32 devices in a mesh: rep: 2 (over x), fsdp: 4 (over y, core), seq: 4 (over z).
Axes of the slice: x: 2, y: 2, z: 4, core: 2. Of those that a mesh axis runs over, the one named last changes fastest.
Arguments:
- tokens: bfloat16 [16, 1024, 1152], P(('rep', 'fsdp'), 'seq'), may hold values from -6 to 6
- condition: bfloat16 [16, 1152], P(('rep', 'fsdp')), may hold values from -6 to 6
- valid_mask: int32 [16, 1024], P(('rep', 'fsdp'), 'seq'), may hold values from 0 to 1, as said below
- teacher: bfloat16 [16, 1024, 1152], P(('rep', 'fsdp'), 'seq'), may hold values from -6 to 6
- out_grad: bfloat16 [16, 1024, 1152], P(('rep', 'fsdp'), 'seq'), may hold values from -96 to 96
- mod_weight: bfloat16 [1152, 6912], P('fsdp'), may hold values from -0.1875 to 0.1875
- mod_bias: bfloat16 [6912], P('fsdp'), may hold values from -3 to 3
- qkv_weight: bfloat16 [1152, 3456], P('fsdp'), may hold values from -0.1875 to 0.1875
- qkv_bias: bfloat16 [2304], P('fsdp'), may hold values from -3 to 3
- out_weight: bfloat16 [1152, 1152], P('fsdp'), may hold values from -2 to 2
- out_bias: bfloat16 [1152], P('fsdp'), may hold values from -3 to 3
- up_weight: bfloat16 [1152, 4608], P('fsdp'), may hold values from -0.1875 to 0.1875
- up_bias: bfloat16 [4608], P('fsdp'), may hold values from -3 to 3
- down_weight: bfloat16 [4608, 1152], P('fsdp'), may hold values from -0.09375 to 0.09375
- down_bias: bfloat16 [1152], P('fsdp'), may hold values from -3 to 3
Outputs:
- block_out: bfloat16 [16, 1024, 1152], P(('rep', 'fsdp'), 'seq')
- loss_value: float32 [], replicated
- tokens_grad: bfloat16 [16, 1024, 1152], P(('rep', 'fsdp'), 'seq')
- condition_grad: float32 [16, 1152], P(('rep', 'fsdp'))
- mod_weight_grad: float32 [1152, 6912], P('fsdp')
- mod_bias_grad: float32 [6912], P('fsdp')
- qkv_weight_grad: float32 [1152, 3456], P('fsdp')
- qkv_bias_grad: float32 [2304], P('fsdp')
- out_weight_grad: float32 [1152, 1152], P('fsdp')
- out_bias_grad: float32 [1152], P('fsdp')
- up_weight_grad: float32 [1152, 4608], P('fsdp')
- up_bias_grad: float32 [4608], P('fsdp')
- down_weight_grad: float32 [4608, 1152], P('fsdp')
- down_bias_grad: float32 [1152], P('fsdp')
The draws below stay inside these ranges and needn't reach their ends.
Inputs may be any that keep to these rules, and one draw needn't show every extreme that they name: `valid_mask`: the first token of every latent is valid.
All inputs are finite; a program needn't handle non-finite values.
Results may differ from the reference program's by a relative error of at most 0.012.
Values may be sent and summed in bfloat16 or wider, within the bound.
A program may use at most 256 MiB of HBM per device.

```python
import math
import jax
import jax.numpy as jnp
from jax import lax

D = 1152
HEADS = 16
HEAD_DIM = 72
FF = 4608
LATENT = 1024
NLAT = 16
LOSS_SCALE = 9437184


def draw_valid_mask(key, part):
    latent_row = jnp.arange(NLAT, dtype=jnp.int32)[:, None]
    position = jnp.arange(LATENT, dtype=jnp.int32)[None, :]
    threshold = 800 + 100 * latent_row // max(NLAT - 1, 1) + 100 * position // max(LATENT - 1, 1)
    rolled = jax.random.randint(key, (NLAT, LATENT), 0, 1000, dtype=jnp.int32)
    return jnp.where((rolled < threshold) | (position == 0), 1, 0).astype(jnp.int32)


def draw_out_grad(key, part):
    scale_key = jax.random.fold_in(key, 11)
    entry_key = jax.random.fold_in(key, 23)
    spread = jax.random.uniform(scale_key, (NLAT, LATENT, 1), jnp.float32, 0.0, 2.0794415416798357)
    scales = 2.0 * jnp.exp(spread)
    entries = jnp.clip(jax.random.normal(entry_key, (NLAT, LATENT, D), jnp.float32), -6.0, 6.0)
    return (scales * entries).astype(jnp.bfloat16)


def block_levels(own_key, dims, cuts, least, largest):
    level = 1.0
    for axis_at, parts in cuts:
        heights = jax.random.uniform(jax.random.fold_in(jax.random.fold_in(own_key, 6), axis_at), (parts,), jnp.float32, least / len(cuts), largest / len(cuts))
        level = level * jnp.repeat(jnp.exp(heights), dims[axis_at] // parts).reshape((-1,) + (1,) * (len(dims) - 1 - axis_at))
    return level


def normal_values(own_key, dims, scale, bound, cuts=(), kind=jnp.bfloat16):
    drawn = scale * jax.random.normal(own_key, dims, jnp.float32)
    if cuts:
        drawn = drawn * block_levels(own_key, dims, cuts, -0.22, 0.18)
    return jnp.clip(drawn, -bound, bound).astype(kind)


def setup_inputs(seed: int = 0) -> dict:
    splits = jax.random.split(jax.random.key(seed), 16)
    tokens = normal_values(splits[0], (NLAT, LATENT, D), 1.0, 6.0, ((0, 8), (1, 4)))
    condition = normal_values(splits[1], (NLAT, D), 1.0, 6.0, ((0, 8),))
    valid_mask = draw_valid_mask(jax.random.fold_in(splits[15], 71), 0)
    teacher = normal_values(splits[3], (NLAT, LATENT, D), 1.0, 6.0, ((0, 8), (1, 4)))
    out_grad = draw_out_grad(jax.random.fold_in(splits[15], 71), 0)
    mod_weight = normal_values(splits[5], (D, 6 * D), D ** -0.5, 0.1875, ((0, 4),))
    mod_bias = normal_values(splits[6], (6 * D,), 0.5, 3.0, ((0, 4),))
    qkv_weight = normal_values(splits[7], (D, 3 * D), D ** -0.5, 0.1875, ((0, 4),))
    qkv_bias = normal_values(splits[8], (2 * D,), 0.5, 3.0, ((0, 4),))
    out_weight = normal_values(splits[9], (D, D), (8 * D // LATENT) ** -0.5, 2.0, ((0, 4),))
    out_bias = normal_values(splits[10], (D,), 0.5, 3.0, ((0, 4),))
    up_weight = normal_values(splits[11], (D, FF), D ** -0.5, 0.1875, ((0, 4),))
    up_bias = normal_values(splits[12], (FF,), 0.5, 3.0, ((0, 4),))
    down_weight = normal_values(splits[13], (FF, D), FF ** -0.5, 0.09375, ((0, 4),))
    down_bias = normal_values(splits[14], (D,), 0.5, 3.0, ((0, 4),))
    return dict(tokens=tokens, condition=condition, valid_mask=valid_mask, teacher=teacher, out_grad=out_grad, mod_weight=mod_weight, mod_bias=mod_bias, qkv_weight=qkv_weight, qkv_bias=qkv_bias, out_weight=out_weight, out_bias=out_bias, up_weight=up_weight, up_bias=up_bias, down_weight=down_weight, down_bias=down_bias)


@jax.custom_vjp
def low(v):
    return lax.optimization_barrier(v.astype(jnp.bfloat16)).astype(jnp.float32)

@jax.custom_vjp
def low_back(v):
    return v

def low_keep(v):
    return (low(v), None)

def low_pass(kept, grad):
    return (grad,)

def back_keep(v):
    return (v, None)

def back_low(kept, grad):
    return (low(grad),)
low.defvjp(low_keep, low_pass)
low_back.defvjp(back_keep, back_low)
EPS = 1e-06
GELU_C = 0.7978845608028654
HIGHEST = lax.Precision.HIGHEST

def norm_rows(inputs):
    centred = inputs - lax.optimization_barrier(jnp.mean(inputs, axis=-1, keepdims=True))
    return centred * lax.rsqrt(lax.optimization_barrier(jnp.mean(centred * centred, axis=-1, keepdims=True)) + EPS)

def gelu_tanh(inputs):
    return 0.5 * inputs * (1.0 + jnp.tanh(GELU_C * (inputs + 0.044715 * inputs * inputs * inputs)))

def rounded_both(inputs):
    return low_back(low(inputs))

def project(left, right):
    return jnp.einsum('gsd,de->gse', left, right, precision=HIGHEST)

def block_group(params, inputs, conds, keyvalid, target):
    mod_w, mod_b, qkv_w, qkv_b, out_w, out_b, up_w, up_b, down_w, down_b = params
    group, length, width = inputs.shape
    factor = HEAD_DIM ** (-0.5)
    modulation = jnp.dot(low(jax.nn.silu(conds)), mod_w, precision=HIGHEST, preferred_element_type=jnp.float32) + mod_b
    pieces = [modulation[:, None, number * width:(number + 1) * width] for number in range(6)]
    shift_one, scale_one, gate_one, shift_two, scale_two, gate_two = pieces
    hidden_one = low(norm_rows(inputs) * (1.0 + scale_one) + shift_one)
    projected = project(hidden_one, qkv_w)
    queries = rounded_both(projected[..., :width] + qkv_b[:width])
    keys_all = rounded_both(projected[..., width:2 * width])
    values_all = rounded_both(projected[..., 2 * width:] + qkv_b[width:])

    def split_heads(tensor):
        return tensor.reshape(group, length, HEADS, HEAD_DIM).transpose(2, 0, 1, 3)
    keep_mask = keyvalid[:, None, :] > 0.5

    def attend(packed):
        q_head, k_head, v_head = packed
        scores = jnp.einsum('gqd,gkd->gqk', q_head, k_head, precision=HIGHEST) * factor
        scores = jnp.where(keep_mask, low_back(scores), -1e+30)
        probability = low(jax.nn.softmax(scores, axis=-1))
        return jnp.einsum('gqk,gkd->gqd', probability, v_head, precision=HIGHEST)
    heads_out = lax.map(jax.checkpoint(attend), (split_heads(queries), split_heads(keys_all), split_heads(values_all)))
    attended = rounded_both(heads_out.transpose(1, 2, 0, 3).reshape(group, length, width))
    branch = low_back(project(attended, out_w) + out_b)
    middle = inputs + gate_one * branch
    hidden_two = low(norm_rows(middle) * (1.0 + scale_two) + shift_two)
    upper = low_back(project(hidden_two, up_w) + up_b)
    activated = low(gelu_tanh(upper))
    mlp_out = low_back(project(activated, down_w) + down_b)
    output = middle + gate_two * mlp_out
    differ = output - target
    return (output, jnp.sum(keyvalid[..., None] * differ * differ))

def reference(tokens, condition, valid_mask, teacher, out_grad, mod_weight, mod_bias, qkv_weight, qkv_bias, out_weight, out_bias, up_weight, up_bias, down_weight, down_bias):
    params = tuple((weight.astype(jnp.float32) for weight in (mod_weight, mod_bias, qkv_weight, qkv_bias, out_weight, out_bias, up_weight, up_bias, down_weight, down_bias)))
    inputs = tokens.astype(jnp.float32)
    conds = condition.astype(jnp.float32)
    keyvalid = valid_mask.astype(jnp.float32)
    target = teacher.astype(jnp.float32)
    counted = jnp.sum(keyvalid)
    group = math.gcd(NLAT, max(1, 4096 // LATENT))
    blocks = NLAT // group
    checked = jax.checkpoint(block_group)

    def forward(weights, values_in, conds_in):

        def step(total, packed):
            x_group, c_group, m_group, t_group = packed
            y_group, err_group = checked(weights, x_group, c_group, m_group, t_group)
            return (total + err_group, y_group)
        total, outputs = lax.scan(step, jnp.zeros((), jnp.float32), (values_in.reshape(blocks, group, LATENT, D), conds_in.reshape(blocks, group, D), keyvalid.reshape(blocks, group, LATENT), target.reshape(blocks, group, LATENT, D)))
        return (outputs.reshape(NLAT, LATENT, D), total / (D * counted))
    (output, loss_value), pull = jax.vjp(forward, params, inputs, conds)
    grads, input_grad, cond_grad = pull((out_grad.astype(jnp.float32), jnp.full((), LOSS_SCALE, jnp.float32)))
    return (output.astype(jnp.bfloat16), loss_value, input_grad.astype(jnp.bfloat16), cond_grad, grads[0], grads[1], grads[2], grads[3], grads[4], grads[5], grads[6], grads[7], grads[8], grads[9])
```

```python
import functools

import jax
import jax.numpy as jnp
from jax import lax
from jax.experimental import pallas as pl
from jax.experimental.pallas import tpu as pltpu
from jax.sharding import PartitionSpec as P

HEADS = 16

EPS = 1e-06
GELU_C = 0.7978845608028654
HIGHEST = lax.Precision.HIGHEST
LOG2E = 1.4426950408889634
NEG = -1e30
BF16 = jnp.bfloat16
F32 = jnp.float32
WINDOW = 256
LANES = 128


def flip(array, axis, bit):
    size = lax.axis_size(axis)
    return lax.ppermute(array, axis, [(i, i ^ bit) for i in range(size)])


def shift(array, axis, step):
    size = lax.axis_size(axis)
    return lax.ppermute(array, axis, [(i, (i + step) % size) for i in range(size)])


def pick(array, index):
    return lax.dynamic_index_in_dim(array, index, 0, keepdims=False)


def in_order(first, second, swapped):
    return jnp.where(swapped, jnp.stack([second, first]), jnp.stack([first, second]))


def to_latent(array):
    seq, fsdp = lax.axis_size("seq"), lax.axis_size("fsdp")
    place = lax.axis_index("seq")
    arrived = []
    for turn in range(2):
        pairs = []
        for f in range(fsdp):
            for s in range(seq):
                pair, core = f // 2, f % 2
                target = (pair * 2 + s // 2, 2 * core + (s + turn) % 2)
                pairs.append((f * seq + s, target[0] * seq + target[1]))
        block = pick(array, (place + turn) % 2)
        arrived.append(lax.ppermute(block, ("fsdp", "seq"), pairs))
    both = in_order(arrived[0], arrived[1], place % 2 == 1)
    return both.reshape((-1,) + both.shape[2:])


def from_latent(array):
    seq, fsdp = lax.axis_size("seq"), lax.axis_size("fsdp")
    place = lax.axis_index("seq")
    halves = array.reshape((2, array.shape[0] // 2) + array.shape[1:])
    arrived = []
    for turn in range(2):
        pairs = []
        for f in range(fsdp):
            for s in range(seq):
                pair, core = f // 2, f % 2
                slot = (s + turn) % 2
                target = (pair * 2 + s // 2, 2 * core + slot)
                pairs.append((f * seq + s, target[0] * seq + target[1]))
        arrived.append(lax.ppermute(pick(halves, (place + turn) % 2), ("fsdp", "seq"), pairs))
    return in_order(arrived[0], arrived[1], place % 2 == 1)


def sum_everywhere(value, fast):
    if not fast:
        return lax.psum(value, ("rep", "fsdp", "seq"))
    for axis, bit in (("fsdp", 1), ("fsdp", 2), ("rep", 1), ("seq", 1), ("seq", 2)):
        value = value + flip(value, axis, bit)
    return value


def gather_rows(row, fast):
    if not fast:
        fsdp = lax.axis_size("fsdp")
        everything = lax.all_gather(row, ("rep", "fsdp", "seq"), axis=0)
        everything = everything.reshape((-1, fsdp // 2, 2, lax.axis_size("seq")) + row.shape)
        return everything[:, :, 0].reshape((-1,) + row.shape)
    seq = lax.axis_size("seq")
    place = lax.axis_index("seq")
    here = [row] + [shift(row, "seq", step) for step in range(1, seq)]
    here = jnp.stack(here)
    here = jnp.concatenate(
        [lax.dynamic_slice_in_dim(here, (place - s) % seq, 1, 0) for s in range(seq)]
    )
    both = in_order(here, flip(here, "fsdp", 2), lax.axis_index("fsdp") >= 2)
    both = both.reshape((-1,) + row.shape)
    quad = in_order(both, flip(both, "rep", 1), lax.axis_index("rep") == 1)
    return quad.reshape((-1,) + row.shape)


def gather_small(vector, fast):
    if not fast:
        return lax.all_gather(vector, "fsdp", axis=0)
    place = lax.axis_index("fsdp")
    pair = in_order(vector, flip(vector, "fsdp", 1), place % 2 == 1)
    quad = in_order(pair, flip(pair, "fsdp", 2), place >= 2)
    return quad.reshape((-1,) + vector.shape)


def assemble_kernel(own, core, first, second, core_first, core_second, out, held, in_sem, out_sem):
    place, replica = lax.axis_index("fsdp"), lax.axis_index("rep")
    rows, half = own.shape[0], first.shape[0]

    def partner(bit):
        return place + bit - 2 * bit * ((place // bit) % 2)

    across = partner(2)
    across_core = across + 1 - 2 * (across % 2)
    moves = [
        (own, place * rows),
        (core, partner(1) * rows),
        (first, across * rows + replica * half),
        (second, across * rows + (1 - replica) * half),
        (core_first, across_core * rows + replica * half),
        (core_second, across_core * rows + (1 - replica) * half),
    ]
    loads, stores = [], []
    for number, (source, start) in enumerate(moves):
        where = pl.ds(pl.multiple_of(start, 16), source.shape[0])
        loads.append(pltpu.make_async_copy(source, held.at[where], in_sem.at[number]))
        stores.append(pltpu.make_async_copy(held.at[where], out.at[where], out_sem.at[number]))
        loads[-1].start()
    for load, store in zip(loads, stores, strict=True):
        load.wait()
        store.start()
    for store in stores:
        store.wait()


def gather_weight(weight, fast):
    if not fast:
        return lax.all_gather(weight, "fsdp", axis=0, tiled=True)
    rows, columns = weight.shape
    half = rows // 2
    mine = lax.dynamic_slice_in_dim(weight, lax.axis_index("rep") * half, half, 0)
    first = flip(mine, "fsdp", 2)
    second = flip(first, "rep", 1)
    core = flip(weight, "fsdp", 1)
    core_first = flip(first, "fsdp", 1)
    core_second = flip(second, "fsdp", 1)
    full = (rows * 4, columns)
    return pl.pallas_call(
        assemble_kernel,
        out_shape=jax.ShapeDtypeStruct(full, weight.dtype),
        in_specs=[pl.BlockSpec(memory_space=pl.ANY)] * 6,
        out_specs=pl.BlockSpec(memory_space=pl.ANY),
        scratch_shapes=[
            pltpu.VMEM(full, weight.dtype),
            pltpu.SemaphoreType.DMA((6,)),
            pltpu.SemaphoreType.DMA((6,)),
        ],
        cost_estimate=pl.CostEstimate(
            flops=0, transcendentals=0, bytes_accessed=4 * rows * columns * 4
        ),
        name="assemble",
    )(weight, core, first, second, core_first, core_second)


def outer_kernel(has_extra, left_own, left_other, right_own, right_other, *rest):
    out = rest[-1]
    dims = (((0,), (0,)), ((), ()))
    total = lax.dot_general(left_own[...], right_own[...], dims, preferred_element_type=F32)
    total += lax.dot_general(left_other[...], right_other[...], dims, preferred_element_type=F32)
    if has_extra:
        total += rest[0][0].astype(F32)
    out[0] = total.astype(out.dtype)


def outer_blocks(left_own, left_other, right_own, right_other, extra=None):
    tokens, rows = left_own.shape
    columns = right_own.shape[1]
    width = 1152
    tall = 384 if rows % 384 == 0 else rows
    blocks = columns // width
    left_spec = pl.BlockSpec((tokens, tall), lambda j, i: (0, i))
    right_spec = pl.BlockSpec((tokens, width), lambda j, i: (0, j))
    out_spec = pl.BlockSpec((1, tall, width), lambda j, i: (j, i, 0))
    operands = [left_own, left_other, right_own, right_other]
    specs = [left_spec, left_spec, right_spec, right_spec]
    if extra is not None:
        operands.append(extra)
        specs.append(out_spec)
    return pl.pallas_call(
        functools.partial(outer_kernel, extra is not None),
        grid=(blocks, rows // tall),
        out_shape=jax.ShapeDtypeStruct((blocks, rows, width), BF16),
        in_specs=specs,
        out_specs=out_spec,
        cost_estimate=pl.CostEstimate(
            flops=4 * tokens * rows * columns,
            transcendentals=0,
            bytes_accessed=2 * (2 * tokens * (rows + columns) + 2 * rows * columns),
        ),
        name="outer",
    )(*operands)


def reduce_start(give):
    return flip(give, "fsdp", 2)


def reduce_rest(kept):
    seq = lax.axis_size("seq")
    place, replica = lax.axis_index("seq"), lax.axis_index("rep")
    width = kept.shape[-1]
    parts = kept.reshape(2, seq, -1, width)
    arrived = flip(pick(parts, 1 - replica), "rep", 1)
    mine = (pick(parts, replica).astype(F32) + arrived.astype(F32)).astype(BF16)
    others = [shift(pick(mine, (place + step) % seq), "seq", step) for step in range(1, seq)]
    total = pick(mine, place).astype(F32)
    for other in others:
        total = total + other.astype(F32)
    total = total.astype(BF16)
    along = [total] + [shift(total, "seq", step) for step in range(1, seq)]
    across = [flip(piece, "rep", 1) for piece in along]
    return along + across


def place_kernel(layout, pieces, outs, held, wide, in_sem, out_sem):
    place, replica = lax.axis_index("seq"), lax.axis_index("rep")
    seq = len(pieces) // 2
    tall, width = pieces[0].shape
    loads = []
    for number, piece in enumerate(pieces):
        loads.append(pltpu.make_async_copy(piece, held.at[number], in_sem.at[number]))
        loads[-1].start()

    def target(number):
        step = number % seq
        side = replica if number < seq else 1 - replica
        return side * seq + (place + seq - step) % seq

    def copies(number):
        index = target(number)
        found = []
        if layout == "tall":
            rows = pl.ds(pl.multiple_of(index * tall, 8), tall)
            found.append((None, outs[0].at[rows]))
        else:
            per_block = outs[0].shape[0] // tall
            rows = pl.ds(pl.multiple_of((index % per_block) * tall, 8), tall)
            block = index // per_block
            low = 0
            for out in outs:
                count = out.shape[1] // width
                columns = pl.ds(pl.multiple_of((block - low) * width, LANES), width)
                inside = (block >= low) & (block < low + count) if len(outs) > 1 else None
                found.append((inside, out.at[rows, columns]))
                low += count
        return [
            (inside, pltpu.make_async_copy(wide.at[number], view, out_sem.at[number]))
            for inside, view in found
        ]

    def each(number, act):
        for inside, copy in copies(number):
            if inside is None:
                act(copy)
            else:
                pl.when(inside)(functools.partial(act, copy))

    for number, load in enumerate(loads):
        load.wait()
        wide[number] = held[number].astype(F32)
        each(number, lambda copy: copy.start())
    for number in range(len(loads)):
        each(number, lambda copy: copy.wait())


def place_pieces(pieces, shapes, layout):
    count = len(pieces)
    tall, width = pieces[0].shape

    def body(*refs):
        place_kernel(
            layout,
            refs[:count],
            refs[count : count + len(shapes)],
            *refs[count + len(shapes) :],
        )

    return pl.pallas_call(
        body,
        out_shape=[jax.ShapeDtypeStruct(shape, F32) for shape in shapes],
        in_specs=[pl.BlockSpec(memory_space=pl.ANY)] * count,
        out_specs=[pl.BlockSpec(memory_space=pl.ANY)] * len(shapes),
        scratch_shapes=[
            pltpu.VMEM((count, tall, width), BF16),
            pltpu.VMEM((count, tall, width), F32),
            pltpu.SemaphoreType.DMA((count,)),
            pltpu.SemaphoreType.DMA((count,)),
        ],
        cost_estimate=pl.CostEstimate(
            flops=0, transcendentals=0, bytes_accessed=6 * count * tall * width
        ),
        name="place",
    )(*pieces)


def head_window(head, head_dim, width):
    start = head * head_dim
    base = jnp.minimum(start // LANES, (width - WINDOW) // LANES) * LANES
    base = pl.multiple_of(base, LANES)
    return start, base


def forward_kernel(
    head_dim, q_ref, k_own, v_own, k_other, v_other, bias_own, bias_other, out_ref, lse_ref
):
    tokens, width = q_ref.shape
    blocks = 2
    tall = tokens // blocks
    scale = head_dim ** (-0.5) * LOG2E
    out_ref[...] = jnp.zeros_like(out_ref)
    lse_ref[...] = jnp.zeros_like(lse_ref)
    b_own, b_other = bias_own[...], bias_other[...]
    dims = (((1,), (1,)), ((), ()))

    def body(head, carry):
        start, base = head_window(head, head_dim, width)
        window = pl.ds(base, WINDOW)
        lane = lax.broadcasted_iota(jnp.int32, (1, WINDOW), 1) + base
        inside = (lane >= start) & (lane < start + head_dim)
        keep = inside.astype(BF16)
        spot = lax.broadcasted_iota(jnp.int32, (1, LANES), 1) == head
        key_one, key_two = k_own[:, window], k_other[:, window]
        val_one, val_two = v_own[:, window] * keep, v_other[:, window] * keep
        for block in range(blocks):
            rows = pl.ds(block * tall, tall)
            query = q_ref[rows, window] * keep
            one = lax.dot_general(query, key_one, dims, preferred_element_type=F32)
            two = lax.dot_general(query, key_two, dims, preferred_element_type=F32)
            one = one * scale + b_own
            two = two * scale + b_other
            top = jnp.maximum(
                jnp.max(one, axis=1, keepdims=True), jnp.max(two, axis=1, keepdims=True)
            )
            one = jnp.exp2(one - top)
            two = jnp.exp2(two - top)
            total = jnp.sum(one, axis=1, keepdims=True) + jnp.sum(two, axis=1, keepdims=True)
            mixed = jnp.dot(one.astype(BF16), val_one, preferred_element_type=F32)
            mixed += jnp.dot(two.astype(BF16), val_two, preferred_element_type=F32)
            mixed = mixed * (1.0 / total)
            out_ref[rows, window] = jnp.where(
                inside, mixed, out_ref[rows, window].astype(F32)
            ).astype(out_ref.dtype)
            lse_ref[rows, :] = jnp.where(spot, top + jnp.log2(total), lse_ref[rows, :])
        return carry

    lax.fori_loop(0, HEADS, body, 0)


def attend(queries, k_own, v_own, k_other, v_other, bias_own, bias_other):
    tokens, width = queries.shape
    return pl.pallas_call(
        functools.partial(forward_kernel, width // HEADS),
        out_shape=[
            jax.ShapeDtypeStruct((tokens, width), BF16),
            jax.ShapeDtypeStruct((tokens, LANES), F32),
        ],
        compiler_params=pltpu.CompilerParams(vmem_limit_bytes=48 * 1024 * 1024),
        cost_estimate=pl.CostEstimate(
            flops=16 * tokens * tokens * 2 * WINDOW * 4,
            transcendentals=HEADS * tokens * tokens * 2,
            bytes_accessed=6 * tokens * width * 2,
        ),
        name="attend",
    )(queries, k_own, v_own, k_other, v_other, bias_own, bias_other)


def backward_kernel(
    head_dim,
    q_ref,
    k_own,
    v_own,
    k_other,
    v_other,
    do_ref,
    lse_ref,
    bias_own,
    bias_other,
    dq_out,
    dk_own_out,
    dv_own_out,
    dk_other_out,
    dv_other_out,
    dq_acc,
    dk_one,
    dv_one,
    dk_two,
    dv_two,
):
    tokens, width = q_ref.shape
    factor = head_dim ** (-0.5)
    scale = factor * LOG2E
    for ref in (dq_acc, dk_one, dv_one, dk_two, dv_two):
        ref[...] = jnp.zeros_like(ref)
    across = (((1,), (1,)), ((), ()))
    down = (((0,), (0,)), ((), ()))
    sides = (
        (k_own, v_own, bias_own, dk_one, dv_one),
        (k_other, v_other, bias_other, dk_two, dv_two),
    )

    def body(head, carry):
        start, base = head_window(head, head_dim, width)
        window = pl.ds(base, WINDOW)
        lane = lax.broadcasted_iota(jnp.int32, (1, WINDOW), 1) + base
        keep = ((lane >= start) & (lane < start + head_dim)).astype(BF16)
        query = q_ref[:, window] * keep
        grad = do_ref[:, window] * keep
        lse = lse_ref[pl.ds(head, 1), :]
        probs, prods = [], []
        delta = None
        for k_ref, v_ref, bias, _, _ in sides:
            scores = lax.dot_general(k_ref[:, window], query, across, preferred_element_type=F32)
            prob = jnp.exp2(scores * scale + bias[...] - lse)
            prob_grad = lax.dot_general(v_ref[:, window], grad, across, preferred_element_type=F32)
            prod = prob * prob_grad
            part = jnp.sum(prod, axis=0, keepdims=True)
            delta = part if delta is None else delta + part
            probs.append(prob)
            prods.append(prod)
        dq = None
        for (k_ref, _, _, dk, dv), prob, prod in zip(sides, probs, prods, strict=True):
            dv[:, window] += jnp.dot(prob.astype(BF16), grad, preferred_element_type=F32)
            score_grad = (prod - prob * delta).astype(BF16)
            dk[:, window] += jnp.dot(score_grad, query, preferred_element_type=F32)
            part = lax.dot_general(
                score_grad, k_ref[:, window] * keep, down, preferred_element_type=F32
            )
            dq = part if dq is None else dq + part
        dq_acc[:, window] += dq
        return carry

    lax.fori_loop(0, HEADS, body, 0)
    dq_out[...] = (dq_acc[...] * factor).astype(dq_out.dtype)
    dk_own_out[...] = (dk_one[...] * factor).astype(dk_own_out.dtype)
    dv_own_out[...] = dv_one[...].astype(dv_own_out.dtype)
    dk_other_out[...] = (dk_two[...] * factor).astype(dk_other_out.dtype)
    dv_other_out[...] = dv_two[...].astype(dv_other_out.dtype)


def attend_back(queries, k_own, v_own, k_other, v_other, grad, lse, bias_own, bias_other):
    tokens, width = queries.shape
    shape = (tokens, width)
    return pl.pallas_call(
        functools.partial(backward_kernel, width // HEADS),
        out_shape=[
            jax.ShapeDtypeStruct(shape, BF16),
            jax.ShapeDtypeStruct(shape, F32),
            jax.ShapeDtypeStruct(shape, F32),
            jax.ShapeDtypeStruct(shape, BF16),
            jax.ShapeDtypeStruct(shape, BF16),
        ],
        scratch_shapes=[pltpu.VMEM(shape, F32) for _ in range(5)],
        compiler_params=pltpu.CompilerParams(vmem_limit_bytes=60 * 1024 * 1024),
        cost_estimate=pl.CostEstimate(
            flops=16 * tokens * tokens * 2 * WINDOW * 10,
            transcendentals=HEADS * tokens * tokens * 2,
            bytes_accessed=13 * tokens * width * 2,
        ),
        name="attend_back",
    )(queries, k_own, v_own, k_other, v_other, grad, lse, bias_own, bias_other)


def dot(left, right):
    return jnp.dot(left, right, preferred_element_type=F32)


def dot_t(left, right):
    return lax.dot_general(left, right, (((1,), (1,)), ((), ())), preferred_element_type=F32)


def norm_parts(inputs):
    centred = inputs - jnp.mean(inputs, axis=-1, keepdims=True)
    rate = lax.rsqrt(jnp.mean(centred * centred, axis=-1, keepdims=True) + EPS)
    return centred * rate, rate


def norm_back(grad, normed, rate):
    return rate * (
        grad
        - jnp.mean(grad, axis=-1, keepdims=True)
        - normed * jnp.mean(grad * normed, axis=-1, keepdims=True)
    )


def gelu_parts(inputs):
    inner = jnp.tanh(GELU_C * (inputs + 0.044715 * inputs * inputs * inputs))
    value = 0.5 * inputs * (1.0 + inner)
    slope = 0.5 * (1.0 + inner) + 0.5 * inputs * (1.0 - inner * inner) * GELU_C * (
        1.0 + 3.0 * 0.044715 * inputs * inputs
    )
    return value, slope


def column_sum(array):
    return jnp.sum(array.astype(F32), axis=0)


def shards(
    tokens,
    condition,
    valid_mask,
    teacher,
    out_grad,
    mod_weight,
    mod_bias,
    qkv_weight,
    qkv_bias,
    out_weight,
    out_bias,
    up_weight,
    up_bias,
    down_weight,
    down_bias,
):
    reps, fsdp, seq = lax.axis_size("rep"), lax.axis_size("fsdp"), lax.axis_size("seq")
    fast = (reps, fsdp, seq) == (2, 4, 4)
    latents, span, width = tokens.shape
    assert 2 * latents == seq and latents == 2
    place_f, place_s = lax.axis_index("fsdp"), lax.axis_index("seq")
    total_tokens = latents * span * reps * fsdp * seq

    inputs_low = to_latent(tokens)
    keyvalid = to_latent(valid_mask.astype(F32))
    counted = sum_everywhere(jnp.sum(valid_mask.astype(F32)).reshape(1, 1), fast)
    cond_row = pick(condition, place_s % 2)
    cond_row = jnp.where(place_f % 2 == place_s // 2, cond_row, flip(cond_row, "fsdp", 1))

    shard_rows = mod_weight.shape[0]
    if fast:
        cond_pair = jnp.stack([cond_row, flip(cond_row, "fsdp", 2)])
    else:
        cond_pair = lax.all_gather(cond_row, "fsdp", axis=0)[::2]
    silu_pair = jax.nn.silu(cond_pair.astype(F32)).astype(BF16)
    silu_cols = lax.dynamic_slice_in_dim(silu_pair, place_f * shard_rows, shard_rows, 1)
    partial = dot(silu_cols, mod_weight)
    if fast:
        mod_row = partial[0] + flip(partial[1], "fsdp", 2)
        mod_row = mod_row + flip(mod_row, "fsdp", 1)
    else:
        mod_row = pick(lax.psum(partial, "fsdp"), place_f // 2)

    biases = jnp.concatenate([mod_bias, qkv_bias, out_bias, up_bias, down_bias])
    bias_all = gather_small(biases, fast).astype(F32)
    cuts = [0]
    for bias in (mod_bias, qkv_bias, out_bias, up_bias, down_bias):
        cuts.append(cuts[-1] + bias.shape[0])
    mod_b, qkv_b, out_b, up_b, down_b = (
        bias_all[:, low:high].reshape(-1) for low, high in zip(cuts[:-1], cuts[1:], strict=True)
    )
    pieces = (mod_row + mod_b).reshape(6, 1, width)
    shift_one, scale_one, gate_one, shift_two, scale_two, gate_two = (pieces[i] for i in range(6))

    qkv_full = gather_weight(qkv_weight, fast)
    out_full = gather_weight(out_weight, fast)
    up_full = gather_weight(up_weight, fast)
    down_full = gather_weight(down_weight, fast)
    teacher_own = to_latent(teacher)
    out_grad_own = to_latent(out_grad)

    inputs = inputs_low.astype(F32)
    normed_one, rate_one = norm_parts(inputs)
    hidden_one = (normed_one * (1.0 + scale_one) + shift_one).astype(BF16)
    projected = dot(hidden_one, qkv_full)
    queries = (projected[:, :width] + qkv_b[:width]).astype(BF16)
    keys_own = projected[:, width : 2 * width].astype(BF16)
    values_own = (projected[:, 2 * width :] + qkv_b[width:]).astype(BF16)
    keys_other, values_other = flip(keys_own, "fsdp", 1), flip(values_own, "fsdp", 1)
    mask_own = (keyvalid - 1.0) * (-NEG)
    mask_other = flip(mask_own, "fsdp", 1)
    attended, lse = attend(
        queries, keys_own, values_own, keys_other, values_other, mask_own[None], mask_other[None]
    )
    branch = dot(attended, out_full) + out_b
    middle = inputs + gate_one * branch
    normed_two, rate_two = norm_parts(middle)
    hidden_two = (normed_two * (1.0 + scale_two) + shift_two).astype(BF16)
    up_pre = dot(hidden_two, up_full) + up_b
    activated, slope = gelu_parts(up_pre)
    activated = activated.astype(BF16)
    mlp_out = dot(activated, down_full) + down_b
    output = middle + gate_two * mlp_out
    block_out = from_latent(output.astype(BF16))
    differ = (output - teacher_own.astype(F32)) * keyvalid[:, None]
    err_total = sum_everywhere(jnp.sum(differ * differ).reshape(1, 1), fast)

    grad_out = out_grad_own.astype(F32) + total_tokens / counted * differ
    grad_mlp = (grad_out * gate_two).astype(BF16)
    gate_two_grad = jnp.sum(grad_out * mlp_out, axis=0)

    def shard_of(array, which):
        rows = array.shape[1] // fsdp
        return lax.dynamic_slice_in_dim(array, which * rows, rows, 1)

    def weight_grad(left, right):
        if not fast:
            whole = lax.dot_general(
                left, right, (((0,), (0,)), ((), ())), preferred_element_type=F32
            )
            mine = lax.psum_scatter(whole.astype(BF16), "fsdp", scatter_dimension=0, tiled=True)
            return lax.psum(mine, ("rep", "seq")).astype(F32)
        right_other = flip(right, "fsdp", 1)
        keep, give = shard_of(left, place_f), shard_of(left, place_f ^ 2)
        keep_other = flip(shard_of(left, place_f ^ 1), "fsdp", 1)
        give_other = flip(shard_of(left, place_f ^ 3), "fsdp", 1)
        arrived = reduce_start(outer_blocks(give, give_other, right, right_other))
        return outer_blocks(keep, keep_other, right, right_other, arrived)

    down_sum = weight_grad(activated, grad_mlp)
    down_bgrad = column_sum(grad_mlp)
    upper_grad = (dot_t(grad_mlp, down_full) * slope).astype(BF16)
    up_sum = weight_grad(hidden_two, upper_grad)
    up_bgrad = column_sum(upper_grad)
    hidden_two_grad = dot_t(upper_grad, up_full)
    scaled_two = hidden_two_grad * (1.0 + scale_two)
    middle_grad = grad_out + norm_back(scaled_two, normed_two, rate_two)
    shift_two_grad = jnp.sum(hidden_two_grad, axis=0)
    scale_two_grad = jnp.sum(hidden_two_grad * normed_two, axis=0)
    branch_grad = (middle_grad * gate_one).astype(BF16)
    gate_one_grad = jnp.sum(middle_grad * branch, axis=0)
    out_sum = weight_grad(attended, branch_grad)
    out_bgrad = column_sum(branch_grad)
    attended_grad = dot_t(branch_grad, out_full).astype(BF16)

    early_row = jnp.concatenate(
        [
            gate_one_grad,
            shift_two_grad,
            scale_two_grad,
            gate_two_grad,
            out_bgrad,
            up_bgrad,
            down_bgrad,
        ]
    )
    early_row = early_row + flip(early_row, "fsdp", 1)
    early_rows = gather_rows(early_row[None], fast)[:, 0]

    query_grad, key_part, value_part, key_away, value_away = attend_back(
        queries,
        keys_own,
        values_own,
        keys_other,
        values_other,
        attended_grad,
        lse.T,
        mask_own[:, None],
        mask_other[:, None],
    )
    key_grad = (key_part + flip(key_away, "fsdp", 1).astype(F32)).astype(BF16)
    value_grad = (value_part + flip(value_away, "fsdp", 1).astype(F32)).astype(BF16)
    qkv_grad = jnp.concatenate([query_grad, key_grad, value_grad], axis=-1)
    qkv_sum = weight_grad(hidden_one, qkv_grad)
    hidden_one_grad = dot_t(qkv_grad, qkv_full)
    scaled_one = hidden_one_grad * (1.0 + scale_one)
    tokens_grad = middle_grad + norm_back(scaled_one, normed_one, rate_one)
    tokens_grad = from_latent(tokens_grad.astype(BF16))
    late_row = jnp.concatenate(
        [
            jnp.sum(hidden_one_grad, axis=0),
            jnp.sum(hidden_one_grad * normed_one, axis=0),
            column_sum(query_grad),
            column_sum(value_grad),
        ]
    )
    late_row = late_row + flip(late_row, "fsdp", 1)
    late_rows = gather_rows(late_row[None], fast)[:, 0]

    mod_grad = jnp.concatenate([late_rows[:, : 2 * width], early_rows[:, : 4 * width]], axis=1)
    silu_row = jax.nn.silu(cond_row.astype(F32)).astype(BF16)
    silu_all = gather_rows(silu_row[None], fast)[:, 0]
    silu_own = lax.dynamic_slice_in_dim(silu_all, place_f * shard_rows, shard_rows, 1)
    mod_wgrad = lax.dot_general(
        silu_own.astype(F32),
        mod_grad,
        (((0,), (0,)), ((), ())),
        precision=HIGHEST,
        preferred_element_type=F32,
    )
    bias_rows = jnp.concatenate([early_rows[:, 4 * width :], late_rows[:, 2 * width :]], axis=1)
    bias_sum = jnp.sum(bias_rows, axis=0)

    def own_bias(low, size):
        own = size // fsdp
        return lax.dynamic_slice_in_dim(bias_sum, low + place_f * own, own, 0)

    up_size = up_b.shape[0]
    out_bg = own_bias(0, width)
    up_bg = own_bias(width, up_size)
    down_bg = own_bias(width + up_size, width)
    qkv_bg = own_bias(2 * width + up_size, 2 * width)
    mod_own = mod_bias.shape[0]
    mod_bg = lax.dynamic_slice_in_dim(jnp.sum(mod_grad, axis=0), place_f * mod_own, mod_own, 0)

    replica = lax.axis_index("rep")
    per_rep = mod_grad.shape[0] // reps
    own_rep = lax.dynamic_slice_in_dim(mod_grad, replica * per_rep, per_rep, 0)
    silu_grad = lax.dot_general(
        own_rep,
        mod_weight.astype(F32),
        (((1,), (1,)), ((), ())),
        precision=HIGHEST,
        preferred_element_type=F32,
    )
    owners = silu_grad.reshape(fsdp, latents, shard_rows)
    if fast:
        found = [pick(owners, place_f)]
        found += [flip(pick(owners, place_f ^ bit), "fsdp", bit) for bit in (1, 2, 3)]
        found = jnp.stack(found)
        found = jnp.concatenate(
            [lax.dynamic_slice_in_dim(found, place_f ^ f, 1, 0) for f in range(fsdp)]
        )
    else:
        found = lax.all_to_all(owners, "fsdp", 0, 0, tiled=True)
    silu_grad = found.transpose(1, 0, 2).reshape(latents, width)
    conds = condition.astype(F32)
    sigmoid = 1.0 / (1.0 + jnp.exp(-conds))
    condition_grad = silu_grad * (sigmoid * (1.0 + conds * (1.0 - sigmoid)))

    if fast:
        down_g = place_pieces(
            reduce_rest(down_sum.reshape(-1, width)), [down_weight.shape], "tall"
        )[0]
        up_g = place_pieces(reduce_rest(up_sum.reshape(-1, width)), [up_weight.shape], "wide")[0]
        tail = jnp.concatenate([out_sum, qkv_sum], axis=0).reshape(-1, width)
        out_g, qkv_g = place_pieces(
            reduce_rest(tail), [out_weight.shape, qkv_weight.shape], "wide"
        )
    else:
        down_g, up_g, out_g, qkv_g = down_sum, up_sum, out_sum, qkv_sum
    loss_value = (err_total / (width * counted))[0, 0]
    return (
        block_out,
        loss_value,
        tokens_grad,
        condition_grad,
        mod_wgrad,
        mod_bg,
        qkv_g,
        qkv_bg,
        out_g,
        out_bg,
        up_g,
        up_bg,
        down_g,
        down_bg,
    )


def solution(mesh):
    batch = P(("rep", "fsdp"), "seq", None)
    matrix, vector = P("fsdp", None), P("fsdp")
    params = (matrix, vector) * 5
    return jax.shard_map(
        shards,
        mesh=mesh,
        in_specs=(batch, P(("rep", "fsdp"), None), P(("rep", "fsdp"), "seq"), batch, batch)
        + params,
        out_specs=(batch, P(), batch, P(("rep", "fsdp"), None)) + params,
        check_vma=False,
    )
```

```python
import functools

import jax
import jax.numpy as jnp
from jax import lax
from jax.experimental import pallas as pl
from jax.experimental.pallas import tpu as pltpu
from jax.sharding import PartitionSpec as P

HEADS = 16

EPS = 1e-06
GELU_C = 0.7978845608028654
HIGHEST = lax.Precision.HIGHEST
LOG2E = 1.4426950408889634
NEG = -1e30
BF16 = jnp.bfloat16
F32 = jnp.float32
WINDOW = 256
LANES = 128


def flip(array, axis, bit):
    size = lax.axis_size(axis)
    return lax.ppermute(array, axis, [(i, i ^ bit) for i in range(size)])


def shift(array, axis, step):
    size = lax.axis_size(axis)
    return lax.ppermute(array, axis, [(i, (i + step) % size) for i in range(size)])


def pick(array, index):
    return lax.dynamic_index_in_dim(array, index, 0, keepdims=False)


def in_order(first, second, swapped):
    return jnp.where(swapped, jnp.stack([second, first]), jnp.stack([first, second]))


def to_latent(array):
    seq, fsdp = lax.axis_size("seq"), lax.axis_size("fsdp")
    place = lax.axis_index("seq")
    arrived = []
    for turn in range(2):
        pairs = []
        for f in range(fsdp):
            for s in range(seq):
                pair, core = f // 2, f % 2
                target = (pair * 2 + s // 2, 2 * core + (s + turn) % 2)
                pairs.append((f * seq + s, target[0] * seq + target[1]))
        block = pick(array, (place + turn) % 2)
        arrived.append(lax.ppermute(block, ("fsdp", "seq"), pairs))
    both = in_order(arrived[0], arrived[1], place % 2 == 1)
    return both.reshape((-1,) + both.shape[2:])


def from_latent(array):
    seq, fsdp = lax.axis_size("seq"), lax.axis_size("fsdp")
    place = lax.axis_index("seq")
    halves = array.reshape((2, array.shape[0] // 2) + array.shape[1:])
    arrived = []
    for turn in range(2):
        pairs = []
        for f in range(fsdp):
            for s in range(seq):
                pair, core = f // 2, f % 2
                slot = (s + turn) % 2
                target = (pair * 2 + s // 2, 2 * core + slot)
                pairs.append((f * seq + s, target[0] * seq + target[1]))
        arrived.append(lax.ppermute(pick(halves, (place + turn) % 2), ("fsdp", "seq"), pairs))
    return in_order(arrived[0], arrived[1], place % 2 == 1)


def sum_everywhere(value, fast):
    if not fast:
        return lax.psum(value, ("rep", "fsdp", "seq"))
    for axis, bit in (("fsdp", 1), ("fsdp", 2), ("rep", 1), ("seq", 1), ("seq", 2)):
        value = value + flip(value, axis, bit)
    return value


def gather_rows(row, fast):
    if not fast:
        fsdp = lax.axis_size("fsdp")
        everything = lax.all_gather(row, ("rep", "fsdp", "seq"), axis=0)
        everything = everything.reshape((-1, fsdp // 2, 2, lax.axis_size("seq")) + row.shape)
        return everything[:, :, 0].reshape((-1,) + row.shape)
    seq = lax.axis_size("seq")
    place = lax.axis_index("seq")
    here = [row] + [shift(row, "seq", step) for step in range(1, seq)]
    here = jnp.stack(here)
    here = jnp.concatenate(
        [lax.dynamic_slice_in_dim(here, (place - s) % seq, 1, 0) for s in range(seq)]
    )
    both = in_order(here, flip(here, "fsdp", 2), lax.axis_index("fsdp") >= 2)
    both = both.reshape((-1,) + row.shape)
    quad = in_order(both, flip(both, "rep", 1), lax.axis_index("rep") == 1)
    return quad.reshape((-1,) + row.shape)


def gather_small(vector, fast):
    if not fast:
        return lax.all_gather(vector, "fsdp", axis=0)
    place = lax.axis_index("fsdp")
    pair = in_order(vector, flip(vector, "fsdp", 1), place % 2 == 1)
    quad = in_order(pair, flip(pair, "fsdp", 2), place >= 2)
    return quad.reshape((-1,) + vector.shape)


def gather_weight(weight):
    return lax.all_gather(weight, "fsdp", axis=0, tiled=True)


MESH = pl.DeviceIdType.MESH


class Spot:
    def __init__(self):
        self.x, self.f, self.s = (lax.axis_index(name) for name in ("rep", "fsdp", "seq"))
        self.core = self.f % 2
        self.pair = self.f // 2

    def other(self, bit):
        if bit == 3:
            return 3 - self.f
        return self.f + bit - 2 * bit * ((self.f // bit) % 2)

    def fsdp(self, bit):
        return (self.x, self.other(bit), self.s)

    def rep(self, bit=0):
        return (1 - self.x, self.other(bit) if bit else self.f, self.s)

    def seq(self, step):
        return (self.x, self.f, lax.rem(self.s + step, 4))

    def token_target(self, turn):
        block = lax.rem(self.s + turn, 2)
        return (self.x, 2 * self.pair + self.s // 2, 2 * self.core + block), block


def greet(devices):
    barrier = pltpu.get_barrier_semaphore()
    for device in devices:
        pl.semaphore_signal(barrier, inc=1, device_id=device, device_id_type=MESH)
    pl.semaphore_wait(barrier, len(devices))


def column_group(spot):
    found = [(spot.x, spot.other(1), spot.s)]
    for step in range(1, 4):
        found.append(spot.seq(step))
        found.append((spot.x, spot.other(1), lax.rem(spot.s + step, 4)))
    return found


class Sender:
    def __init__(self, send_sems, recv_sems):
        self.send_sems, self.recv_sems = send_sems, recv_sems
        self.used = 0
        self.open = []

    def slot(self):
        self.used += 1
        return self.used - 1

    def start(self, slot, source, target, device):
        copy = pltpu.make_async_remote_copy(
            source, target, self.send_sems.at[slot], self.recv_sems.at[slot], device, MESH
        )
        copy.start()
        self.open.append(copy)

    def arrived(self, slot, view):
        pltpu.make_async_copy(view, view, self.recv_sems.at[slot]).wait()

    def finish(self):
        for copy in self.open:
            copy.wait_send()
        self.open = []


class Locals:
    def __init__(self, sems):
        self.sems = sems
        self.used = 0
        self.open = []

    def start(self, source, target):
        copy = pltpu.make_async_copy(source, target, self.sems.at[self.used])
        self.used += 1
        copy.start()
        return copy


class TokenMove:
    def __init__(self, sender, spot, source, target):
        self.sender, self.spot, self.source, self.target = sender, spot, source, target
        self.slots = [sender.slot(), sender.slot()]

    def start(self):
        spot = self.spot
        self.remote = []
        for turn, slot in enumerate(self.slots):
            device, block = spot.token_target(turn)
            stays = (device[1] == spot.f) & (device[2] == spot.s)
            source = self.source.at[block]
            target = self.target.at[lax.rem(spot.s, 2)]
            remote = pltpu.make_async_remote_copy(
                source,
                target,
                self.sender.send_sems.at[slot],
                self.sender.recv_sems.at[slot],
                device,
                MESH,
            )
            local = pltpu.make_async_copy(source, target, self.sender.recv_sems.at[slot])
            pl.when(jnp.logical_not(stays))(lambda remote=remote: remote.start())
            pl.when(stays)(lambda local=local: local.start())
            self.remote.append((stays, remote))

    def finish(self):
        for turn, slot in enumerate(self.slots):
            self.sender.arrived(slot, self.target.at[lax.rem(self.spot.s + turn, 2)])
        for stays, remote in self.remote:
            pl.when(jnp.logical_not(stays))(lambda remote=remote: remote.wait_send())


class WeightMove:
    def __init__(self, sender, local, spot, own, full, stage, chunks):
        self.sender, self.local, self.spot = sender, local, spot
        self.own, self.full, self.stage = own, full, stage
        self.rows, self.chunks = own.shape[0], chunks
        self.half = self.rows // 2
        self.tall = self.half // chunks
        self.slots = {
            kind: [sender.slot() for _ in range(1 if kind == "core" else chunks)]
            for kind in ("core", "far", "side", "far_core", "side_core")
        }

    def view(self, bits, side, chunk):
        shard = self.spot.other(bits) if bits else self.spot.f
        half = self.spot.x if side == 0 else 1 - self.spot.x
        start = shard * self.rows + half * self.half + chunk * self.tall
        return self.full.at[pl.ds(pl.multiple_of(start, 16), self.tall)]

    def shard_view(self, bits):
        shard = self.spot.other(bits) if bits else self.spot.f
        return self.full.at[pl.ds(pl.multiple_of(shard * self.rows, 16), self.rows)]

    def start_far(self):
        spot = self.spot
        for chunk, slot in enumerate(self.slots["far"]):
            start = pl.multiple_of(spot.x * self.half + chunk * self.tall, 16)
            self.sender.start(
                slot, self.own.at[pl.ds(start, self.tall)], self.view(0, 0, chunk), spot.fsdp(2)
            )

    def start_near(self):
        self.sender.start(self.slots["core"][0], self.own, self.shard_view(0), self.spot.fsdp(1))
        self.load = self.local.start(self.own, self.stage)

    def store(self):
        self.load.wait()
        self.kept = self.local.start(self.stage, self.shard_view(0))

    def pass_far(self, chunk):
        view = self.view(2, 0, chunk)
        self.sender.arrived(self.slots["far"][chunk], view)
        self.sender.start(self.slots["side"][chunk], view, view, self.spot.rep())
        self.sender.start(self.slots["far_core"][chunk], view, view, self.spot.fsdp(1))

    def pass_side(self, chunk):
        view = self.view(2, 1, chunk)
        self.sender.arrived(self.slots["side"][chunk], view)
        self.sender.start(self.slots["side_core"][chunk], view, view, self.spot.fsdp(1))

    def finish(self):
        self.kept.wait()
        self.sender.arrived(self.slots["core"][0], self.shard_view(1))
        for chunk in range(self.chunks):
            self.sender.arrived(self.slots["far_core"][chunk], self.view(3, 0, chunk))
            self.sender.arrived(self.slots["side_core"][chunk], self.view(3, 1, chunk))


def entry_kernel(
    tokens,
    valid,
    cond,
    biases,
    mod_weight,
    qkv_weight,
    out_weight,
    tokens_own,
    valid_all,
    mod_parts,
    bias_all,
    qkv_full,
    out_full,
    mod_held,
    cond_held,
    partial,
    qkv_stage,
    out_stage,
    send_sems,
    recv_sems,
    local_sems,
):
    spot = Spot()
    sender, local = Sender(send_sems, recv_sems), Locals(local_sems)
    mod_load = local.start(mod_weight, mod_held)
    greet(column_group(spot) + [spot.fsdp(2), spot.fsdp(3), spot.rep()])

    row = lax.rem(spot.s, 2)
    cond_slots, bias_slots = {}, {}
    for bit in (1, 2, 3):
        cond_slots[bit], bias_slots[bit] = sender.slot(), sender.slot()
        target = spot.other(bit)
        sender.start(
            cond_slots[bit], cond.at[row, target], cond_held.at[spot.f], spot.fsdp(bit)
        )
    for bit in (1, 2, 3):
        sender.start(bias_slots[bit], biases, bias_all.at[spot.f], spot.fsdp(bit))
    cond_own = local.start(cond.at[row, spot.f], cond_held.at[spot.f])
    bias_own = local.start(biases, bias_all.at[spot.f])

    qkv = WeightMove(sender, local, spot, qkv_weight, qkv_full, qkv_stage, 3)
    out = WeightMove(sender, local, spot, out_weight, out_full, out_stage, 1)
    mod_slots = {bit: sender.slot() for bit in (1, 2, 3)}
    move = TokenMove(sender, spot, tokens, tokens_own)
    valid_base = [sender.slot() for _ in range(4)][0]
    valid_open = []
    for turn in range(2):
        device, block = spot.token_target(turn)
        for core in range(2):
            goal = (device[0], 2 * spot.pair + core, device[2])
            stays = (goal[1] == spot.f) & (goal[2] == spot.s)
            source, target = valid.at[block], valid_all.at[spot.s]
            arrival = recv_sems.at[valid_base + spot.s]
            remote = pltpu.make_async_remote_copy(
                source, target, send_sems.at[valid_base + 2 * turn + core], arrival, goal, MESH
            )
            near = pltpu.make_async_copy(source, target, arrival)
            pl.when(jnp.logical_not(stays))(lambda remote=remote: remote.start())
            pl.when(stays)(lambda near=near: near.start())
            valid_open.append((stays, remote))
    move.start()
    qkv.start_far()
    qkv.start_near()
    out.start_near()

    cond_own.wait()
    for bit in (1, 2, 3):
        sender.arrived(cond_slots[bit], cond_held.at[spot.other(bit)])
    first, second = cond_held[spot.s // 2], cond_held[2 + spot.s // 2]
    which = lax.broadcasted_iota(jnp.int32, (16, first.shape[-1]), 0)
    conds = jnp.where(which == 0, first, second)
    silu = (conds / (1.0 + jnp.exp(-conds))).astype(BF16)
    mod_load.wait()
    width = mod_held.shape[1] // 6
    for piece in range(6):
        columns = slice(piece * width, (piece + 1) * width)
        product = jnp.dot(silu, mod_held[:, columns], preferred_element_type=F32)
        partial[0, :, columns] = product[0:1]
        partial[1, :, columns] = product[1:2]
    for bit in (1, 2, 3):
        pair = spot.pair if bit == 1 else 1 - spot.pair
        sender.start(
            mod_slots[bit], partial.at[pair], mod_parts.at[spot.f], spot.fsdp(bit)
        )
    mod_own = local.start(partial.at[spot.pair], mod_parts.at[spot.f])
    out.start_far()
    qkv.store()
    out.store()
    for chunk in range(3):
        qkv.pass_far(chunk)
        if chunk:
            qkv.pass_side(chunk - 1)
    qkv.pass_side(2)
    out.pass_far(0)
    out.pass_side(0)

    bias_own.wait()
    mod_own.wait()
    for bit in (1, 2, 3):
        sender.arrived(bias_slots[bit], bias_all.at[spot.other(bit)])
        sender.arrived(mod_slots[bit], mod_parts.at[spot.other(bit)])
    for place in range(4):
        sender.arrived(valid_base + place, valid_all.at[place])
    for stays, remote in valid_open:
        pl.when(jnp.logical_not(stays))(lambda remote=remote: remote.wait_send())
    move.finish()
    qkv.finish()
    out.finish()
    sender.finish()


def sems(count):
    return pltpu.SemaphoreType.DMA((count,))


def enter(tokens, valid, cond, biases, mod_weight, qkv_weight, out_weight):
    anywhere = pl.BlockSpec(memory_space=pl.ANY)
    return pl.pallas_call(
        entry_kernel,
        out_shape=[
            jax.ShapeDtypeStruct(tokens.shape, tokens.dtype),
            jax.ShapeDtypeStruct((4,) + valid.shape[1:], F32),
            jax.ShapeDtypeStruct((4, 1, mod_weight.shape[1]), F32),
            jax.ShapeDtypeStruct((4,) + biases.shape, F32),
            jax.ShapeDtypeStruct((4 * qkv_weight.shape[0], qkv_weight.shape[1]), BF16),
            jax.ShapeDtypeStruct((4 * out_weight.shape[0], out_weight.shape[1]), BF16),
        ],
        in_specs=[anywhere] * 7,
        out_specs=[anywhere] * 6,
        scratch_shapes=[
            pltpu.VMEM(mod_weight.shape, BF16),
            pltpu.VMEM((4,) + cond.shape[2:], F32),
            pltpu.VMEM((2, 1, mod_weight.shape[1]), F32),
            pltpu.VMEM(qkv_weight.shape, BF16),
            pltpu.VMEM(out_weight.shape, BF16),
            sems(40),
            sems(40),
            sems(12),
        ],
        compiler_params=pltpu.CompilerParams(
            collective_id=1, has_side_effects=True, vmem_limit_bytes=32 * 1024 * 1024
        ),
        name="enter",
    )(tokens, valid, cond, biases, mod_weight, qkv_weight, out_weight)


def outer_kernel(has_extra, left_own, left_other, right_own, right_other, *rest):
    out = rest[-1]
    dims = (((0,), (0,)), ((), ()))
    total = lax.dot_general(left_own[...], right_own[...], dims, preferred_element_type=F32)
    total += lax.dot_general(left_other[...], right_other[...], dims, preferred_element_type=F32)
    if has_extra:
        total += rest[0][0].astype(F32)
    out[0] = total.astype(out.dtype)


def outer_blocks(left_own, left_other, right_own, right_other, extra=None):
    tokens, rows = left_own.shape
    columns = right_own.shape[1]
    width = 1152
    tall = 384 if rows % 384 == 0 else rows
    blocks = columns // width
    left_spec = pl.BlockSpec((tokens, tall), lambda j, i: (0, i))
    right_spec = pl.BlockSpec((tokens, width), lambda j, i: (0, j))
    out_spec = pl.BlockSpec((1, tall, width), lambda j, i: (j, i, 0))
    operands = [left_own, left_other, right_own, right_other]
    specs = [left_spec, left_spec, right_spec, right_spec]
    if extra is not None:
        operands.append(extra)
        specs.append(out_spec)
    return pl.pallas_call(
        functools.partial(outer_kernel, extra is not None),
        grid=(blocks, rows // tall),
        out_shape=jax.ShapeDtypeStruct((blocks, rows, width), BF16),
        in_specs=specs,
        out_specs=out_spec,
        cost_estimate=pl.CostEstimate(
            flops=4 * tokens * rows * columns,
            transcendentals=0,
            bytes_accessed=2 * (2 * tokens * (rows + columns) + 2 * rows * columns),
        ),
        name="outer",
    )(*operands)


def reduce_start(give):
    return flip(give, "fsdp", 2)


def reduce_rest(kept):
    seq = lax.axis_size("seq")
    place, replica = lax.axis_index("seq"), lax.axis_index("rep")
    width = kept.shape[-1]
    parts = kept.reshape(2, seq, -1, width)
    arrived = flip(pick(parts, 1 - replica), "rep", 1)
    mine = (pick(parts, replica).astype(F32) + arrived.astype(F32)).astype(BF16)
    others = [shift(pick(mine, (place + step) % seq), "seq", step) for step in range(1, seq)]
    total = pick(mine, place).astype(F32)
    for other in others:
        total = total + other.astype(F32)
    total = total.astype(BF16)
    along = [total] + [shift(total, "seq", step) for step in range(1, seq)]
    across = [flip(piece, "rep", 1) for piece in along]
    return along + across


def place_kernel(layout, pieces, outs, held, wide, in_sem, out_sem):
    place, replica = lax.axis_index("seq"), lax.axis_index("rep")
    seq = len(pieces) // 2
    tall, width = pieces[0].shape
    loads = []
    for number, piece in enumerate(pieces):
        loads.append(pltpu.make_async_copy(piece, held.at[number], in_sem.at[number]))
        loads[-1].start()

    def target(number):
        step = number % seq
        side = replica if number < seq else 1 - replica
        return side * seq + (place + seq - step) % seq

    def copies(number):
        index = target(number)
        found = []
        if layout == "tall":
            rows = pl.ds(pl.multiple_of(index * tall, 8), tall)
            found.append((None, outs[0].at[rows]))
        else:
            per_block = outs[0].shape[0] // tall
            rows = pl.ds(pl.multiple_of((index % per_block) * tall, 8), tall)
            block = index // per_block
            low = 0
            for out in outs:
                count = out.shape[1] // width
                columns = pl.ds(pl.multiple_of((block - low) * width, LANES), width)
                inside = (block >= low) & (block < low + count) if len(outs) > 1 else None
                found.append((inside, out.at[rows, columns]))
                low += count
        return [
            (inside, pltpu.make_async_copy(wide.at[number], view, out_sem.at[number]))
            for inside, view in found
        ]

    def each(number, act):
        for inside, copy in copies(number):
            if inside is None:
                act(copy)
            else:
                pl.when(inside)(functools.partial(act, copy))

    for number, load in enumerate(loads):
        load.wait()
        wide[number] = held[number].astype(F32)
        each(number, lambda copy: copy.start())
    for number in range(len(loads)):
        each(number, lambda copy: copy.wait())


def place_pieces(pieces, shapes, layout):
    count = len(pieces)
    tall, width = pieces[0].shape

    def body(*refs):
        place_kernel(
            layout,
            refs[:count],
            refs[count : count + len(shapes)],
            *refs[count + len(shapes) :],
        )

    return pl.pallas_call(
        body,
        out_shape=[jax.ShapeDtypeStruct(shape, F32) for shape in shapes],
        in_specs=[pl.BlockSpec(memory_space=pl.ANY)] * count,
        out_specs=[pl.BlockSpec(memory_space=pl.ANY)] * len(shapes),
        scratch_shapes=[
            pltpu.VMEM((count, tall, width), BF16),
            pltpu.VMEM((count, tall, width), F32),
            pltpu.SemaphoreType.DMA((count,)),
            pltpu.SemaphoreType.DMA((count,)),
        ],
        cost_estimate=pl.CostEstimate(
            flops=0, transcendentals=0, bytes_accessed=6 * count * tall * width
        ),
        name="place",
    )(*pieces)


def head_window(head, head_dim, width):
    start = head * head_dim
    base = jnp.minimum(start // LANES, (width - WINDOW) // LANES) * LANES
    base = pl.multiple_of(base, LANES)
    return start, base


def forward_heads(
    low,
    high,
    q_ref,
    k_own,
    v_own,
    k_other,
    v_other,
    bias_own,
    bias_other,
    out_ref,
    lse_ref,
):
    tokens, width = q_ref.shape
    head_dim = width // HEADS
    blocks = 2
    tall = tokens // blocks
    scale = head_dim ** (-0.5) * LOG2E
    b_own, b_other = bias_own[...], bias_other[...]
    dims = (((1,), (1,)), ((), ()))

    def body(head, carry):
        start, base = head_window(head, head_dim, width)
        window = pl.ds(base, WINDOW)
        lane = lax.broadcasted_iota(jnp.int32, (1, WINDOW), 1) + base
        inside = (lane >= start) & (lane < start + head_dim)
        keep = inside.astype(BF16)
        spot = lax.broadcasted_iota(jnp.int32, (1, LANES), 1) == head
        key_one, key_two = k_own[:, window], k_other[:, window]
        val_one, val_two = v_own[:, window] * keep, v_other[:, window] * keep
        for block in range(blocks):
            rows = pl.ds(block * tall, tall)
            query = q_ref[rows, window] * keep
            one = lax.dot_general(query, key_one, dims, preferred_element_type=F32)
            two = lax.dot_general(query, key_two, dims, preferred_element_type=F32)
            one = one * scale + b_own
            two = two * scale + b_other
            top = jnp.maximum(
                jnp.max(one, axis=1, keepdims=True), jnp.max(two, axis=1, keepdims=True)
            )
            one = jnp.exp2(one - top)
            two = jnp.exp2(two - top)
            total = jnp.sum(one, axis=1, keepdims=True) + jnp.sum(two, axis=1, keepdims=True)
            mixed = jnp.dot(one.astype(BF16), val_one, preferred_element_type=F32)
            mixed += jnp.dot(two.astype(BF16), val_two, preferred_element_type=F32)
            mixed = mixed * (1.0 / total)
            out_ref[rows, window] = jnp.where(
                inside, mixed, out_ref[rows, window].astype(F32)
            ).astype(out_ref.dtype)
            lse_ref[rows, :] = jnp.where(spot, top + jnp.log2(total), lse_ref[rows, :])
        return carry

    lax.fori_loop(low, high, body, 0)


def forward_kernel(*refs):
    out_ref, lse_ref = refs[-2:]
    out_ref[...] = jnp.zeros_like(out_ref)
    lse_ref[...] = jnp.zeros_like(lse_ref)
    forward_heads(0, HEADS, *refs)


def forward_send_kernel(
    q_ref,
    k_own,
    v_own,
    bias_own,
    bias_other,
    count_in,
    up_weight,
    down_weight,
    teacher,
    out_grad,
    out_ref,
    lse_ref,
    k_other,
    v_other,
    count_out,
    up_full,
    down_full,
    teacher_own,
    out_grad_own,
    counts,
    count_sum,
    far_counts,
    up_stage,
    down_stage,
    send_sems,
    recv_sems,
    local_sems,
):
    spot = Spot()
    sender, local = Sender(send_sems, recv_sems), Locals(local_sems)
    greet(column_group(spot) + [spot.fsdp(2), spot.rep(), spot.rep(2)])
    count_slots = [sender.slot() for _ in range(3)]
    for step in range(1, 4):
        sender.start(count_slots[step - 1], count_in, counts.at[step - 1], spot.seq(step))
    key_slot, value_slot = sender.slot(), sender.slot()
    sender.start(key_slot, k_own, k_other, spot.fsdp(1))
    sender.start(value_slot, v_own, v_other, spot.fsdp(1))
    moves = [
        TokenMove(sender, spot, teacher, teacher_own),
        TokenMove(sender, spot, out_grad, out_grad_own),
    ]
    up = WeightMove(sender, local, spot, up_weight, up_full, up_stage, 3)
    down = WeightMove(sender, local, spot, down_weight, down_full, down_stage, 4)
    far_slots = [sender.slot() for _ in range(3)]

    total = count_in[...]
    for step in range(1, 4):
        sender.arrived(count_slots[step - 1], counts.at[step - 1])
        total = total + counts[step - 1]
    count_sum[...] = total
    for number, device in enumerate((spot.fsdp(2), spot.rep(), spot.rep(2))):
        sender.start(far_slots[number], count_sum, far_counts.at[number], device)
    up.start_far()
    down.start_far()
    for move in moves:
        move.start()
    sender.arrived(key_slot, k_other)
    sender.arrived(value_slot, v_other)
    up.start_near()
    down.start_near()
    out_ref[...] = jnp.zeros_like(out_ref)
    lse_ref[...] = jnp.zeros_like(lse_ref)
    data = (q_ref, k_own, v_own, k_other, v_other, bias_own, bias_other, out_ref, lse_ref)
    forward_heads(0, 8, *data)
    up.store()
    down.store()
    up.pass_far(0)
    forward_heads(8, HEADS, *data)
    up.pass_far(1)
    up.pass_side(0)
    up.pass_far(2)
    up.pass_side(1)
    down.pass_far(0)
    up.pass_side(2)
    for chunk in range(1, 4):
        down.pass_far(chunk)
        down.pass_side(chunk - 1)
    down.pass_side(3)
    total = count_sum[...]
    for number in range(3):
        sender.arrived(far_slots[number], far_counts.at[number])
        total = total + far_counts[number]
    count_out[...] = total
    for move in moves:
        move.finish()
    up.finish()
    down.finish()
    sender.finish()


def attend_and_gather(
    queries,
    keys,
    values,
    bias_own,
    bias_other,
    count,
    up_weight,
    down_weight,
    teacher,
    out_grad,
):
    tokens, width = queries.shape
    anywhere = pl.BlockSpec(memory_space=pl.ANY)
    near = pl.BlockSpec(memory_space=pltpu.VMEM)
    shape = (tokens, width)
    return pl.pallas_call(
        forward_send_kernel,
        out_shape=[
            jax.ShapeDtypeStruct(shape, BF16),
            jax.ShapeDtypeStruct((tokens, LANES), F32),
            jax.ShapeDtypeStruct(shape, BF16),
            jax.ShapeDtypeStruct(shape, BF16),
            jax.ShapeDtypeStruct(count.shape, F32),
            jax.ShapeDtypeStruct((4 * up_weight.shape[0], up_weight.shape[1]), BF16),
            jax.ShapeDtypeStruct((4 * down_weight.shape[0], down_weight.shape[1]), BF16),
            jax.ShapeDtypeStruct(teacher.shape, BF16),
            jax.ShapeDtypeStruct(out_grad.shape, BF16),
        ],
        in_specs=[near] * 6 + [anywhere] * 4,
        out_specs=[near] * 5 + [anywhere] * 4,
        scratch_shapes=[
            pltpu.VMEM((3,) + count.shape, F32),
            pltpu.VMEM(count.shape, F32),
            pltpu.VMEM((3,) + count.shape, F32),
            pltpu.VMEM(up_weight.shape, BF16),
            pltpu.VMEM(down_weight.shape, BF16),
            sems(48),
            sems(48),
            sems(8),
        ],
        compiler_params=pltpu.CompilerParams(
            collective_id=2, has_side_effects=True, vmem_limit_bytes=56 * 1024 * 1024
        ),
        name="attend_and_gather",
    )(
        queries,
        keys,
        values,
        bias_own,
        bias_other,
        count,
        up_weight,
        down_weight,
        teacher,
        out_grad,
    )


def attend(queries, k_own, v_own, k_other, v_other, bias_own, bias_other):
    tokens, width = queries.shape
    return pl.pallas_call(
        forward_kernel,
        out_shape=[
            jax.ShapeDtypeStruct((tokens, width), BF16),
            jax.ShapeDtypeStruct((tokens, LANES), F32),
        ],
        compiler_params=pltpu.CompilerParams(vmem_limit_bytes=48 * 1024 * 1024),
        cost_estimate=pl.CostEstimate(
            flops=16 * tokens * tokens * 2 * WINDOW * 4,
            transcendentals=HEADS * tokens * tokens * 2,
            bytes_accessed=6 * tokens * width * 2,
        ),
        name="attend",
    )(queries, k_own, v_own, k_other, v_other, bias_own, bias_other)


def backward_kernel(
    head_dim,
    q_ref,
    k_own,
    v_own,
    k_other,
    v_other,
    do_ref,
    lse_ref,
    bias_own,
    bias_other,
    dq_out,
    dk_own_out,
    dv_own_out,
    dk_other_out,
    dv_other_out,
    dq_acc,
    dk_one,
    dv_one,
    dk_two,
    dv_two,
):
    tokens, width = q_ref.shape
    factor = head_dim ** (-0.5)
    scale = factor * LOG2E
    for ref in (dq_acc, dk_one, dv_one, dk_two, dv_two):
        ref[...] = jnp.zeros_like(ref)
    across = (((1,), (1,)), ((), ()))
    down = (((0,), (0,)), ((), ()))
    sides = (
        (k_own, v_own, bias_own, dk_one, dv_one),
        (k_other, v_other, bias_other, dk_two, dv_two),
    )

    def body(head, carry):
        start, base = head_window(head, head_dim, width)
        window = pl.ds(base, WINDOW)
        lane = lax.broadcasted_iota(jnp.int32, (1, WINDOW), 1) + base
        keep = ((lane >= start) & (lane < start + head_dim)).astype(BF16)
        query = q_ref[:, window] * keep
        grad = do_ref[:, window] * keep
        lse = lse_ref[pl.ds(head, 1), :]
        probs, prods = [], []
        delta = None
        for k_ref, v_ref, bias, _, _ in sides:
            scores = lax.dot_general(k_ref[:, window], query, across, preferred_element_type=F32)
            prob = jnp.exp2(scores * scale + bias[...] - lse)
            prob_grad = lax.dot_general(v_ref[:, window], grad, across, preferred_element_type=F32)
            prod = prob * prob_grad
            part = jnp.sum(prod, axis=0, keepdims=True)
            delta = part if delta is None else delta + part
            probs.append(prob)
            prods.append(prod)
        dq = None
        for (k_ref, _, _, dk, dv), prob, prod in zip(sides, probs, prods, strict=True):
            dv[:, window] += jnp.dot(prob.astype(BF16), grad, preferred_element_type=F32)
            score_grad = (prod - prob * delta).astype(BF16)
            dk[:, window] += jnp.dot(score_grad, query, preferred_element_type=F32)
            part = lax.dot_general(
                score_grad, k_ref[:, window] * keep, down, preferred_element_type=F32
            )
            dq = part if dq is None else dq + part
        dq_acc[:, window] += dq
        return carry

    lax.fori_loop(0, HEADS, body, 0)
    dq_out[...] = (dq_acc[...] * factor).astype(dq_out.dtype)
    dk_own_out[...] = (dk_one[...] * factor).astype(dk_own_out.dtype)
    dv_own_out[...] = dv_one[...].astype(dv_own_out.dtype)
    dk_other_out[...] = (dk_two[...] * factor).astype(dk_other_out.dtype)
    dv_other_out[...] = dv_two[...].astype(dv_other_out.dtype)


def attend_back(queries, k_own, v_own, k_other, v_other, grad, lse, bias_own, bias_other):
    tokens, width = queries.shape
    shape = (tokens, width)
    return pl.pallas_call(
        functools.partial(backward_kernel, width // HEADS),
        out_shape=[
            jax.ShapeDtypeStruct(shape, BF16),
            jax.ShapeDtypeStruct(shape, F32),
            jax.ShapeDtypeStruct(shape, F32),
            jax.ShapeDtypeStruct(shape, BF16),
            jax.ShapeDtypeStruct(shape, BF16),
        ],
        scratch_shapes=[pltpu.VMEM(shape, F32) for _ in range(5)],
        compiler_params=pltpu.CompilerParams(vmem_limit_bytes=60 * 1024 * 1024),
        cost_estimate=pl.CostEstimate(
            flops=16 * tokens * tokens * 2 * WINDOW * 10,
            transcendentals=HEADS * tokens * tokens * 2,
            bytes_accessed=13 * tokens * width * 2,
        ),
        name="attend_back",
    )(queries, k_own, v_own, k_other, v_other, grad, lse, bias_own, bias_other)


def dot(left, right):
    return jnp.dot(left, right, preferred_element_type=F32)


def dot_t(left, right):
    return lax.dot_general(left, right, (((1,), (1,)), ((), ())), preferred_element_type=F32)


def norm_parts(inputs):
    centred = inputs - jnp.mean(inputs, axis=-1, keepdims=True)
    rate = lax.rsqrt(jnp.mean(centred * centred, axis=-1, keepdims=True) + EPS)
    return centred * rate, rate


def norm_back(grad, normed, rate):
    return rate * (
        grad
        - jnp.mean(grad, axis=-1, keepdims=True)
        - normed * jnp.mean(grad * normed, axis=-1, keepdims=True)
    )


def gelu_parts(inputs):
    inner = jnp.tanh(GELU_C * (inputs + 0.044715 * inputs * inputs * inputs))
    value = 0.5 * inputs * (1.0 + inner)
    slope = 0.5 * (1.0 + inner) + 0.5 * inputs * (1.0 - inner * inner) * GELU_C * (
        1.0 + 3.0 * 0.044715 * inputs * inputs
    )
    return value, slope


def column_sum(array):
    return jnp.sum(array.astype(F32), axis=0)


def shards(
    tokens,
    condition,
    valid_mask,
    teacher,
    out_grad,
    mod_weight,
    mod_bias,
    qkv_weight,
    qkv_bias,
    out_weight,
    out_bias,
    up_weight,
    up_bias,
    down_weight,
    down_bias,
):
    reps, fsdp, seq = lax.axis_size("rep"), lax.axis_size("fsdp"), lax.axis_size("seq")
    fast = (reps, fsdp, seq) == (2, 4, 4)
    latents, span, width = tokens.shape
    assert 2 * latents == seq and latents == 2
    place_f, place_s = lax.axis_index("fsdp"), lax.axis_index("seq")
    total_tokens = latents * span * reps * fsdp * seq

    biases = jnp.concatenate([mod_bias, qkv_bias, out_bias, up_bias, down_bias])
    shard_rows = mod_weight.shape[0]
    cond_row = pick(condition, place_s % 2)
    keep_mask = valid_mask.astype(F32)

    if fast:
        inputs_low, valid_all, mod_parts, bias_all, qkv_full, out_full = enter(
            tokens,
            keep_mask.reshape(latents, 1, span),
            condition.astype(F32).reshape(latents, fsdp, 1, shard_rows),
            biases.astype(F32)[None],
            mod_weight,
            qkv_weight,
            out_weight,
        )
        inputs_low = inputs_low.reshape(-1, width)
        valid_all = valid_all.reshape(2, -1)
        keyvalid, valid_other = pick(valid_all, place_f % 2), pick(valid_all, 1 - place_f % 2)
        mod_row = jnp.sum(mod_parts, axis=(0, 1))
        bias_all = bias_all[:, 0]
    else:
        inputs_low = to_latent(tokens)
        keyvalid = to_latent(keep_mask)
        valid_other = flip(keyvalid, "fsdp", 1)
        counted = lax.psum(jnp.sum(keep_mask), ("rep", "fsdp", "seq")).reshape(1, 1)
        own_row = jnp.where(place_f % 2 == place_s // 2, cond_row, flip(cond_row, "fsdp", 1))
        cond_pair = lax.all_gather(own_row, "fsdp", axis=0)[::2]
        silu_pair = jax.nn.silu(cond_pair.astype(F32)).astype(BF16)
        silu_cols = lax.dynamic_slice_in_dim(silu_pair, place_f * shard_rows, shard_rows, 1)
        mod_row = pick(lax.psum(dot(silu_cols, mod_weight), "fsdp"), place_f // 2)
        bias_all = lax.all_gather(biases, "fsdp", axis=0).astype(F32)
        qkv_full, out_full = gather_weight(qkv_weight), gather_weight(out_weight)
        up_full, down_full = gather_weight(up_weight), gather_weight(down_weight)
        teacher_own, out_grad_own = to_latent(teacher), to_latent(out_grad)
    mask_own = (keyvalid - 1.0) * (-NEG)
    mask_other = (valid_other - 1.0) * (-NEG)

    cuts = [0]
    for bias in (mod_bias, qkv_bias, out_bias, up_bias, down_bias):
        cuts.append(cuts[-1] + bias.shape[0])
    mod_b, qkv_b, out_b, up_b, down_b = (
        bias_all[:, low:high].reshape(-1) for low, high in zip(cuts[:-1], cuts[1:], strict=True)
    )
    pieces = (mod_row + mod_b).reshape(6, 1, width)
    shift_one, scale_one, gate_one, shift_two, scale_two, gate_two = (pieces[i] for i in range(6))

    inputs = inputs_low.astype(F32)
    normed_one, rate_one = norm_parts(inputs)
    hidden_one = (normed_one * (1.0 + scale_one) + shift_one).astype(BF16)
    projected = dot(hidden_one, qkv_full)
    queries = (projected[:, :width] + qkv_b[:width]).astype(BF16)
    keys_own = projected[:, width : 2 * width].astype(BF16)
    values_own = (projected[:, 2 * width :] + qkv_b[width:]).astype(BF16)
    if fast:
        (
            attended,
            lse,
            keys_other,
            values_other,
            counted,
            up_full,
            down_full,
            teacher_own,
            out_grad_own,
        ) = attend_and_gather(
            queries,
            keys_own,
            values_own,
            mask_own[None],
            mask_other[None],
            jnp.full((1, LANES), jnp.sum(valid_all)),
            up_weight,
            down_weight,
            teacher,
            out_grad,
        )
        counted = counted[:, :1]
        teacher_own = teacher_own.reshape(-1, width)
        out_grad_own = out_grad_own.reshape(-1, width)
    else:
        keys_other, values_other = flip(keys_own, "fsdp", 1), flip(values_own, "fsdp", 1)
        attended, lse = attend(
            queries,
            keys_own,
            values_own,
            keys_other,
            values_other,
            mask_own[None],
            mask_other[None],
        )
    branch = dot(attended, out_full) + out_b
    middle = inputs + gate_one * branch
    normed_two, rate_two = norm_parts(middle)
    hidden_two = (normed_two * (1.0 + scale_two) + shift_two).astype(BF16)
    up_pre = dot(hidden_two, up_full) + up_b
    activated, slope = gelu_parts(up_pre)
    activated = activated.astype(BF16)
    mlp_out = dot(activated, down_full) + down_b
    output = middle + gate_two * mlp_out
    block_out = from_latent(output.astype(BF16))
    differ = (output - teacher_own.astype(F32)) * keyvalid[:, None]
    err_total = sum_everywhere(jnp.sum(differ * differ).reshape(1, 1), fast)

    grad_out = out_grad_own.astype(F32) + total_tokens / counted * differ
    grad_mlp = (grad_out * gate_two).astype(BF16)
    gate_two_grad = jnp.sum(grad_out * mlp_out, axis=0)

    def shard_of(array, which):
        rows = array.shape[1] // fsdp
        return lax.dynamic_slice_in_dim(array, which * rows, rows, 1)

    def weight_grad(left, right):
        if not fast:
            whole = lax.dot_general(
                left, right, (((0,), (0,)), ((), ())), preferred_element_type=F32
            )
            mine = lax.psum_scatter(whole.astype(BF16), "fsdp", scatter_dimension=0, tiled=True)
            return lax.psum(mine, ("rep", "seq")).astype(F32)
        right_other = flip(right, "fsdp", 1)
        keep, give = shard_of(left, place_f), shard_of(left, place_f ^ 2)
        keep_other = flip(shard_of(left, place_f ^ 1), "fsdp", 1)
        give_other = flip(shard_of(left, place_f ^ 3), "fsdp", 1)
        arrived = reduce_start(outer_blocks(give, give_other, right, right_other))
        return outer_blocks(keep, keep_other, right, right_other, arrived)

    down_sum = weight_grad(activated, grad_mlp)
    down_bgrad = column_sum(grad_mlp)
    upper_grad = (dot_t(grad_mlp, down_full) * slope).astype(BF16)
    up_sum = weight_grad(hidden_two, upper_grad)
    up_bgrad = column_sum(upper_grad)
    hidden_two_grad = dot_t(upper_grad, up_full)
    scaled_two = hidden_two_grad * (1.0 + scale_two)
    middle_grad = grad_out + norm_back(scaled_two, normed_two, rate_two)
    shift_two_grad = jnp.sum(hidden_two_grad, axis=0)
    scale_two_grad = jnp.sum(hidden_two_grad * normed_two, axis=0)
    branch_grad = (middle_grad * gate_one).astype(BF16)
    gate_one_grad = jnp.sum(middle_grad * branch, axis=0)
    out_sum = weight_grad(attended, branch_grad)
    out_bgrad = column_sum(branch_grad)
    attended_grad = dot_t(branch_grad, out_full).astype(BF16)

    early_row = jnp.concatenate(
        [
            gate_one_grad,
            shift_two_grad,
            scale_two_grad,
            gate_two_grad,
            out_bgrad,
            up_bgrad,
            down_bgrad,
        ]
    )
    early_row = early_row + flip(early_row, "fsdp", 1)
    early_rows = gather_rows(early_row[None], fast)[:, 0]

    query_grad, key_part, value_part, key_away, value_away = attend_back(
        queries,
        keys_own,
        values_own,
        keys_other,
        values_other,
        attended_grad,
        lse.T,
        mask_own[:, None],
        mask_other[:, None],
    )
    key_grad = (key_part + flip(key_away, "fsdp", 1).astype(F32)).astype(BF16)
    value_grad = (value_part + flip(value_away, "fsdp", 1).astype(F32)).astype(BF16)
    qkv_grad = jnp.concatenate([query_grad, key_grad, value_grad], axis=-1)
    qkv_sum = weight_grad(hidden_one, qkv_grad)
    hidden_one_grad = dot_t(qkv_grad, qkv_full)
    scaled_one = hidden_one_grad * (1.0 + scale_one)
    tokens_grad = middle_grad + norm_back(scaled_one, normed_one, rate_one)
    tokens_grad = from_latent(tokens_grad.astype(BF16))
    late_row = jnp.concatenate(
        [
            jnp.sum(hidden_one_grad, axis=0),
            jnp.sum(hidden_one_grad * normed_one, axis=0),
            column_sum(query_grad),
            column_sum(value_grad),
        ]
    )
    late_row = late_row + flip(late_row, "fsdp", 1)
    late_rows = gather_rows(late_row[None], fast)[:, 0]

    mod_grad = jnp.concatenate([late_rows[:, : 2 * width], early_rows[:, : 4 * width]], axis=1)
    if not fast:
        cond_row = own_row
    else:
        cond_row = jnp.where(place_f % 2 == place_s // 2, cond_row, flip(cond_row, "fsdp", 1))
    silu_row = jax.nn.silu(cond_row.astype(F32)).astype(BF16)
    silu_all = gather_rows(silu_row[None], fast)[:, 0]
    silu_own = lax.dynamic_slice_in_dim(silu_all, place_f * shard_rows, shard_rows, 1)
    mod_wgrad = lax.dot_general(
        silu_own.astype(F32),
        mod_grad,
        (((0,), (0,)), ((), ())),
        precision=HIGHEST,
        preferred_element_type=F32,
    )
    bias_rows = jnp.concatenate([early_rows[:, 4 * width :], late_rows[:, 2 * width :]], axis=1)
    bias_sum = jnp.sum(bias_rows, axis=0)

    def own_bias(low, size):
        own = size // fsdp
        return lax.dynamic_slice_in_dim(bias_sum, low + place_f * own, own, 0)

    up_size = up_b.shape[0]
    out_bg = own_bias(0, width)
    up_bg = own_bias(width, up_size)
    down_bg = own_bias(width + up_size, width)
    qkv_bg = own_bias(2 * width + up_size, 2 * width)
    mod_own = mod_bias.shape[0]
    mod_bg = lax.dynamic_slice_in_dim(jnp.sum(mod_grad, axis=0), place_f * mod_own, mod_own, 0)

    replica = lax.axis_index("rep")
    per_rep = mod_grad.shape[0] // reps
    own_rep = lax.dynamic_slice_in_dim(mod_grad, replica * per_rep, per_rep, 0)
    silu_grad = lax.dot_general(
        own_rep,
        mod_weight.astype(F32),
        (((1,), (1,)), ((), ())),
        precision=HIGHEST,
        preferred_element_type=F32,
    )
    owners = silu_grad.reshape(fsdp, latents, shard_rows)
    if fast:
        found = [pick(owners, place_f)]
        found += [flip(pick(owners, place_f ^ bit), "fsdp", bit) for bit in (1, 2, 3)]
        found = jnp.stack(found)
        found = jnp.concatenate(
            [lax.dynamic_slice_in_dim(found, place_f ^ f, 1, 0) for f in range(fsdp)]
        )
    else:
        found = lax.all_to_all(owners, "fsdp", 0, 0, tiled=True)
    silu_grad = found.transpose(1, 0, 2).reshape(latents, width)
    conds = condition.astype(F32)
    sigmoid = 1.0 / (1.0 + jnp.exp(-conds))
    condition_grad = silu_grad * (sigmoid * (1.0 + conds * (1.0 - sigmoid)))

    if fast:
        down_g = place_pieces(
            reduce_rest(down_sum.reshape(-1, width)), [down_weight.shape], "tall"
        )[0]
        up_g = place_pieces(reduce_rest(up_sum.reshape(-1, width)), [up_weight.shape], "wide")[0]
        tail = jnp.concatenate([out_sum, qkv_sum], axis=0).reshape(-1, width)
        out_g, qkv_g = place_pieces(
            reduce_rest(tail), [out_weight.shape, qkv_weight.shape], "wide"
        )
    else:
        down_g, up_g, out_g, qkv_g = down_sum, up_sum, out_sum, qkv_sum
    loss_value = (err_total / (width * counted))[0, 0]
    return (
        block_out,
        loss_value,
        tokens_grad,
        condition_grad,
        mod_wgrad,
        mod_bg,
        qkv_g,
        qkv_bg,
        out_g,
        out_bg,
        up_g,
        up_bg,
        down_g,
        down_bg,
    )


def solution(mesh):
    batch = P(("rep", "fsdp"), "seq", None)
    matrix, vector = P("fsdp", None), P("fsdp")
    params = (matrix, vector) * 5
    return jax.shard_map(
        shards,
        mesh=mesh,
        in_specs=(batch, P(("rep", "fsdp"), None), P(("rep", "fsdp"), "seq"), batch, batch)
        + params,
        out_specs=(batch, P(), batch, P(("rep", "fsdp"), None)) + params,
        check_vma=False,
    )
```

```python
import functools

import jax
import jax.numpy as jnp
from jax import lax
from jax.experimental import pallas as pl
from jax.experimental.pallas import tpu as pltpu
from jax.sharding import PartitionSpec as P

HEADS = 16

EPS = 1e-06
GELU_C = 0.7978845608028654
HIGHEST = lax.Precision.HIGHEST
LOG2E = 1.4426950408889634
NEG = -1e30
BF16 = jnp.bfloat16
F32 = jnp.float32
WINDOW = 256
LANES = 128


def flip(array, axis, bit):
    size = lax.axis_size(axis)
    return lax.ppermute(array, axis, [(i, i ^ bit) for i in range(size)])


def pick(array, index):
    return lax.dynamic_index_in_dim(array, index, 0, keepdims=False)


def in_order(first, second, swapped):
    return jnp.where(swapped, jnp.stack([second, first]), jnp.stack([first, second]))


def to_latent(array):
    seq, fsdp = lax.axis_size("seq"), lax.axis_size("fsdp")
    place = lax.axis_index("seq")
    arrived = []
    for turn in range(2):
        pairs = []
        for f in range(fsdp):
            for s in range(seq):
                pair, core = f // 2, f % 2
                target = (pair * 2 + s // 2, 2 * core + (s + turn) % 2)
                pairs.append((f * seq + s, target[0] * seq + target[1]))
        block = pick(array, (place + turn) % 2)
        arrived.append(lax.ppermute(block, ("fsdp", "seq"), pairs))
    both = in_order(arrived[0], arrived[1], place % 2 == 1)
    return both.reshape((-1,) + both.shape[2:])


def from_latent(array):
    seq, fsdp = lax.axis_size("seq"), lax.axis_size("fsdp")
    place = lax.axis_index("seq")
    halves = array.reshape((2, array.shape[0] // 2) + array.shape[1:])
    arrived = []
    for turn in range(2):
        pairs = []
        for f in range(fsdp):
            for s in range(seq):
                pair, core = f // 2, f % 2
                slot = (s + turn) % 2
                target = (pair * 2 + s // 2, 2 * core + slot)
                pairs.append((f * seq + s, target[0] * seq + target[1]))
        arrived.append(lax.ppermute(pick(halves, (place + turn) % 2), ("fsdp", "seq"), pairs))
    return in_order(arrived[0], arrived[1], place % 2 == 1)


def gather_rows(row):
    fsdp = lax.axis_size("fsdp")
    everything = lax.all_gather(row, ("rep", "fsdp", "seq"), axis=0)
    everything = everything.reshape((-1, fsdp // 2, 2, lax.axis_size("seq")) + row.shape)
    return everything[:, :, 0].reshape((-1,) + row.shape)


def gather_weight(weight):
    return lax.all_gather(weight, "fsdp", axis=0, tiled=True)


MESH = pl.DeviceIdType.MESH


class Spot:
    def __init__(self):
        self.x, self.f, self.s = (lax.axis_index(name) for name in ("rep", "fsdp", "seq"))
        self.core = self.f % 2
        self.pair = self.f // 2

    def other(self, bit):
        if bit == 3:
            return 3 - self.f
        return self.f + bit - 2 * bit * ((self.f // bit) % 2)

    def fsdp(self, bit):
        return (self.x, self.other(bit), self.s)

    def rep(self, bit=0):
        return (1 - self.x, self.other(bit) if bit else self.f, self.s)

    def seq(self, step):
        return (self.x, self.f, lax.rem(self.s + step, 4))

    def token_target(self, turn):
        block = lax.rem(self.s + turn, 2)
        return (self.x, 2 * self.pair + self.s // 2, 2 * self.core + block), block


def greet(devices):
    barrier = pltpu.get_barrier_semaphore()
    for device in devices:
        pl.semaphore_signal(barrier, inc=1, device_id=device, device_id_type=MESH)
    pl.semaphore_wait(barrier, len(devices))


def column_group(spot):
    found = [(spot.x, spot.other(1), spot.s)]
    for step in range(1, 4):
        found.append(spot.seq(step))
        found.append((spot.x, spot.other(1), lax.rem(spot.s + step, 4)))
    return found


class Sender:
    def __init__(self, send_sems, recv_sems):
        self.send_sems, self.recv_sems = send_sems, recv_sems
        self.used = 0
        self.open = []

    def slot(self):
        self.used += 1
        return self.used - 1

    def start(self, slot, source, target, device):
        copy = pltpu.make_async_remote_copy(
            source, target, self.send_sems.at[slot], self.recv_sems.at[slot], device, MESH
        )
        copy.start()
        self.open.append(copy)

    def start_if(self, wanted, send_slot, recv_slot, source, target, device):
        copy = pltpu.make_async_remote_copy(
            source, target, self.send_sems.at[send_slot], self.recv_sems.at[recv_slot], device, MESH
        )
        pl.when(wanted)(lambda: copy.start())
        return wanted, copy

    def slots(self, count):
        self.used += count
        return self.used - count

    def sent(self, slot, view):
        pltpu.make_async_copy(view, view, self.send_sems.at[slot]).wait()

    def arrived(self, slot, view):
        pltpu.make_async_copy(view, view, self.recv_sems.at[slot]).wait()

    def finish(self):
        for copy in self.open:
            copy.wait_send()
        self.open = []


class Locals:
    def __init__(self, sems):
        self.sems = sems
        self.used = 0
        self.open = []

    def start(self, source, target):
        copy = pltpu.make_async_copy(source, target, self.sems.at[self.used])
        self.used += 1
        copy.start()
        return copy


class TokenMove:
    def __init__(self, sender, spot, source, target):
        self.sender, self.spot, self.source, self.target = sender, spot, source, target
        self.slots = [sender.slot(), sender.slot()]

    def start(self):
        spot = self.spot
        self.remote = []
        for turn, slot in enumerate(self.slots):
            device, block = spot.token_target(turn)
            stays = (device[1] == spot.f) & (device[2] == spot.s)
            source = self.source.at[block]
            target = self.target.at[lax.rem(spot.s, 2)]
            remote = pltpu.make_async_remote_copy(
                source,
                target,
                self.sender.send_sems.at[slot],
                self.sender.recv_sems.at[slot],
                device,
                MESH,
            )
            local = pltpu.make_async_copy(source, target, self.sender.recv_sems.at[slot])
            pl.when(jnp.logical_not(stays))(lambda remote=remote: remote.start())
            pl.when(stays)(lambda local=local: local.start())
            self.remote.append((stays, remote))

    def finish(self):
        for turn, slot in enumerate(self.slots):
            self.sender.arrived(slot, self.target.at[lax.rem(self.spot.s + turn, 2)])
        for stays, remote in self.remote:
            pl.when(jnp.logical_not(stays))(lambda remote=remote: remote.wait_send())


class WeightMove:
    def __init__(self, sender, local, spot, own, full, stage, chunks):
        self.sender, self.local, self.spot = sender, local, spot
        self.own, self.full, self.stage = own, full, stage
        self.rows, self.chunks = own.shape[0], chunks
        self.half = self.rows // 2
        self.tall = self.half // chunks
        self.slots = {
            kind: [sender.slot() for _ in range(1 if kind == "core" else chunks)]
            for kind in ("core", "far", "side", "far_core", "side_core")
        }

    def view(self, bits, side, chunk):
        shard = self.spot.other(bits) if bits else self.spot.f
        half = self.spot.x if side == 0 else 1 - self.spot.x
        start = shard * self.rows + half * self.half + chunk * self.tall
        return self.full.at[pl.ds(pl.multiple_of(start, 16), self.tall)]

    def shard_view(self, bits):
        shard = self.spot.other(bits) if bits else self.spot.f
        return self.full.at[pl.ds(pl.multiple_of(shard * self.rows, 16), self.rows)]

    def start_far(self):
        spot = self.spot
        for chunk, slot in enumerate(self.slots["far"]):
            start = pl.multiple_of(spot.x * self.half + chunk * self.tall, 16)
            self.sender.start(
                slot, self.own.at[pl.ds(start, self.tall)], self.view(0, 0, chunk), spot.fsdp(2)
            )

    def start_near(self):
        self.sender.start(self.slots["core"][0], self.own, self.shard_view(0), self.spot.fsdp(1))
        self.load = self.local.start(self.own, self.stage)

    def store(self):
        self.load.wait()
        self.kept = self.local.start(self.stage, self.shard_view(0))

    def pass_far(self, chunk):
        view = self.view(2, 0, chunk)
        self.sender.arrived(self.slots["far"][chunk], view)
        self.sender.start(self.slots["side"][chunk], view, view, self.spot.rep())
        self.sender.start(self.slots["far_core"][chunk], view, view, self.spot.fsdp(1))

    def pass_side(self, chunk):
        view = self.view(2, 1, chunk)
        self.sender.arrived(self.slots["side"][chunk], view)
        self.sender.start(self.slots["side_core"][chunk], view, view, self.spot.fsdp(1))

    def finish(self):
        self.kept.wait()
        self.sender.arrived(self.slots["core"][0], self.shard_view(1))
        for chunk in range(self.chunks):
            self.sender.arrived(self.slots["far_core"][chunk], self.view(3, 0, chunk))
            self.sender.arrived(self.slots["side_core"][chunk], self.view(3, 1, chunk))


def entry_kernel(
    tokens,
    valid,
    cond,
    biases,
    mod_weight,
    qkv_weight,
    out_weight,
    tokens_own,
    valid_all,
    mod_parts,
    bias_all,
    qkv_full,
    out_full,
    mod_held,
    cond_held,
    partial,
    qkv_stage,
    out_stage,
    send_sems,
    recv_sems,
    local_sems,
):
    spot = Spot()
    sender, local = Sender(send_sems, recv_sems), Locals(local_sems)
    mod_load = local.start(mod_weight, mod_held)
    greet(column_group(spot) + [spot.fsdp(2), spot.fsdp(3), spot.rep()])

    row = lax.rem(spot.s, 2)
    cond_slots, bias_slots = {}, {}
    for bit in (1, 2, 3):
        cond_slots[bit], bias_slots[bit] = sender.slot(), sender.slot()
        target = spot.other(bit)
        sender.start(
            cond_slots[bit], cond.at[row, target], cond_held.at[spot.f], spot.fsdp(bit)
        )
    for bit in (1, 2, 3):
        sender.start(bias_slots[bit], biases, bias_all.at[spot.f], spot.fsdp(bit))
    cond_own = local.start(cond.at[row, spot.f], cond_held.at[spot.f])
    bias_own = local.start(biases, bias_all.at[spot.f])

    qkv = WeightMove(sender, local, spot, qkv_weight, qkv_full, qkv_stage, 3)
    out = WeightMove(sender, local, spot, out_weight, out_full, out_stage, 1)
    mod_slots = {bit: sender.slot() for bit in (1, 2, 3)}
    move = TokenMove(sender, spot, tokens, tokens_own)
    valid_base = [sender.slot() for _ in range(4)][0]
    valid_open = []
    for turn in range(2):
        device, block = spot.token_target(turn)
        for core in range(2):
            goal = (device[0], 2 * spot.pair + core, device[2])
            stays = (goal[1] == spot.f) & (goal[2] == spot.s)
            source, target = valid.at[block], valid_all.at[spot.s]
            arrival = recv_sems.at[valid_base + spot.s]
            remote = pltpu.make_async_remote_copy(
                source, target, send_sems.at[valid_base + 2 * turn + core], arrival, goal, MESH
            )
            near = pltpu.make_async_copy(source, target, arrival)
            pl.when(jnp.logical_not(stays))(lambda remote=remote: remote.start())
            pl.when(stays)(lambda near=near: near.start())
            valid_open.append((stays, remote))
    move.start()
    qkv.start_far()
    qkv.start_near()
    out.start_near()

    cond_own.wait()
    for bit in (1, 2, 3):
        sender.arrived(cond_slots[bit], cond_held.at[spot.other(bit)])
    first, second = cond_held[spot.s // 2], cond_held[2 + spot.s // 2]
    which = lax.broadcasted_iota(jnp.int32, (16, first.shape[-1]), 0)
    conds = jnp.where(which == 0, first, second)
    silu = (conds / (1.0 + jnp.exp(-conds))).astype(BF16)
    mod_load.wait()
    width = mod_held.shape[1] // 6
    for piece in range(6):
        columns = slice(piece * width, (piece + 1) * width)
        product = jnp.dot(silu, mod_held[:, columns], preferred_element_type=F32)
        partial[0, :, columns] = product[0:1]
        partial[1, :, columns] = product[1:2]
    for bit in (1, 2, 3):
        pair = spot.pair if bit == 1 else 1 - spot.pair
        sender.start(
            mod_slots[bit], partial.at[pair], mod_parts.at[spot.f], spot.fsdp(bit)
        )
    mod_own = local.start(partial.at[spot.pair], mod_parts.at[spot.f])
    out.start_far()
    qkv.store()
    out.store()
    for chunk in range(3):
        qkv.pass_far(chunk)
        if chunk:
            qkv.pass_side(chunk - 1)
    qkv.pass_side(2)
    out.pass_far(0)
    out.pass_side(0)

    bias_own.wait()
    mod_own.wait()
    for bit in (1, 2, 3):
        sender.arrived(bias_slots[bit], bias_all.at[spot.other(bit)])
        sender.arrived(mod_slots[bit], mod_parts.at[spot.other(bit)])
    for place in range(4):
        sender.arrived(valid_base + place, valid_all.at[place])
    for stays, remote in valid_open:
        pl.when(jnp.logical_not(stays))(lambda remote=remote: remote.wait_send())
    move.finish()
    qkv.finish()
    out.finish()
    sender.finish()


def sems(count):
    return pltpu.SemaphoreType.DMA((count,))


def enter(tokens, valid, cond, biases, mod_weight, qkv_weight, out_weight):
    anywhere = pl.BlockSpec(memory_space=pl.ANY)
    return pl.pallas_call(
        entry_kernel,
        out_shape=[
            jax.ShapeDtypeStruct(tokens.shape, tokens.dtype),
            jax.ShapeDtypeStruct((4,) + valid.shape[1:], F32),
            jax.ShapeDtypeStruct((4, 1, mod_weight.shape[1]), F32),
            jax.ShapeDtypeStruct((4,) + biases.shape, F32),
            jax.ShapeDtypeStruct((4 * qkv_weight.shape[0], qkv_weight.shape[1]), BF16),
            jax.ShapeDtypeStruct((4 * out_weight.shape[0], out_weight.shape[1]), BF16),
        ],
        in_specs=[anywhere] * 7,
        out_specs=[anywhere] * 6,
        scratch_shapes=[
            pltpu.VMEM(mod_weight.shape, BF16),
            pltpu.VMEM((4,) + cond.shape[2:], F32),
            pltpu.VMEM((2, 1, mod_weight.shape[1]), F32),
            pltpu.VMEM(qkv_weight.shape, BF16),
            pltpu.VMEM(out_weight.shape, BF16),
            sems(40),
            sems(40),
            sems(12),
        ],
        compiler_params=pltpu.CompilerParams(
            collective_id=1, has_side_effects=True, vmem_limit_bytes=32 * 1024 * 1024
        ),
        name="enter",
    )(tokens, valid, cond, biases, mod_weight, qkv_weight, out_weight)


class TokenReturn:
    def __init__(self, sender, spot, source, target):
        self.sender, self.spot, self.source, self.target = sender, spot, source, target
        self.slots = [sender.slot(), sender.slot()]

    def start(self):
        spot = self.spot
        self.remote = []
        for turn, slot in enumerate(self.slots):
            half = lax.rem(spot.s + turn, 2)
            device = (spot.x, 2 * spot.pair + spot.s // 2, 2 * spot.core + half)
            stays = (device[1] == spot.f) & (device[2] == spot.s)
            source, target = self.source.at[half], self.target.at[lax.rem(spot.s, 2)]
            arrival = self.sender.recv_sems.at[slot]
            remote = pltpu.make_async_remote_copy(
                source, target, self.sender.send_sems.at[slot], arrival, device, MESH
            )
            local = pltpu.make_async_copy(source, target, arrival)
            pl.when(jnp.logical_not(stays))(lambda remote=remote: remote.start())
            pl.when(stays)(lambda local=local: local.start())
            self.remote.append((stays, remote))

    def finish(self):
        for turn, slot in enumerate(self.slots):
            self.sender.arrived(slot, self.target.at[lax.rem(self.spot.s + turn, 2)])
        for stays, remote in self.remote:
            pl.when(jnp.logical_not(stays))(lambda remote=remote: remote.wait_send())


ORDER = (0, 3, 1, 2)


class GradMove:
    def __init__(self, sender, local, spot, far, side, depth, total, final):
        self.sender, self.local, self.spot = sender, local, spot
        self.far, self.side, self.depth, self.total, self.final = far, side, depth, total, final
        self.tall = far.shape[1] // 2
        self.y, self.x, self.z, self.g, self.relay, self.fx = (sender.slots(4) for _ in range(6))
        self.kept = local.used
        local.used += 1
        self.z_open, self.g_open = [], []

    def send_far(self, j, give):
        self.sender.start(self.y + j, give, self.far.at[j], self.spot.fsdp(2))

    def half(self, side):
        return pl.ds(pl.multiple_of(side * self.tall, 16), self.tall)

    def fold(self, j, kept, arrives=True):
        if arrives:
            self.sender.arrived(self.y + j, self.far.at[j])
        self.far[j] = (self.far[j].astype(F32) + kept.astype(F32)).astype(BF16)
        self.sender.start(
            self.x + j, self.far.at[j, self.half(1 - self.spot.x)], self.side.at[j], self.spot.rep()
        )

    def cross(self, j):
        spot = self.spot
        self.sender.arrived(self.x + j, self.side.at[j])
        mine = self.far[j, self.half(spot.x), :].astype(F32)
        self.side[j] = (mine + self.side[j].astype(F32)).astype(BF16)
        step = lax.rem(spot.s - j + 4, 4)
        index = jnp.maximum(step - 1, 0)
        self.z_open.append(
            self.sender.start_if(
                spot.s != j,
                self.z + j,
                self.z + index,
                self.side.at[j],
                self.depth.at[index],
                (spot.x, spot.f, j),
            )
        )

    def settle(self, j):
        spot, sender = self.spot, self.sender
        target = self.final.at[j, spot.x]

        @pl.when(spot.s == j)
        def _():
            total = self.side[j].astype(F32)
            for index in range(3):
                sender.arrived(self.z + index, self.depth.at[index])
                total = total + self.depth[index].astype(F32)
            self.total[...] = total.astype(BF16)
            if j > 0:
                pltpu.make_async_remote_copy(
                    self.total,
                    target,
                    sender.send_sems.at[self.g],
                    sender.recv_sems.at[self.g + j],
                    (spot.x, spot.f, j - 1),
                    MESH,
                ).start()
            if j < 3:
                pltpu.make_async_remote_copy(
                    self.total,
                    target,
                    sender.send_sems.at[self.g + 1],
                    sender.recv_sems.at[self.g + j],
                    (spot.x, spot.f, j + 1),
                    MESH,
                ).start()
            pltpu.make_async_remote_copy(
                self.total,
                target,
                sender.send_sems.at[self.fx + j],
                sender.recv_sems.at[self.fx + j],
                spot.rep(),
                MESH,
            ).start()
            pltpu.make_async_copy(self.total, target, self.local.sems.at[self.kept]).start()

    def pass_on(self, j):
        spot, sender = self.spot, self.sender
        target = self.final.at[j, spot.x]

        @pl.when(spot.s != j)
        def _():
            sender.arrived(self.g + j, target)
            pltpu.make_async_remote_copy(
                target,
                target,
                sender.send_sems.at[self.fx + j],
                sender.recv_sems.at[self.fx + j],
                spot.rep(),
                MESH,
            ).start()

        up = (spot.s > j) & (spot.s < 3)
        down = (spot.s < j) & (spot.s > 0)
        onward = jnp.where(up, jnp.minimum(spot.s + 1, 3), jnp.maximum(spot.s - 1, 0))
        self.g_open.append(
            sender.start_if(
                up | down, self.relay + j, self.g + j, target, target, (spot.x, spot.f, onward)
            )
        )

    def finish(self):
        spot, sender = self.spot, self.sender
        for j in range(4):
            sender.arrived(self.fx + j, self.final.at[j, 1 - spot.x])
            sender.sent(self.fx + j, self.total)
        for wanted, copy in self.z_open + self.g_open:
            pl.when(wanted)(lambda copy=copy: copy.wait_send())
        pl.when(spot.s > 0)(lambda: sender.sent(self.g, self.total))
        pl.when(spot.s < 3)(lambda: sender.sent(self.g + 1, self.total))
        pltpu.make_async_copy(
            self.total, self.total, self.local.sems.at[self.kept]
        ).wait()


DOWN = (((0,), (0,)), ((), ()))


def outer(left_own, left_other, right_own, right_other):
    total = lax.dot_general(left_own, right_own, DOWN, preferred_element_type=F32)
    return total + lax.dot_general(left_other, right_other, DOWN, preferred_element_type=F32)


def lane_block(index, size):
    return pl.ds(pl.multiple_of(index * size, LANES), size)


def backward_send_kernel(
    q_ref,
    k_own,
    v_own,
    k_other,
    v_other,
    do_ref,
    lse_ref,
    bias_own,
    bias_other,
    grad_mlp,
    error_in,
    activated,
    hidden,
    upper_grad,
    block_out,
    dq_out,
    dk_out,
    dv_out,
    error_out,
    down_final,
    up_far,
    up_kept,
    upper_other,
    block_back,
    act_give,
    act_keep,
    act_give_other,
    act_keep_other,
    mlp_other,
    hid,
    rights,
    give,
    kept,
    far,
    side,
    depth,
    total,
    errors,
    error_core,
    error_row,
    dk_one,
    dv_one,
    dk_two,
    dv_two,
    dk_in,
    dv_in,
    send_sems,
    recv_sems,
    local_sems,
):
    spot = Spot()
    sender, local = Sender(send_sems, recv_sems), Locals(local_sems)
    width = q_ref.shape[1]
    shard = activated.shape[1] // 4
    f, core = spot.f, spot.fsdp(1)
    loads = [
        local.start(activated.at[:, lane_block(spot.other(2), shard)], act_give),
        local.start(activated.at[:, lane_block(f, shard)], act_keep),
        local.start(hidden.at[spot.other(2)], hid.at[0]),
        local.start(hidden.at[f], hid.at[1]),
    ]
    right_base = local.used
    local.used += 4

    def right_copies(j):
        slot = j % 2
        columns = pl.ds(j * width, width)
        return (
            pltpu.make_async_copy(
                upper_grad.at[:, columns], rights.at[0, slot], local.sems.at[right_base + slot]
            ),
            pltpu.make_async_copy(
                upper_other.at[:, columns], rights.at[1, slot], local.sems.at[right_base + 2 + slot]
            ),
        )

    greet(column_group(spot) + [spot.fsdp(2), spot.rep()])
    error_core_slot = sender.slot()
    sender.start(error_core_slot, error_in, error_core, core)
    pieces = [sender.slot() for _ in range(6)]
    sender.start(
        pieces[0], activated.at[:, lane_block(spot.other(3), shard)], act_give_other, core
    )
    sender.start(pieces[1], grad_mlp, mlp_other, core)
    sender.start(
        pieces[2], activated.at[:, lane_block(spot.other(1), shard)], act_keep_other, core
    )
    sender.start(pieces[3], hidden.at[spot.other(3)], hid.at[2], core)
    sender.start(pieces[4], hidden.at[spot.other(1)], hid.at[3], core)
    sender.start(pieces[5], upper_grad, upper_other, core)
    back = TokenReturn(sender, spot, block_out, block_back)
    down = GradMove(sender, local, spot, far, side, depth, total, down_final)
    up_slots = sender.slots(4)
    error_slots, error_far, error_side = sender.slots(4), sender.slot(), sender.slot()
    back.start()

    for load in loads[:2]:
        load.wait()
    sender.arrived(pieces[0], act_give_other)
    sender.arrived(pieces[1], mlp_other)
    block = 384

    def fill(target, left, left_other):
        def body(i, carry):
            columns = lane_block(i, block)
            rows = pl.ds(pl.multiple_of(i * block, 16), block)
            target[rows, :] = outer(
                left[:, columns], left_other[:, columns], grad_mlp[...], mlp_other[...]
            ).astype(BF16)
            return carry

        lax.fori_loop(0, shard // block, body, 0)

    tall = shard // 4
    fill(give.at[0], act_give, act_give_other)
    for j in ORDER:
        down.send_far(j, give.at[0, pl.ds(j * tall, tall)])
    sender.arrived(pieces[2], act_keep_other)
    fill(kept.at[0], act_keep, act_keep_other)

    sender.arrived(error_core_slot, error_core)
    errors[spot.s] = error_in[...] + error_core[...]
    error_open = []
    for step in range(1, 4):
        copy = pltpu.make_async_remote_copy(
            errors.at[spot.s],
            errors.at[spot.s],
            send_sems.at[error_slots + step - 1],
            recv_sems.at[error_slots + spot.s],
            spot.seq(step),
            MESH,
        )
        copy.start()
        error_open.append(copy)

    for load in loads[2:]:
        load.wait()
    for slot, place in ((3, 2), (4, 3)):
        sender.arrived(pieces[slot], hid.at[place])
    sender.arrived(pieces[5], upper_other)
    for copy in right_copies(0):
        copy.start()
    stored = []
    for j in range(4):
        if j < 3:
            for copy in right_copies(j + 1):
                copy.start()
        for copy in right_copies(j):
            copy.wait()
        right, right_other = rights[0, j % 2], rights[1, j % 2]
        rows = pl.ds(j * tall, tall)
        give[1, rows, :] = outer(hid[0], hid[2], right, right_other).astype(BF16)
        sender.start(up_slots + j, give.at[1, rows], up_far.at[j], spot.fsdp(2))
        kept[1, rows, :] = outer(hid[1], hid[3], right, right_other).astype(BF16)
        stored.append(local.start(kept.at[1, rows], up_kept.at[j]))

    data = (
        q_ref,
        k_own,
        v_own,
        k_other,
        v_other,
        do_ref,
        lse_ref,
        bias_own,
        bias_other,
        dq_out,
        dk_one,
        dv_one,
        dk_two,
        dv_two,
    )

    def fold(j):
        down.fold(j, kept[0, pl.ds(j * tall, tall), :])

    a, b, c, d = ORDER
    fold(a)
    backward_heads(0, 4, *data)
    fold(b)
    down.cross(a)
    backward_heads(4, 8, *data)
    fold(c)
    down.cross(b)
    down.settle(a)
    for place in range(4):

        @pl.when(spot.s != place)
        def _():
            sender.arrived(error_slots + place, errors.at[place])

    error_row[0] = errors[0] + errors[1] + errors[2] + errors[3]
    sender.start(error_far, error_row.at[0], error_row.at[1], spot.fsdp(2))
    backward_heads(8, 12, *data)
    fold(d)
    down.cross(c)
    down.settle(b)
    down.pass_on(a)
    backward_heads(12, HEADS, *data)
    dk_slot, dv_slot = sender.slot(), sender.slot()
    sender.start(dk_slot, dk_two, dk_in, core)
    sender.start(dv_slot, dv_two, dv_in, core)
    down.cross(d)
    down.settle(c)
    down.pass_on(b)
    sender.arrived(error_far, error_row.at[1])
    error_row[2] = error_row[0] + error_row[1]
    sender.start(error_side, error_row.at[2], error_row.at[3], spot.rep())
    sender.arrived(dk_slot, dk_in)
    dk_out[...] = (dk_one[...] + dk_in[...].astype(F32)).astype(BF16)
    sender.arrived(dv_slot, dv_in)
    dv_out[...] = (dv_one[...] + dv_in[...].astype(F32)).astype(BF16)
    down.settle(d)
    down.pass_on(c)
    down.pass_on(d)
    sender.arrived(error_side, error_row.at[3])
    error_out[...] = error_row[2] + error_row[3]
    for copy in error_open:
        copy.wait_send()
    for copy in stored:
        copy.wait()
    back.finish()
    for j in range(4):
        sender.arrived(up_slots + j, up_far.at[j])
    down.finish()
    sender.finish()


def attend_back_and_reduce(
    queries,
    keys,
    values,
    keys_other,
    values_other,
    grad,
    lse,
    bias_own,
    bias_other,
    grad_mlp,
    error,
    activated,
    hidden,
    upper_grad,
    block_out,
):
    tokens, width = queries.shape
    shape = (tokens, width)
    shard = activated.shape[1] // 4
    tall = shard // 4
    anywhere = pl.BlockSpec(memory_space=pl.ANY)
    near = pl.BlockSpec(memory_space=pltpu.VMEM)
    return pl.pallas_call(
        backward_send_kernel,
        out_shape=[
            jax.ShapeDtypeStruct(shape, BF16),
            jax.ShapeDtypeStruct(shape, BF16),
            jax.ShapeDtypeStruct(shape, BF16),
            jax.ShapeDtypeStruct(error.shape, F32),
            jax.ShapeDtypeStruct((4, 2, tall // 2, width), BF16),
            jax.ShapeDtypeStruct((4, tall, width), BF16),
            jax.ShapeDtypeStruct((4, tall, width), BF16),
            jax.ShapeDtypeStruct(upper_grad.shape, BF16),
            jax.ShapeDtypeStruct(block_out.shape, BF16),
        ],
        in_specs=[near] * 11 + [anywhere] * 4,
        out_specs=[near] * 4 + [anywhere] * 5,
        scratch_shapes=[
            pltpu.VMEM((tokens, shard), BF16),
            pltpu.VMEM((tokens, shard), BF16),
            pltpu.VMEM((tokens, shard), BF16),
            pltpu.VMEM((tokens, shard), BF16),
            pltpu.VMEM(shape, BF16),
            pltpu.VMEM((4,) + hidden.shape[1:], BF16),
            pltpu.VMEM((2, 2) + shape, BF16),
            pltpu.VMEM((2, shard, width), BF16),
            pltpu.VMEM((2, shard, width), BF16),
            pltpu.VMEM((4, tall, width), BF16),
            pltpu.VMEM((4, tall // 2, width), BF16),
            pltpu.VMEM((3, tall // 2, width), BF16),
            pltpu.VMEM((tall // 2, width), BF16),
            pltpu.VMEM((4,) + error.shape, F32),
            pltpu.VMEM(error.shape, F32),
            pltpu.VMEM((4,) + error.shape, F32),
            pltpu.VMEM(shape, F32),
            pltpu.VMEM(shape, F32),
            pltpu.VMEM(shape, BF16),
            pltpu.VMEM(shape, BF16),
            pltpu.VMEM(shape, BF16),
            pltpu.VMEM(shape, BF16),
            sems(64),
            sems(64),
            sems(16),
        ],
        compiler_params=pltpu.CompilerParams(
            collective_id=3, has_side_effects=True, vmem_limit_bytes=67043328
        ),
        name="attend_back_and_reduce",
    )(
        queries,
        keys,
        values,
        keys_other,
        values_other,
        grad,
        lse,
        bias_own,
        bias_other,
        grad_mlp,
        error,
        activated,
        hidden,
        upper_grad,
        block_out,
    )


def finish_kernel(
    branch_grad,
    qkv_grad,
    row,
    attended,
    hidden,
    up_far,
    up_kept,
    tokens_grad,
    rows,
    up_final,
    tail_final,
    tokens_back,
    branch_other,
    qkv_other,
    att,
    hid,
    up_sum,
    up_own,
    up_side,
    up_depth,
    up_total,
    give,
    far,
    side,
    depth,
    total,
    row_in,
    send_sems,
    recv_sems,
    local_sems,
):
    spot = Spot()
    sender, local = Sender(send_sems, recv_sems), Locals(local_sems)
    width = branch_grad.shape[1]
    f, core = spot.f, spot.fsdp(1)
    load_up = [
        (local.start(up_far.at[j], up_sum.at[j]), local.start(up_kept.at[j], up_own.at[j]))
        for j in ORDER
    ]
    loads = [
        local.start(attended.at[spot.other(2)], att.at[0]),
        local.start(attended.at[f], att.at[1]),
        local.start(hidden.at[spot.other(2)], hid.at[0]),
        local.start(hidden.at[f], hid.at[1]),
    ]
    greet(column_group(spot) + [spot.fsdp(2), spot.rep()])
    row_slot = sender.slot()
    sender.start(row_slot, row, row_in, core)
    slots = [sender.slot() for _ in range(6)]
    sender.start(slots[0], attended.at[spot.other(3)], att.at[2], core)
    sender.start(slots[1], branch_grad, branch_other, core)
    sender.start(slots[2], hidden.at[spot.other(3)], hid.at[2], core)
    sender.start(slots[3], qkv_grad, qkv_other, core)
    sender.start(slots[4], attended.at[spot.other(1)], att.at[3], core)
    sender.start(slots[5], hidden.at[spot.other(1)], hid.at[3], core)
    up = GradMove(sender, local, spot, up_sum, up_side, up_depth, up_total, up_final)
    tail = GradMove(sender, local, spot, far, side, depth, total, tail_final)
    back = TokenReturn(sender, spot, tokens_grad, tokens_back)
    row_z, row_y, row_x = sender.slots(4), sender.slot(), sender.slot()
    for j, (first, second) in zip(ORDER, load_up, strict=True):
        first.wait()
        second.wait()
        up.fold(j, up_own[j], arrives=False)

    sender.arrived(row_slot, row_in)
    column = (spot.x * 2 + spot.pair) * 4
    rows[column + spot.s] = row[...] + row_in[...]
    row_open = []
    for step in range(1, 4):
        copy = pltpu.make_async_remote_copy(
            rows.at[column + spot.s],
            rows.at[column + spot.s],
            send_sems.at[row_z + step - 1],
            recv_sems.at[row_z + spot.s],
            spot.seq(step),
            MESH,
        )
        copy.start()
        row_open.append(copy)

    for load in loads:
        load.wait()

    def operands(j):
        if j == 0:
            return att, branch_grad[...], branch_other[...]
        columns = slice((j - 1) * width, j * width)
        return hid, qkv_grad[:, columns], qkv_other[:, columns]

    sender.arrived(slots[0], att.at[2])
    sender.arrived(slots[1], branch_other)
    for j in ORDER:
        if j == ORDER[1]:
            sender.arrived(slots[2], hid.at[2])
            sender.arrived(slots[3], qkv_other)
        left, right, right_other = operands(j)
        give[j] = outer(left[0], left[2], right, right_other).astype(BF16)
        tail.send_far(j, give.at[j])
    sender.arrived(slots[4], att.at[3])
    sender.arrived(slots[5], hid.at[3])

    def fold(j):
        left, right, right_other = operands(j)
        tail.fold(j, outer(left[1], left[3], right, right_other))

    a, b, c, d = ORDER
    up.cross(a)
    up.cross(b)
    fold(a)
    up.cross(c)
    up.cross(d)
    back.start()
    for place in range(4):

        @pl.when(spot.s != place)
        def _():
            sender.arrived(row_z + place, rows.at[column + place])

    span = pl.ds(column, 4)
    sender.start(row_y, rows.at[span], rows.at[span], spot.fsdp(2))
    up.settle(a)
    up.settle(b)
    tail.cross(a)
    fold(b)
    up.pass_on(a)
    up.settle(c)
    tail.cross(b)
    up.settle(d)
    up.pass_on(b)
    fold(c)
    tail.settle(a)
    up.pass_on(c)
    tail.cross(c)
    up.pass_on(d)
    far_column = (spot.x * 2 + 1 - spot.pair) * 4
    sender.arrived(row_y, rows.at[pl.ds(far_column, 4)])
    half = pl.ds(spot.x * 8, 8)
    sender.start(row_x, rows.at[half], rows.at[half], spot.rep())
    fold(d)
    tail.settle(b)
    tail.pass_on(a)
    tail.cross(d)
    tail.settle(c)
    tail.pass_on(b)
    tail.settle(d)
    tail.pass_on(c)
    tail.pass_on(d)
    sender.arrived(row_x, rows.at[pl.ds((1 - spot.x) * 8, 8)])
    for copy in row_open:
        copy.wait_send()
    back.finish()
    up.finish()
    tail.finish()
    sender.finish()


def finish(branch_grad, qkv_grad, row, attended, hidden, up_far, up_kept, tokens_grad):
    tokens, width = branch_grad.shape
    tall = up_far.shape[1]
    anywhere = pl.BlockSpec(memory_space=pl.ANY)
    near = pl.BlockSpec(memory_space=pltpu.VMEM)
    final = jax.ShapeDtypeStruct((4, 2, tall // 2, width), BF16)
    group = [
        pltpu.VMEM((4, tall, width), BF16),
        pltpu.VMEM((4, tall, width), BF16),
        pltpu.VMEM((4, tall // 2, width), BF16),
        pltpu.VMEM((3, tall // 2, width), BF16),
        pltpu.VMEM((tall // 2, width), BF16),
    ]
    return pl.pallas_call(
        finish_kernel,
        out_shape=[
            jax.ShapeDtypeStruct((16,) + row.shape, F32),
            final,
            final,
            jax.ShapeDtypeStruct(tokens_grad.shape, BF16),
        ],
        in_specs=[near] * 3 + [anywhere] * 5,
        out_specs=[near] + [anywhere] * 3,
        scratch_shapes=[
            pltpu.VMEM(branch_grad.shape, BF16),
            pltpu.VMEM(qkv_grad.shape, BF16),
            pltpu.VMEM((4,) + attended.shape[1:], BF16),
            pltpu.VMEM((4,) + hidden.shape[1:], BF16),
        ]
        + group
        + group
        + [pltpu.VMEM(row.shape, F32), sems(72), sems(72), sems(20)],
        compiler_params=pltpu.CompilerParams(
            collective_id=4, has_side_effects=True, vmem_limit_bytes=56 * 1024 * 1024
        ),
        name="finish",
    )(branch_grad, qkv_grad, row, attended, hidden, up_far, up_kept, tokens_grad)


def spread_kernel(block, out):
    out[...] = block[0].astype(F32)


def spread(blocks):
    count, rows, width = blocks.shape
    return pl.pallas_call(
        spread_kernel,
        grid=(count,),
        out_shape=jax.ShapeDtypeStruct((rows, count * width), F32),
        in_specs=[pl.BlockSpec((1, rows, width), lambda j: (j, 0, 0))],
        out_specs=pl.BlockSpec((rows, width), lambda j: (0, j)),
        name="spread",
    )(blocks)


def head_window(head, head_dim, width):
    start = head * head_dim
    base = jnp.minimum(start // LANES, (width - WINDOW) // LANES) * LANES
    base = pl.multiple_of(base, LANES)
    return start, base


def forward_heads(
    low,
    high,
    q_ref,
    k_own,
    v_own,
    k_other,
    v_other,
    bias_own,
    bias_other,
    out_ref,
    lse_ref,
):
    tokens, width = q_ref.shape
    head_dim = width // HEADS
    blocks = 2
    tall = tokens // blocks
    scale = head_dim ** (-0.5) * LOG2E
    b_own, b_other = bias_own[...], bias_other[...]
    dims = (((1,), (1,)), ((), ()))

    def body(head, carry):
        start, base = head_window(head, head_dim, width)
        window = pl.ds(base, WINDOW)
        lane = lax.broadcasted_iota(jnp.int32, (1, WINDOW), 1) + base
        inside = (lane >= start) & (lane < start + head_dim)
        keep = inside.astype(BF16)
        spot = lax.broadcasted_iota(jnp.int32, (1, LANES), 1) == head
        key_one, key_two = k_own[:, window], k_other[:, window]
        val_one, val_two = v_own[:, window] * keep, v_other[:, window] * keep
        for block in range(blocks):
            rows = pl.ds(block * tall, tall)
            query = q_ref[rows, window] * keep
            one = lax.dot_general(query, key_one, dims, preferred_element_type=F32)
            two = lax.dot_general(query, key_two, dims, preferred_element_type=F32)
            one = one * scale + b_own
            two = two * scale + b_other
            top = jnp.maximum(
                jnp.max(one, axis=1, keepdims=True), jnp.max(two, axis=1, keepdims=True)
            )
            one = jnp.exp2(one - top)
            two = jnp.exp2(two - top)
            total = jnp.sum(one, axis=1, keepdims=True) + jnp.sum(two, axis=1, keepdims=True)
            mixed = jnp.dot(one.astype(BF16), val_one, preferred_element_type=F32)
            mixed += jnp.dot(two.astype(BF16), val_two, preferred_element_type=F32)
            mixed = mixed * (1.0 / total)
            out_ref[rows, window] = jnp.where(
                inside, mixed, out_ref[rows, window].astype(F32)
            ).astype(out_ref.dtype)
            lse_ref[rows, :] = jnp.where(spot, top + jnp.log2(total), lse_ref[rows, :])
        return carry

    lax.fori_loop(low, high, body, 0)


def forward_kernel(*refs):
    out_ref, lse_ref = refs[-2:]
    out_ref[...] = jnp.zeros_like(out_ref)
    lse_ref[...] = jnp.zeros_like(lse_ref)
    forward_heads(0, HEADS, *refs)


def forward_send_kernel(
    q_ref,
    k_own,
    v_own,
    bias_own,
    bias_other,
    count_in,
    up_weight,
    down_weight,
    teacher,
    out_grad,
    out_ref,
    lse_ref,
    k_other,
    v_other,
    count_out,
    up_full,
    down_full,
    teacher_own,
    out_grad_own,
    counts,
    count_sum,
    far_counts,
    up_stage,
    down_stage,
    send_sems,
    recv_sems,
    local_sems,
):
    spot = Spot()
    sender, local = Sender(send_sems, recv_sems), Locals(local_sems)
    greet(column_group(spot) + [spot.fsdp(2), spot.rep(), spot.rep(2)])
    count_slots = [sender.slot() for _ in range(3)]
    for step in range(1, 4):
        sender.start(count_slots[step - 1], count_in, counts.at[step - 1], spot.seq(step))
    key_slot, value_slot = sender.slot(), sender.slot()
    sender.start(key_slot, k_own, k_other, spot.fsdp(1))
    sender.start(value_slot, v_own, v_other, spot.fsdp(1))
    moves = [
        TokenMove(sender, spot, teacher, teacher_own),
        TokenMove(sender, spot, out_grad, out_grad_own),
    ]
    up = WeightMove(sender, local, spot, up_weight, up_full, up_stage, 3)
    down = WeightMove(sender, local, spot, down_weight, down_full, down_stage, 4)
    far_slots = [sender.slot() for _ in range(3)]

    total = count_in[...]
    for step in range(1, 4):
        sender.arrived(count_slots[step - 1], counts.at[step - 1])
        total = total + counts[step - 1]
    count_sum[...] = total
    for number, device in enumerate((spot.fsdp(2), spot.rep(), spot.rep(2))):
        sender.start(far_slots[number], count_sum, far_counts.at[number], device)
    up.start_far()
    down.start_far()
    for move in moves:
        move.start()
    sender.arrived(key_slot, k_other)
    sender.arrived(value_slot, v_other)
    up.start_near()
    down.start_near()
    out_ref[...] = jnp.zeros_like(out_ref)
    lse_ref[...] = jnp.zeros_like(lse_ref)
    data = (q_ref, k_own, v_own, k_other, v_other, bias_own, bias_other, out_ref, lse_ref)
    forward_heads(0, 8, *data)
    up.store()
    down.store()
    up.pass_far(0)
    forward_heads(8, HEADS, *data)
    up.pass_far(1)
    up.pass_side(0)
    up.pass_far(2)
    up.pass_side(1)
    down.pass_far(0)
    up.pass_side(2)
    for chunk in range(1, 4):
        down.pass_far(chunk)
        down.pass_side(chunk - 1)
    down.pass_side(3)
    total = count_sum[...]
    for number in range(3):
        sender.arrived(far_slots[number], far_counts.at[number])
        total = total + far_counts[number]
    count_out[...] = total
    for move in moves:
        move.finish()
    up.finish()
    down.finish()
    sender.finish()


def attend_and_gather(
    queries,
    keys,
    values,
    bias_own,
    bias_other,
    count,
    up_weight,
    down_weight,
    teacher,
    out_grad,
):
    tokens, width = queries.shape
    anywhere = pl.BlockSpec(memory_space=pl.ANY)
    near = pl.BlockSpec(memory_space=pltpu.VMEM)
    shape = (tokens, width)
    return pl.pallas_call(
        forward_send_kernel,
        out_shape=[
            jax.ShapeDtypeStruct(shape, BF16),
            jax.ShapeDtypeStruct((tokens, LANES), F32),
            jax.ShapeDtypeStruct(shape, BF16),
            jax.ShapeDtypeStruct(shape, BF16),
            jax.ShapeDtypeStruct(count.shape, F32),
            jax.ShapeDtypeStruct((4 * up_weight.shape[0], up_weight.shape[1]), BF16),
            jax.ShapeDtypeStruct((4 * down_weight.shape[0], down_weight.shape[1]), BF16),
            jax.ShapeDtypeStruct(teacher.shape, BF16),
            jax.ShapeDtypeStruct(out_grad.shape, BF16),
        ],
        in_specs=[near] * 6 + [anywhere] * 4,
        out_specs=[near] * 5 + [anywhere] * 4,
        scratch_shapes=[
            pltpu.VMEM((3,) + count.shape, F32),
            pltpu.VMEM(count.shape, F32),
            pltpu.VMEM((3,) + count.shape, F32),
            pltpu.VMEM(up_weight.shape, BF16),
            pltpu.VMEM(down_weight.shape, BF16),
            sems(48),
            sems(48),
            sems(8),
        ],
        compiler_params=pltpu.CompilerParams(
            collective_id=2, has_side_effects=True, vmem_limit_bytes=56 * 1024 * 1024
        ),
        name="attend_and_gather",
    )(
        queries,
        keys,
        values,
        bias_own,
        bias_other,
        count,
        up_weight,
        down_weight,
        teacher,
        out_grad,
    )


def attend(queries, k_own, v_own, k_other, v_other, bias_own, bias_other):
    tokens, width = queries.shape
    return pl.pallas_call(
        forward_kernel,
        out_shape=[
            jax.ShapeDtypeStruct((tokens, width), BF16),
            jax.ShapeDtypeStruct((tokens, LANES), F32),
        ],
        compiler_params=pltpu.CompilerParams(vmem_limit_bytes=48 * 1024 * 1024),
        cost_estimate=pl.CostEstimate(
            flops=16 * tokens * tokens * 2 * WINDOW * 4,
            transcendentals=HEADS * tokens * tokens * 2,
            bytes_accessed=6 * tokens * width * 2,
        ),
        name="attend",
    )(queries, k_own, v_own, k_other, v_other, bias_own, bias_other)


def backward_heads(
    low,
    high,
    q_ref,
    k_own,
    v_own,
    k_other,
    v_other,
    do_ref,
    lse_ref,
    bias_own,
    bias_other,
    dq_ref,
    dk_one,
    dv_one,
    dk_two,
    dv_two,
):
    tokens, width = q_ref.shape
    head_dim = width // HEADS
    factor = head_dim ** (-0.5)
    scale = factor * LOG2E
    across = (((1,), (1,)), ((), ()))
    sides = (
        (k_own, v_own, bias_own, dk_one, dv_one),
        (k_other, v_other, bias_other, dk_two, dv_two),
    )

    def body(head, carry):
        start, base = head_window(head, head_dim, width)
        window = pl.ds(base, WINDOW)
        lane = lax.broadcasted_iota(jnp.int32, (1, WINDOW), 1) + base
        inside = (lane >= start) & (lane < start + head_dim)
        keep = inside.astype(BF16)
        query = q_ref[:, window] * keep
        grad = do_ref[:, window] * keep
        lse = lse_ref[pl.ds(head, 1), :]

        def put(ref, value):
            ref[:, window] = jnp.where(inside, value, ref[:, window].astype(F32)).astype(ref.dtype)

        probs, prods = [], []
        delta = None
        for k_ref, v_ref, bias, _, _ in sides:
            scores = lax.dot_general(k_ref[:, window], query, across, preferred_element_type=F32)
            prob = jnp.exp2(scores * scale + bias[...] - lse)
            prob_grad = lax.dot_general(v_ref[:, window], grad, across, preferred_element_type=F32)
            prod = prob * prob_grad
            part = jnp.sum(prod, axis=0, keepdims=True)
            delta = part if delta is None else delta + part
            probs.append(prob)
            prods.append(prod)
        dq = None
        for (k_ref, _, _, dk, dv), prob, prod in zip(sides, probs, prods, strict=True):
            put(dv, jnp.dot(prob.astype(BF16), grad, preferred_element_type=F32))
            score_grad = (prod - prob * delta).astype(BF16)
            put(dk, jnp.dot(score_grad, query, preferred_element_type=F32) * factor)
            part = lax.dot_general(
                score_grad, k_ref[:, window], DOWN, preferred_element_type=F32
            )
            dq = part if dq is None else dq + part
        put(dq_ref, dq * factor)
        return carry

    lax.fori_loop(low, high, body, 0)


def backward_kernel(*refs):
    for ref in refs[-5:]:
        ref[...] = jnp.zeros_like(ref)
    backward_heads(0, HEADS, *refs)


def attend_back(queries, k_own, v_own, k_other, v_other, grad, lse, bias_own, bias_other):
    tokens, width = queries.shape
    shape = (tokens, width)
    return pl.pallas_call(
        backward_kernel,
        out_shape=[
            jax.ShapeDtypeStruct(shape, BF16),
            jax.ShapeDtypeStruct(shape, F32),
            jax.ShapeDtypeStruct(shape, F32),
            jax.ShapeDtypeStruct(shape, BF16),
            jax.ShapeDtypeStruct(shape, BF16),
        ],
        compiler_params=pltpu.CompilerParams(vmem_limit_bytes=60 * 1024 * 1024),
        name="attend_back",
    )(queries, k_own, v_own, k_other, v_other, grad, lse, bias_own, bias_other)


def dot(left, right):
    return jnp.dot(left, right, preferred_element_type=F32)


def dot_t(left, right):
    return lax.dot_general(left, right, (((1,), (1,)), ((), ())), preferred_element_type=F32)


def norm_parts(inputs):
    centred = inputs - jnp.mean(inputs, axis=-1, keepdims=True)
    rate = lax.rsqrt(jnp.mean(centred * centred, axis=-1, keepdims=True) + EPS)
    return centred * rate, rate


def norm_back(grad, normed, rate):
    return rate * (
        grad
        - jnp.mean(grad, axis=-1, keepdims=True)
        - normed * jnp.mean(grad * normed, axis=-1, keepdims=True)
    )


def gelu_parts(inputs):
    inner = jnp.tanh(GELU_C * (inputs + 0.044715 * inputs * inputs * inputs))
    value = 0.5 * inputs * (1.0 + inner)
    slope = 0.5 * (1.0 + inner) + 0.5 * inputs * (1.0 - inner * inner) * GELU_C * (
        1.0 + 3.0 * 0.044715 * inputs * inputs
    )
    return value, slope


def column_sum(array):
    return jnp.sum(array.astype(F32), axis=0)


def shards(
    tokens,
    condition,
    valid_mask,
    teacher,
    out_grad,
    mod_weight,
    mod_bias,
    qkv_weight,
    qkv_bias,
    out_weight,
    out_bias,
    up_weight,
    up_bias,
    down_weight,
    down_bias,
):
    reps, fsdp, seq = lax.axis_size("rep"), lax.axis_size("fsdp"), lax.axis_size("seq")
    fast = (reps, fsdp, seq) == (2, 4, 4)
    latents, span, width = tokens.shape
    assert 2 * latents == seq and latents == 2
    place_f, place_s = lax.axis_index("fsdp"), lax.axis_index("seq")
    total_tokens = latents * span * reps * fsdp * seq

    biases = jnp.concatenate([mod_bias, qkv_bias, out_bias, up_bias, down_bias])
    shard_rows = mod_weight.shape[0]
    cond_row = pick(condition, place_s % 2)
    keep_mask = valid_mask.astype(F32)

    if fast:
        inputs_low, valid_all, mod_parts, bias_all, qkv_full, out_full = enter(
            tokens,
            keep_mask.reshape(latents, 1, span),
            condition.astype(F32).reshape(latents, fsdp, 1, shard_rows),
            biases.astype(F32)[None],
            mod_weight,
            qkv_weight,
            out_weight,
        )
        inputs_low = inputs_low.reshape(-1, width)
        valid_all = valid_all.reshape(2, -1)
        keyvalid, valid_other = pick(valid_all, place_f % 2), pick(valid_all, 1 - place_f % 2)
        mod_row = jnp.sum(mod_parts, axis=(0, 1))
        bias_all = bias_all[:, 0]
    else:
        inputs_low = to_latent(tokens)
        keyvalid = to_latent(keep_mask)
        valid_other = flip(keyvalid, "fsdp", 1)
        counted = lax.psum(jnp.sum(keep_mask), ("rep", "fsdp", "seq")).reshape(1, 1)
        own_row = jnp.where(place_f % 2 == place_s // 2, cond_row, flip(cond_row, "fsdp", 1))
        cond_pair = lax.all_gather(own_row, "fsdp", axis=0)[::2]
        silu_pair = jax.nn.silu(cond_pair.astype(F32)).astype(BF16)
        silu_cols = lax.dynamic_slice_in_dim(silu_pair, place_f * shard_rows, shard_rows, 1)
        mod_row = pick(lax.psum(dot(silu_cols, mod_weight), "fsdp"), place_f // 2)
        bias_all = lax.all_gather(biases, "fsdp", axis=0).astype(F32)
        qkv_full, out_full = gather_weight(qkv_weight), gather_weight(out_weight)
        up_full, down_full = gather_weight(up_weight), gather_weight(down_weight)
        teacher_own, out_grad_own = to_latent(teacher), to_latent(out_grad)
    mask_own = (keyvalid - 1.0) * (-NEG)
    mask_other = (valid_other - 1.0) * (-NEG)

    cuts = [0]
    for bias in (mod_bias, qkv_bias, out_bias, up_bias, down_bias):
        cuts.append(cuts[-1] + bias.shape[0])
    mod_b, qkv_b, out_b, up_b, down_b = (
        bias_all[:, low:high].reshape(-1) for low, high in zip(cuts[:-1], cuts[1:], strict=True)
    )
    pieces = (mod_row + mod_b).reshape(6, 1, width)
    shift_one, scale_one, gate_one, shift_two, scale_two, gate_two = (pieces[i] for i in range(6))

    inputs = inputs_low.astype(F32)
    normed_one, rate_one = norm_parts(inputs)
    hidden_one = (normed_one * (1.0 + scale_one) + shift_one).astype(BF16)
    projected = dot(hidden_one, qkv_full)
    queries = (projected[:, :width] + qkv_b[:width]).astype(BF16)
    keys_own = projected[:, width : 2 * width].astype(BF16)
    values_own = (projected[:, 2 * width :] + qkv_b[width:]).astype(BF16)
    if fast:
        (
            attended,
            lse,
            keys_other,
            values_other,
            counted,
            up_full,
            down_full,
            teacher_own,
            out_grad_own,
        ) = attend_and_gather(
            queries,
            keys_own,
            values_own,
            mask_own[None],
            mask_other[None],
            jnp.full((1, LANES), jnp.sum(valid_all)),
            up_weight,
            down_weight,
            teacher,
            out_grad,
        )
        counted = counted[:, :1]
        teacher_own = teacher_own.reshape(-1, width)
        out_grad_own = out_grad_own.reshape(-1, width)
    else:
        keys_other, values_other = flip(keys_own, "fsdp", 1), flip(values_own, "fsdp", 1)
        attended, lse = attend(
            queries,
            keys_own,
            values_own,
            keys_other,
            values_other,
            mask_own[None],
            mask_other[None],
        )
    branch = dot(attended, out_full) + out_b
    middle = inputs + gate_one * branch
    normed_two, rate_two = norm_parts(middle)
    hidden_two = (normed_two * (1.0 + scale_two) + shift_two).astype(BF16)
    up_pre = dot(hidden_two, up_full) + up_b
    activated, slope = gelu_parts(up_pre)
    activated = activated.astype(BF16)
    mlp_out = dot(activated, down_full) + down_b
    output = middle + gate_two * mlp_out
    block_out = output.astype(BF16)
    differ = (output - teacher_own.astype(F32)) * keyvalid[:, None]
    error = jnp.sum(differ * differ)

    grad_out = out_grad_own.astype(F32) + total_tokens / counted * differ
    grad_mlp = (grad_out * gate_two).astype(BF16)
    gate_two_grad = jnp.sum(grad_out * mlp_out, axis=0)

    def slices(array):
        return array.reshape(array.shape[0], fsdp, -1).transpose(1, 0, 2)

    def weight_grad(left, right):
        whole = lax.dot_general(left, right, DOWN, preferred_element_type=F32)
        mine = lax.psum_scatter(whole.astype(BF16), "fsdp", scatter_dimension=0, tiled=True)
        return lax.psum(mine, ("rep", "seq")).astype(F32)

    down_bgrad = column_sum(grad_mlp)
    upper_grad = (dot_t(grad_mlp, down_full) * slope).astype(BF16)
    up_bgrad = column_sum(upper_grad)
    hidden_two_grad = dot_t(upper_grad, up_full)
    scaled_two = hidden_two_grad * (1.0 + scale_two)
    middle_grad = grad_out + norm_back(scaled_two, normed_two, rate_two)
    shift_two_grad = jnp.sum(hidden_two_grad, axis=0)
    scale_two_grad = jnp.sum(hidden_two_grad * normed_two, axis=0)
    branch_grad = (middle_grad * gate_one).astype(BF16)
    gate_one_grad = jnp.sum(middle_grad * branch, axis=0)
    out_bgrad = column_sum(branch_grad)
    attended_grad = dot_t(branch_grad, out_full).astype(BF16)

    if fast:
        (
            query_grad,
            key_grad,
            value_grad,
            error_sum,
            down_final,
            up_far,
            up_kept,
            _,
            block_out,
        ) = attend_back_and_reduce(
            queries,
            keys_own,
            values_own,
            keys_other,
            values_other,
            attended_grad,
            lse.T,
            mask_own[:, None],
            mask_other[:, None],
            grad_mlp,
            jnp.full((1, LANES), error),
            activated,
            slices(hidden_two),
            upper_grad,
            block_out.reshape(2, span, width),
        )
        err_total = error_sum[:, :1]
    else:
        query_grad, key_part, value_part, key_away, value_away = attend_back(
            queries,
            keys_own,
            values_own,
            keys_other,
            values_other,
            attended_grad,
            lse.T,
            mask_own[:, None],
            mask_other[:, None],
        )
        key_grad = (key_part + flip(key_away, "fsdp", 1).astype(F32)).astype(BF16)
        value_grad = (value_part + flip(value_away, "fsdp", 1).astype(F32)).astype(BF16)
        err_total = lax.psum(error, ("rep", "fsdp", "seq")).reshape(1, 1)
        block_out = from_latent(block_out)
    qkv_grad = jnp.concatenate([query_grad, key_grad, value_grad], axis=-1)
    hidden_one_grad = dot_t(qkv_grad, qkv_full)
    scaled_one = hidden_one_grad * (1.0 + scale_one)
    tokens_grad = middle_grad + norm_back(scaled_one, normed_one, rate_one)
    tokens_grad = tokens_grad.astype(BF16)
    row = jnp.concatenate(
        [
            jnp.sum(hidden_one_grad, axis=0),
            jnp.sum(hidden_one_grad * normed_one, axis=0),
            gate_one_grad,
            shift_two_grad,
            scale_two_grad,
            gate_two_grad,
            out_bgrad,
            up_bgrad,
            down_bgrad,
            column_sum(query_grad),
            column_sum(value_grad),
            jnp.where(place_f % 2 == place_s // 2, cond_row.astype(F32), 0.0),
        ]
    )
    if fast:
        length = row.shape[0]
        deep = -(-length // (8 * LANES)) * 8
        row = jnp.pad(row, (0, deep * LANES - length)).reshape(deep, LANES)
        rows, up_final, tail_final, tokens_grad = finish(
            branch_grad,
            qkv_grad,
            row,
            slices(attended),
            slices(hidden_one),
            up_far,
            up_kept,
            tokens_grad.reshape(2, span, width),
        )
        rows = rows.reshape(-1, deep * LANES)[:, :length]
        down_g = down_final.reshape(down_weight.shape).astype(F32)
        up_g = spread(up_final.reshape(4, -1, width))
        tail_final = tail_final.reshape(4, -1, width)
        out_g = tail_final[0].astype(F32)
        qkv_g = spread(tail_final[1:])
    else:
        row = row + flip(row, "fsdp", 1)
        rows = gather_rows(row)
        tokens_grad = from_latent(tokens_grad)
        down_g = weight_grad(activated, grad_mlp)
        up_g = weight_grad(hidden_two, upper_grad)
        out_g = weight_grad(attended, branch_grad)
        qkv_g = weight_grad(hidden_one, qkv_grad)

    mod_grad = rows[:, : 6 * width]
    silu_all = jax.nn.silu(rows[:, -width:]).astype(BF16)
    silu_own = lax.dynamic_slice_in_dim(silu_all, place_f * shard_rows, shard_rows, 1)
    mod_wgrad = lax.dot_general(
        silu_own.astype(F32),
        mod_grad,
        (((0,), (0,)), ((), ())),
        precision=HIGHEST,
        preferred_element_type=F32,
    )
    bias_sum = jnp.sum(rows[:, 6 * width : -width], axis=0)

    def own_bias(low, size):
        own = size // fsdp
        return lax.dynamic_slice_in_dim(bias_sum, low + place_f * own, own, 0)

    up_size = up_b.shape[0]
    out_bg = own_bias(0, width)
    up_bg = own_bias(width, up_size)
    down_bg = own_bias(width + up_size, width)
    qkv_bg = own_bias(2 * width + up_size, 2 * width)
    mod_own = mod_bias.shape[0]
    mod_bg = lax.dynamic_slice_in_dim(jnp.sum(mod_grad, axis=0), place_f * mod_own, mod_own, 0)

    replica = lax.axis_index("rep")
    per_rep = mod_grad.shape[0] // reps
    own_rep = lax.dynamic_slice_in_dim(mod_grad, replica * per_rep, per_rep, 0)
    silu_grad = lax.dot_general(
        own_rep,
        mod_weight.astype(F32),
        (((1,), (1,)), ((), ())),
        precision=HIGHEST,
        preferred_element_type=F32,
    )
    owners = silu_grad.reshape(fsdp, latents, shard_rows)
    if fast:
        found = [pick(owners, place_f)]
        found += [flip(pick(owners, place_f ^ bit), "fsdp", bit) for bit in (1, 2, 3)]
        found = jnp.stack(found)
        found = jnp.concatenate(
            [lax.dynamic_slice_in_dim(found, place_f ^ f, 1, 0) for f in range(fsdp)]
        )
    else:
        found = lax.all_to_all(owners, "fsdp", 0, 0, tiled=True)
    silu_grad = found.transpose(1, 0, 2).reshape(latents, width)
    conds = condition.astype(F32)
    sigmoid = 1.0 / (1.0 + jnp.exp(-conds))
    condition_grad = silu_grad * (sigmoid * (1.0 + conds * (1.0 - sigmoid)))

    loss_value = (err_total / (width * counted))[0, 0]
    return (
        block_out,
        loss_value,
        tokens_grad,
        condition_grad,
        mod_wgrad,
        mod_bg,
        qkv_g,
        qkv_bg,
        out_g,
        out_bg,
        up_g,
        up_bg,
        down_g,
        down_bg,
    )


def solution(mesh):
    batch = P(("rep", "fsdp"), "seq", None)
    matrix, vector = P("fsdp", None), P("fsdp")
    params = (matrix, vector) * 5
    return jax.shard_map(
        shards,
        mesh=mesh,
        in_specs=(batch, P(("rep", "fsdp"), None), P(("rep", "fsdp"), "seq"), batch, batch)
        + params,
        out_specs=(batch, P(), batch, P(("rep", "fsdp"), None)) + params,
        check_vma=False,
    )
```

```python
import functools

import jax
import jax.numpy as jnp
from jax import lax
from jax.experimental import pallas as pl
from jax.experimental.pallas import tpu as pltpu
from jax.sharding import PartitionSpec as P

HEADS = 16

EPS = 1e-06
GELU_C = 0.7978845608028654
HIGHEST = lax.Precision.HIGHEST
LOG2E = 1.4426950408889634
NEG = -1e30
BF16 = jnp.bfloat16
F32 = jnp.float32
WINDOW = 256
LANES = 128


def flip(array, axis, bit):
    size = lax.axis_size(axis)
    return lax.ppermute(array, axis, [(i, i ^ bit) for i in range(size)])


def pick(array, index):
    return lax.dynamic_index_in_dim(array, index, 0, keepdims=False)


def in_order(first, second, swapped):
    return jnp.where(swapped, jnp.stack([second, first]), jnp.stack([first, second]))


def to_latent(array):
    seq, fsdp = lax.axis_size("seq"), lax.axis_size("fsdp")
    place = lax.axis_index("seq")
    arrived = []
    for turn in range(2):
        pairs = []
        for f in range(fsdp):
            for s in range(seq):
                pair, core = f // 2, f % 2
                target = (pair * 2 + s // 2, 2 * core + (s + turn) % 2)
                pairs.append((f * seq + s, target[0] * seq + target[1]))
        block = pick(array, (place + turn) % 2)
        arrived.append(lax.ppermute(block, ("fsdp", "seq"), pairs))
    both = in_order(arrived[0], arrived[1], place % 2 == 1)
    return both.reshape((-1,) + both.shape[2:])


def from_latent(array):
    seq, fsdp = lax.axis_size("seq"), lax.axis_size("fsdp")
    place = lax.axis_index("seq")
    halves = array.reshape((2, array.shape[0] // 2) + array.shape[1:])
    arrived = []
    for turn in range(2):
        pairs = []
        for f in range(fsdp):
            for s in range(seq):
                pair, core = f // 2, f % 2
                slot = (s + turn) % 2
                target = (pair * 2 + s // 2, 2 * core + slot)
                pairs.append((f * seq + s, target[0] * seq + target[1]))
        arrived.append(lax.ppermute(pick(halves, (place + turn) % 2), ("fsdp", "seq"), pairs))
    return in_order(arrived[0], arrived[1], place % 2 == 1)


def gather_rows(row):
    fsdp = lax.axis_size("fsdp")
    everything = lax.all_gather(row, ("rep", "fsdp", "seq"), axis=0)
    everything = everything.reshape((-1, fsdp // 2, 2, lax.axis_size("seq")) + row.shape)
    return everything[:, :, 0].reshape((-1,) + row.shape)


def gather_weight(weight):
    return lax.all_gather(weight, "fsdp", axis=0, tiled=True)


MESH = pl.DeviceIdType.MESH


class Spot:
    def __init__(self):
        self.x, self.f, self.s = (lax.axis_index(name) for name in ("rep", "fsdp", "seq"))
        self.core = self.f % 2
        self.pair = self.f // 2

    def other(self, bit):
        if bit == 3:
            return 3 - self.f
        return self.f + bit - 2 * bit * ((self.f // bit) % 2)

    def fsdp(self, bit):
        return (self.x, self.other(bit), self.s)

    def rep(self, bit=0):
        return (1 - self.x, self.other(bit) if bit else self.f, self.s)

    def seq(self, step):
        return (self.x, self.f, lax.rem(self.s + step, 4))

    def token_target(self, turn):
        block = lax.rem(self.s + turn, 2)
        return (self.x, 2 * self.pair + self.s // 2, 2 * self.core + block), block


def greet(devices):
    barrier = pltpu.get_barrier_semaphore()
    for device in devices:
        pl.semaphore_signal(barrier, inc=1, device_id=device, device_id_type=MESH)
    pl.semaphore_wait(barrier, len(devices))


def column_group(spot):
    found = [(spot.x, spot.other(1), spot.s)]
    for step in range(1, 4):
        found.append(spot.seq(step))
        found.append((spot.x, spot.other(1), lax.rem(spot.s + step, 4)))
    return found


class Sender:
    def __init__(self, send_sems, recv_sems):
        self.send_sems, self.recv_sems = send_sems, recv_sems
        self.used = 0
        self.open = []

    def slot(self):
        self.used += 1
        return self.used - 1

    def start(self, slot, source, target, device):
        copy = pltpu.make_async_remote_copy(
            source, target, self.send_sems.at[slot], self.recv_sems.at[slot], device, MESH
        )
        copy.start()
        self.open.append(copy)

    def start_if(self, wanted, send_slot, recv_slot, source, target, device):
        copy = pltpu.make_async_remote_copy(
            source, target, self.send_sems.at[send_slot], self.recv_sems.at[recv_slot], device, MESH
        )
        pl.when(wanted)(lambda: copy.start())
        return wanted, copy

    def slots(self, count):
        self.used += count
        return self.used - count

    def sent(self, slot, view):
        pltpu.make_async_copy(view, view, self.send_sems.at[slot]).wait()

    def arrived(self, slot, view):
        pltpu.make_async_copy(view, view, self.recv_sems.at[slot]).wait()

    def finish(self):
        for copy in self.open:
            copy.wait_send()
        self.open = []


class Locals:
    def __init__(self, sems):
        self.sems = sems
        self.used = 0
        self.open = []

    def start(self, source, target):
        copy = pltpu.make_async_copy(source, target, self.sems.at[self.used])
        self.used += 1
        copy.start()
        return copy


class TokenMove:
    def __init__(self, sender, spot, source, target):
        self.sender, self.spot, self.source, self.target = sender, spot, source, target
        self.slots = [sender.slot(), sender.slot()]

    def start(self):
        spot = self.spot
        self.remote = []
        for turn, slot in enumerate(self.slots):
            device, block = spot.token_target(turn)
            stays = (device[1] == spot.f) & (device[2] == spot.s)
            source = self.source.at[block]
            target = self.target.at[lax.rem(spot.s, 2)]
            remote = pltpu.make_async_remote_copy(
                source,
                target,
                self.sender.send_sems.at[slot],
                self.sender.recv_sems.at[slot],
                device,
                MESH,
            )
            local = pltpu.make_async_copy(source, target, self.sender.recv_sems.at[slot])
            pl.when(jnp.logical_not(stays))(lambda remote=remote: remote.start())
            pl.when(stays)(lambda local=local: local.start())
            self.remote.append((stays, remote))

    def finish(self):
        for turn, slot in enumerate(self.slots):
            self.sender.arrived(slot, self.target.at[lax.rem(self.spot.s + turn, 2)])
        for stays, remote in self.remote:
            pl.when(jnp.logical_not(stays))(lambda remote=remote: remote.wait_send())


class WeightMove:
    def __init__(self, sender, local, spot, own, full, stage, chunks):
        self.sender, self.local, self.spot = sender, local, spot
        self.own, self.full, self.stage = own, full, stage
        self.rows, self.chunks = own.shape[0], chunks
        self.half = self.rows // 2
        self.tall = self.half // chunks
        self.slots = {
            kind: [sender.slot() for _ in range(1 if kind == "core" else chunks)]
            for kind in ("core", "far", "side", "far_core", "side_core")
        }

    def view(self, bits, side, chunk):
        shard = self.spot.other(bits) if bits else self.spot.f
        half = self.spot.x if side == 0 else 1 - self.spot.x
        start = shard * self.rows + half * self.half + chunk * self.tall
        return self.full.at[pl.ds(pl.multiple_of(start, 16), self.tall)]

    def shard_view(self, bits):
        shard = self.spot.other(bits) if bits else self.spot.f
        return self.full.at[pl.ds(pl.multiple_of(shard * self.rows, 16), self.rows)]

    def start_far(self):
        spot = self.spot
        for chunk, slot in enumerate(self.slots["far"]):
            start = pl.multiple_of(spot.x * self.half + chunk * self.tall, 16)
            self.sender.start(
                slot, self.own.at[pl.ds(start, self.tall)], self.view(0, 0, chunk), spot.fsdp(2)
            )

    def start_near(self):
        self.sender.start(self.slots["core"][0], self.own, self.shard_view(0), self.spot.fsdp(1))
        self.load = self.local.start(self.own, self.stage)

    def store(self):
        self.load.wait()
        self.kept = self.local.start(self.stage, self.shard_view(0))

    def pass_far(self, chunk):
        view = self.view(2, 0, chunk)
        self.sender.arrived(self.slots["far"][chunk], view)
        self.sender.start(self.slots["side"][chunk], view, view, self.spot.rep())
        self.sender.start(self.slots["far_core"][chunk], view, view, self.spot.fsdp(1))

    def pass_side(self, chunk):
        view = self.view(2, 1, chunk)
        self.sender.arrived(self.slots["side"][chunk], view)
        self.sender.start(self.slots["side_core"][chunk], view, view, self.spot.fsdp(1))

    def finish(self):
        self.kept.wait()
        self.sender.arrived(self.slots["core"][0], self.shard_view(1))
        for chunk in range(self.chunks):
            self.sender.arrived(self.slots["far_core"][chunk], self.view(3, 0, chunk))
            self.sender.arrived(self.slots["side_core"][chunk], self.view(3, 1, chunk))


def entry_kernel(
    tokens,
    valid,
    cond,
    biases,
    mod_weight,
    qkv_weight,
    out_weight,
    tokens_own,
    valid_all,
    mod_parts,
    bias_all,
    qkv_full,
    out_full,
    mod_held,
    cond_held,
    partial,
    qkv_stage,
    out_stage,
    send_sems,
    recv_sems,
    local_sems,
):
    spot = Spot()
    sender, local = Sender(send_sems, recv_sems), Locals(local_sems)
    mod_load = local.start(mod_weight, mod_held)
    greet(column_group(spot) + [spot.fsdp(2), spot.fsdp(3), spot.rep()])

    row = lax.rem(spot.s, 2)
    cond_slots, bias_slots = {}, {}
    for bit in (1, 2, 3):
        cond_slots[bit], bias_slots[bit] = sender.slot(), sender.slot()
        target = spot.other(bit)
        sender.start(
            cond_slots[bit], cond.at[row, target], cond_held.at[spot.f], spot.fsdp(bit)
        )
    for bit in (1, 2, 3):
        sender.start(bias_slots[bit], biases, bias_all.at[spot.f], spot.fsdp(bit))
    cond_own = local.start(cond.at[row, spot.f], cond_held.at[spot.f])
    bias_own = local.start(biases, bias_all.at[spot.f])

    qkv = WeightMove(sender, local, spot, qkv_weight, qkv_full, qkv_stage, 3)
    out = WeightMove(sender, local, spot, out_weight, out_full, out_stage, 1)
    mod_slots = {bit: sender.slot() for bit in (1, 2, 3)}
    move = TokenMove(sender, spot, tokens, tokens_own)
    valid_base = [sender.slot() for _ in range(4)][0]
    valid_open = []
    for turn in range(2):
        device, block = spot.token_target(turn)
        for core in range(2):
            goal = (device[0], 2 * spot.pair + core, device[2])
            stays = (goal[1] == spot.f) & (goal[2] == spot.s)
            source, target = valid.at[block], valid_all.at[spot.s]
            arrival = recv_sems.at[valid_base + spot.s]
            remote = pltpu.make_async_remote_copy(
                source, target, send_sems.at[valid_base + 2 * turn + core], arrival, goal, MESH
            )
            near = pltpu.make_async_copy(source, target, arrival)
            pl.when(jnp.logical_not(stays))(lambda remote=remote: remote.start())
            pl.when(stays)(lambda near=near: near.start())
            valid_open.append((stays, remote))
    move.start()
    qkv.start_far()
    qkv.start_near()
    out.start_near()

    cond_own.wait()
    for bit in (1, 2, 3):
        sender.arrived(cond_slots[bit], cond_held.at[spot.other(bit)])
    first, second = cond_held[spot.s // 2], cond_held[2 + spot.s // 2]
    which = lax.broadcasted_iota(jnp.int32, (16, first.shape[-1]), 0)
    conds = jnp.where(which == 0, first, second)
    silu = (conds / (1.0 + jnp.exp(-conds))).astype(BF16)
    mod_load.wait()
    width = mod_held.shape[1] // 6
    for piece in range(6):
        columns = slice(piece * width, (piece + 1) * width)
        product = jnp.dot(silu, mod_held[:, columns], preferred_element_type=F32)
        partial[0, :, columns] = product[0:1]
        partial[1, :, columns] = product[1:2]
    for bit in (1, 2, 3):
        pair = spot.pair if bit == 1 else 1 - spot.pair
        sender.start(
            mod_slots[bit], partial.at[pair], mod_parts.at[spot.f], spot.fsdp(bit)
        )
    mod_own = local.start(partial.at[spot.pair], mod_parts.at[spot.f])
    out.start_far()
    qkv.store()
    out.store()
    for chunk in range(3):
        qkv.pass_far(chunk)
        if chunk:
            qkv.pass_side(chunk - 1)
    qkv.pass_side(2)
    out.pass_far(0)
    out.pass_side(0)

    bias_own.wait()
    mod_own.wait()
    for bit in (1, 2, 3):
        sender.arrived(bias_slots[bit], bias_all.at[spot.other(bit)])
        sender.arrived(mod_slots[bit], mod_parts.at[spot.other(bit)])
    for place in range(4):
        sender.arrived(valid_base + place, valid_all.at[place])
    for stays, remote in valid_open:
        pl.when(jnp.logical_not(stays))(lambda remote=remote: remote.wait_send())
    move.finish()
    qkv.finish()
    out.finish()
    sender.finish()


def sems(count):
    return pltpu.SemaphoreType.DMA((count,))


def enter(tokens, valid, cond, biases, mod_weight, qkv_weight, out_weight):
    anywhere = pl.BlockSpec(memory_space=pl.ANY)
    return pl.pallas_call(
        entry_kernel,
        out_shape=[
            jax.ShapeDtypeStruct(tokens.shape, tokens.dtype),
            jax.ShapeDtypeStruct((4,) + valid.shape[1:], F32),
            jax.ShapeDtypeStruct((4, 1, mod_weight.shape[1]), F32),
            jax.ShapeDtypeStruct((4,) + biases.shape, F32),
            jax.ShapeDtypeStruct((4 * qkv_weight.shape[0], qkv_weight.shape[1]), BF16),
            jax.ShapeDtypeStruct((4 * out_weight.shape[0], out_weight.shape[1]), BF16),
        ],
        in_specs=[anywhere] * 7,
        out_specs=[anywhere] * 6,
        scratch_shapes=[
            pltpu.VMEM(mod_weight.shape, BF16),
            pltpu.VMEM((4,) + cond.shape[2:], F32),
            pltpu.VMEM((2, 1, mod_weight.shape[1]), F32),
            pltpu.VMEM(qkv_weight.shape, BF16),
            pltpu.VMEM(out_weight.shape, BF16),
            sems(40),
            sems(40),
            sems(12),
        ],
        compiler_params=pltpu.CompilerParams(
            collective_id=1, has_side_effects=True, vmem_limit_bytes=32 * 1024 * 1024
        ),
        name="enter",
    )(tokens, valid, cond, biases, mod_weight, qkv_weight, out_weight)


class TokenReturn:
    def __init__(self, sender, spot, source, target):
        self.sender, self.spot, self.source, self.target = sender, spot, source, target
        self.slots = [sender.slot(), sender.slot()]

    def start(self):
        spot = self.spot
        self.remote = []
        for turn, slot in enumerate(self.slots):
            half = lax.rem(spot.s + turn, 2)
            device = (spot.x, 2 * spot.pair + spot.s // 2, 2 * spot.core + half)
            stays = (device[1] == spot.f) & (device[2] == spot.s)
            source, target = self.source.at[half], self.target.at[lax.rem(spot.s, 2)]
            arrival = self.sender.recv_sems.at[slot]
            remote = pltpu.make_async_remote_copy(
                source, target, self.sender.send_sems.at[slot], arrival, device, MESH
            )
            local = pltpu.make_async_copy(source, target, arrival)
            pl.when(jnp.logical_not(stays))(lambda remote=remote: remote.start())
            pl.when(stays)(lambda local=local: local.start())
            self.remote.append((stays, remote))

    def finish(self):
        for turn, slot in enumerate(self.slots):
            self.sender.arrived(slot, self.target.at[lax.rem(self.spot.s + turn, 2)])
        for stays, remote in self.remote:
            pl.when(jnp.logical_not(stays))(lambda remote=remote: remote.wait_send())


ORDER = (0, 3, 1, 2)


class GradMove:
    def __init__(self, sender, local, spot, far, side, depth, total, final):
        self.sender, self.local, self.spot = sender, local, spot
        self.far, self.side, self.depth, self.total, self.final = far, side, depth, total, final
        self.tall = total.shape[0]
        self.y, self.x, self.z, self.g, self.fx = (sender.slots(4) for _ in range(5))
        self.kept = local.used
        local.used += 1
        self.z_open = []

    def send_far(self, j, give):
        self.sender.start(self.y + j, give, self.far.at[j], self.spot.fsdp(2))

    def half(self, side):
        return pl.ds(pl.multiple_of(side * self.tall, 16), self.tall)

    def fold(self, j, kept, arrives=True):
        if arrives:
            self.sender.arrived(self.y + j, self.far.at[j])
        self.far[j] = (self.far[j].astype(F32) + kept.astype(F32)).astype(BF16)
        self.sender.start(
            self.x + j, self.far.at[j, self.half(1 - self.spot.x)], self.side.at[j], self.spot.rep()
        )

    def cross(self, j):
        spot = self.spot
        self.sender.arrived(self.x + j, self.side.at[j])
        mine = self.far[j, self.half(spot.x), :].astype(F32)
        self.side[j] = (mine + self.side[j].astype(F32)).astype(BF16)
        step = lax.rem(spot.s - j + 4, 4)
        index = jnp.maximum(step - 1, 0)
        self.z_open.append(
            self.sender.start_if(
                spot.s != j,
                self.z + j,
                self.z + index,
                self.side.at[j],
                self.depth.at[index],
                (spot.x, spot.f, j),
            )
        )

    def gather(self, j):
        @pl.when(self.spot.s == j)
        def _():
            total = self.side[j].astype(F32)
            for index in range(3):
                self.sender.arrived(self.z + index, self.depth.at[index])
                total = total + self.depth[index].astype(F32)
            self.total[...] = total.astype(BF16)

    def give_back(self, j):
        spot, sender = self.spot, self.sender
        target = self.final.at[j, spot.x]

        @pl.when(spot.s == j)
        def _():
            for step in range(1, 4):
                pltpu.make_async_remote_copy(
                    self.total,
                    target,
                    sender.send_sems.at[self.g + step],
                    sender.recv_sems.at[self.g + j],
                    (spot.x, spot.f, (j + step) % 4),
                    MESH,
                ).start()
            pltpu.make_async_remote_copy(
                self.total,
                target,
                sender.send_sems.at[self.fx + j],
                sender.recv_sems.at[self.fx + j],
                spot.rep(),
                MESH,
            ).start()
            pltpu.make_async_copy(self.total, target, self.local.sems.at[self.kept]).start()

    def settle(self, j):
        self.gather(j)
        self.give_back(j)

    def pass_on(self, j):
        spot, sender = self.spot, self.sender
        target = self.final.at[j, spot.x]

        @pl.when(spot.s != j)
        def _():
            sender.arrived(self.g + j, target)
            pltpu.make_async_remote_copy(
                target,
                target,
                sender.send_sems.at[self.fx + j],
                sender.recv_sems.at[self.fx + j],
                spot.rep(),
                MESH,
            ).start()

    def finish_sums(self):
        for wanted, copy in self.z_open:
            pl.when(wanted)(lambda copy=copy: copy.wait_send())

    def finish_back(self):
        spot, sender = self.spot, self.sender
        for j in range(4):
            sender.arrived(self.fx + j, self.final.at[j, 1 - spot.x])
            sender.sent(self.fx + j, self.total)
        for step in range(1, 4):
            sender.sent(self.g + step, self.total)
        pltpu.make_async_copy(self.total, self.total, self.local.sems.at[self.kept]).wait()

    def finish(self):
        self.finish_sums()
        self.finish_back()


DOWN = (((0,), (0,)), ((), ()))


def outer(left_own, left_other, right_own, right_other):
    total = lax.dot_general(left_own, right_own, DOWN, preferred_element_type=F32)
    return total + lax.dot_general(left_other, right_other, DOWN, preferred_element_type=F32)


def lane_block(index, size):
    return pl.ds(pl.multiple_of(index * size, LANES), size)


def backward_send_kernel(
    q_ref,
    k_own,
    v_own,
    k_other,
    v_other,
    do_ref,
    lse_ref,
    bias_own,
    bias_other,
    grad_mlp,
    error_in,
    activated,
    hidden,
    upper_grad,
    block_out,
    qkv_out,
    error_out,
    up_total,
    down_final,
    upper_other,
    block_back,
    act_give,
    act_keep,
    act_give_other,
    act_keep_other,
    mlp_other,
    hid,
    rights,
    give,
    kept,
    far,
    side,
    depth,
    total,
    up_far,
    up_side,
    up_depth,
    errors,
    dk_one,
    dv_one,
    dk_two,
    dv_two,
    dk_in,
    dv_in,
    send_sems,
    recv_sems,
    local_sems,
):
    spot = Spot()
    sender, local = Sender(send_sems, recv_sems), Locals(local_sems)
    width = q_ref.shape[1]
    shard = activated.shape[1] // 4
    f, core = spot.f, spot.fsdp(1)
    loads = [
        local.start(activated.at[:, lane_block(spot.other(2), shard)], act_give),
        local.start(activated.at[:, lane_block(f, shard)], act_keep),
        local.start(hidden.at[spot.other(2)], hid.at[0]),
        local.start(hidden.at[f], hid.at[1]),
    ]
    right_base = local.used
    local.used += 4

    def right_copies(number):
        j, slot = ORDER[number], number % 2
        columns = pl.ds(j * width, width)
        return (
            pltpu.make_async_copy(
                upper_grad.at[:, columns], rights.at[0, slot], local.sems.at[right_base + slot]
            ),
            pltpu.make_async_copy(
                upper_other.at[:, columns], rights.at[1, slot], local.sems.at[right_base + 2 + slot]
            ),
        )

    greet(column_group(spot) + [spot.fsdp(2), spot.rep()])
    error_slots = [sender.slot() for _ in range(3)]
    error_z = sender.slots(4)
    sender.start(error_slots[0], error_in, errors.at[4], core)
    pieces = [sender.slot() for _ in range(6)]
    sender.start(
        pieces[0], activated.at[:, lane_block(spot.other(3), shard)], act_give_other, core
    )
    sender.start(pieces[1], grad_mlp, mlp_other, core)
    sender.start(
        pieces[2], activated.at[:, lane_block(spot.other(1), shard)], act_keep_other, core
    )
    sender.start(pieces[3], hidden.at[spot.other(3)], hid.at[2], core)
    sender.start(pieces[4], hidden.at[spot.other(1)], hid.at[3], core)
    sender.start(pieces[5], upper_grad, upper_other, core)
    back = TokenReturn(sender, spot, block_out, block_back)
    down = GradMove(sender, local, spot, far, side, depth, total, down_final)
    up = GradMove(sender, local, spot, up_far, up_side, up_depth, up_total, None)

    sender.arrived(error_slots[0], errors.at[4])
    errors[5] = error_in[...] + errors[4]
    sender.start(error_slots[1], errors.at[5], errors.at[6], spot.fsdp(2))
    for load in loads[:2]:
        load.wait()
    sender.arrived(pieces[0], act_give_other)
    sender.arrived(error_slots[1], errors.at[6])
    errors[7] = errors[5] + errors[6]
    sender.start(error_slots[2], errors.at[7], errors.at[8], spot.rep())
    sender.arrived(pieces[1], mlp_other)
    block = 384

    def fill(target, left, left_other):
        def body(i, carry):
            columns = lane_block(i, block)
            rows = pl.ds(pl.multiple_of(i * block, 16), block)
            target[rows, :] = outer(
                left[:, columns], left_other[:, columns], grad_mlp[...], mlp_other[...]
            ).astype(BF16)
            return carry

        lax.fori_loop(0, shard // block, body, 0)

    tall = shard // 4
    fill(give.at[0], act_give, act_give_other)
    for j in ORDER:
        down.send_far(j, give.at[0, pl.ds(j * tall, tall)])
    sender.arrived(error_slots[2], errors.at[8])
    errors[spot.s] = errors[7] + errors[8]
    error_open = []
    for step in range(1, 4):
        copy = pltpu.make_async_remote_copy(
            errors.at[spot.s],
            errors.at[spot.s],
            send_sems.at[error_z + step],
            recv_sems.at[error_z + spot.s],
            spot.seq(step),
            MESH,
        )
        copy.start()
        error_open.append(copy)
    back.start()
    sender.arrived(pieces[2], act_keep_other)
    fill(kept.at[0], act_keep, act_keep_other)

    for load in loads[2:]:
        load.wait()
    for slot, place in ((3, 2), (4, 3)):
        sender.arrived(pieces[slot], hid.at[place])
    sender.arrived(pieces[5], upper_other)
    for copy in right_copies(0):
        copy.start()
    for number, j in enumerate(ORDER):
        if number < 3:
            for copy in right_copies(number + 1):
                copy.start()
        for copy in right_copies(number):
            copy.wait()
        right, right_other = rights[0, number % 2], rights[1, number % 2]
        rows = pl.ds(j * tall, tall)
        give[1, rows, :] = outer(hid[0], hid[2], right, right_other).astype(BF16)
        up.send_far(j, give.at[1, rows])
        kept[1, rows, :] = outer(hid[1], hid[3], right, right_other).astype(BF16)

    data = (
        q_ref,
        k_own,
        v_own,
        k_other,
        v_other,
        do_ref,
        lse_ref,
        bias_own,
        bias_other,
        qkv_out.at[:, pl.ds(0, width)],
        dk_one,
        dv_one,
        dk_two,
        dv_two,
    )

    def fold(group, index, j):
        group.fold(j, kept[index, pl.ds(j * tall, tall), :])

    a, b, c, d = ORDER
    fold(down, 0, a)
    backward_heads(0, 4, *data)
    down.cross(a)
    fold(down, 0, b)
    backward_heads(4, 8, *data)
    down.cross(b)
    fold(down, 0, c)
    backward_heads(8, 12, *data)
    down.cross(c)
    down.settle(a)
    fold(down, 0, d)
    backward_heads(12, HEADS, *data)
    dk_slot, dv_slot = sender.slot(), sender.slot()
    sender.start(dk_slot, dk_two, dk_in, core)
    sender.start(dv_slot, dv_two, dv_in, core)
    down.cross(d)
    down.settle(b)
    fold(up, 1, a)
    sender.arrived(dk_slot, dk_in)
    qkv_out[:, width : 2 * width] = (dk_one[...] + dk_in[...].astype(F32)).astype(BF16)
    sender.arrived(dv_slot, dv_in)
    qkv_out[:, 2 * width :] = (dv_one[...] + dv_in[...].astype(F32)).astype(BF16)
    down.settle(c)
    up.cross(a)
    fold(up, 1, b)
    down.settle(d)
    up.cross(b)
    down.pass_on(a)
    fold(up, 1, c)
    down.pass_on(b)
    up.cross(c)
    down.pass_on(c)
    for place in range(4):

        @pl.when(spot.s != place)
        def _():
            sender.arrived(error_z + place, errors.at[place])

    error_out[...] = errors[0] + errors[1] + errors[2] + errors[3]
    for copy in error_open:
        copy.wait_send()
    fold(up, 1, d)
    down.pass_on(d)
    up.cross(d)
    up.gather(a)
    up.gather(b)
    up.gather(c)
    back.finish()
    down.finish()
    up.gather(d)
    up.finish_sums()
    sender.finish()


def attend_back_and_reduce(
    queries,
    keys,
    values,
    keys_other,
    values_other,
    grad,
    lse,
    bias_own,
    bias_other,
    grad_mlp,
    error,
    activated,
    hidden,
    upper_grad,
    block_out,
):
    tokens, width = queries.shape
    shape = (tokens, width)
    shard = activated.shape[1] // 4
    tall = shard // 4
    anywhere = pl.BlockSpec(memory_space=pl.ANY)
    near = pl.BlockSpec(memory_space=pltpu.VMEM)
    piece = (tall // 2, width)
    return pl.pallas_call(
        backward_send_kernel,
        out_shape=[
            jax.ShapeDtypeStruct((tokens, 3 * width), BF16),
            jax.ShapeDtypeStruct(error.shape, F32),
            jax.ShapeDtypeStruct(piece, BF16),
            jax.ShapeDtypeStruct((4, 2) + piece, BF16),
            jax.ShapeDtypeStruct(upper_grad.shape, BF16),
            jax.ShapeDtypeStruct(block_out.shape, BF16),
        ],
        in_specs=[near] * 11 + [anywhere] * 4,
        out_specs=[near] * 3 + [anywhere] * 3,
        scratch_shapes=[
            pltpu.VMEM((tokens, shard), BF16),
            pltpu.VMEM((tokens, shard), BF16),
            pltpu.VMEM((tokens, shard), BF16),
            pltpu.VMEM((tokens, shard), BF16),
            pltpu.VMEM(shape, BF16),
            pltpu.VMEM((4,) + hidden.shape[1:], BF16),
            pltpu.VMEM((2, 2) + shape, BF16),
            pltpu.VMEM((2, shard, width), BF16),
            pltpu.VMEM((2, shard, width), BF16),
            pltpu.VMEM((4, tall, width), BF16),
            pltpu.VMEM((4,) + piece, BF16),
            pltpu.VMEM((3,) + piece, BF16),
            pltpu.VMEM(piece, BF16),
            pltpu.VMEM((4, tall, width), BF16),
            pltpu.VMEM((4,) + piece, BF16),
            pltpu.VMEM((3,) + piece, BF16),
            pltpu.VMEM((9,) + error.shape, F32),
            pltpu.VMEM(shape, F32),
            pltpu.VMEM(shape, F32),
            pltpu.VMEM(shape, BF16),
            pltpu.VMEM(shape, BF16),
            pltpu.VMEM(shape, BF16),
            pltpu.VMEM(shape, BF16),
            sems(72),
            sems(72),
            sems(16),
        ],
        compiler_params=pltpu.CompilerParams(
            collective_id=3, has_side_effects=True, vmem_limit_bytes=67043328
        ),
        name="attend_back_and_reduce",
    )(
        queries,
        keys,
        values,
        keys_other,
        values_other,
        grad,
        lse,
        bias_own,
        bias_other,
        grad_mlp,
        error,
        activated,
        hidden,
        upper_grad,
        block_out,
    )


ROW_PARTS = 16


def finish_kernel(count, *refs):
    (branch_grad, qkv_grad, up_total), parts, refs = refs[:3], refs[3 : 3 + count], refs[3 + count :]
    (
        attended,
        hidden,
        mod_weight,
        tokens_grad,
        rows,
        cond_parts,
        up_final,
        tail_final,
        tokens_back,
        branch_other,
        qkv_other,
        att,
        hid,
        mod_held,
        give,
        far,
        side,
        depth,
        total,
        row,
        row_in,
        cond_send,
        send_sems,
        recv_sems,
        local_sems,
    ) = refs
    spot = Spot()
    sender, local = Sender(send_sems, recv_sems), Locals(local_sems)
    width = branch_grad.shape[1]
    f, core = spot.f, spot.fsdp(1)
    loads = [
        local.start(attended.at[spot.other(2)], att.at[0]),
        local.start(attended.at[f], att.at[1]),
        local.start(hidden.at[spot.other(2)], hid.at[0]),
        local.start(hidden.at[f], hid.at[1]),
    ]
    mod_load = local.start(mod_weight, mod_held)
    place = 0
    for part in parts:
        for column in range(part.shape[1] // width):
            row[place : place + 1, :] = part[:, column * width : (column + 1) * width]
            place += 1
    row[place:, :] = jnp.zeros((ROW_PARTS - place, width), F32)
    greet(column_group(spot) + [spot.fsdp(2), spot.fsdp(3), spot.rep()])
    row_slot = sender.slot()
    sender.start(row_slot, row, row_in, core)
    slots = [sender.slot() for _ in range(6)]
    sender.start(slots[0], attended.at[spot.other(3)], att.at[2], core)
    sender.start(slots[1], branch_grad, branch_other, core)
    sender.start(slots[2], hidden.at[spot.other(3)], hid.at[2], core)
    sender.start(slots[3], qkv_grad, qkv_other, core)
    sender.start(slots[4], attended.at[spot.other(1)], att.at[3], core)
    sender.start(slots[5], hidden.at[spot.other(1)], hid.at[3], core)
    up = GradMove(sender, local, spot, None, None, None, up_total, up_final)
    tail = GradMove(sender, local, spot, far, side, depth, total, tail_final)
    back = TokenReturn(sender, spot, tokens_grad, tokens_back)
    row_z, row_y, row_x = sender.slots(4), sender.slot(), sender.slot()
    cond_slots = {bit: sender.slot() for bit in (1, 2, 3)}

    sender.arrived(row_slot, row_in)
    column = (spot.x * 2 + spot.pair) * 4
    rows[column + spot.s] = row[...] + row_in[...]
    row_open = []
    for step in range(1, 4):
        copy = pltpu.make_async_remote_copy(
            rows.at[column + spot.s],
            rows.at[column + spot.s],
            send_sems.at[row_z + step],
            recv_sems.at[row_z + spot.s],
            spot.seq(step),
            MESH,
        )
        copy.start()
        row_open.append(copy)
    for j in ORDER:
        up.give_back(j)
    back.start()
    for load in loads:
        load.wait()

    def operands(j):
        if j == 0:
            return att, branch_grad[...], branch_other[...]
        columns = slice((j - 1) * width, j * width)
        return hid, qkv_grad[:, columns], qkv_other[:, columns]

    sender.arrived(slots[0], att.at[2])
    sender.arrived(slots[1], branch_other)
    a, b, c, d = ORDER
    for j in ORDER:
        if j == b:
            sender.arrived(slots[2], hid.at[2])
            sender.arrived(slots[3], qkv_other)
        left, right, right_other = operands(j)
        give[j] = outer(left[0], left[2], right, right_other).astype(BF16)
        tail.send_far(j, give.at[j])
    for place in range(4):

        @pl.when(spot.s != place)
        def _():
            sender.arrived(row_z + place, rows.at[column + place])

    span = pl.ds(column, 4)
    sender.start(row_y, rows.at[span], rows.at[span], spot.fsdp(2))
    sender.arrived(slots[4], att.at[3])
    sender.arrived(slots[5], hid.at[3])

    def fold(j):
        left, right, right_other = operands(j)
        tail.fold(j, outer(left[1], left[3], right, right_other))

    up.pass_on(a)
    fold(a)
    tail.cross(a)
    up.pass_on(b)
    fold(b)
    tail.cross(b)
    fold(c)
    up.pass_on(c)
    tail.cross(c)
    tail.settle(a)
    fold(d)
    tail.cross(d)
    up.pass_on(d)
    far_column = (spot.x * 2 + 1 - spot.pair) * 4
    sender.arrived(row_y, rows.at[pl.ds(far_column, 4)])
    half = pl.ds(spot.x * 8, 8)
    sender.start(row_x, rows.at[half], rows.at[half], spot.rep())
    tail.settle(b)
    tail.settle(c)

    mod_load.wait()
    products = jnp.zeros((16, mod_held.shape[0]), F32)
    for part in range(6):
        grad = rows[half, part, :]
        high = grad.astype(BF16)
        low = (grad - high.astype(F32)).astype(BF16)
        products += lax.dot_general(
            jnp.concatenate([high, low], axis=0),
            mod_held[:, part * width : (part + 1) * width],
            (((1,), (1,)), ((), ())),
            preferred_element_type=F32,
        )
    silu_grad = products[:8] + products[8:]
    for latent in range(8):
        cond_send[latent // 2, latent % 2 : latent % 2 + 1, :] = silu_grad[latent : latent + 1]
    cond_parts[f] = cond_send[f]
    for bit in (1, 2, 3):
        sender.start(
            cond_slots[bit], cond_send.at[spot.other(bit)], cond_parts.at[f], spot.fsdp(bit)
        )

    tail.pass_on(a)
    tail.settle(d)
    tail.pass_on(b)
    tail.pass_on(c)
    tail.pass_on(d)
    for bit in (1, 2, 3):
        sender.arrived(cond_slots[bit], cond_parts.at[spot.other(bit)])
    sender.arrived(row_x, rows.at[pl.ds((1 - spot.x) * 8, 8)])
    for copy in row_open:
        copy.wait_send()
    back.finish()
    up.finish_back()
    tail.finish()
    sender.finish()


def finish(branch_grad, qkv_grad, up_total, parts, attended, hidden, mod_weight, tokens_grad):
    tokens, width = branch_grad.shape
    piece = up_total.shape
    anywhere = pl.BlockSpec(memory_space=pl.ANY)
    near = pl.BlockSpec(memory_space=pltpu.VMEM)
    final = jax.ShapeDtypeStruct((4, 2) + piece, BF16)
    tall = 2 * piece[0]
    return pl.pallas_call(
        functools.partial(finish_kernel, len(parts)),
        out_shape=[
            jax.ShapeDtypeStruct((16, ROW_PARTS, width), F32),
            jax.ShapeDtypeStruct((4, 2, mod_weight.shape[0]), F32),
            final,
            final,
            jax.ShapeDtypeStruct(tokens_grad.shape, BF16),
        ],
        in_specs=[near] * (3 + len(parts)) + [anywhere] * 4,
        out_specs=[near] * 2 + [anywhere] * 3,
        scratch_shapes=[
            pltpu.VMEM(branch_grad.shape, BF16),
            pltpu.VMEM(qkv_grad.shape, BF16),
            pltpu.VMEM((4,) + attended.shape[1:], BF16),
            pltpu.VMEM((4,) + hidden.shape[1:], BF16),
            pltpu.VMEM(mod_weight.shape, BF16),
            pltpu.VMEM((4, tall, width), BF16),
            pltpu.VMEM((4, tall, width), BF16),
            pltpu.VMEM((4,) + piece, BF16),
            pltpu.VMEM((3,) + piece, BF16),
            pltpu.VMEM(piece, BF16),
            pltpu.VMEM((ROW_PARTS, width), F32),
            pltpu.VMEM((ROW_PARTS, width), F32),
            pltpu.VMEM((4, 2, mod_weight.shape[0]), F32),
            sems(72),
            sems(72),
            sems(20),
        ],
        compiler_params=pltpu.CompilerParams(
            collective_id=4, has_side_effects=True, vmem_limit_bytes=56 * 1024 * 1024
        ),
        name="finish",
    )(branch_grad, qkv_grad, up_total, *parts, attended, hidden, mod_weight, tokens_grad)


def spread_kernel(block, out):
    out[...] = block[0].astype(F32)


def spread(blocks):
    count, rows, width = blocks.shape
    return pl.pallas_call(
        spread_kernel,
        grid=(count,),
        out_shape=jax.ShapeDtypeStruct((rows, count * width), F32),
        in_specs=[pl.BlockSpec((1, rows, width), lambda j: (j, 0, 0))],
        out_specs=pl.BlockSpec((rows, width), lambda j: (0, j)),
        name="spread",
    )(blocks)


def head_window(head, head_dim, width):
    start = head * head_dim
    base = jnp.minimum(start // LANES, (width - WINDOW) // LANES) * LANES
    base = pl.multiple_of(base, LANES)
    return start, base


def forward_heads(
    low,
    high,
    q_ref,
    k_own,
    v_own,
    k_other,
    v_other,
    bias_own,
    bias_other,
    out_ref,
    lse_ref,
):
    tokens, width = q_ref.shape
    head_dim = width // HEADS
    blocks = 2
    tall = tokens // blocks
    scale = head_dim ** (-0.5) * LOG2E
    b_own, b_other = bias_own[...], bias_other[...]
    dims = (((1,), (1,)), ((), ()))

    def body(head, carry):
        start, base = head_window(head, head_dim, width)
        window = pl.ds(base, WINDOW)
        lane = lax.broadcasted_iota(jnp.int32, (1, WINDOW), 1) + base
        inside = (lane >= start) & (lane < start + head_dim)
        keep = inside.astype(BF16)
        spot = lax.broadcasted_iota(jnp.int32, (1, LANES), 1) == head
        key_one, key_two = k_own[:, window], k_other[:, window]
        val_one, val_two = v_own[:, window] * keep, v_other[:, window] * keep
        for block in range(blocks):
            rows = pl.ds(block * tall, tall)
            query = q_ref[rows, window] * keep
            one = lax.dot_general(query, key_one, dims, preferred_element_type=F32)
            two = lax.dot_general(query, key_two, dims, preferred_element_type=F32)
            one = one * scale + b_own
            two = two * scale + b_other
            top = jnp.maximum(
                jnp.max(one, axis=1, keepdims=True), jnp.max(two, axis=1, keepdims=True)
            )
            one = jnp.exp2(one - top)
            two = jnp.exp2(two - top)
            total = jnp.sum(one, axis=1, keepdims=True) + jnp.sum(two, axis=1, keepdims=True)
            mixed = jnp.dot(one.astype(BF16), val_one, preferred_element_type=F32)
            mixed += jnp.dot(two.astype(BF16), val_two, preferred_element_type=F32)
            mixed = mixed * (1.0 / total)
            out_ref[rows, window] = jnp.where(
                inside, mixed, out_ref[rows, window].astype(F32)
            ).astype(out_ref.dtype)
            lse_ref[rows, :] = jnp.where(spot, top + jnp.log2(total), lse_ref[rows, :])
        return carry

    lax.fori_loop(low, high, body, 0)


def forward_kernel(*refs):
    out_ref, lse_ref = refs[-2:]
    out_ref[...] = jnp.zeros_like(out_ref)
    lse_ref[...] = jnp.zeros_like(lse_ref)
    forward_heads(0, HEADS, *refs)


def forward_send_kernel(
    q_ref,
    k_own,
    v_own,
    bias_own,
    bias_other,
    count_in,
    up_weight,
    down_weight,
    teacher,
    out_grad,
    out_ref,
    lse_ref,
    k_other,
    v_other,
    count_out,
    up_full,
    down_full,
    teacher_own,
    out_grad_own,
    counts,
    count_sum,
    far_counts,
    up_stage,
    down_stage,
    send_sems,
    recv_sems,
    local_sems,
):
    spot = Spot()
    sender, local = Sender(send_sems, recv_sems), Locals(local_sems)
    greet(column_group(spot) + [spot.fsdp(2), spot.rep(), spot.rep(2)])
    count_slots = [sender.slot() for _ in range(3)]
    for step in range(1, 4):
        sender.start(count_slots[step - 1], count_in, counts.at[step - 1], spot.seq(step))
    key_slot, value_slot = sender.slot(), sender.slot()
    sender.start(key_slot, k_own, k_other, spot.fsdp(1))
    sender.start(value_slot, v_own, v_other, spot.fsdp(1))
    moves = [
        TokenMove(sender, spot, teacher, teacher_own),
        TokenMove(sender, spot, out_grad, out_grad_own),
    ]
    up = WeightMove(sender, local, spot, up_weight, up_full, up_stage, 3)
    down = WeightMove(sender, local, spot, down_weight, down_full, down_stage, 4)
    far_slots = [sender.slot() for _ in range(3)]

    total = count_in[...]
    for step in range(1, 4):
        sender.arrived(count_slots[step - 1], counts.at[step - 1])
        total = total + counts[step - 1]
    count_sum[...] = total
    for number, device in enumerate((spot.fsdp(2), spot.rep(), spot.rep(2))):
        sender.start(far_slots[number], count_sum, far_counts.at[number], device)
    up.start_far()
    down.start_far()
    for move in moves:
        move.start()
    sender.arrived(key_slot, k_other)
    sender.arrived(value_slot, v_other)
    up.start_near()
    down.start_near()
    out_ref[...] = jnp.zeros_like(out_ref)
    lse_ref[...] = jnp.zeros_like(lse_ref)
    data = (q_ref, k_own, v_own, k_other, v_other, bias_own, bias_other, out_ref, lse_ref)
    forward_heads(0, 8, *data)
    up.store()
    down.store()
    up.pass_far(0)
    forward_heads(8, HEADS, *data)
    up.pass_far(1)
    up.pass_side(0)
    up.pass_far(2)
    up.pass_side(1)
    down.pass_far(0)
    up.pass_side(2)
    for chunk in range(1, 4):
        down.pass_far(chunk)
        down.pass_side(chunk - 1)
    down.pass_side(3)
    total = count_sum[...]
    for number in range(3):
        sender.arrived(far_slots[number], far_counts.at[number])
        total = total + far_counts[number]
    count_out[...] = total
    for move in moves:
        move.finish()
    up.finish()
    down.finish()
    sender.finish()


def attend_and_gather(
    queries,
    keys,
    values,
    bias_own,
    bias_other,
    count,
    up_weight,
    down_weight,
    teacher,
    out_grad,
):
    tokens, width = queries.shape
    anywhere = pl.BlockSpec(memory_space=pl.ANY)
    near = pl.BlockSpec(memory_space=pltpu.VMEM)
    shape = (tokens, width)
    return pl.pallas_call(
        forward_send_kernel,
        out_shape=[
            jax.ShapeDtypeStruct(shape, BF16),
            jax.ShapeDtypeStruct((tokens, LANES), F32),
            jax.ShapeDtypeStruct(shape, BF16),
            jax.ShapeDtypeStruct(shape, BF16),
            jax.ShapeDtypeStruct(count.shape, F32),
            jax.ShapeDtypeStruct((4 * up_weight.shape[0], up_weight.shape[1]), BF16),
            jax.ShapeDtypeStruct((4 * down_weight.shape[0], down_weight.shape[1]), BF16),
            jax.ShapeDtypeStruct(teacher.shape, BF16),
            jax.ShapeDtypeStruct(out_grad.shape, BF16),
        ],
        in_specs=[near] * 6 + [anywhere] * 4,
        out_specs=[near] * 5 + [anywhere] * 4,
        scratch_shapes=[
            pltpu.VMEM((3,) + count.shape, F32),
            pltpu.VMEM(count.shape, F32),
            pltpu.VMEM((3,) + count.shape, F32),
            pltpu.VMEM(up_weight.shape, BF16),
            pltpu.VMEM(down_weight.shape, BF16),
            sems(48),
            sems(48),
            sems(8),
        ],
        compiler_params=pltpu.CompilerParams(
            collective_id=2, has_side_effects=True, vmem_limit_bytes=56 * 1024 * 1024
        ),
        name="attend_and_gather",
    )(
        queries,
        keys,
        values,
        bias_own,
        bias_other,
        count,
        up_weight,
        down_weight,
        teacher,
        out_grad,
    )


def attend(queries, k_own, v_own, k_other, v_other, bias_own, bias_other):
    tokens, width = queries.shape
    return pl.pallas_call(
        forward_kernel,
        out_shape=[
            jax.ShapeDtypeStruct((tokens, width), BF16),
            jax.ShapeDtypeStruct((tokens, LANES), F32),
        ],
        compiler_params=pltpu.CompilerParams(vmem_limit_bytes=48 * 1024 * 1024),
        cost_estimate=pl.CostEstimate(
            flops=16 * tokens * tokens * 2 * WINDOW * 4,
            transcendentals=HEADS * tokens * tokens * 2,
            bytes_accessed=6 * tokens * width * 2,
        ),
        name="attend",
    )(queries, k_own, v_own, k_other, v_other, bias_own, bias_other)


def backward_heads(
    low,
    high,
    q_ref,
    k_own,
    v_own,
    k_other,
    v_other,
    do_ref,
    lse_ref,
    bias_own,
    bias_other,
    dq_ref,
    dk_one,
    dv_one,
    dk_two,
    dv_two,
):
    tokens, width = q_ref.shape
    head_dim = width // HEADS
    factor = head_dim ** (-0.5)
    scale = factor * LOG2E
    across = (((1,), (1,)), ((), ()))
    sides = (
        (k_own, v_own, bias_own, dk_one, dv_one),
        (k_other, v_other, bias_other, dk_two, dv_two),
    )

    def body(head, carry):
        start, base = head_window(head, head_dim, width)
        window = pl.ds(base, WINDOW)
        lane = lax.broadcasted_iota(jnp.int32, (1, WINDOW), 1) + base
        inside = (lane >= start) & (lane < start + head_dim)
        keep = inside.astype(BF16)
        query = q_ref[:, window] * keep
        grad = do_ref[:, window] * keep
        lse = lse_ref[pl.ds(head, 1), :]

        def put(ref, value):
            ref[:, window] = jnp.where(inside, value, ref[:, window].astype(F32)).astype(ref.dtype)

        probs, prods = [], []
        delta = None
        for k_ref, v_ref, bias, _, _ in sides:
            scores = lax.dot_general(k_ref[:, window], query, across, preferred_element_type=F32)
            prob = jnp.exp2(scores * scale + bias[...] - lse)
            prob_grad = lax.dot_general(v_ref[:, window], grad, across, preferred_element_type=F32)
            prod = prob * prob_grad
            part = jnp.sum(prod, axis=0, keepdims=True)
            delta = part if delta is None else delta + part
            probs.append(prob)
            prods.append(prod)
        dq = None
        for (k_ref, _, _, dk, dv), prob, prod in zip(sides, probs, prods, strict=True):
            put(dv, jnp.dot(prob.astype(BF16), grad, preferred_element_type=F32))
            score_grad = (prod - prob * delta).astype(BF16)
            put(dk, jnp.dot(score_grad, query, preferred_element_type=F32) * factor)
            part = lax.dot_general(
                score_grad, k_ref[:, window], DOWN, preferred_element_type=F32
            )
            dq = part if dq is None else dq + part
        put(dq_ref, dq * factor)
        return carry

    lax.fori_loop(low, high, body, 0)


def backward_kernel(*refs):
    for ref in refs[-5:]:
        ref[...] = jnp.zeros_like(ref)
    backward_heads(0, HEADS, *refs)


def attend_back(queries, k_own, v_own, k_other, v_other, grad, lse, bias_own, bias_other):
    tokens, width = queries.shape
    shape = (tokens, width)
    return pl.pallas_call(
        backward_kernel,
        out_shape=[
            jax.ShapeDtypeStruct(shape, BF16),
            jax.ShapeDtypeStruct(shape, F32),
            jax.ShapeDtypeStruct(shape, F32),
            jax.ShapeDtypeStruct(shape, BF16),
            jax.ShapeDtypeStruct(shape, BF16),
        ],
        compiler_params=pltpu.CompilerParams(vmem_limit_bytes=60 * 1024 * 1024),
        name="attend_back",
    )(queries, k_own, v_own, k_other, v_other, grad, lse, bias_own, bias_other)


def dot(left, right):
    return jnp.dot(left, right, preferred_element_type=F32)


def dot_t(left, right):
    return lax.dot_general(left, right, (((1,), (1,)), ((), ())), preferred_element_type=F32)


def norm_parts(inputs):
    centred = inputs - jnp.mean(inputs, axis=-1, keepdims=True)
    rate = lax.rsqrt(jnp.mean(centred * centred, axis=-1, keepdims=True) + EPS)
    return centred * rate, rate


def norm_back(grad, normed, rate):
    return rate * (
        grad
        - jnp.mean(grad, axis=-1, keepdims=True)
        - normed * jnp.mean(grad * normed, axis=-1, keepdims=True)
    )


def gelu_parts(inputs):
    inner = jnp.tanh(GELU_C * (inputs + 0.044715 * inputs * inputs * inputs))
    value = 0.5 * inputs * (1.0 + inner)
    slope = 0.5 * (1.0 + inner) + 0.5 * inputs * (1.0 - inner * inner) * GELU_C * (
        1.0 + 3.0 * 0.044715 * inputs * inputs
    )
    return value, slope


def column_sum(array):
    return jnp.sum(array.astype(F32), axis=0)


def shards(
    tokens,
    condition,
    valid_mask,
    teacher,
    out_grad,
    mod_weight,
    mod_bias,
    qkv_weight,
    qkv_bias,
    out_weight,
    out_bias,
    up_weight,
    up_bias,
    down_weight,
    down_bias,
):
    reps, fsdp, seq = lax.axis_size("rep"), lax.axis_size("fsdp"), lax.axis_size("seq")
    fast = (reps, fsdp, seq) == (2, 4, 4)
    latents, span, width = tokens.shape
    assert 2 * latents == seq and latents == 2
    place_f, place_s = lax.axis_index("fsdp"), lax.axis_index("seq")
    total_tokens = latents * span * reps * fsdp * seq

    biases = jnp.concatenate([mod_bias, qkv_bias, out_bias, up_bias, down_bias])
    shard_rows = mod_weight.shape[0]
    cond_row = pick(condition, place_s % 2)
    keep_mask = valid_mask.astype(F32)

    if fast:
        inputs_low, valid_all, mod_parts, bias_all, qkv_full, out_full = enter(
            tokens,
            keep_mask.reshape(latents, 1, span),
            condition.astype(F32).reshape(latents, fsdp, 1, shard_rows),
            biases.astype(F32)[None],
            mod_weight,
            qkv_weight,
            out_weight,
        )
        inputs_low = inputs_low.reshape(-1, width)
        valid_all = valid_all.reshape(2, -1)
        keyvalid, valid_other = pick(valid_all, place_f % 2), pick(valid_all, 1 - place_f % 2)
        mod_row = jnp.sum(mod_parts, axis=(0, 1))
        bias_all = bias_all[:, 0]
    else:
        inputs_low = to_latent(tokens)
        keyvalid = to_latent(keep_mask)
        valid_other = flip(keyvalid, "fsdp", 1)
        counted = lax.psum(jnp.sum(keep_mask), ("rep", "fsdp", "seq")).reshape(1, 1)
        own_row = jnp.where(place_f % 2 == place_s // 2, cond_row, flip(cond_row, "fsdp", 1))
        cond_pair = lax.all_gather(own_row, "fsdp", axis=0)[::2]
        silu_pair = jax.nn.silu(cond_pair.astype(F32)).astype(BF16)
        silu_cols = lax.dynamic_slice_in_dim(silu_pair, place_f * shard_rows, shard_rows, 1)
        mod_row = pick(lax.psum(dot(silu_cols, mod_weight), "fsdp"), place_f // 2)
        bias_all = lax.all_gather(biases, "fsdp", axis=0).astype(F32)
        qkv_full, out_full = gather_weight(qkv_weight), gather_weight(out_weight)
        up_full, down_full = gather_weight(up_weight), gather_weight(down_weight)
        teacher_own, out_grad_own = to_latent(teacher), to_latent(out_grad)
    mask_own = (keyvalid - 1.0) * (-NEG)
    mask_other = (valid_other - 1.0) * (-NEG)

    cuts = [0]
    for bias in (mod_bias, qkv_bias, out_bias, up_bias, down_bias):
        cuts.append(cuts[-1] + bias.shape[0])
    mod_b, qkv_b, out_b, up_b, down_b = (
        bias_all[:, low:high].reshape(-1) for low, high in zip(cuts[:-1], cuts[1:], strict=True)
    )
    pieces = (mod_row + mod_b).reshape(6, 1, width)
    shift_one, scale_one, gate_one, shift_two, scale_two, gate_two = (pieces[i] for i in range(6))

    inputs = inputs_low.astype(F32)
    normed_one, rate_one = norm_parts(inputs)
    hidden_one = (normed_one * (1.0 + scale_one) + shift_one).astype(BF16)
    projected = dot(hidden_one, qkv_full)
    queries = (projected[:, :width] + qkv_b[:width]).astype(BF16)
    keys_own = projected[:, width : 2 * width].astype(BF16)
    values_own = (projected[:, 2 * width :] + qkv_b[width:]).astype(BF16)
    if fast:
        (
            attended,
            lse,
            keys_other,
            values_other,
            counted,
            up_full,
            down_full,
            teacher_own,
            out_grad_own,
        ) = attend_and_gather(
            queries,
            keys_own,
            values_own,
            mask_own[None],
            mask_other[None],
            jnp.full((1, LANES), jnp.sum(valid_all)),
            up_weight,
            down_weight,
            teacher,
            out_grad,
        )
        counted = counted[:, :1]
        teacher_own = teacher_own.reshape(-1, width)
        out_grad_own = out_grad_own.reshape(-1, width)
    else:
        keys_other, values_other = flip(keys_own, "fsdp", 1), flip(values_own, "fsdp", 1)
        attended, lse = attend(
            queries,
            keys_own,
            values_own,
            keys_other,
            values_other,
            mask_own[None],
            mask_other[None],
        )
    branch = dot(attended, out_full) + out_b
    middle = inputs + gate_one * branch
    normed_two, rate_two = norm_parts(middle)
    hidden_two = (normed_two * (1.0 + scale_two) + shift_two).astype(BF16)
    up_pre = dot(hidden_two, up_full) + up_b
    activated, slope = gelu_parts(up_pre)
    activated = activated.astype(BF16)
    mlp_out = dot(activated, down_full) + down_b
    output = middle + gate_two * mlp_out
    block_out = output.astype(BF16)
    differ = (output - teacher_own.astype(F32)) * keyvalid[:, None]
    error = jnp.sum(differ * differ)

    grad_out = out_grad_own.astype(F32) + total_tokens / counted * differ
    grad_mlp = (grad_out * gate_two).astype(BF16)
    gate_two_grad = jnp.sum(grad_out * mlp_out, axis=0)

    def slices(array):
        return array.reshape(array.shape[0], fsdp, -1).transpose(1, 0, 2)

    def weight_grad(left, right):
        whole = lax.dot_general(left, right, DOWN, preferred_element_type=F32)
        mine = lax.psum_scatter(whole.astype(BF16), "fsdp", scatter_dimension=0, tiled=True)
        return lax.psum(mine, ("rep", "seq")).astype(F32)

    down_bgrad = column_sum(grad_mlp)
    upper_grad = (dot_t(grad_mlp, down_full) * slope).astype(BF16)
    up_bgrad = column_sum(upper_grad)
    hidden_two_grad = dot_t(upper_grad, up_full)
    scaled_two = hidden_two_grad * (1.0 + scale_two)
    middle_grad = grad_out + norm_back(scaled_two, normed_two, rate_two)
    shift_two_grad = jnp.sum(hidden_two_grad, axis=0)
    scale_two_grad = jnp.sum(hidden_two_grad * normed_two, axis=0)
    branch_grad = (middle_grad * gate_one).astype(BF16)
    gate_one_grad = jnp.sum(middle_grad * branch, axis=0)
    out_bgrad = column_sum(branch_grad)
    attended_grad = dot_t(branch_grad, out_full).astype(BF16)

    if fast:
        qkv_grad, error_sum, up_total, down_final, _, block_out = attend_back_and_reduce(
            queries,
            keys_own,
            values_own,
            keys_other,
            values_other,
            attended_grad,
            lse.T,
            mask_own[:, None],
            mask_other[:, None],
            grad_mlp,
            jnp.full((1, LANES), error),
            activated,
            slices(hidden_two),
            upper_grad,
            block_out.reshape(2, span, width),
        )
        err_total = error_sum[:, :1]
    else:
        query_grad, key_part, value_part, key_away, value_away = attend_back(
            queries,
            keys_own,
            values_own,
            keys_other,
            values_other,
            attended_grad,
            lse.T,
            mask_own[:, None],
            mask_other[:, None],
        )
        key_grad = (key_part + flip(key_away, "fsdp", 1).astype(F32)).astype(BF16)
        value_grad = (value_part + flip(value_away, "fsdp", 1).astype(F32)).astype(BF16)
        err_total = lax.psum(error, ("rep", "fsdp", "seq")).reshape(1, 1)
        block_out = from_latent(block_out)
        qkv_grad = jnp.concatenate([query_grad, key_grad, value_grad], axis=-1)
    hidden_one_grad = dot_t(qkv_grad, qkv_full)
    scaled_one = hidden_one_grad * (1.0 + scale_one)
    tokens_grad = middle_grad + norm_back(scaled_one, normed_one, rate_one)
    tokens_grad = tokens_grad.astype(BF16)
    qkv_bgrad = column_sum(qkv_grad)
    parts = [
        jnp.sum(hidden_one_grad, axis=0),
        jnp.sum(hidden_one_grad * normed_one, axis=0),
        gate_one_grad,
        shift_two_grad,
        scale_two_grad,
        gate_two_grad,
        out_bgrad,
        up_bgrad,
        down_bgrad,
        qkv_bgrad[:width],
        qkv_bgrad[2 * width :],
        jnp.where(place_f % 2 == place_s // 2, cond_row.astype(F32), 0.0),
    ]
    length = sum(part.shape[0] for part in parts)
    if fast:
        rows, cond_parts, up_final, tail_final, tokens_grad = finish(
            branch_grad,
            qkv_grad,
            up_total,
            [part[None] for part in parts],
            slices(attended),
            slices(hidden_one),
            mod_weight,
            tokens_grad.reshape(2, span, width),
        )
        rows = rows.reshape(-1, ROW_PARTS * width)[:, :length]
        down_g = down_final.reshape(down_weight.shape).astype(F32)
        up_g = spread(up_final.reshape(4, -1, width))
        tail_final = tail_final.reshape(4, -1, width)
        out_g = tail_final[0].astype(F32)
        qkv_g = spread(tail_final[1:])
    else:
        row = jnp.concatenate(parts)
        row = row + flip(row, "fsdp", 1)
        rows = gather_rows(row)
        tokens_grad = from_latent(tokens_grad)
        down_g = weight_grad(activated, grad_mlp)
        up_g = weight_grad(hidden_two, upper_grad)
        out_g = weight_grad(attended, branch_grad)
        qkv_g = weight_grad(hidden_one, qkv_grad)

    mod_grad = rows[:, : 6 * width]
    silu_all = jax.nn.silu(rows[:, -width:]).astype(BF16)
    silu_own = lax.dynamic_slice_in_dim(silu_all, place_f * shard_rows, shard_rows, 1)
    mod_wgrad = lax.dot_general(
        silu_own.astype(F32),
        mod_grad,
        (((0,), (0,)), ((), ())),
        precision=HIGHEST,
        preferred_element_type=F32,
    )
    bias_sum = jnp.sum(rows[:, 6 * width : -width], axis=0)

    def own_bias(low, size):
        own = size // fsdp
        return lax.dynamic_slice_in_dim(bias_sum, low + place_f * own, own, 0)

    up_size = up_b.shape[0]
    out_bg = own_bias(0, width)
    up_bg = own_bias(width, up_size)
    down_bg = own_bias(width + up_size, width)
    qkv_bg = own_bias(2 * width + up_size, 2 * width)
    mod_own = mod_bias.shape[0]
    mod_bg = lax.dynamic_slice_in_dim(jnp.sum(mod_grad, axis=0), place_f * mod_own, mod_own, 0)

    if fast:
        found = cond_parts
    else:
        replica = lax.axis_index("rep")
        per_rep = mod_grad.shape[0] // reps
        own_rep = lax.dynamic_slice_in_dim(mod_grad, replica * per_rep, per_rep, 0)
        silu_grad = lax.dot_general(
            own_rep,
            mod_weight.astype(F32),
            (((1,), (1,)), ((), ())),
            precision=HIGHEST,
            preferred_element_type=F32,
        )
        owners = silu_grad.reshape(fsdp, latents, shard_rows)
        found = lax.all_to_all(owners, "fsdp", 0, 0, tiled=True)
    silu_grad = found.transpose(1, 0, 2).reshape(latents, width)
    conds = condition.astype(F32)
    sigmoid = 1.0 / (1.0 + jnp.exp(-conds))
    condition_grad = silu_grad * (sigmoid * (1.0 + conds * (1.0 - sigmoid)))

    loss_value = (err_total / (width * counted))[0, 0]
    return (
        block_out,
        loss_value,
        tokens_grad,
        condition_grad,
        mod_wgrad,
        mod_bg,
        qkv_g,
        qkv_bg,
        out_g,
        out_bg,
        up_g,
        up_bg,
        down_g,
        down_bg,
    )


def solution(mesh):
    batch = P(("rep", "fsdp"), "seq", None)
    matrix, vector = P("fsdp", None), P("fsdp")
    params = (matrix, vector) * 5
    return jax.shard_map(
        shards,
        mesh=mesh,
        in_specs=(batch, P(("rep", "fsdp"), None), P(("rep", "fsdp"), "seq"), batch, batch)
        + params,
        out_specs=(batch, P(), batch, P(("rep", "fsdp"), None)) + params,
        check_vma=False,
    )
```

```python
import functools

import jax
import jax.numpy as jnp
from jax import lax
from jax.experimental import pallas as pl
from jax.experimental.pallas import tpu as pltpu
from jax.sharding import PartitionSpec as P

HEADS = 16

EPS = 1e-06
GELU_C = 0.7978845608028654
HIGHEST = lax.Precision.HIGHEST
LOG2E = 1.4426950408889634
NEG = -1e30
BF16 = jnp.bfloat16
F32 = jnp.float32
WINDOW = 256
LANES = 128


def flip(array, axis, bit):
    size = lax.axis_size(axis)
    return lax.ppermute(array, axis, [(i, i ^ bit) for i in range(size)])


def pick(array, index):
    return lax.dynamic_index_in_dim(array, index, 0, keepdims=False)


def in_order(first, second, swapped):
    return jnp.where(swapped, jnp.stack([second, first]), jnp.stack([first, second]))


def to_latent(array):
    seq, fsdp = lax.axis_size("seq"), lax.axis_size("fsdp")
    place = lax.axis_index("seq")
    arrived = []
    for turn in range(2):
        pairs = []
        for f in range(fsdp):
            for s in range(seq):
                pair, core = f // 2, f % 2
                target = (pair * 2 + s // 2, 2 * core + (s + turn) % 2)
                pairs.append((f * seq + s, target[0] * seq + target[1]))
        block = pick(array, (place + turn) % 2)
        arrived.append(lax.ppermute(block, ("fsdp", "seq"), pairs))
    both = in_order(arrived[0], arrived[1], place % 2 == 1)
    return both.reshape((-1,) + both.shape[2:])


def from_latent(array):
    seq, fsdp = lax.axis_size("seq"), lax.axis_size("fsdp")
    place = lax.axis_index("seq")
    halves = array.reshape((2, array.shape[0] // 2) + array.shape[1:])
    arrived = []
    for turn in range(2):
        pairs = []
        for f in range(fsdp):
            for s in range(seq):
                pair, core = f // 2, f % 2
                slot = (s + turn) % 2
                target = (pair * 2 + s // 2, 2 * core + slot)
                pairs.append((f * seq + s, target[0] * seq + target[1]))
        arrived.append(lax.ppermute(pick(halves, (place + turn) % 2), ("fsdp", "seq"), pairs))
    return in_order(arrived[0], arrived[1], place % 2 == 1)


def gather_rows(row):
    fsdp = lax.axis_size("fsdp")
    everything = lax.all_gather(row, ("rep", "fsdp", "seq"), axis=0)
    everything = everything.reshape((-1, fsdp // 2, 2, lax.axis_size("seq")) + row.shape)
    return everything[:, :, 0].reshape((-1,) + row.shape)


def gather_weight(weight):
    return lax.all_gather(weight, "fsdp", axis=0, tiled=True)


MESH = pl.DeviceIdType.MESH


class Spot:
    def __init__(self):
        self.x, self.f, self.s = (lax.axis_index(name) for name in ("rep", "fsdp", "seq"))
        self.core = self.f % 2
        self.pair = self.f // 2

    def other(self, bit):
        if bit == 3:
            return 3 - self.f
        return self.f + bit - 2 * bit * ((self.f // bit) % 2)

    def fsdp(self, bit):
        return (self.x, self.other(bit), self.s)

    def rep(self, bit=0):
        return (1 - self.x, self.other(bit) if bit else self.f, self.s)

    def seq(self, step):
        return (self.x, self.f, lax.rem(self.s + step, 4))

    def token_target(self, turn):
        block = lax.rem(self.s + turn, 2)
        return (self.x, 2 * self.pair + self.s // 2, 2 * self.core + block), block


def greet(devices):
    barrier = pltpu.get_barrier_semaphore()
    for device in devices:
        pl.semaphore_signal(barrier, inc=1, device_id=device, device_id_type=MESH)
    pl.semaphore_wait(barrier, len(devices))


def column_group(spot):
    found = [(spot.x, spot.other(1), spot.s)]
    for step in range(1, 4):
        found.append(spot.seq(step))
        found.append((spot.x, spot.other(1), lax.rem(spot.s + step, 4)))
    return found


class Sender:
    def __init__(self, send_sems, recv_sems):
        self.send_sems, self.recv_sems = send_sems, recv_sems
        self.used = 0
        self.open = []

    def slot(self):
        self.used += 1
        return self.used - 1

    def start(self, slot, source, target, device):
        copy = pltpu.make_async_remote_copy(
            source, target, self.send_sems.at[slot], self.recv_sems.at[slot], device, MESH
        )
        copy.start()
        self.open.append(copy)

    def start_if(self, wanted, send_slot, recv_slot, source, target, device):
        copy = pltpu.make_async_remote_copy(
            source, target, self.send_sems.at[send_slot], self.recv_sems.at[recv_slot], device, MESH
        )
        pl.when(wanted)(lambda: copy.start())
        return wanted, copy

    def slots(self, count):
        self.used += count
        return self.used - count

    def sent(self, slot, view):
        pltpu.make_async_copy(view, view, self.send_sems.at[slot]).wait()

    def arrived(self, slot, view):
        pltpu.make_async_copy(view, view, self.recv_sems.at[slot]).wait()

    def finish(self):
        for copy in self.open:
            copy.wait_send()
        self.open = []


class Locals:
    def __init__(self, sems):
        self.sems = sems
        self.used = 0
        self.open = []

    def start(self, source, target):
        copy = pltpu.make_async_copy(source, target, self.sems.at[self.used])
        self.used += 1
        copy.start()
        return copy


class TokenMove:
    def __init__(self, sender, spot, source, target):
        self.sender, self.spot, self.source, self.target = sender, spot, source, target
        self.slots = [sender.slot(), sender.slot()]

    def start(self):
        spot = self.spot
        self.remote = []
        for turn, slot in enumerate(self.slots):
            device, block = spot.token_target(turn)
            stays = (device[1] == spot.f) & (device[2] == spot.s)
            source = self.source.at[block]
            target = self.target.at[lax.rem(spot.s, 2)]
            remote = pltpu.make_async_remote_copy(
                source,
                target,
                self.sender.send_sems.at[slot],
                self.sender.recv_sems.at[slot],
                device,
                MESH,
            )
            local = pltpu.make_async_copy(source, target, self.sender.recv_sems.at[slot])
            pl.when(jnp.logical_not(stays))(lambda remote=remote: remote.start())
            pl.when(stays)(lambda local=local: local.start())
            self.remote.append((stays, remote))

    def finish(self):
        for turn, slot in enumerate(self.slots):
            self.sender.arrived(slot, self.target.at[lax.rem(self.spot.s + turn, 2)])
        for stays, remote in self.remote:
            pl.when(jnp.logical_not(stays))(lambda remote=remote: remote.wait_send())


class WeightMove:
    def __init__(self, sender, local, spot, own, full, stage, chunks):
        self.sender, self.local, self.spot = sender, local, spot
        self.own, self.full, self.stage = own, full, stage
        self.rows, self.chunks = own.shape[0], chunks
        self.half = self.rows // 2
        self.tall = self.half // chunks
        self.slots = {
            kind: [sender.slot() for _ in range(1 if kind == "core" else chunks)]
            for kind in ("core", "far", "side", "far_core", "side_core")
        }

    def view(self, bits, side, chunk):
        shard = self.spot.other(bits) if bits else self.spot.f
        half = self.spot.x if side == 0 else 1 - self.spot.x
        start = shard * self.rows + half * self.half + chunk * self.tall
        return self.full.at[pl.ds(pl.multiple_of(start, 16), self.tall)]

    def shard_view(self, bits):
        shard = self.spot.other(bits) if bits else self.spot.f
        return self.full.at[pl.ds(pl.multiple_of(shard * self.rows, 16), self.rows)]

    def start_far(self):
        spot = self.spot
        for chunk, slot in enumerate(self.slots["far"]):
            start = pl.multiple_of(spot.x * self.half + chunk * self.tall, 16)
            self.sender.start(
                slot, self.own.at[pl.ds(start, self.tall)], self.view(0, 0, chunk), spot.fsdp(2)
            )

    def start_near(self):
        self.sender.start(self.slots["core"][0], self.own, self.shard_view(0), self.spot.fsdp(1))
        self.load = self.local.start(self.own, self.stage)

    def store(self):
        self.load.wait()
        self.kept = self.local.start(self.stage, self.shard_view(0))

    def pass_far(self, chunk):
        view = self.view(2, 0, chunk)
        self.sender.arrived(self.slots["far"][chunk], view)
        self.sender.start(self.slots["side"][chunk], view, view, self.spot.rep())
        self.sender.start(self.slots["far_core"][chunk], view, view, self.spot.fsdp(1))

    def pass_side(self, chunk):
        view = self.view(2, 1, chunk)
        self.sender.arrived(self.slots["side"][chunk], view)
        self.sender.start(self.slots["side_core"][chunk], view, view, self.spot.fsdp(1))

    def finish(self):
        self.kept.wait()
        self.sender.arrived(self.slots["core"][0], self.shard_view(1))
        for chunk in range(self.chunks):
            self.sender.arrived(self.slots["far_core"][chunk], self.view(3, 0, chunk))
            self.sender.arrived(self.slots["side_core"][chunk], self.view(3, 1, chunk))


def entry_kernel(
    tokens,
    valid,
    cond,
    biases,
    mod_weight,
    qkv_weight,
    out_weight,
    tokens_own,
    valid_all,
    mod_parts,
    bias_all,
    qkv_full,
    out_full,
    mod_held,
    cond_held,
    partial,
    qkv_stage,
    out_stage,
    send_sems,
    recv_sems,
    local_sems,
):
    spot = Spot()
    sender, local = Sender(send_sems, recv_sems), Locals(local_sems)
    mod_load = local.start(mod_weight, mod_held)
    greet(column_group(spot) + [spot.fsdp(2), spot.fsdp(3), spot.rep()])

    row = lax.rem(spot.s, 2)
    cond_slots, bias_slots = {}, {}
    for bit in (1, 2, 3):
        cond_slots[bit], bias_slots[bit] = sender.slot(), sender.slot()
        target = spot.other(bit)
        sender.start(
            cond_slots[bit], cond.at[row, target], cond_held.at[spot.f], spot.fsdp(bit)
        )
    for bit in (1, 2, 3):
        sender.start(bias_slots[bit], biases, bias_all.at[spot.f], spot.fsdp(bit))
    cond_own = local.start(cond.at[row, spot.f], cond_held.at[spot.f])
    bias_own = local.start(biases, bias_all.at[spot.f])

    qkv = WeightMove(sender, local, spot, qkv_weight, qkv_full, qkv_stage, 3)
    out = WeightMove(sender, local, spot, out_weight, out_full, out_stage, 1)
    mod_slots = {bit: sender.slot() for bit in (1, 2, 3)}
    move = TokenMove(sender, spot, tokens, tokens_own)
    valid_base = [sender.slot() for _ in range(4)][0]
    valid_open = []
    for turn in range(2):
        device, block = spot.token_target(turn)
        for core in range(2):
            goal = (device[0], 2 * spot.pair + core, device[2])
            stays = (goal[1] == spot.f) & (goal[2] == spot.s)
            source, target = valid.at[block], valid_all.at[spot.s]
            arrival = recv_sems.at[valid_base + spot.s]
            remote = pltpu.make_async_remote_copy(
                source, target, send_sems.at[valid_base + 2 * turn + core], arrival, goal, MESH
            )
            near = pltpu.make_async_copy(source, target, arrival)
            pl.when(jnp.logical_not(stays))(lambda remote=remote: remote.start())
            pl.when(stays)(lambda near=near: near.start())
            valid_open.append((stays, remote))
    move.start()
    qkv.start_far()
    qkv.start_near()
    out.start_near()

    cond_own.wait()
    for bit in (1, 2, 3):
        sender.arrived(cond_slots[bit], cond_held.at[spot.other(bit)])
    first, second = cond_held[spot.s // 2], cond_held[2 + spot.s // 2]
    which = lax.broadcasted_iota(jnp.int32, (16, first.shape[-1]), 0)
    conds = jnp.where(which == 0, first, second)
    silu = (conds / (1.0 + jnp.exp(-conds))).astype(BF16)
    mod_load.wait()
    width = mod_held.shape[1] // 6
    for piece in range(6):
        columns = slice(piece * width, (piece + 1) * width)
        product = jnp.dot(silu, mod_held[:, columns], preferred_element_type=F32)
        partial[0, :, columns] = product[0:1]
        partial[1, :, columns] = product[1:2]
    for bit in (1, 2, 3):
        pair = spot.pair if bit == 1 else 1 - spot.pair
        sender.start(
            mod_slots[bit], partial.at[pair], mod_parts.at[spot.f], spot.fsdp(bit)
        )
    mod_own = local.start(partial.at[spot.pair], mod_parts.at[spot.f])
    out.start_far()
    qkv.store()
    out.store()
    for chunk in range(3):
        qkv.pass_far(chunk)
        if chunk:
            qkv.pass_side(chunk - 1)
    qkv.pass_side(2)
    out.pass_far(0)
    out.pass_side(0)

    bias_own.wait()
    mod_own.wait()
    for bit in (1, 2, 3):
        sender.arrived(bias_slots[bit], bias_all.at[spot.other(bit)])
        sender.arrived(mod_slots[bit], mod_parts.at[spot.other(bit)])
    for place in range(4):
        sender.arrived(valid_base + place, valid_all.at[place])
    for stays, remote in valid_open:
        pl.when(jnp.logical_not(stays))(lambda remote=remote: remote.wait_send())
    move.finish()
    qkv.finish()
    out.finish()
    sender.finish()


def sems(count):
    return pltpu.SemaphoreType.DMA((count,))


def enter(tokens, valid, cond, biases, mod_weight, qkv_weight, out_weight):
    anywhere = pl.BlockSpec(memory_space=pl.ANY)
    return pl.pallas_call(
        entry_kernel,
        out_shape=[
            jax.ShapeDtypeStruct(tokens.shape, tokens.dtype),
            jax.ShapeDtypeStruct((4,) + valid.shape[1:], F32),
            jax.ShapeDtypeStruct((4, 1, mod_weight.shape[1]), F32),
            jax.ShapeDtypeStruct((4,) + biases.shape, F32),
            jax.ShapeDtypeStruct((4 * qkv_weight.shape[0], qkv_weight.shape[1]), BF16),
            jax.ShapeDtypeStruct((4 * out_weight.shape[0], out_weight.shape[1]), BF16),
        ],
        in_specs=[anywhere] * 7,
        out_specs=[anywhere] * 6,
        scratch_shapes=[
            pltpu.VMEM(mod_weight.shape, BF16),
            pltpu.VMEM((4,) + cond.shape[2:], F32),
            pltpu.VMEM((2, 1, mod_weight.shape[1]), F32),
            pltpu.VMEM(qkv_weight.shape, BF16),
            pltpu.VMEM(out_weight.shape, BF16),
            sems(40),
            sems(40),
            sems(12),
        ],
        compiler_params=pltpu.CompilerParams(
            collective_id=1, has_side_effects=True, vmem_limit_bytes=67043328
        ),
        name="enter",
    )(tokens, valid, cond, biases, mod_weight, qkv_weight, out_weight)


class TokenReturn:
    def __init__(self, sender, spot, source, target):
        self.sender, self.spot, self.source, self.target = sender, spot, source, target
        self.slots = [sender.slot(), sender.slot()]

    def start(self):
        spot = self.spot
        self.remote = []
        for turn, slot in enumerate(self.slots):
            half = lax.rem(spot.s + turn, 2)
            device = (spot.x, 2 * spot.pair + spot.s // 2, 2 * spot.core + half)
            stays = (device[1] == spot.f) & (device[2] == spot.s)
            source, target = self.source.at[half], self.target.at[lax.rem(spot.s, 2)]
            arrival = self.sender.recv_sems.at[slot]
            remote = pltpu.make_async_remote_copy(
                source, target, self.sender.send_sems.at[slot], arrival, device, MESH
            )
            local = pltpu.make_async_copy(source, target, arrival)
            pl.when(jnp.logical_not(stays))(lambda remote=remote: remote.start())
            pl.when(stays)(lambda local=local: local.start())
            self.remote.append((stays, remote))

    def finish(self):
        for turn, slot in enumerate(self.slots):
            self.sender.arrived(slot, self.target.at[lax.rem(self.spot.s + turn, 2)])
        for stays, remote in self.remote:
            pl.when(jnp.logical_not(stays))(lambda remote=remote: remote.wait_send())


ORDER = (0, 3, 1, 2)
STRIP = 64


def row_norm(inputs):
    centred = inputs - jnp.mean(inputs, axis=-1, keepdims=True)
    rate = lax.rsqrt(jnp.mean(centred * centred, axis=-1, keepdims=True) + EPS)
    return centred * rate, rate


class ColumnStream:
    def __init__(self, local, source, held, width):
        self.local, self.source, self.held, self.width = local, source, held, width
        self.base = local.used
        local.used += 2

    def copy(self, j):
        return pltpu.make_async_copy(
            self.source.at[:, pl.ds(j * self.width, self.width)],
            self.held.at[j % 2],
            self.local.sems.at[self.base + j % 2],
        )

    def start(self, j):
        self.copy(j).start()

    def wait(self, j):
        self.copy(j).wait()
        return self.held[j % 2]


class GradMove:
    def __init__(self, sender, local, spot, far, side, depth, total, final):
        self.sender, self.local, self.spot = sender, local, spot
        self.far, self.side, self.depth, self.total, self.final = far, side, depth, total, final
        self.tall = total.shape[0]
        self.y, self.x, self.z, self.g, self.fx = (sender.slots(4) for _ in range(5))
        self.kept = local.used
        local.used += 1
        self.z_open = []

    def send_far(self, j, give):
        self.sender.start(self.y + j, give, self.far.at[j], self.spot.fsdp(2))

    def half(self, side):
        return pl.ds(pl.multiple_of(side * self.tall, 16), self.tall)

    def fold(self, j, kept, arrives=True):
        if arrives:
            self.sender.arrived(self.y + j, self.far.at[j])
        self.far[j] = (self.far[j].astype(F32) + kept.astype(F32)).astype(BF16)
        self.sender.start(
            self.x + j, self.far.at[j, self.half(1 - self.spot.x)], self.side.at[j], self.spot.rep()
        )

    def cross(self, j):
        spot = self.spot
        self.sender.arrived(self.x + j, self.side.at[j])
        mine = self.far[j, self.half(spot.x), :].astype(F32)
        self.side[j] = (mine + self.side[j].astype(F32)).astype(BF16)
        step = lax.rem(spot.s - j + 4, 4)
        index = jnp.maximum(step - 1, 0)
        self.z_open.append(
            self.sender.start_if(
                spot.s != j,
                self.z + j,
                self.z + index,
                self.side.at[j],
                self.depth.at[index],
                (spot.x, spot.f, j),
            )
        )

    def gather(self, j):
        @pl.when(self.spot.s == j)
        def _():
            total = self.side[j].astype(F32)
            for index in range(3):
                self.sender.arrived(self.z + index, self.depth.at[index])
                total = total + self.depth[index].astype(F32)
            self.total[...] = total.astype(BF16)

    def give_back(self, j):
        spot, sender = self.spot, self.sender
        target = self.final.at[j, spot.x]

        @pl.when(spot.s == j)
        def _():
            for step in range(1, 4):
                pltpu.make_async_remote_copy(
                    self.total,
                    target,
                    sender.send_sems.at[self.g + step],
                    sender.recv_sems.at[self.g + j],
                    (spot.x, spot.f, (j + step) % 4),
                    MESH,
                ).start()
            pltpu.make_async_remote_copy(
                self.total,
                target,
                sender.send_sems.at[self.fx + j],
                sender.recv_sems.at[self.fx + j],
                spot.rep(),
                MESH,
            ).start()
            pltpu.make_async_copy(self.total, target, self.local.sems.at[self.kept]).start()

    def settle(self, j):
        self.gather(j)
        self.give_back(j)

    def pass_on(self, j):
        spot, sender = self.spot, self.sender
        target = self.final.at[j, spot.x]

        @pl.when(spot.s != j)
        def _():
            sender.arrived(self.g + j, target)
            pltpu.make_async_remote_copy(
                target,
                target,
                sender.send_sems.at[self.fx + j],
                sender.recv_sems.at[self.fx + j],
                spot.rep(),
                MESH,
            ).start()

    def finish_sums(self):
        for wanted, copy in self.z_open:
            pl.when(wanted)(lambda copy=copy: copy.wait_send())

    def finish_back(self):
        spot, sender = self.spot, self.sender
        for j in range(4):
            sender.arrived(self.fx + j, self.final.at[j, 1 - spot.x])
            sender.sent(self.fx + j, self.total)
        for step in range(1, 4):
            sender.sent(self.g + step, self.total)
        pltpu.make_async_copy(self.total, self.total, self.local.sems.at[self.kept]).wait()

    def finish(self):
        self.finish_sums()
        self.finish_back()


DOWN = (((0,), (0,)), ((), ()))


def outer(left_own, left_other, right_own, right_other):
    total = lax.dot_general(left_own, right_own, DOWN, preferred_element_type=F32)
    return total + lax.dot_general(left_other, right_other, DOWN, preferred_element_type=F32)


def lane_block(index, size):
    return pl.ds(pl.multiple_of(index * size, LANES), size)


def middle_kernel(
    grad_mlp,
    grad_out,
    middle,
    branch,
    stretch,
    gate,
    error_in,
    activated,
    slope,
    hidden,
    down_full,
    up_full,
    out_full,
    block_out,
    attended_grad,
    branch_grad,
    middle_grad,
    sums,
    error_out,
    up_total,
    down_final,
    upper_other,
    block_back,
    act_give,
    act_keep,
    act_give_other,
    act_keep_other,
    mlp_other,
    hid,
    held,
    slopes,
    uppers,
    others,
    hidden_grad,
    out_held,
    give,
    kept,
    far,
    side,
    depth,
    total,
    up_far,
    up_side,
    up_depth,
    errors,
    send_sems,
    recv_sems,
    local_sems,
):
    spot = Spot()
    sender, local = Sender(send_sems, recv_sems), Locals(local_sems)
    tokens, width = grad_mlp.shape
    shard = activated.shape[1] // 4
    f, core = spot.f, spot.fsdp(1)
    loads = [
        local.start(activated.at[:, lane_block(spot.other(2), shard)], act_give),
        local.start(activated.at[:, lane_block(f, shard)], act_keep),
        local.start(hidden.at[spot.other(2)], hid.at[0]),
        local.start(hidden.at[f], hid.at[1]),
    ]
    out_load = local.start(out_full, out_held)
    base = local.used
    local.used += 6

    def weight_copy(number, which):
        units = pl.ds(ORDER[number] * width, width)
        if which == 0:
            return pltpu.make_async_copy(down_full.at[units], held.at[0], local.sems.at[base])
        if which == 1:
            slot = number % 2
            return pltpu.make_async_copy(
                slope.at[:, units], slopes.at[slot], local.sems.at[base + 1 + slot]
            )
        return pltpu.make_async_copy(up_full.at[:, units], held.at[1], local.sems.at[base + 3])

    def other_copy(number):
        slot = number % 2
        return pltpu.make_async_copy(
            upper_other.at[ORDER[number]], others.at[slot], local.sems.at[base + 4 + slot]
        )

    for which in range(3):
        weight_copy(0, which).start()
    greet(column_group(spot) + [spot.fsdp(2), spot.rep()])
    error_slots = [sender.slot() for _ in range(3)]
    error_z = sender.slots(4)
    sender.start(error_slots[0], error_in, errors.at[4], core)
    pieces = [sender.slot() for _ in range(5)]
    upper_slots = sender.slots(4)
    sender.start(
        pieces[0], activated.at[:, lane_block(spot.other(3), shard)], act_give_other, core
    )
    sender.start(pieces[1], grad_mlp, mlp_other, core)
    sender.start(
        pieces[2], activated.at[:, lane_block(spot.other(1), shard)], act_keep_other, core
    )
    sender.start(pieces[3], hidden.at[spot.other(3)], hid.at[2], core)
    sender.start(pieces[4], hidden.at[spot.other(1)], hid.at[3], core)
    back = TokenReturn(sender, spot, block_out, block_back)
    down = GradMove(sender, local, spot, far, side, depth, total, down_final)
    up = GradMove(sender, local, spot, up_far, up_side, up_depth, up_total, None)

    sender.arrived(error_slots[0], errors.at[4])
    errors[5] = error_in[...] + errors[4]
    sender.start(error_slots[1], errors.at[5], errors.at[6], spot.fsdp(2))
    for load in loads[:2]:
        load.wait()
    sender.arrived(pieces[0], act_give_other)
    sender.arrived(error_slots[1], errors.at[6])
    errors[7] = errors[5] + errors[6]
    sender.start(error_slots[2], errors.at[7], errors.at[8], spot.rep())
    sender.arrived(pieces[1], mlp_other)
    block = 384

    def fill(target, left, left_other):
        def body(i, carry):
            columns = lane_block(i, block)
            rows = pl.ds(pl.multiple_of(i * block, 16), block)
            target[rows, :] = outer(
                left[:, columns], left_other[:, columns], grad_mlp[...], mlp_other[...]
            ).astype(BF16)
            return carry

        lax.fori_loop(0, shard // block, body, 0)

    tall = shard // 4
    fill(give.at[0], act_give, act_give_other)
    for j in ORDER:
        down.send_far(j, give.at[0, pl.ds(j * tall, tall)])
    sender.arrived(error_slots[2], errors.at[8])
    errors[spot.s] = errors[7] + errors[8]
    error_open = []
    for step in range(1, 4):
        copy = pltpu.make_async_remote_copy(
            errors.at[spot.s],
            errors.at[spot.s],
            send_sems.at[error_z + step],
            recv_sems.at[error_z + spot.s],
            spot.seq(step),
            MESH,
        )
        copy.start()
        error_open.append(copy)
    back.start()
    sender.arrived(pieces[2], act_keep_other)
    fill(kept.at[0], act_keep, act_keep_other)

    across = (((1,), (1,)), ((), ()))
    sums[...] = jnp.zeros_like(sums)

    def upper(number):
        j = ORDER[number]
        weight_copy(number, 0).wait()
        weight_copy(number, 1).wait()
        grad = lax.dot_general(grad_mlp[...], held[0], across, preferred_element_type=F32)
        grad = (grad * slopes[number % 2].astype(F32)).astype(BF16)
        uppers[j] = grad
        sender.start(upper_slots + j, uppers.at[j], upper_other.at[j], core)
        if number < 3:
            weight_copy(number + 1, 0).start()
            weight_copy(number + 1, 1).start()
        weight_copy(number, 2).wait()
        product = lax.dot_general(uppers[j], held[1], across, preferred_element_type=F32)
        if number == 0:
            hidden_grad[...] = product
        else:
            hidden_grad[...] += product
        if number < 3:
            weight_copy(number + 1, 2).start()
        sums[5 + j : 6 + j, :] = jnp.sum(uppers[j].astype(F32), axis=0, keepdims=True)

    def up_outer(number):
        j = ORDER[number]
        other_copy(number).wait()
        if number < 3:
            sender.arrived(upper_slots + ORDER[number + 1], upper_other.at[ORDER[number + 1]])
            other_copy(number + 1).start()
        rows = pl.ds(j * tall, tall)
        right_other = others[number % 2]
        give[1, rows, :] = outer(hid[0], hid[2], uppers[j], right_other).astype(BF16)
        up.send_far(j, give.at[1, rows])
        kept[1, rows, :] = outer(hid[1], hid[3], uppers[j], right_other).astype(BF16)

    def fold(group, index, j):
        group.fold(j, kept[index, pl.ds(j * tall, tall), :])

    a, b, c, d = ORDER
    upper(0)
    fold(down, 0, a)
    upper(1)
    down.cross(a)
    upper(2)
    fold(down, 0, b)
    upper(3)
    down.cross(b)
    for load in loads[2:]:
        load.wait()
    for slot, place in ((3, 2), (4, 3)):
        sender.arrived(pieces[slot], hid.at[place])
    sender.arrived(upper_slots + a, upper_other.at[a])
    other_copy(0).start()
    up_outer(0)
    up_outer(1)
    fold(down, 0, c)
    up_outer(2)
    up_outer(3)
    down.cross(c)
    down.settle(a)

    def strip_step(i, found):
        strip = pl.ds(pl.multiple_of(i * STRIP, STRIP), STRIP)
        normed, rate = row_norm(middle[strip, :])
        grad = hidden_grad[strip, :]
        scaled = grad * (1.0 + stretch[...])
        result = grad_out[strip, :] + rate * (
            scaled
            - jnp.mean(scaled, axis=-1, keepdims=True)
            - normed * jnp.mean(scaled * normed, axis=-1, keepdims=True)
        )
        middle_grad[strip, :] = result
        low = (result * gate[...]).astype(BF16)
        branch_grad[strip, :] = low
        terms = (
            result * branch[strip, :],
            grad,
            grad * normed,
            low.astype(F32),
            grad_mlp[strip, :].astype(F32),
        )
        return tuple(
            kept_sum + jnp.sum(term, axis=0, keepdims=True)
            for kept_sum, term in zip(found, terms, strict=True)
        )

    zero = jnp.zeros((1, width), F32)
    found = lax.fori_loop(0, tokens // STRIP, strip_step, (zero,) * 5)
    for place, value in zip((0, 1, 2, 4, 9), found, strict=True):
        sums[place : place + 1, :] = value
    fold(down, 0, d)
    out_load.wait()
    attended_grad[...] = lax.dot_general(
        branch_grad[...], out_held[...], across, preferred_element_type=F32
    ).astype(BF16)
    down.cross(d)
    down.settle(b)
    fold(up, 1, a)
    down.settle(c)
    up.cross(a)
    fold(up, 1, b)
    down.settle(d)
    up.cross(b)
    down.pass_on(a)
    fold(up, 1, c)
    down.pass_on(b)
    up.cross(c)
    down.pass_on(c)
    for place in range(4):

        @pl.when(spot.s != place)
        def _():
            sender.arrived(error_z + place, errors.at[place])

    error_out[...] = errors[0] + errors[1] + errors[2] + errors[3]
    for copy in error_open:
        copy.wait_send()
    fold(up, 1, d)
    down.pass_on(d)
    up.cross(d)
    up.gather(a)
    up.gather(b)
    up.gather(c)
    back.finish()
    down.finish()
    up.gather(d)
    up.finish_sums()
    sender.finish()


def middle_back(near_operands, activated, slope, hidden, down_full, up_full, out_full, block_out):
    grad_mlp = near_operands[0]
    error = near_operands[-1]
    tokens, width = grad_mlp.shape
    shape = (tokens, width)
    shard = activated.shape[1] // 4
    tall = shard // 4
    anywhere = pl.BlockSpec(memory_space=pl.ANY)
    near = pl.BlockSpec(memory_space=pltpu.VMEM)
    piece = (tall // 2, width)
    return pl.pallas_call(
        middle_kernel,
        out_shape=[
            jax.ShapeDtypeStruct(shape, BF16),
            jax.ShapeDtypeStruct(shape, BF16),
            jax.ShapeDtypeStruct(shape, F32),
            jax.ShapeDtypeStruct((ROW_PARTS, width), F32),
            jax.ShapeDtypeStruct(error.shape, F32),
            jax.ShapeDtypeStruct(piece, BF16),
            jax.ShapeDtypeStruct((4, 2) + piece, BF16),
            jax.ShapeDtypeStruct((4,) + shape, BF16),
            jax.ShapeDtypeStruct(block_out.shape, BF16),
        ],
        in_specs=[near] * len(near_operands) + [anywhere] * 7,
        out_specs=[near] * 6 + [anywhere] * 3,
        scratch_shapes=[
            pltpu.VMEM((tokens, shard), BF16),
            pltpu.VMEM((tokens, shard), BF16),
            pltpu.VMEM((tokens, shard), BF16),
            pltpu.VMEM((tokens, shard), BF16),
            pltpu.VMEM(shape, BF16),
            pltpu.VMEM((4,) + hidden.shape[1:], BF16),
            pltpu.VMEM((2, width, width), BF16),
            pltpu.VMEM((2,) + shape, BF16),
            pltpu.VMEM((4,) + shape, BF16),
            pltpu.VMEM((2,) + shape, BF16),
            pltpu.VMEM(shape, F32),
            pltpu.VMEM(out_full.shape, BF16),
            pltpu.VMEM((2, shard, width), BF16),
            pltpu.VMEM((2, shard, width), BF16),
            pltpu.VMEM((4, tall, width), BF16),
            pltpu.VMEM((4,) + piece, BF16),
            pltpu.VMEM((3,) + piece, BF16),
            pltpu.VMEM(piece, BF16),
            pltpu.VMEM((4, tall, width), BF16),
            pltpu.VMEM((4,) + piece, BF16),
            pltpu.VMEM((3,) + piece, BF16),
            pltpu.VMEM((9,) + error.shape, F32),
            sems(72),
            sems(72),
            sems(20),
        ],
        compiler_params=pltpu.CompilerParams(
            collective_id=3, has_side_effects=True, vmem_limit_bytes=67043328
        ),
        name="middle_back",
    )(*near_operands, activated, slope, hidden, down_full, up_full, out_full, block_out)


ROW_PARTS = 16


def finish_kernel(*refs):
    (
        branch_grad,
        up_total,
        middle_grad,
        inputs,
        stretch,
        q_ref,
        k_own,
        v_own,
        k_other,
        v_other,
        do_ref,
        lse_ref,
        bias_own,
        bias_other,
        sums_in,
        gate_sum,
        cond_part,
        attended,
        hidden,
        mod_weight,
        qkv_full,
        rows,
        cond_parts,
        up_final,
        tail_final,
        tokens_back,
        branch_other,
        qkv_grad,
        qkv_other,
        att,
        hid,
        mod_held,
        qkv_held,
        hidden_grad,
        dv_one,
        dk_two,
        dv_two,
        dk_in,
        dv_in,
        tokens_grad,
        give,
        far,
        side,
        depth,
        total,
        row,
        row_in,
        cond_send,
        send_sems,
        recv_sems,
        local_sems,
    ) = refs
    spot = Spot()
    sender, local = Sender(send_sems, recv_sems), Locals(local_sems)
    width = branch_grad.shape[1]
    f, core = spot.f, spot.fsdp(1)
    loads = [
        local.start(attended.at[spot.other(2)], att.at[0]),
        local.start(attended.at[f], att.at[1]),
        local.start(hidden.at[spot.other(2)], hid.at[0]),
        local.start(hidden.at[f], hid.at[1]),
    ]
    mod_load = local.start(mod_weight, mod_held)
    stream = ColumnStream(local, qkv_full, qkv_held, width)
    stream.start(0)
    stream.start(1)
    greet(column_group(spot) + [spot.fsdp(2), spot.fsdp(3), spot.rep()])
    slots = [sender.slot() for _ in range(6)]
    sender.start(slots[0], attended.at[spot.other(3)], att.at[2], core)
    sender.start(slots[1], branch_grad, branch_other, core)
    sender.start(slots[2], hidden.at[spot.other(3)], hid.at[2], core)
    sender.start(slots[4], attended.at[spot.other(1)], att.at[3], core)
    sender.start(slots[5], hidden.at[spot.other(1)], hid.at[3], core)
    up = GradMove(sender, local, spot, None, None, None, up_total, up_final)
    tail = GradMove(sender, local, spot, far, side, depth, total, tail_final)
    back = TokenReturn(sender, spot, tokens_grad, tokens_back)
    row_slot = sender.slot()
    row_z, row_y, row_x = sender.slots(4), sender.slot(), sender.slot()
    cond_slots = {bit: sender.slot() for bit in (1, 2, 3)}
    dk_slot, dv_slot = sender.slot(), sender.slot()
    for j in ORDER:
        up.give_back(j)
    for load in loads:
        load.wait()

    def operands(j):
        if j == 0:
            return att, branch_grad[...], branch_other[...]
        columns = slice((j - 1) * width, j * width)
        return hid, qkv_grad[:, columns], qkv_other[:, columns]

    def give_far(j):
        left, right, right_other = operands(j)
        give[j] = outer(left[0], left[2], right, right_other).astype(BF16)
        tail.send_far(j, give.at[j])

    a, b, c, d = ORDER
    sender.arrived(slots[0], att.at[2])
    sender.arrived(slots[1], branch_other)
    give_far(a)
    data = (
        q_ref,
        k_own,
        v_own,
        k_other,
        v_other,
        do_ref,
        lse_ref,
        bias_own,
        bias_other,
        qkv_grad.at[:, pl.ds(0, width)],
        hidden_grad,
        dv_one,
        dk_two,
        dv_two,
    )
    sender.arrived(slots[4], att.at[3])

    def fold(j):
        left, right, right_other = operands(j)
        tail.fold(j, outer(left[1], left[3], right, right_other))

    backward_heads(0, 5, *data)
    up.pass_on(a)
    backward_heads(5, 10, *data)
    fold(a)
    up.pass_on(b)
    backward_heads(10, HEADS, *data)
    sender.start(dk_slot, dk_two, dk_in, core)
    sender.start(dv_slot, dv_two, dv_in, core)
    tail.cross(a)
    sender.arrived(dk_slot, dk_in)
    qkv_grad[:, width : 2 * width] = (hidden_grad[...] + dk_in[...].astype(F32)).astype(BF16)
    sender.arrived(dv_slot, dv_in)
    qkv_grad[:, 2 * width :] = (dv_one[...] + dv_in[...].astype(F32)).astype(BF16)
    sender.start(slots[3], qkv_grad, qkv_other, core)

    across = (((1,), (1,)), ((), ()))
    for j in range(3):
        product = lax.dot_general(
            qkv_grad[:, j * width : (j + 1) * width],
            stream.wait(j),
            across,
            preferred_element_type=F32,
        )
        if j == 0:
            hidden_grad[...] = product
            stream.start(2)
        else:
            hidden_grad[...] += product
    sender.arrived(slots[2], hid.at[2])
    sender.arrived(slots[3], qkv_other)
    give_far(b)
    give_far(c)
    give_far(d)

    def norm_step(i, sums):
        strip = pl.ds(pl.multiple_of(i * STRIP, STRIP), STRIP)
        normed, rate = row_norm(inputs[strip, :].astype(F32))
        grad = hidden_grad[strip, :]
        scaled = grad * (1.0 + stretch[...])
        result = middle_grad[strip, :] + rate * (
            scaled
            - jnp.mean(scaled, axis=-1, keepdims=True)
            - normed * jnp.mean(scaled * normed, axis=-1, keepdims=True)
        )
        tokens_grad[i // per_half, pl.ds(pl.multiple_of((i % per_half) * STRIP, STRIP), STRIP), :] = (
            result.astype(BF16)
        )
        return (
            sums[0] + jnp.sum(grad, axis=0, keepdims=True),
            sums[1] + jnp.sum(grad * normed, axis=0, keepdims=True),
            sums[2] + jnp.sum(qkv_grad[strip, :width].astype(F32), axis=0, keepdims=True),
            sums[3] + jnp.sum(qkv_grad[strip, 2 * width :].astype(F32), axis=0, keepdims=True),
        )

    per_half = tokens_grad.shape[1] // STRIP
    zero = jnp.zeros((1, width), F32)
    sums = lax.fori_loop(0, 2 * per_half, norm_step, (zero,) * 4)
    row[0:2, :] = jnp.concatenate(sums[:2], axis=0)
    row[2:, :] = sums_in[: ROW_PARTS - 2, :]
    row[5:6, :] = gate_sum[...]
    row[12:15, :] = jnp.concatenate(sums[2:] + (cond_part[...],), axis=0)
    sender.start(row_slot, row, row_in, core)
    sender.arrived(row_slot, row_in)
    column = (spot.x * 2 + spot.pair) * 4
    rows[column + spot.s] = row[...] + row_in[...]
    row_open = []
    for step in range(1, 4):
        copy = pltpu.make_async_remote_copy(
            rows.at[column + spot.s],
            rows.at[column + spot.s],
            send_sems.at[row_z + step],
            recv_sems.at[row_z + spot.s],
            spot.seq(step),
            MESH,
        )
        copy.start()
        row_open.append(copy)
    back.start()
    sender.arrived(slots[5], hid.at[3])
    fold(b)
    tail.cross(b)
    for place in range(4):

        @pl.when(spot.s != place)
        def _():
            sender.arrived(row_z + place, rows.at[column + place])

    span = pl.ds(column, 4)
    sender.start(row_y, rows.at[span], rows.at[span], spot.fsdp(2))
    fold(c)
    up.pass_on(c)
    tail.cross(c)
    tail.settle(a)
    fold(d)
    tail.cross(d)
    up.pass_on(d)
    far_column = (spot.x * 2 + 1 - spot.pair) * 4
    sender.arrived(row_y, rows.at[pl.ds(far_column, 4)])
    half = pl.ds(spot.x * 8, 8)
    sender.start(row_x, rows.at[half], rows.at[half], spot.rep())
    tail.settle(b)
    tail.settle(c)

    mod_load.wait()
    products = jnp.zeros((16, mod_held.shape[0]), F32)
    for part in range(6):
        grad = rows[half, part, :]
        high = grad.astype(BF16)
        low = (grad - high.astype(F32)).astype(BF16)
        products += lax.dot_general(
            jnp.concatenate([high, low], axis=0),
            mod_held[:, part * width : (part + 1) * width],
            (((1,), (1,)), ((), ())),
            preferred_element_type=F32,
        )
    silu_grad = products[:8] + products[8:]
    for latent in range(8):
        cond_send[latent // 2, latent % 2 : latent % 2 + 1, :] = silu_grad[latent : latent + 1]
    cond_parts[f] = cond_send[f]
    for bit in (1, 2, 3):
        sender.start(
            cond_slots[bit], cond_send.at[spot.other(bit)], cond_parts.at[f], spot.fsdp(bit)
        )

    tail.pass_on(a)
    tail.settle(d)
    tail.pass_on(b)
    tail.pass_on(c)
    tail.pass_on(d)
    for bit in (1, 2, 3):
        sender.arrived(cond_slots[bit], cond_parts.at[spot.other(bit)])
    sender.arrived(row_x, rows.at[pl.ds((1 - spot.x) * 8, 8)])
    for copy in row_open:
        copy.wait_send()
    back.finish()
    up.finish_back()
    tail.finish()
    sender.finish()


def finish(near_operands, attended, hidden, mod_weight, qkv_full, token_shape):
    branch_grad, up_total = near_operands[:2]
    tokens, width = branch_grad.shape
    shape = (tokens, width)
    piece = up_total.shape
    anywhere = pl.BlockSpec(memory_space=pl.ANY)
    near = pl.BlockSpec(memory_space=pltpu.VMEM)
    final = jax.ShapeDtypeStruct((4, 2) + piece, BF16)
    tall = 2 * piece[0]
    return pl.pallas_call(
        finish_kernel,
        out_shape=[
            jax.ShapeDtypeStruct((16, ROW_PARTS, width), F32),
            jax.ShapeDtypeStruct((4, 2, mod_weight.shape[0]), F32),
            final,
            final,
            jax.ShapeDtypeStruct(token_shape, BF16),
        ],
        in_specs=[near] * len(near_operands) + [anywhere] * 4,
        out_specs=[near] * 2 + [anywhere] * 3,
        scratch_shapes=[
            pltpu.VMEM(shape, BF16),
            pltpu.VMEM((tokens, 3 * width), BF16),
            pltpu.VMEM((tokens, 3 * width), BF16),
            pltpu.VMEM((4,) + attended.shape[1:], BF16),
            pltpu.VMEM((4,) + hidden.shape[1:], BF16),
            pltpu.VMEM(mod_weight.shape, BF16),
            pltpu.VMEM((2, width, width), BF16),
            pltpu.VMEM(shape, F32),
            pltpu.VMEM(shape, F32),
            pltpu.VMEM(shape, BF16),
            pltpu.VMEM(shape, BF16),
            pltpu.VMEM(shape, BF16),
            pltpu.VMEM(shape, BF16),
            pltpu.VMEM(token_shape, BF16),
            pltpu.VMEM((4, tall, width), BF16),
            pltpu.VMEM((4, tall, width), BF16),
            pltpu.VMEM((4,) + piece, BF16),
            pltpu.VMEM((3,) + piece, BF16),
            pltpu.VMEM(piece, BF16),
            pltpu.VMEM((ROW_PARTS, width), F32),
            pltpu.VMEM((ROW_PARTS, width), F32),
            pltpu.VMEM((4, 2, mod_weight.shape[0]), F32),
            sems(72),
            sems(72),
            sems(24),
        ],
        compiler_params=pltpu.CompilerParams(
            collective_id=4, has_side_effects=True, vmem_limit_bytes=67043328
        ),
        name="finish",
    )(*near_operands, attended, hidden, mod_weight, qkv_full)


def spread_kernel(block, out):
    out[...] = block[0].astype(F32)


def spread(blocks):
    count, rows, width = blocks.shape
    return pl.pallas_call(
        spread_kernel,
        grid=(count,),
        out_shape=jax.ShapeDtypeStruct((rows, count * width), F32),
        in_specs=[pl.BlockSpec((1, rows, width), lambda j: (j, 0, 0))],
        out_specs=pl.BlockSpec((rows, width), lambda j: (0, j)),
        name="spread",
    )(blocks)


def head_window(head, head_dim, width):
    start = head * head_dim
    base = jnp.minimum(start // LANES, (width - WINDOW) // LANES) * LANES
    base = pl.multiple_of(base, LANES)
    return start, base


def forward_heads(
    low,
    high,
    q_ref,
    k_own,
    v_own,
    k_other,
    v_other,
    bias_own,
    bias_other,
    out_ref,
    lse_ref,
):
    tokens, width = q_ref.shape
    head_dim = width // HEADS
    blocks = 2
    tall = tokens // blocks
    scale = head_dim ** (-0.5) * LOG2E
    b_own, b_other = bias_own[...], bias_other[...]
    dims = (((1,), (1,)), ((), ()))

    def body(head, carry):
        start, base = head_window(head, head_dim, width)
        window = pl.ds(base, WINDOW)
        lane = lax.broadcasted_iota(jnp.int32, (1, WINDOW), 1) + base
        inside = (lane >= start) & (lane < start + head_dim)
        keep = inside.astype(BF16)
        spot = lax.broadcasted_iota(jnp.int32, (1, LANES), 1) == head
        key_one, key_two = k_own[:, window], k_other[:, window]
        val_one, val_two = v_own[:, window] * keep, v_other[:, window] * keep
        for block in range(blocks):
            rows = pl.ds(block * tall, tall)
            query = q_ref[rows, window] * keep
            one = lax.dot_general(query, key_one, dims, preferred_element_type=F32)
            two = lax.dot_general(query, key_two, dims, preferred_element_type=F32)
            one = one * scale + b_own
            two = two * scale + b_other
            top = jnp.maximum(
                jnp.max(one, axis=1, keepdims=True), jnp.max(two, axis=1, keepdims=True)
            )
            one = jnp.exp2(one - top)
            two = jnp.exp2(two - top)
            total = jnp.sum(one, axis=1, keepdims=True) + jnp.sum(two, axis=1, keepdims=True)
            mixed = jnp.dot(one.astype(BF16), val_one, preferred_element_type=F32)
            mixed += jnp.dot(two.astype(BF16), val_two, preferred_element_type=F32)
            mixed = mixed * (1.0 / total)
            out_ref[rows, window] = jnp.where(
                inside, mixed, out_ref[rows, window].astype(F32)
            ).astype(out_ref.dtype)
            lse_ref[rows, :] = jnp.where(spot, top + jnp.log2(total), lse_ref[rows, :])
        return carry

    lax.fori_loop(low, high, body, 0)


def forward_kernel(*refs):
    out_ref, lse_ref = refs[-2:]
    out_ref[...] = jnp.zeros_like(out_ref)
    lse_ref[...] = jnp.zeros_like(lse_ref)
    forward_heads(0, HEADS, *refs)


def forward_send_kernel(
    inputs,
    shift,
    stretch,
    q_bias,
    v_bias,
    bias_own,
    bias_other,
    count_in,
    qkv_full,
    up_weight,
    down_weight,
    teacher,
    out_grad,
    hidden,
    q_ref,
    k_own,
    v_own,
    out_ref,
    lse_ref,
    k_other,
    v_other,
    count_out,
    up_full,
    down_full,
    teacher_own,
    out_grad_own,
    qkv_held,
    counts,
    count_sum,
    far_counts,
    up_stage,
    down_stage,
    send_sems,
    recv_sems,
    local_sems,
):
    spot = Spot()
    sender, local = Sender(send_sems, recv_sems), Locals(local_sems)
    width = q_ref.shape[1]
    stream = ColumnStream(local, qkv_full, qkv_held, width)
    stream.start(0)
    stream.start(1)
    greet(column_group(spot) + [spot.fsdp(2), spot.rep(), spot.rep(2)])
    count_slots = [sender.slot() for _ in range(3)]
    for step in range(1, 4):
        sender.start(count_slots[step - 1], count_in, counts.at[step - 1], spot.seq(step))
    key_slot, value_slot = sender.slot(), sender.slot()
    moves = [
        TokenMove(sender, spot, teacher, teacher_own),
        TokenMove(sender, spot, out_grad, out_grad_own),
    ]
    up = WeightMove(sender, local, spot, up_weight, up_full, up_stage, 3)
    down = WeightMove(sender, local, spot, down_weight, down_full, down_stage, 4)
    far_slots = [sender.slot() for _ in range(3)]

    total = count_in[...]
    for step in range(1, 4):
        sender.arrived(count_slots[step - 1], counts.at[step - 1])
        total = total + counts[step - 1]
    count_sum[...] = total
    for number, device in enumerate((spot.fsdp(2), spot.rep(), spot.rep(2))):
        sender.start(far_slots[number], count_sum, far_counts.at[number], device)
    up.start_far()
    down.start_far()
    for move in moves:
        move.start()

    def normalise(i, carry):
        rows = pl.ds(pl.multiple_of(i * STRIP, STRIP), STRIP)
        normed, _ = row_norm(inputs[rows, :].astype(F32))
        hidden[rows, :] = (normed * (1.0 + stretch[...]) + shift[...]).astype(BF16)
        return carry

    lax.fori_loop(0, q_ref.shape[0] // STRIP, normalise, 0)
    q_ref[...] = (
        jnp.dot(hidden[...], stream.wait(0), preferred_element_type=F32) + q_bias[...]
    ).astype(BF16)
    stream.start(2)
    k_own[...] = jnp.dot(hidden[...], stream.wait(1), preferred_element_type=F32).astype(BF16)
    sender.start(key_slot, k_own, k_other, spot.fsdp(1))
    v_own[...] = (
        jnp.dot(hidden[...], stream.wait(2), preferred_element_type=F32) + v_bias[...]
    ).astype(BF16)
    sender.start(value_slot, v_own, v_other, spot.fsdp(1))
    up.start_near()
    down.start_near()
    up.pass_far(0)
    out_ref[...] = jnp.zeros_like(out_ref)
    lse_ref[...] = jnp.zeros_like(lse_ref)
    sender.arrived(key_slot, k_other)
    sender.arrived(value_slot, v_other)
    data = (q_ref, k_own, v_own, k_other, v_other, bias_own, bias_other, out_ref, lse_ref)
    forward_heads(0, 8, *data)
    up.store()
    down.store()
    up.pass_far(1)
    up.pass_side(0)
    forward_heads(8, HEADS, *data)
    up.pass_far(2)
    up.pass_side(1)
    down.pass_far(0)
    up.pass_side(2)
    for chunk in range(1, 4):
        down.pass_far(chunk)
        down.pass_side(chunk - 1)
    down.pass_side(3)
    total = count_sum[...]
    for number in range(3):
        sender.arrived(far_slots[number], far_counts.at[number])
        total = total + far_counts[number]
    count_out[...] = total
    for move in moves:
        move.finish()
    up.finish()
    down.finish()
    sender.finish()


def attend_and_gather(inputs, near_operands, qkv_full, up_weight, down_weight, teacher, out_grad):
    tokens, width = inputs.shape
    count = near_operands[-1]
    anywhere = pl.BlockSpec(memory_space=pl.ANY)
    near = pl.BlockSpec(memory_space=pltpu.VMEM)
    shape = (tokens, width)
    return pl.pallas_call(
        forward_send_kernel,
        out_shape=[jax.ShapeDtypeStruct(shape, BF16)] * 5
        + [
            jax.ShapeDtypeStruct((tokens, LANES), F32),
            jax.ShapeDtypeStruct(shape, BF16),
            jax.ShapeDtypeStruct(shape, BF16),
            jax.ShapeDtypeStruct(count.shape, F32),
            jax.ShapeDtypeStruct((4 * up_weight.shape[0], up_weight.shape[1]), BF16),
            jax.ShapeDtypeStruct((4 * down_weight.shape[0], down_weight.shape[1]), BF16),
            jax.ShapeDtypeStruct(teacher.shape, BF16),
            jax.ShapeDtypeStruct(out_grad.shape, BF16),
        ],
        in_specs=[near] * (1 + len(near_operands)) + [anywhere] * 5,
        out_specs=[near] * 9 + [anywhere] * 4,
        scratch_shapes=[
            pltpu.VMEM((2, width, width), BF16),
            pltpu.VMEM((3,) + count.shape, F32),
            pltpu.VMEM(count.shape, F32),
            pltpu.VMEM((3,) + count.shape, F32),
            pltpu.VMEM(up_weight.shape, BF16),
            pltpu.VMEM(down_weight.shape, BF16),
            sems(48),
            sems(48),
            sems(12),
        ],
        compiler_params=pltpu.CompilerParams(
            collective_id=2, has_side_effects=True, vmem_limit_bytes=67043328
        ),
        name="attend_and_gather",
    )(inputs, *near_operands, qkv_full, up_weight, down_weight, teacher, out_grad)


def attend(queries, k_own, v_own, k_other, v_other, bias_own, bias_other):
    tokens, width = queries.shape
    return pl.pallas_call(
        forward_kernel,
        out_shape=[
            jax.ShapeDtypeStruct((tokens, width), BF16),
            jax.ShapeDtypeStruct((tokens, LANES), F32),
        ],
        compiler_params=pltpu.CompilerParams(vmem_limit_bytes=48 * 1024 * 1024),
        cost_estimate=pl.CostEstimate(
            flops=16 * tokens * tokens * 2 * WINDOW * 4,
            transcendentals=HEADS * tokens * tokens * 2,
            bytes_accessed=6 * tokens * width * 2,
        ),
        name="attend",
    )(queries, k_own, v_own, k_other, v_other, bias_own, bias_other)


def backward_heads(
    low,
    high,
    q_ref,
    k_own,
    v_own,
    k_other,
    v_other,
    do_ref,
    lse_ref,
    bias_own,
    bias_other,
    dq_ref,
    dk_one,
    dv_one,
    dk_two,
    dv_two,
):
    tokens, width = q_ref.shape
    head_dim = width // HEADS
    factor = head_dim ** (-0.5)
    scale = factor * LOG2E
    across = (((1,), (1,)), ((), ()))
    sides = (
        (k_own, v_own, bias_own, dk_one, dv_one),
        (k_other, v_other, bias_other, dk_two, dv_two),
    )

    def body(head, carry):
        start, base = head_window(head, head_dim, width)
        window = pl.ds(base, WINDOW)
        lane = lax.broadcasted_iota(jnp.int32, (1, WINDOW), 1) + base
        inside = (lane >= start) & (lane < start + head_dim)
        keep = inside.astype(BF16)
        query = q_ref[:, window] * keep
        grad = do_ref[:, window] * keep
        lse = lse_ref[pl.ds(head, 1), :]

        def put(ref, value):
            ref[:, window] = jnp.where(inside, value, ref[:, window].astype(F32)).astype(ref.dtype)

        probs, prods = [], []
        delta = None
        for k_ref, v_ref, bias, _, _ in sides:
            scores = lax.dot_general(k_ref[:, window], query, across, preferred_element_type=F32)
            prob = jnp.exp2(scores * scale + bias[...] - lse)
            prob_grad = lax.dot_general(v_ref[:, window], grad, across, preferred_element_type=F32)
            prod = prob * prob_grad
            part = jnp.sum(prod, axis=0, keepdims=True)
            delta = part if delta is None else delta + part
            probs.append(prob)
            prods.append(prod)
        dq = None
        for (k_ref, _, _, dk, dv), prob, prod in zip(sides, probs, prods, strict=True):
            put(dv, jnp.dot(prob.astype(BF16), grad, preferred_element_type=F32))
            score_grad = (prod - prob * delta).astype(BF16)
            put(dk, jnp.dot(score_grad, query, preferred_element_type=F32) * factor)
            part = lax.dot_general(
                score_grad, k_ref[:, window], DOWN, preferred_element_type=F32
            )
            dq = part if dq is None else dq + part
        put(dq_ref, dq * factor)
        return carry

    lax.fori_loop(low, high, body, 0)


def backward_kernel(*refs):
    for ref in refs[-5:]:
        ref[...] = jnp.zeros_like(ref)
    backward_heads(0, HEADS, *refs)


def attend_back(queries, k_own, v_own, k_other, v_other, grad, lse, bias_own, bias_other):
    tokens, width = queries.shape
    shape = (tokens, width)
    return pl.pallas_call(
        backward_kernel,
        out_shape=[
            jax.ShapeDtypeStruct(shape, BF16),
            jax.ShapeDtypeStruct(shape, F32),
            jax.ShapeDtypeStruct(shape, F32),
            jax.ShapeDtypeStruct(shape, BF16),
            jax.ShapeDtypeStruct(shape, BF16),
        ],
        compiler_params=pltpu.CompilerParams(vmem_limit_bytes=60 * 1024 * 1024),
        name="attend_back",
    )(queries, k_own, v_own, k_other, v_other, grad, lse, bias_own, bias_other)


def dot(left, right):
    return jnp.dot(left, right, preferred_element_type=F32)


def dot_t(left, right):
    return lax.dot_general(left, right, (((1,), (1,)), ((), ())), preferred_element_type=F32)


def norm_parts(inputs):
    centred = inputs - jnp.mean(inputs, axis=-1, keepdims=True)
    rate = lax.rsqrt(jnp.mean(centred * centred, axis=-1, keepdims=True) + EPS)
    return centred * rate, rate


def norm_back(grad, normed, rate):
    return rate * (
        grad
        - jnp.mean(grad, axis=-1, keepdims=True)
        - normed * jnp.mean(grad * normed, axis=-1, keepdims=True)
    )


def gelu_parts(inputs):
    inner = jnp.tanh(GELU_C * (inputs + 0.044715 * inputs * inputs * inputs))
    value = 0.5 * inputs * (1.0 + inner)
    slope = 0.5 * (1.0 + inner) + 0.5 * inputs * (1.0 - inner * inner) * GELU_C * (
        1.0 + 3.0 * 0.044715 * inputs * inputs
    )
    return value, slope


def column_sum(array):
    return jnp.sum(array.astype(F32), axis=0)


def shards(
    tokens,
    condition,
    valid_mask,
    teacher,
    out_grad,
    mod_weight,
    mod_bias,
    qkv_weight,
    qkv_bias,
    out_weight,
    out_bias,
    up_weight,
    up_bias,
    down_weight,
    down_bias,
):
    reps, fsdp, seq = lax.axis_size("rep"), lax.axis_size("fsdp"), lax.axis_size("seq")
    fast = (reps, fsdp, seq) == (2, 4, 4)
    latents, span, width = tokens.shape
    assert 2 * latents == seq and latents == 2
    place_f, place_s = lax.axis_index("fsdp"), lax.axis_index("seq")
    total_tokens = latents * span * reps * fsdp * seq

    biases = jnp.concatenate([mod_bias, qkv_bias, out_bias, up_bias, down_bias])
    shard_rows = mod_weight.shape[0]
    cond_row = pick(condition, place_s % 2)
    keep_mask = valid_mask.astype(F32)

    if fast:
        inputs_low, valid_all, mod_parts, bias_all, qkv_full, out_full = enter(
            tokens,
            keep_mask.reshape(latents, 1, span),
            condition.astype(F32).reshape(latents, fsdp, 1, shard_rows),
            biases.astype(F32)[None],
            mod_weight,
            qkv_weight,
            out_weight,
        )
        inputs_low = inputs_low.reshape(-1, width)
        valid_all = valid_all.reshape(2, -1)
        keyvalid, valid_other = pick(valid_all, place_f % 2), pick(valid_all, 1 - place_f % 2)
        mod_row = jnp.sum(mod_parts, axis=(0, 1))
        bias_all = bias_all[:, 0]
    else:
        inputs_low = to_latent(tokens)
        keyvalid = to_latent(keep_mask)
        valid_other = flip(keyvalid, "fsdp", 1)
        counted = lax.psum(jnp.sum(keep_mask), ("rep", "fsdp", "seq")).reshape(1, 1)
        own_row = jnp.where(place_f % 2 == place_s // 2, cond_row, flip(cond_row, "fsdp", 1))
        cond_pair = lax.all_gather(own_row, "fsdp", axis=0)[::2]
        silu_pair = jax.nn.silu(cond_pair.astype(F32)).astype(BF16)
        silu_cols = lax.dynamic_slice_in_dim(silu_pair, place_f * shard_rows, shard_rows, 1)
        mod_row = pick(lax.psum(dot(silu_cols, mod_weight), "fsdp"), place_f // 2)
        bias_all = lax.all_gather(biases, "fsdp", axis=0).astype(F32)
        qkv_full, out_full = gather_weight(qkv_weight), gather_weight(out_weight)
        up_full, down_full = gather_weight(up_weight), gather_weight(down_weight)
        teacher_own, out_grad_own = to_latent(teacher), to_latent(out_grad)
    mask_own = (keyvalid - 1.0) * (-NEG)
    mask_other = (valid_other - 1.0) * (-NEG)

    cuts = [0]
    for bias in (mod_bias, qkv_bias, out_bias, up_bias, down_bias):
        cuts.append(cuts[-1] + bias.shape[0])
    mod_b, qkv_b, out_b, up_b, down_b = (
        bias_all[:, low:high].reshape(-1) for low, high in zip(cuts[:-1], cuts[1:], strict=True)
    )
    pieces = (mod_row + mod_b).reshape(6, 1, width)
    shift_one, scale_one, gate_one, shift_two, scale_two, gate_two = (pieces[i] for i in range(6))

    inputs = inputs_low.astype(F32)
    if fast:
        (
            hidden_one,
            queries,
            keys_own,
            values_own,
            attended,
            lse,
            keys_other,
            values_other,
            counted,
            up_full,
            down_full,
            teacher_own,
            out_grad_own,
        ) = attend_and_gather(
            inputs_low,
            (
                shift_one,
                scale_one,
                qkv_b[None, :width],
                qkv_b[None, width:],
                mask_own[None],
                mask_other[None],
                jnp.full((1, LANES), jnp.sum(valid_all)),
            ),
            qkv_full,
            up_weight,
            down_weight,
            teacher,
            out_grad,
        )
        counted = counted[:, :1]
        teacher_own = teacher_own.reshape(-1, width)
        out_grad_own = out_grad_own.reshape(-1, width)
    else:
        normed_one, rate_one = norm_parts(inputs)
        hidden_one = (normed_one * (1.0 + scale_one) + shift_one).astype(BF16)
        projected = dot(hidden_one, qkv_full)
        queries = (projected[:, :width] + qkv_b[:width]).astype(BF16)
        keys_own = projected[:, width : 2 * width].astype(BF16)
        values_own = (projected[:, 2 * width :] + qkv_b[width:]).astype(BF16)
        keys_other, values_other = flip(keys_own, "fsdp", 1), flip(values_own, "fsdp", 1)
        attended, lse = attend(
            queries,
            keys_own,
            values_own,
            keys_other,
            values_other,
            mask_own[None],
            mask_other[None],
        )
    branch = dot(attended, out_full) + out_b
    middle = inputs + gate_one * branch
    normed_two, rate_two = norm_parts(middle)
    hidden_two = (normed_two * (1.0 + scale_two) + shift_two).astype(BF16)
    up_pre = dot(hidden_two, up_full) + up_b
    activated, slope = gelu_parts(up_pre)
    activated = activated.astype(BF16)
    mlp_out = dot(activated, down_full) + down_b
    output = middle + gate_two * mlp_out
    block_out = output.astype(BF16)
    differ = (output - teacher_own.astype(F32)) * keyvalid[:, None]
    error = jnp.sum(differ * differ)

    grad_out = out_grad_own.astype(F32) + total_tokens / counted * differ
    grad_mlp = (grad_out * gate_two).astype(BF16)
    gate_two_grad = jnp.sum(grad_out * mlp_out, axis=0, keepdims=True)

    def slices(array):
        return array.reshape(array.shape[0], fsdp, -1).transpose(1, 0, 2)

    def weight_grad(left, right):
        whole = lax.dot_general(left, right, DOWN, preferred_element_type=F32)
        mine = lax.psum_scatter(whole.astype(BF16), "fsdp", scatter_dimension=0, tiled=True)
        return lax.psum(mine, ("rep", "seq")).astype(F32)

    cond_part = jnp.where(place_f % 2 == place_s // 2, cond_row.astype(F32), 0.0)[None]
    length = (11 + up_weight.shape[1] // width) * width
    if fast:
        (
            attended_grad,
            branch_grad,
            middle_grad,
            sums,
            error_sum,
            up_total,
            down_final,
            _,
            block_out,
        ) = middle_back(
            (
                grad_mlp,
                grad_out,
                middle,
                branch,
                scale_two,
                gate_one,
                jnp.full((1, LANES), error),
            ),
            activated,
            slope.astype(BF16),
            slices(hidden_two),
            down_full,
            up_full,
            out_full,
            block_out.reshape(2, span, width),
        )
        err_total = error_sum[:, :1]
        rows, cond_parts, up_final, tail_final, tokens_grad = finish(
            (
                branch_grad,
                up_total,
                middle_grad,
                inputs_low,
                scale_one,
                queries,
                keys_own,
                values_own,
                keys_other,
                values_other,
                attended_grad,
                lse.T,
                mask_own[:, None],
                mask_other[:, None],
                sums,
                gate_two_grad,
                cond_part,
            ),
            slices(attended),
            slices(hidden_one),
            mod_weight,
            qkv_full,
            (2, span, width),
        )
        rows = rows.reshape(-1, ROW_PARTS * width)[:, :length]
        down_g = down_final.reshape(down_weight.shape).astype(F32)
        up_g = spread(up_final.reshape(4, -1, width))
        tail_final = tail_final.reshape(4, -1, width)
        out_g = tail_final[0].astype(F32)
        qkv_g = spread(tail_final[1:])
    else:
        upper_grad = (dot_t(grad_mlp, down_full) * slope).astype(BF16)
        hidden_two_grad = dot_t(upper_grad, up_full)
        scaled_two = hidden_two_grad * (1.0 + scale_two)
        middle_grad = grad_out + norm_back(scaled_two, normed_two, rate_two)
        branch_grad = (middle_grad * gate_one).astype(BF16)
        attended_grad = dot_t(branch_grad, out_full).astype(BF16)
        query_grad, key_part, value_part, key_away, value_away = attend_back(
            queries,
            keys_own,
            values_own,
            keys_other,
            values_other,
            attended_grad,
            lse.T,
            mask_own[:, None],
            mask_other[:, None],
        )
        key_grad = (key_part + flip(key_away, "fsdp", 1).astype(F32)).astype(BF16)
        value_grad = (value_part + flip(value_away, "fsdp", 1).astype(F32)).astype(BF16)
        err_total = lax.psum(error, ("rep", "fsdp", "seq")).reshape(1, 1)
        block_out = from_latent(block_out)
        qkv_grad = jnp.concatenate([query_grad, key_grad, value_grad], axis=-1)
        hidden_one_grad = dot_t(qkv_grad, qkv_full)
        scaled_one = hidden_one_grad * (1.0 + scale_one)
        tokens_grad = middle_grad + norm_back(scaled_one, normed_one, rate_one)
        tokens_grad = tokens_grad.astype(BF16)
        row = jnp.concatenate(
            [
                column_sum(hidden_one_grad),
                column_sum(hidden_one_grad * normed_one),
                column_sum(middle_grad * branch),
                column_sum(hidden_two_grad),
                column_sum(hidden_two_grad * normed_two),
                gate_two_grad[0],
                column_sum(branch_grad),
                column_sum(upper_grad),
                column_sum(grad_mlp),
                column_sum(query_grad),
                column_sum(value_grad),
                cond_part[0],
            ]
        )
        row = row + flip(row, "fsdp", 1)
        rows = gather_rows(row)
        tokens_grad = from_latent(tokens_grad)
        down_g = weight_grad(activated, grad_mlp)
        up_g = weight_grad(hidden_two, upper_grad)
        out_g = weight_grad(attended, branch_grad)
        qkv_g = weight_grad(hidden_one, qkv_grad)

    mod_grad = rows[:, : 6 * width]
    silu_all = jax.nn.silu(rows[:, -width:]).astype(BF16)
    silu_own = lax.dynamic_slice_in_dim(silu_all, place_f * shard_rows, shard_rows, 1)
    mod_wgrad = lax.dot_general(
        silu_own.astype(F32),
        mod_grad,
        (((0,), (0,)), ((), ())),
        precision=HIGHEST,
        preferred_element_type=F32,
    )
    bias_sum = jnp.sum(rows[:, 6 * width : -width], axis=0)

    def own_bias(low, size):
        own = size // fsdp
        return lax.dynamic_slice_in_dim(bias_sum, low + place_f * own, own, 0)

    up_size = up_b.shape[0]
    out_bg = own_bias(0, width)
    up_bg = own_bias(width, up_size)
    down_bg = own_bias(width + up_size, width)
    qkv_bg = own_bias(2 * width + up_size, 2 * width)
    mod_own = mod_bias.shape[0]
    mod_bg = lax.dynamic_slice_in_dim(jnp.sum(mod_grad, axis=0), place_f * mod_own, mod_own, 0)

    if fast:
        found = cond_parts
    else:
        replica = lax.axis_index("rep")
        per_rep = mod_grad.shape[0] // reps
        own_rep = lax.dynamic_slice_in_dim(mod_grad, replica * per_rep, per_rep, 0)
        silu_grad = lax.dot_general(
            own_rep,
            mod_weight.astype(F32),
            (((1,), (1,)), ((), ())),
            precision=HIGHEST,
            preferred_element_type=F32,
        )
        owners = silu_grad.reshape(fsdp, latents, shard_rows)
        found = lax.all_to_all(owners, "fsdp", 0, 0, tiled=True)
    silu_grad = found.transpose(1, 0, 2).reshape(latents, width)
    conds = condition.astype(F32)
    sigmoid = 1.0 / (1.0 + jnp.exp(-conds))
    condition_grad = silu_grad * (sigmoid * (1.0 + conds * (1.0 - sigmoid)))

    loss_value = (err_total / (width * counted))[0, 0]
    return (
        block_out,
        loss_value,
        tokens_grad,
        condition_grad,
        mod_wgrad,
        mod_bg,
        qkv_g,
        qkv_bg,
        out_g,
        out_bg,
        up_g,
        up_bg,
        down_g,
        down_bg,
    )


def solution(mesh):
    batch = P(("rep", "fsdp"), "seq", None)
    matrix, vector = P("fsdp", None), P("fsdp")
    params = (matrix, vector) * 5
    return jax.shard_map(
        shards,
        mesh=mesh,
        in_specs=(batch, P(("rep", "fsdp"), None), P(("rep", "fsdp"), "seq"), batch, batch)
        + params,
        out_specs=(batch, P(), batch, P(("rep", "fsdp"), None)) + params,
        check_vma=False,
    )
```

```python
import functools

import jax
import jax.numpy as jnp
from jax import lax
from jax.experimental import pallas as pl
from jax.experimental.pallas import tpu as pltpu
from jax.sharding import PartitionSpec as P

HEADS = 16

EPS = 1e-06
GELU_C = 0.7978845608028654
HIGHEST = lax.Precision.HIGHEST
LOG2E = 1.4426950408889634
NEG = -1e30
BF16 = jnp.bfloat16
F32 = jnp.float32
WINDOW = 256
LANES = 128


def flip(array, axis, bit):
    size = lax.axis_size(axis)
    return lax.ppermute(array, axis, [(i, i ^ bit) for i in range(size)])


def pick(array, index):
    return lax.dynamic_index_in_dim(array, index, 0, keepdims=False)


def in_order(first, second, swapped):
    return jnp.where(swapped, jnp.stack([second, first]), jnp.stack([first, second]))


def to_latent(array):
    seq, fsdp = lax.axis_size("seq"), lax.axis_size("fsdp")
    place = lax.axis_index("seq")
    arrived = []
    for turn in range(2):
        pairs = []
        for f in range(fsdp):
            for s in range(seq):
                pair, core = f // 2, f % 2
                target = (pair * 2 + s // 2, 2 * core + (s + turn) % 2)
                pairs.append((f * seq + s, target[0] * seq + target[1]))
        block = pick(array, (place + turn) % 2)
        arrived.append(lax.ppermute(block, ("fsdp", "seq"), pairs))
    both = in_order(arrived[0], arrived[1], place % 2 == 1)
    return both.reshape((-1,) + both.shape[2:])


def from_latent(array):
    seq, fsdp = lax.axis_size("seq"), lax.axis_size("fsdp")
    place = lax.axis_index("seq")
    halves = array.reshape((2, array.shape[0] // 2) + array.shape[1:])
    arrived = []
    for turn in range(2):
        pairs = []
        for f in range(fsdp):
            for s in range(seq):
                pair, core = f // 2, f % 2
                slot = (s + turn) % 2
                target = (pair * 2 + s // 2, 2 * core + slot)
                pairs.append((f * seq + s, target[0] * seq + target[1]))
        arrived.append(lax.ppermute(pick(halves, (place + turn) % 2), ("fsdp", "seq"), pairs))
    return in_order(arrived[0], arrived[1], place % 2 == 1)


def gather_rows(row):
    fsdp = lax.axis_size("fsdp")
    everything = lax.all_gather(row, ("rep", "fsdp", "seq"), axis=0)
    everything = everything.reshape((-1, fsdp // 2, 2, lax.axis_size("seq")) + row.shape)
    return everything[:, :, 0].reshape((-1,) + row.shape)


def gather_weight(weight):
    return lax.all_gather(weight, "fsdp", axis=0, tiled=True)


MESH = pl.DeviceIdType.MESH


class Spot:
    def __init__(self):
        self.x, self.f, self.s = (lax.axis_index(name) for name in ("rep", "fsdp", "seq"))
        self.core = self.f % 2
        self.pair = self.f // 2

    def other(self, bit):
        if bit == 3:
            return 3 - self.f
        return self.f + bit - 2 * bit * ((self.f // bit) % 2)

    def fsdp(self, bit):
        return (self.x, self.other(bit), self.s)

    def rep(self, bit=0):
        return (1 - self.x, self.other(bit) if bit else self.f, self.s)

    def seq(self, step):
        return (self.x, self.f, lax.rem(self.s + step, 4))

    def token_target(self, turn):
        block = lax.rem(self.s + turn, 2)
        return (self.x, 2 * self.pair + self.s // 2, 2 * self.core + block), block


def greet(devices):
    barrier = pltpu.get_barrier_semaphore()
    for device in devices:
        pl.semaphore_signal(barrier, inc=1, device_id=device, device_id_type=MESH)
    pl.semaphore_wait(barrier, len(devices))


def column_group(spot):
    found = [(spot.x, spot.other(1), spot.s)]
    for step in range(1, 4):
        found.append(spot.seq(step))
        found.append((spot.x, spot.other(1), lax.rem(spot.s + step, 4)))
    return found


class Sender:
    def __init__(self, send_sems, recv_sems):
        self.send_sems, self.recv_sems = send_sems, recv_sems
        self.used = 0
        self.open = []

    def slot(self):
        self.used += 1
        return self.used - 1

    def start(self, slot, source, target, device):
        copy = pltpu.make_async_remote_copy(
            source, target, self.send_sems.at[slot], self.recv_sems.at[slot], device, MESH
        )
        copy.start()
        self.open.append(copy)

    def start_if(self, wanted, send_slot, recv_slot, source, target, device):
        copy = pltpu.make_async_remote_copy(
            source, target, self.send_sems.at[send_slot], self.recv_sems.at[recv_slot], device, MESH
        )
        pl.when(wanted)(lambda: copy.start())
        return wanted, copy

    def slots(self, count):
        self.used += count
        return self.used - count

    def sent(self, slot, view):
        pltpu.make_async_copy(view, view, self.send_sems.at[slot]).wait()

    def arrived(self, slot, view):
        pltpu.make_async_copy(view, view, self.recv_sems.at[slot]).wait()

    def finish(self):
        for copy in self.open:
            copy.wait_send()
        self.open = []


class Locals:
    def __init__(self, sems):
        self.sems = sems
        self.used = 0
        self.open = []

    def start(self, source, target):
        copy = pltpu.make_async_copy(source, target, self.sems.at[self.used])
        self.used += 1
        copy.start()
        return copy


class TokenMove:
    def __init__(self, sender, spot, source, target):
        self.sender, self.spot, self.source, self.target = sender, spot, source, target
        self.slots = [sender.slot(), sender.slot()]

    def start(self):
        spot = self.spot
        self.remote = []
        for turn, slot in enumerate(self.slots):
            device, block = spot.token_target(turn)
            stays = (device[1] == spot.f) & (device[2] == spot.s)
            source = self.source.at[block]
            target = self.target.at[lax.rem(spot.s, 2)]
            remote = pltpu.make_async_remote_copy(
                source,
                target,
                self.sender.send_sems.at[slot],
                self.sender.recv_sems.at[slot],
                device,
                MESH,
            )
            local = pltpu.make_async_copy(source, target, self.sender.recv_sems.at[slot])
            pl.when(jnp.logical_not(stays))(lambda remote=remote: remote.start())
            pl.when(stays)(lambda local=local: local.start())
            self.remote.append((stays, remote))

    def finish(self):
        for turn, slot in enumerate(self.slots):
            self.sender.arrived(slot, self.target.at[lax.rem(self.spot.s + turn, 2)])
        for stays, remote in self.remote:
            pl.when(jnp.logical_not(stays))(lambda remote=remote: remote.wait_send())


class WeightMove:
    def __init__(self, sender, local, spot, own, full, stage, chunks):
        self.sender, self.local, self.spot = sender, local, spot
        self.own, self.full, self.stage = own, full, stage
        self.rows, self.chunks = own.shape[0], chunks
        self.half = self.rows // 2
        self.tall = self.half // chunks
        self.slots = {
            kind: [sender.slot() for _ in range(1 if kind == "core" else chunks)]
            for kind in ("core", "far", "side", "far_core", "side_core")
        }

    def view(self, bits, side, chunk):
        shard = self.spot.other(bits) if bits else self.spot.f
        half = self.spot.x if side == 0 else 1 - self.spot.x
        start = shard * self.rows + half * self.half + chunk * self.tall
        return self.full.at[pl.ds(pl.multiple_of(start, 16), self.tall)]

    def shard_view(self, bits):
        shard = self.spot.other(bits) if bits else self.spot.f
        return self.full.at[pl.ds(pl.multiple_of(shard * self.rows, 16), self.rows)]

    def start_far(self):
        spot = self.spot
        for chunk, slot in enumerate(self.slots["far"]):
            start = pl.multiple_of(spot.x * self.half + chunk * self.tall, 16)
            self.sender.start(
                slot, self.own.at[pl.ds(start, self.tall)], self.view(0, 0, chunk), spot.fsdp(2)
            )

    def start_near(self):
        self.sender.start(self.slots["core"][0], self.own, self.shard_view(0), self.spot.fsdp(1))
        self.load = self.local.start(self.own, self.stage)

    def store(self):
        self.load.wait()
        self.kept = self.local.start(self.stage, self.shard_view(0))

    def pass_far(self, chunk):
        view = self.view(2, 0, chunk)
        self.sender.arrived(self.slots["far"][chunk], view)
        self.sender.start(self.slots["side"][chunk], view, view, self.spot.rep())
        self.sender.start(self.slots["far_core"][chunk], view, view, self.spot.fsdp(1))

    def pass_side(self, chunk):
        view = self.view(2, 1, chunk)
        self.sender.arrived(self.slots["side"][chunk], view)
        self.sender.start(self.slots["side_core"][chunk], view, view, self.spot.fsdp(1))

    def finish(self):
        self.kept.wait()
        self.sender.arrived(self.slots["core"][0], self.shard_view(1))
        for chunk in range(self.chunks):
            self.sender.arrived(self.slots["far_core"][chunk], self.view(3, 0, chunk))
            self.sender.arrived(self.slots["side_core"][chunk], self.view(3, 1, chunk))


def entry_kernel(
    tokens,
    valid,
    cond,
    biases,
    mod_weight,
    qkv_weight,
    out_weight,
    tokens_own,
    valid_all,
    mod_parts,
    bias_all,
    qkv_full,
    out_full,
    mod_held,
    cond_held,
    partial,
    qkv_stage,
    out_stage,
    send_sems,
    recv_sems,
    local_sems,
):
    spot = Spot()
    sender, local = Sender(send_sems, recv_sems), Locals(local_sems)
    mod_load = local.start(mod_weight, mod_held)
    greet(column_group(spot) + [spot.fsdp(2), spot.fsdp(3), spot.rep()])

    row = lax.rem(spot.s, 2)
    cond_slots, bias_slots = {}, {}
    for bit in (1, 2, 3):
        cond_slots[bit], bias_slots[bit] = sender.slot(), sender.slot()
        target = spot.other(bit)
        sender.start(
            cond_slots[bit], cond.at[row, target], cond_held.at[spot.f], spot.fsdp(bit)
        )
    for bit in (1, 2, 3):
        sender.start(bias_slots[bit], biases, bias_all.at[spot.f], spot.fsdp(bit))
    cond_own = local.start(cond.at[row, spot.f], cond_held.at[spot.f])
    bias_own = local.start(biases, bias_all.at[spot.f])

    qkv = WeightMove(sender, local, spot, qkv_weight, qkv_full, qkv_stage, 3)
    out = WeightMove(sender, local, spot, out_weight, out_full, out_stage, 1)
    mod_slots = {bit: sender.slot() for bit in (1, 2, 3)}
    move = TokenMove(sender, spot, tokens, tokens_own)
    valid_base = [sender.slot() for _ in range(4)][0]
    valid_open = []
    for turn in range(2):
        device, block = spot.token_target(turn)
        for core in range(2):
            goal = (device[0], 2 * spot.pair + core, device[2])
            stays = (goal[1] == spot.f) & (goal[2] == spot.s)
            source, target = valid.at[block], valid_all.at[spot.s]
            arrival = recv_sems.at[valid_base + spot.s]
            remote = pltpu.make_async_remote_copy(
                source, target, send_sems.at[valid_base + 2 * turn + core], arrival, goal, MESH
            )
            near = pltpu.make_async_copy(source, target, arrival)
            pl.when(jnp.logical_not(stays))(lambda remote=remote: remote.start())
            pl.when(stays)(lambda near=near: near.start())
            valid_open.append((stays, remote))
    move.start()
    qkv.start_far()
    qkv.start_near()
    out.start_near()

    cond_own.wait()
    for bit in (1, 2, 3):
        sender.arrived(cond_slots[bit], cond_held.at[spot.other(bit)])
    first, second = cond_held[spot.s // 2], cond_held[2 + spot.s // 2]
    which = lax.broadcasted_iota(jnp.int32, (16, first.shape[-1]), 0)
    conds = jnp.where(which == 0, first, second)
    silu = (conds / (1.0 + jnp.exp(-conds))).astype(BF16)
    mod_load.wait()
    width = mod_held.shape[1] // 6
    for piece in range(6):
        columns = slice(piece * width, (piece + 1) * width)
        product = jnp.dot(silu, mod_held[:, columns], preferred_element_type=F32)
        partial[0, :, columns] = product[0:1]
        partial[1, :, columns] = product[1:2]
    for bit in (1, 2, 3):
        pair = spot.pair if bit == 1 else 1 - spot.pair
        sender.start(
            mod_slots[bit], partial.at[pair], mod_parts.at[spot.f], spot.fsdp(bit)
        )
    mod_own = local.start(partial.at[spot.pair], mod_parts.at[spot.f])
    out.start_far()
    qkv.store()
    out.store()
    for chunk in range(3):
        qkv.pass_far(chunk)
        if chunk:
            qkv.pass_side(chunk - 1)
    qkv.pass_side(2)
    out.pass_far(0)
    out.pass_side(0)

    bias_own.wait()
    mod_own.wait()
    for bit in (1, 2, 3):
        sender.arrived(bias_slots[bit], bias_all.at[spot.other(bit)])
        sender.arrived(mod_slots[bit], mod_parts.at[spot.other(bit)])
    for place in range(4):
        sender.arrived(valid_base + place, valid_all.at[place])
    for stays, remote in valid_open:
        pl.when(jnp.logical_not(stays))(lambda remote=remote: remote.wait_send())
    move.finish()
    qkv.finish()
    out.finish()
    sender.finish()


def sems(count):
    return pltpu.SemaphoreType.DMA((count,))


def enter(tokens, valid, cond, biases, mod_weight, qkv_weight, out_weight):
    anywhere = pl.BlockSpec(memory_space=pl.ANY)
    return pl.pallas_call(
        entry_kernel,
        out_shape=[
            jax.ShapeDtypeStruct(tokens.shape, tokens.dtype),
            jax.ShapeDtypeStruct((4,) + valid.shape[1:], F32),
            jax.ShapeDtypeStruct((4, 1, mod_weight.shape[1]), F32),
            jax.ShapeDtypeStruct((4,) + biases.shape, F32),
            jax.ShapeDtypeStruct((4 * qkv_weight.shape[0], qkv_weight.shape[1]), BF16),
            jax.ShapeDtypeStruct((4 * out_weight.shape[0], out_weight.shape[1]), BF16),
        ],
        in_specs=[anywhere] * 7,
        out_specs=[anywhere] * 6,
        scratch_shapes=[
            pltpu.VMEM(mod_weight.shape, BF16),
            pltpu.VMEM((4,) + cond.shape[2:], F32),
            pltpu.VMEM((2, 1, mod_weight.shape[1]), F32),
            pltpu.VMEM(qkv_weight.shape, BF16),
            pltpu.VMEM(out_weight.shape, BF16),
            sems(40),
            sems(40),
            sems(12),
        ],
        compiler_params=pltpu.CompilerParams(
            collective_id=1, has_side_effects=True, vmem_limit_bytes=67043328
        ),
        name="enter",
    )(tokens, valid, cond, biases, mod_weight, qkv_weight, out_weight)


class TokenReturn:
    def __init__(self, sender, spot, source, target):
        self.sender, self.spot, self.source, self.target = sender, spot, source, target
        self.slots = [sender.slot(), sender.slot()]

    def start(self):
        spot = self.spot
        self.remote = []
        for turn, slot in enumerate(self.slots):
            half = lax.rem(spot.s + turn, 2)
            device = (spot.x, 2 * spot.pair + spot.s // 2, 2 * spot.core + half)
            stays = (device[1] == spot.f) & (device[2] == spot.s)
            source, target = self.source.at[half], self.target.at[lax.rem(spot.s, 2)]
            arrival = self.sender.recv_sems.at[slot]
            remote = pltpu.make_async_remote_copy(
                source, target, self.sender.send_sems.at[slot], arrival, device, MESH
            )
            local = pltpu.make_async_copy(source, target, arrival)
            pl.when(jnp.logical_not(stays))(lambda remote=remote: remote.start())
            pl.when(stays)(lambda local=local: local.start())
            self.remote.append((stays, remote))

    def finish(self):
        for turn, slot in enumerate(self.slots):
            self.sender.arrived(slot, self.target.at[lax.rem(self.spot.s + turn, 2)])
        for stays, remote in self.remote:
            pl.when(jnp.logical_not(stays))(lambda remote=remote: remote.wait_send())


ORDER = (0, 3, 1, 2)
STRIP = 64


def row_norm(inputs):
    centred = inputs - jnp.mean(inputs, axis=-1, keepdims=True)
    rate = lax.rsqrt(jnp.mean(centred * centred, axis=-1, keepdims=True) + EPS)
    return centred * rate, rate


class ColumnStream:
    def __init__(self, local, source, held, width):
        self.local, self.source, self.held, self.width = local, source, held, width
        self.base = local.used
        local.used += 2

    def copy(self, j):
        return pltpu.make_async_copy(
            self.source.at[:, pl.ds(j * self.width, self.width)],
            self.held.at[j % 2],
            self.local.sems.at[self.base + j % 2],
        )

    def start(self, j):
        self.copy(j).start()

    def wait(self, j):
        self.copy(j).wait()
        return self.held[j % 2]


class GradMove:
    def __init__(self, sender, local, spot, far, side, depth, total, final):
        self.sender, self.local, self.spot = sender, local, spot
        self.far, self.side, self.depth, self.total, self.final = far, side, depth, total, final
        self.tall = total.shape[0]
        self.y, self.x, self.z, self.g, self.fx = (sender.slots(4) for _ in range(5))
        self.kept = local.used
        local.used += 1
        self.z_open = []

    def send_far(self, j, give):
        self.sender.start(self.y + j, give, self.far.at[j], self.spot.fsdp(2))

    def half(self, side):
        return pl.ds(pl.multiple_of(side * self.tall, 16), self.tall)

    def fold(self, j, kept, arrives=True):
        if arrives:
            self.sender.arrived(self.y + j, self.far.at[j])
        self.far[j] = (self.far[j].astype(F32) + kept.astype(F32)).astype(BF16)
        self.sender.start(
            self.x + j, self.far.at[j, self.half(1 - self.spot.x)], self.side.at[j], self.spot.rep()
        )

    def cross(self, j):
        spot = self.spot
        self.sender.arrived(self.x + j, self.side.at[j])
        mine = self.far[j, self.half(spot.x), :].astype(F32)
        self.side[j] = (mine + self.side[j].astype(F32)).astype(BF16)
        step = lax.rem(spot.s - j + 4, 4)
        index = jnp.maximum(step - 1, 0)
        self.z_open.append(
            self.sender.start_if(
                spot.s != j,
                self.z + j,
                self.z + index,
                self.side.at[j],
                self.depth.at[index],
                (spot.x, spot.f, j),
            )
        )

    def gather(self, j):
        @pl.when(self.spot.s == j)
        def _():
            total = self.side[j].astype(F32)
            for index in range(3):
                self.sender.arrived(self.z + index, self.depth.at[index])
                total = total + self.depth[index].astype(F32)
            self.total[...] = total.astype(BF16)

    def give_back(self, j):
        spot, sender = self.spot, self.sender
        target = self.final.at[j, spot.x]

        @pl.when(spot.s == j)
        def _():
            for step in range(1, 4):
                pltpu.make_async_remote_copy(
                    self.total,
                    target,
                    sender.send_sems.at[self.g + step],
                    sender.recv_sems.at[self.g + j],
                    (spot.x, spot.f, (j + step) % 4),
                    MESH,
                ).start()
            pltpu.make_async_remote_copy(
                self.total,
                target,
                sender.send_sems.at[self.fx + j],
                sender.recv_sems.at[self.fx + j],
                spot.rep(),
                MESH,
            ).start()
            pltpu.make_async_copy(self.total, target, self.local.sems.at[self.kept]).start()

    def settle(self, j):
        self.gather(j)
        self.give_back(j)

    def pass_on(self, j):
        spot, sender = self.spot, self.sender
        target = self.final.at[j, spot.x]

        @pl.when(spot.s != j)
        def _():
            sender.arrived(self.g + j, target)
            pltpu.make_async_remote_copy(
                target,
                target,
                sender.send_sems.at[self.fx + j],
                sender.recv_sems.at[self.fx + j],
                spot.rep(),
                MESH,
            ).start()

    def finish_sums(self):
        for wanted, copy in self.z_open:
            pl.when(wanted)(lambda copy=copy: copy.wait_send())

    def finish_back(self):
        spot, sender = self.spot, self.sender
        for j in range(4):
            sender.arrived(self.fx + j, self.final.at[j, 1 - spot.x])
            sender.sent(self.fx + j, self.total)
        for step in range(1, 4):
            sender.sent(self.g + step, self.total)
        pltpu.make_async_copy(self.total, self.total, self.local.sems.at[self.kept]).wait()

    def finish(self):
        self.finish_sums()
        self.finish_back()


DOWN = (((0,), (0,)), ((), ()))


def outer(left_own, left_other, right_own, right_other):
    total = lax.dot_general(left_own, right_own, DOWN, preferred_element_type=F32)
    return total + lax.dot_general(left_other, right_other, DOWN, preferred_element_type=F32)


def lane_block(index, size):
    return pl.ds(pl.multiple_of(index * size, LANES), size)


def middle_kernel(
    grad_mlp,
    grad_out,
    middle,
    branch,
    stretch,
    gate,
    error_in,
    activated,
    slope,
    hidden,
    down_full,
    up_full,
    out_full,
    block_out,
    attended_grad,
    branch_grad,
    middle_grad,
    sums,
    error_out,
    up_total,
    down_final,
    upper_other,
    block_back,
    act_give,
    act_keep,
    act_give_other,
    act_keep_other,
    mlp_other,
    hid,
    held,
    slopes,
    uppers,
    others,
    hidden_grad,
    out_held,
    give,
    kept,
    far,
    side,
    depth,
    total,
    up_far,
    up_side,
    up_depth,
    errors,
    send_sems,
    recv_sems,
    local_sems,
):
    spot = Spot()
    sender, local = Sender(send_sems, recv_sems), Locals(local_sems)
    tokens, width = grad_mlp.shape
    shard = activated.shape[1] // 4
    f, core = spot.f, spot.fsdp(1)
    loads = [
        local.start(activated.at[:, lane_block(spot.other(2), shard)], act_give),
        local.start(activated.at[:, lane_block(f, shard)], act_keep),
        local.start(hidden.at[spot.other(2)], hid.at[0]),
        local.start(hidden.at[f], hid.at[1]),
    ]
    out_load = local.start(out_full, out_held)
    base = local.used
    local.used += 6

    def weight_copy(number, which):
        units = pl.ds(ORDER[number] * width, width)
        if which == 0:
            return pltpu.make_async_copy(down_full.at[units], held.at[0], local.sems.at[base])
        if which == 1:
            slot = number % 2
            return pltpu.make_async_copy(
                slope.at[:, units], slopes.at[slot], local.sems.at[base + 1 + slot]
            )
        return pltpu.make_async_copy(up_full.at[:, units], held.at[1], local.sems.at[base + 3])

    def other_copy(number):
        slot = number % 2
        return pltpu.make_async_copy(
            upper_other.at[ORDER[number]], others.at[slot], local.sems.at[base + 4 + slot]
        )

    for which in range(3):
        weight_copy(0, which).start()
    greet(column_group(spot) + [spot.fsdp(2), spot.rep()])
    error_slots = [sender.slot() for _ in range(3)]
    error_z = sender.slots(4)
    sender.start(error_slots[0], error_in, errors.at[4], core)
    pieces = [sender.slot() for _ in range(5)]
    upper_slots = sender.slots(4)
    sender.start(
        pieces[0], activated.at[:, lane_block(spot.other(3), shard)], act_give_other, core
    )
    sender.start(pieces[1], grad_mlp, mlp_other, core)
    sender.start(
        pieces[2], activated.at[:, lane_block(spot.other(1), shard)], act_keep_other, core
    )
    sender.start(pieces[3], hidden.at[spot.other(3)], hid.at[2], core)
    sender.start(pieces[4], hidden.at[spot.other(1)], hid.at[3], core)
    back = TokenReturn(sender, spot, block_out, block_back)
    down = GradMove(sender, local, spot, far, side, depth, total, down_final)
    up = GradMove(sender, local, spot, up_far, up_side, up_depth, up_total, None)

    sender.arrived(error_slots[0], errors.at[4])
    errors[5] = error_in[...] + errors[4]
    sender.start(error_slots[1], errors.at[5], errors.at[6], spot.fsdp(2))
    for load in loads[:2]:
        load.wait()
    sender.arrived(pieces[0], act_give_other)
    sender.arrived(error_slots[1], errors.at[6])
    errors[7] = errors[5] + errors[6]
    sender.start(error_slots[2], errors.at[7], errors.at[8], spot.rep())
    sender.arrived(pieces[1], mlp_other)
    block = 384

    def fill(target, left, left_other):
        def body(i, carry):
            columns = lane_block(i, block)
            rows = pl.ds(pl.multiple_of(i * block, 16), block)
            target[rows, :] = outer(
                left[:, columns], left_other[:, columns], grad_mlp[...], mlp_other[...]
            ).astype(BF16)
            return carry

        lax.fori_loop(0, shard // block, body, 0)

    tall = shard // 4
    fill(give.at[0], act_give, act_give_other)
    for j in ORDER:
        down.send_far(j, give.at[0, pl.ds(j * tall, tall)])
    sender.arrived(error_slots[2], errors.at[8])
    errors[spot.s] = errors[7] + errors[8]
    error_open = []
    for step in range(1, 4):
        copy = pltpu.make_async_remote_copy(
            errors.at[spot.s],
            errors.at[spot.s],
            send_sems.at[error_z + step],
            recv_sems.at[error_z + spot.s],
            spot.seq(step),
            MESH,
        )
        copy.start()
        error_open.append(copy)
    back.start()
    sender.arrived(pieces[2], act_keep_other)
    fill(kept.at[0], act_keep, act_keep_other)

    across = (((1,), (1,)), ((), ()))
    sums[...] = jnp.zeros_like(sums)

    def upper(number):
        j = ORDER[number]
        weight_copy(number, 0).wait()
        weight_copy(number, 1).wait()
        grad = lax.dot_general(grad_mlp[...], held[0], across, preferred_element_type=F32)
        grad = (grad * slopes[number % 2].astype(F32)).astype(BF16)
        uppers[j] = grad
        sender.start(upper_slots + j, uppers.at[j], upper_other.at[j], core)
        if number < 3:
            weight_copy(number + 1, 0).start()
            weight_copy(number + 1, 1).start()
        weight_copy(number, 2).wait()
        product = lax.dot_general(uppers[j], held[1], across, preferred_element_type=F32)
        if number == 0:
            hidden_grad[...] = product
        else:
            hidden_grad[...] += product
        if number < 3:
            weight_copy(number + 1, 2).start()
        sums[5 + j : 6 + j, :] = jnp.sum(uppers[j].astype(F32), axis=0, keepdims=True)

    def up_outer(number):
        j = ORDER[number]
        other_copy(number).wait()
        if number < 3:
            sender.arrived(upper_slots + ORDER[number + 1], upper_other.at[ORDER[number + 1]])
            other_copy(number + 1).start()
        rows = pl.ds(j * tall, tall)
        right_other = others[number % 2]
        give[1, rows, :] = outer(hid[0], hid[2], uppers[j], right_other).astype(BF16)
        up.send_far(j, give.at[1, rows])
        kept[1, rows, :] = outer(hid[1], hid[3], uppers[j], right_other).astype(BF16)

    def fold(group, index, j):
        group.fold(j, kept[index, pl.ds(j * tall, tall), :])

    a, b, c, d = ORDER
    upper(0)
    fold(down, 0, a)
    upper(1)
    down.cross(a)
    upper(2)
    fold(down, 0, b)
    upper(3)
    down.cross(b)
    for load in loads[2:]:
        load.wait()
    for slot, place in ((3, 2), (4, 3)):
        sender.arrived(pieces[slot], hid.at[place])
    sender.arrived(upper_slots + a, upper_other.at[a])
    other_copy(0).start()
    up_outer(0)
    up_outer(1)
    fold(down, 0, c)
    up_outer(2)
    up_outer(3)
    down.cross(c)
    down.settle(a)

    def strip_step(i, found):
        strip = pl.ds(pl.multiple_of(i * STRIP, STRIP), STRIP)
        normed, rate = row_norm(middle[strip, :])
        grad = hidden_grad[strip, :]
        scaled = grad * (1.0 + stretch[...])
        result = grad_out[strip, :] + rate * (
            scaled
            - jnp.mean(scaled, axis=-1, keepdims=True)
            - normed * jnp.mean(scaled * normed, axis=-1, keepdims=True)
        )
        middle_grad[strip, :] = result
        low = (result * gate[...]).astype(BF16)
        branch_grad[strip, :] = low
        terms = (
            result * branch[strip, :],
            grad,
            grad * normed,
            low.astype(F32),
            grad_mlp[strip, :].astype(F32),
        )
        return tuple(
            kept_sum + jnp.sum(term, axis=0, keepdims=True)
            for kept_sum, term in zip(found, terms, strict=True)
        )

    zero = jnp.zeros((1, width), F32)
    found = lax.fori_loop(0, tokens // STRIP, strip_step, (zero,) * 5)
    for place, value in zip((0, 1, 2, 4, 9), found, strict=True):
        sums[place : place + 1, :] = value
    fold(down, 0, d)
    out_load.wait()
    attended_grad[...] = lax.dot_general(
        branch_grad[...], out_held[...], across, preferred_element_type=F32
    ).astype(BF16)
    down.cross(d)
    down.settle(b)
    fold(up, 1, a)
    down.settle(c)
    up.cross(a)
    fold(up, 1, b)
    down.settle(d)
    up.cross(b)
    down.pass_on(a)
    fold(up, 1, c)
    down.pass_on(b)
    up.cross(c)
    down.pass_on(c)
    for place in range(4):

        @pl.when(spot.s != place)
        def _():
            sender.arrived(error_z + place, errors.at[place])

    error_out[...] = errors[0] + errors[1] + errors[2] + errors[3]
    for copy in error_open:
        copy.wait_send()
    fold(up, 1, d)
    down.pass_on(d)
    up.cross(d)
    up.gather(a)
    up.gather(b)
    up.gather(c)
    back.finish()
    down.finish()
    up.gather(d)
    up.finish_sums()
    sender.finish()


def middle_back(near_operands, activated, slope, hidden, down_full, up_full, out_full, block_out):
    grad_mlp = near_operands[0]
    error = near_operands[-1]
    tokens, width = grad_mlp.shape
    shape = (tokens, width)
    shard = activated.shape[1] // 4
    tall = shard // 4
    anywhere = pl.BlockSpec(memory_space=pl.ANY)
    near = pl.BlockSpec(memory_space=pltpu.VMEM)
    piece = (tall // 2, width)
    return pl.pallas_call(
        middle_kernel,
        out_shape=[
            jax.ShapeDtypeStruct(shape, BF16),
            jax.ShapeDtypeStruct(shape, BF16),
            jax.ShapeDtypeStruct(shape, F32),
            jax.ShapeDtypeStruct((ROW_PARTS, width), F32),
            jax.ShapeDtypeStruct(error.shape, F32),
            jax.ShapeDtypeStruct(piece, BF16),
            jax.ShapeDtypeStruct((4, 2) + piece, BF16),
            jax.ShapeDtypeStruct((4,) + shape, BF16),
            jax.ShapeDtypeStruct(block_out.shape, BF16),
        ],
        in_specs=[near] * len(near_operands) + [anywhere] * 7,
        out_specs=[near] * 6 + [anywhere] * 3,
        scratch_shapes=[
            pltpu.VMEM((tokens, shard), BF16),
            pltpu.VMEM((tokens, shard), BF16),
            pltpu.VMEM((tokens, shard), BF16),
            pltpu.VMEM((tokens, shard), BF16),
            pltpu.VMEM(shape, BF16),
            pltpu.VMEM((4,) + hidden.shape[1:], BF16),
            pltpu.VMEM((2, width, width), BF16),
            pltpu.VMEM((2,) + shape, BF16),
            pltpu.VMEM((4,) + shape, BF16),
            pltpu.VMEM((2,) + shape, BF16),
            pltpu.VMEM(shape, F32),
            pltpu.VMEM(out_full.shape, BF16),
            pltpu.VMEM((2, shard, width), BF16),
            pltpu.VMEM((2, shard, width), BF16),
            pltpu.VMEM((4, tall, width), BF16),
            pltpu.VMEM((4,) + piece, BF16),
            pltpu.VMEM((3,) + piece, BF16),
            pltpu.VMEM(piece, BF16),
            pltpu.VMEM((4, tall, width), BF16),
            pltpu.VMEM((4,) + piece, BF16),
            pltpu.VMEM((3,) + piece, BF16),
            pltpu.VMEM((9,) + error.shape, F32),
            sems(72),
            sems(72),
            sems(20),
        ],
        compiler_params=pltpu.CompilerParams(
            collective_id=3, has_side_effects=True, vmem_limit_bytes=67043328
        ),
        name="middle_back",
    )(*near_operands, activated, slope, hidden, down_full, up_full, out_full, block_out)


ROW_PARTS = 16


def finish_kernel(*refs):
    (
        branch_grad,
        up_total,
        middle_grad,
        inputs,
        stretch,
        q_ref,
        k_own,
        v_own,
        k_other,
        v_other,
        do_ref,
        lse_ref,
        bias_own,
        bias_other,
        sums_in,
        gate_sum,
        cond_part,
        attended,
        hidden,
        mod_weight,
        qkv_full,
        rows,
        cond_parts,
        up_final,
        tail_final,
        tokens_back,
        branch_other,
        qkv_grad,
        qkv_other,
        att,
        hid,
        mod_held,
        qkv_held,
        hidden_grad,
        dv_one,
        dk_two,
        dv_two,
        dk_in,
        dv_in,
        tokens_grad,
        give,
        far,
        side,
        depth,
        total,
        row,
        row_in,
        cond_send,
        send_sems,
        recv_sems,
        local_sems,
    ) = refs
    spot = Spot()
    sender, local = Sender(send_sems, recv_sems), Locals(local_sems)
    width = branch_grad.shape[1]
    f, core = spot.f, spot.fsdp(1)
    loads = [
        local.start(attended.at[spot.other(2)], att.at[0]),
        local.start(attended.at[f], att.at[1]),
        local.start(hidden.at[spot.other(2)], hid.at[0]),
        local.start(hidden.at[f], hid.at[1]),
    ]
    mod_load = local.start(mod_weight, mod_held)
    stream = ColumnStream(local, qkv_full, qkv_held, width)
    stream.start(0)
    stream.start(1)
    greet(column_group(spot) + [spot.fsdp(2), spot.fsdp(3), spot.rep()])
    slots = [sender.slot() for _ in range(6)]
    sender.start(slots[0], attended.at[spot.other(3)], att.at[2], core)
    sender.start(slots[1], branch_grad, branch_other, core)
    sender.start(slots[2], hidden.at[spot.other(3)], hid.at[2], core)
    sender.start(slots[4], attended.at[spot.other(1)], att.at[3], core)
    sender.start(slots[5], hidden.at[spot.other(1)], hid.at[3], core)
    up = GradMove(sender, local, spot, None, None, None, up_total, up_final)
    tail = GradMove(sender, local, spot, far, side, depth, total, tail_final)
    back = TokenReturn(sender, spot, tokens_grad, tokens_back)
    row_slot = sender.slot()
    row_z, row_y, row_x = sender.slots(4), sender.slot(), sender.slot()
    cond_slots = {bit: sender.slot() for bit in (1, 2, 3)}
    dk_slot, dv_slot = sender.slot(), sender.slot()
    for j in ORDER:
        up.give_back(j)
    for load in loads:
        load.wait()

    def operands(j):
        if j == 0:
            return att, branch_grad[...], branch_other[...]
        columns = slice((j - 1) * width, j * width)
        return hid, qkv_grad[:, columns], qkv_other[:, columns]

    def give_far(j):
        left, right, right_other = operands(j)
        give[j] = outer(left[0], left[2], right, right_other).astype(BF16)
        tail.send_far(j, give.at[j])

    a, b, c, d = ORDER
    sender.arrived(slots[0], att.at[2])
    sender.arrived(slots[1], branch_other)
    give_far(a)
    data = (
        q_ref,
        k_own,
        v_own,
        k_other,
        v_other,
        do_ref,
        lse_ref,
        bias_own,
        bias_other,
        qkv_grad.at[:, pl.ds(0, width)],
        hidden_grad,
        dv_one,
        dk_two,
        dv_two,
    )
    sender.arrived(slots[4], att.at[3])

    def fold(j):
        left, right, right_other = operands(j)
        tail.fold(j, outer(left[1], left[3], right, right_other))

    backward_heads(0, 5, *data)
    up.pass_on(a)
    backward_heads(5, 10, *data)
    fold(a)
    up.pass_on(b)
    backward_heads(10, HEADS, *data)
    sender.start(dk_slot, dk_two, dk_in, core)
    sender.start(dv_slot, dv_two, dv_in, core)
    tail.cross(a)
    sender.arrived(dk_slot, dk_in)
    qkv_grad[:, width : 2 * width] = (hidden_grad[...] + dk_in[...].astype(F32)).astype(BF16)
    sender.arrived(dv_slot, dv_in)
    qkv_grad[:, 2 * width :] = (dv_one[...] + dv_in[...].astype(F32)).astype(BF16)
    sender.start(slots[3], qkv_grad, qkv_other, core)

    across = (((1,), (1,)), ((), ()))
    for j in range(3):
        product = lax.dot_general(
            qkv_grad[:, j * width : (j + 1) * width],
            stream.wait(j),
            across,
            preferred_element_type=F32,
        )
        if j == 0:
            hidden_grad[...] = product
            stream.start(2)
        else:
            hidden_grad[...] += product
    sender.arrived(slots[2], hid.at[2])
    sender.arrived(slots[3], qkv_other)
    give_far(b)
    give_far(c)
    give_far(d)

    def norm_step(i, sums):
        strip = pl.ds(pl.multiple_of(i * STRIP, STRIP), STRIP)
        normed, rate = row_norm(inputs[strip, :].astype(F32))
        grad = hidden_grad[strip, :]
        scaled = grad * (1.0 + stretch[...])
        result = middle_grad[strip, :] + rate * (
            scaled
            - jnp.mean(scaled, axis=-1, keepdims=True)
            - normed * jnp.mean(scaled * normed, axis=-1, keepdims=True)
        )
        tokens_grad[i // per_half, pl.ds(pl.multiple_of((i % per_half) * STRIP, STRIP), STRIP), :] = (
            result.astype(BF16)
        )
        return (
            sums[0] + jnp.sum(grad, axis=0, keepdims=True),
            sums[1] + jnp.sum(grad * normed, axis=0, keepdims=True),
            sums[2] + jnp.sum(qkv_grad[strip, :width].astype(F32), axis=0, keepdims=True),
            sums[3] + jnp.sum(qkv_grad[strip, 2 * width :].astype(F32), axis=0, keepdims=True),
        )

    per_half = tokens_grad.shape[1] // STRIP
    zero = jnp.zeros((1, width), F32)
    sums = lax.fori_loop(0, 2 * per_half, norm_step, (zero,) * 4)
    row[0:2, :] = jnp.concatenate(sums[:2], axis=0)
    row[2:, :] = sums_in[: ROW_PARTS - 2, :]
    row[5:6, :] = gate_sum[...]
    row[12:15, :] = jnp.concatenate(sums[2:] + (cond_part[...],), axis=0)
    sender.start(row_slot, row, row_in, core)
    sender.arrived(row_slot, row_in)
    column = (spot.x * 2 + spot.pair) * 4
    rows[column + spot.s] = row[...] + row_in[...]
    row_open = []
    for step in range(1, 4):
        copy = pltpu.make_async_remote_copy(
            rows.at[column + spot.s],
            rows.at[column + spot.s],
            send_sems.at[row_z + step],
            recv_sems.at[row_z + spot.s],
            spot.seq(step),
            MESH,
        )
        copy.start()
        row_open.append(copy)
    back.start()
    sender.arrived(slots[5], hid.at[3])
    fold(b)
    tail.cross(b)
    for place in range(4):

        @pl.when(spot.s != place)
        def _():
            sender.arrived(row_z + place, rows.at[column + place])

    span = pl.ds(column, 4)
    sender.start(row_y, rows.at[span], rows.at[span], spot.fsdp(2))
    fold(c)
    up.pass_on(c)
    tail.cross(c)
    tail.settle(a)
    fold(d)
    tail.cross(d)
    up.pass_on(d)
    far_column = (spot.x * 2 + 1 - spot.pair) * 4
    sender.arrived(row_y, rows.at[pl.ds(far_column, 4)])
    half = pl.ds(spot.x * 8, 8)
    sender.start(row_x, rows.at[half], rows.at[half], spot.rep())
    tail.settle(b)
    tail.settle(c)

    mod_load.wait()
    products = jnp.zeros((16, mod_held.shape[0]), F32)
    for part in range(6):
        grad = rows[half, part, :]
        high = grad.astype(BF16)
        low = (grad - high.astype(F32)).astype(BF16)
        products += lax.dot_general(
            jnp.concatenate([high, low], axis=0),
            mod_held[:, part * width : (part + 1) * width],
            (((1,), (1,)), ((), ())),
            preferred_element_type=F32,
        )
    silu_grad = products[:8] + products[8:]
    for latent in range(8):
        cond_send[latent // 2, latent % 2 : latent % 2 + 1, :] = silu_grad[latent : latent + 1]
    cond_parts[f] = cond_send[f]
    for bit in (1, 2, 3):
        sender.start(
            cond_slots[bit], cond_send.at[spot.other(bit)], cond_parts.at[f], spot.fsdp(bit)
        )

    tail.pass_on(a)
    tail.settle(d)
    tail.pass_on(b)
    tail.pass_on(c)
    tail.pass_on(d)
    for bit in (1, 2, 3):
        sender.arrived(cond_slots[bit], cond_parts.at[spot.other(bit)])
    sender.arrived(row_x, rows.at[pl.ds((1 - spot.x) * 8, 8)])
    for copy in row_open:
        copy.wait_send()
    back.finish()
    up.finish_back()
    tail.finish()
    sender.finish()


def finish(near_operands, attended, hidden, mod_weight, qkv_full, token_shape):
    branch_grad, up_total = near_operands[:2]
    tokens, width = branch_grad.shape
    shape = (tokens, width)
    piece = up_total.shape
    anywhere = pl.BlockSpec(memory_space=pl.ANY)
    near = pl.BlockSpec(memory_space=pltpu.VMEM)
    final = jax.ShapeDtypeStruct((4, 2) + piece, BF16)
    tall = 2 * piece[0]
    return pl.pallas_call(
        finish_kernel,
        out_shape=[
            jax.ShapeDtypeStruct((16, ROW_PARTS, width), F32),
            jax.ShapeDtypeStruct((4, 2, mod_weight.shape[0]), F32),
            final,
            final,
            jax.ShapeDtypeStruct(token_shape, BF16),
        ],
        in_specs=[near] * len(near_operands) + [anywhere] * 4,
        out_specs=[near] * 2 + [anywhere] * 3,
        scratch_shapes=[
            pltpu.VMEM(shape, BF16),
            pltpu.VMEM((tokens, 3 * width), BF16),
            pltpu.VMEM((tokens, 3 * width), BF16),
            pltpu.VMEM((4,) + attended.shape[1:], BF16),
            pltpu.VMEM((4,) + hidden.shape[1:], BF16),
            pltpu.VMEM(mod_weight.shape, BF16),
            pltpu.VMEM((2, width, width), BF16),
            pltpu.VMEM(shape, F32),
            pltpu.VMEM(shape, F32),
            pltpu.VMEM(shape, BF16),
            pltpu.VMEM(shape, BF16),
            pltpu.VMEM(shape, BF16),
            pltpu.VMEM(shape, BF16),
            pltpu.VMEM(token_shape, BF16),
            pltpu.VMEM((4, tall, width), BF16),
            pltpu.VMEM((4, tall, width), BF16),
            pltpu.VMEM((4,) + piece, BF16),
            pltpu.VMEM((3,) + piece, BF16),
            pltpu.VMEM(piece, BF16),
            pltpu.VMEM((ROW_PARTS, width), F32),
            pltpu.VMEM((ROW_PARTS, width), F32),
            pltpu.VMEM((4, 2, mod_weight.shape[0]), F32),
            sems(72),
            sems(72),
            sems(24),
        ],
        compiler_params=pltpu.CompilerParams(
            collective_id=4, has_side_effects=True, vmem_limit_bytes=67043328
        ),
        name="finish",
    )(*near_operands, attended, hidden, mod_weight, qkv_full)


def spread_kernel(block, out):
    out[...] = block[0].astype(F32)


def spread(blocks):
    count, rows, width = blocks.shape
    return pl.pallas_call(
        spread_kernel,
        grid=(count,),
        out_shape=jax.ShapeDtypeStruct((rows, count * width), F32),
        in_specs=[pl.BlockSpec((1, rows, width), lambda j: (j, 0, 0))],
        out_specs=pl.BlockSpec((rows, width), lambda j: (0, j)),
        name="spread",
    )(blocks)


def head_window(head, head_dim, width):
    start = head * head_dim
    base = jnp.minimum(start // LANES, (width - WINDOW) // LANES) * LANES
    base = pl.multiple_of(base, LANES)
    return start, base


def forward_heads(
    low,
    high,
    q_ref,
    k_own,
    v_own,
    k_other,
    v_other,
    bias_own,
    bias_other,
    out_ref,
    lse_ref,
):
    tokens, width = q_ref.shape
    head_dim = width // HEADS
    blocks = 2
    tall = tokens // blocks
    scale = head_dim ** (-0.5) * LOG2E
    b_own, b_other = bias_own[...], bias_other[...]
    dims = (((1,), (1,)), ((), ()))

    def body(head, carry):
        start, base = head_window(head, head_dim, width)
        window = pl.ds(base, WINDOW)
        lane = lax.broadcasted_iota(jnp.int32, (1, WINDOW), 1) + base
        inside = (lane >= start) & (lane < start + head_dim)
        keep = inside.astype(BF16)
        spot = lax.broadcasted_iota(jnp.int32, (1, LANES), 1) == head
        key_one, key_two = k_own[:, window], k_other[:, window]
        val_one, val_two = v_own[:, window] * keep, v_other[:, window] * keep
        for block in range(blocks):
            rows = pl.ds(block * tall, tall)
            query = q_ref[rows, window] * keep
            one = lax.dot_general(query, key_one, dims, preferred_element_type=F32)
            two = lax.dot_general(query, key_two, dims, preferred_element_type=F32)
            one = one * scale + b_own
            two = two * scale + b_other
            top = jnp.maximum(
                jnp.max(one, axis=1, keepdims=True), jnp.max(two, axis=1, keepdims=True)
            )
            one = jnp.exp2(one - top)
            two = jnp.exp2(two - top)
            total = jnp.sum(one, axis=1, keepdims=True) + jnp.sum(two, axis=1, keepdims=True)
            mixed = jnp.dot(one.astype(BF16), val_one, preferred_element_type=F32)
            mixed += jnp.dot(two.astype(BF16), val_two, preferred_element_type=F32)
            mixed = mixed * (1.0 / total)
            out_ref[rows, window] = jnp.where(
                inside, mixed, out_ref[rows, window].astype(F32)
            ).astype(out_ref.dtype)
            lse_ref[rows, :] = jnp.where(spot, top + jnp.log2(total), lse_ref[rows, :])
        return carry

    lax.fori_loop(low, high, body, 0)


def forward_kernel(*refs):
    out_ref, lse_ref = refs[-2:]
    out_ref[...] = jnp.zeros_like(out_ref)
    lse_ref[...] = jnp.zeros_like(lse_ref)
    forward_heads(0, HEADS, *refs)


def forward_send_kernel(
    inputs,
    shift,
    stretch,
    q_bias,
    v_bias,
    bias_own,
    bias_other,
    gate,
    out_bias,
    shift_two,
    stretch_two,
    up_bias,
    count_in,
    qkv_full,
    out_full,
    up_weight,
    down_weight,
    teacher,
    out_grad,
    hidden,
    q_ref,
    k_own,
    v_own,
    out_ref,
    lse_ref,
    k_other,
    v_other,
    hidden_two,
    count_out,
    up_full,
    down_full,
    teacher_own,
    out_grad_own,
    middle_out,
    branch_out,
    activated,
    slope,
    qkv_held,
    middle,
    branch,
    upper,
    values,
    slopes,
    counts,
    count_sum,
    far_counts,
    up_stage,
    down_stage,
    send_sems,
    recv_sems,
    local_sems,
):
    spot = Spot()
    sender, local = Sender(send_sems, recv_sems), Locals(local_sems)
    width = q_ref.shape[1]
    stream = ColumnStream(local, qkv_full, qkv_held, width)
    stream.start(0)
    stream.start(1)
    greet(column_group(spot) + [spot.fsdp(2), spot.rep(), spot.rep(2)])
    count_slots = [sender.slot() for _ in range(3)]
    for step in range(1, 4):
        sender.start(count_slots[step - 1], count_in, counts.at[step - 1], spot.seq(step))
    key_slot, value_slot = sender.slot(), sender.slot()
    moves = [
        TokenMove(sender, spot, teacher, teacher_own),
        TokenMove(sender, spot, out_grad, out_grad_own),
    ]
    up = WeightMove(sender, local, spot, up_weight, up_full, up_stage, 3)
    down = WeightMove(sender, local, spot, down_weight, down_full, down_stage, 4)
    far_slots = [sender.slot() for _ in range(3)]

    up.start_far()
    down.start_far()
    for move in moves:
        move.start()

    def normalise(i, carry):
        rows = pl.ds(pl.multiple_of(i * STRIP, STRIP), STRIP)
        normed, _ = row_norm(inputs[rows, :].astype(F32))
        hidden[rows, :] = (normed * (1.0 + stretch[...]) + shift[...]).astype(BF16)
        return carry

    lax.fori_loop(0, q_ref.shape[0] // STRIP, normalise, 0)
    q_ref[...] = (
        jnp.dot(hidden[...], stream.wait(0), preferred_element_type=F32) + q_bias[...]
    ).astype(BF16)
    stream.start(2)
    k_own[...] = jnp.dot(hidden[...], stream.wait(1), preferred_element_type=F32).astype(BF16)
    sender.start(key_slot, k_own, k_other, spot.fsdp(1))
    v_own[...] = (
        jnp.dot(hidden[...], stream.wait(2), preferred_element_type=F32) + v_bias[...]
    ).astype(BF16)
    sender.start(value_slot, v_own, v_other, spot.fsdp(1))
    up.start_near()
    down.start_near()
    out_load = pltpu.make_async_copy(out_full, qkv_held.at[1], local.sems.at[stream.base + 1])
    out_load.start()

    total = count_in[...]
    for step in range(1, 4):
        sender.arrived(count_slots[step - 1], counts.at[step - 1])
        total = total + counts[step - 1]
    count_sum[...] = total
    for number, device in enumerate((spot.fsdp(2), spot.rep(), spot.rep(2))):
        sender.start(far_slots[number], count_sum, far_counts.at[number], device)
    up.pass_far(0)
    out_ref[...] = jnp.zeros_like(out_ref)
    lse_ref[...] = jnp.zeros_like(lse_ref)
    sender.arrived(key_slot, k_other)
    sender.arrived(value_slot, v_other)
    data = (q_ref, k_own, v_own, k_other, v_other, bias_own, bias_other, out_ref, lse_ref)
    forward_heads(0, 8, *data)
    up.store()
    down.store()
    up.pass_far(1)
    up.pass_side(0)
    forward_heads(8, HEADS, *data)
    up.pass_far(2)
    up.pass_side(1)
    down.pass_far(0)

    out_load.wait()
    branch[...] = (
        jnp.dot(out_ref[...], qkv_held[1], preferred_element_type=F32) + out_bias[...]
    )

    def norm_two(i, carry):
        rows = pl.ds(pl.multiple_of(i * STRIP, STRIP), STRIP)
        result = inputs[rows, :].astype(F32) + gate[...] * branch[rows, :]
        middle[rows, :] = result
        normed, _ = row_norm(result)
        hidden_two[rows, :] = (normed * (1.0 + stretch_two[...]) + shift_two[...]).astype(BF16)
        return carry

    lax.fori_loop(0, q_ref.shape[0] // STRIP, norm_two, 0)
    stored = [local.start(middle, middle_out), local.start(branch, branch_out)]
    up.pass_side(2)
    down.pass_far(1)
    down.pass_side(0)
    up.finish()

    up_stream = ColumnStream(local, up_full, qkv_held, width)
    up_stream.start(0)
    up_stream.start(1)
    kept = []
    for j in range(4):
        columns = slice(j * width, (j + 1) * width)
        upper[...] = jnp.dot(hidden_two[...], up_stream.wait(j), preferred_element_type=F32)
        if j < 2:
            up_stream.start(j + 2)
            down.pass_far(j + 2)
            down.pass_side(j + 1)
        else:
            for copy in kept[j - 2]:
                copy.wait()
        if j == 2:
            down.pass_side(3)

        def activate(i, carry):
            rows = pl.ds(pl.multiple_of(i * STRIP, STRIP), STRIP)
            value, rise = gelu_parts(upper[rows, :] + up_bias[:, columns])
            values[j % 2, rows, :] = value.astype(BF16)
            slopes[j % 2, rows, :] = rise.astype(BF16)
            return carry

        lax.fori_loop(0, q_ref.shape[0] // STRIP, activate, 0)
        kept.append(
            (
                local.start(values.at[j % 2], activated.at[:, pl.ds(j * width, width)]),
                local.start(slopes.at[j % 2], slope.at[:, pl.ds(j * width, width)]),
            )
        )
    for copy in stored + list(kept[2] + kept[3]):
        copy.wait()
    total = count_sum[...]
    for number in range(3):
        sender.arrived(far_slots[number], far_counts.at[number])
        total = total + far_counts[number]
    count_out[...] = total
    for move in moves:
        move.finish()
    down.finish()
    sender.finish()


def attend_and_gather(
    inputs, near_operands, qkv_full, out_full, up_weight, down_weight, teacher, out_grad
):
    tokens, width = inputs.shape
    count = near_operands[-1]
    anywhere = pl.BlockSpec(memory_space=pl.ANY)
    near = pl.BlockSpec(memory_space=pltpu.VMEM)
    shape = (tokens, width)
    return pl.pallas_call(
        forward_send_kernel,
        out_shape=[jax.ShapeDtypeStruct(shape, BF16)] * 5
        + [
            jax.ShapeDtypeStruct((tokens, LANES), F32),
            jax.ShapeDtypeStruct(shape, BF16),
            jax.ShapeDtypeStruct(shape, BF16),
            jax.ShapeDtypeStruct(shape, BF16),
            jax.ShapeDtypeStruct(count.shape, F32),
            jax.ShapeDtypeStruct((4 * up_weight.shape[0], up_weight.shape[1]), BF16),
            jax.ShapeDtypeStruct((4 * down_weight.shape[0], down_weight.shape[1]), BF16),
            jax.ShapeDtypeStruct(teacher.shape, BF16),
            jax.ShapeDtypeStruct(out_grad.shape, BF16),
            jax.ShapeDtypeStruct(shape, F32),
            jax.ShapeDtypeStruct(shape, F32),
            jax.ShapeDtypeStruct((tokens, up_weight.shape[1]), BF16),
            jax.ShapeDtypeStruct((tokens, up_weight.shape[1]), BF16),
        ],
        in_specs=[near] * (1 + len(near_operands)) + [anywhere] * 6,
        out_specs=[near] * 10 + [anywhere] * 8,
        scratch_shapes=[
            pltpu.VMEM((2, width, width), BF16),
            pltpu.VMEM(shape, F32),
            pltpu.VMEM(shape, F32),
            pltpu.VMEM(shape, F32),
            pltpu.VMEM((2,) + shape, BF16),
            pltpu.VMEM((2,) + shape, BF16),
            pltpu.VMEM((3,) + count.shape, F32),
            pltpu.VMEM(count.shape, F32),
            pltpu.VMEM((3,) + count.shape, F32),
            pltpu.VMEM(up_weight.shape, BF16),
            pltpu.VMEM(down_weight.shape, BF16),
            sems(48),
            sems(48),
            sems(24),
        ],
        compiler_params=pltpu.CompilerParams(
            collective_id=2, has_side_effects=True, vmem_limit_bytes=67043328
        ),
        name="attend_and_gather",
    )(inputs, *near_operands, qkv_full, out_full, up_weight, down_weight, teacher, out_grad)


def attend(queries, k_own, v_own, k_other, v_other, bias_own, bias_other):
    tokens, width = queries.shape
    return pl.pallas_call(
        forward_kernel,
        out_shape=[
            jax.ShapeDtypeStruct((tokens, width), BF16),
            jax.ShapeDtypeStruct((tokens, LANES), F32),
        ],
        compiler_params=pltpu.CompilerParams(vmem_limit_bytes=48 * 1024 * 1024),
        cost_estimate=pl.CostEstimate(
            flops=16 * tokens * tokens * 2 * WINDOW * 4,
            transcendentals=HEADS * tokens * tokens * 2,
            bytes_accessed=6 * tokens * width * 2,
        ),
        name="attend",
    )(queries, k_own, v_own, k_other, v_other, bias_own, bias_other)


def backward_heads(
    low,
    high,
    q_ref,
    k_own,
    v_own,
    k_other,
    v_other,
    do_ref,
    lse_ref,
    bias_own,
    bias_other,
    dq_ref,
    dk_one,
    dv_one,
    dk_two,
    dv_two,
):
    tokens, width = q_ref.shape
    head_dim = width // HEADS
    factor = head_dim ** (-0.5)
    scale = factor * LOG2E
    across = (((1,), (1,)), ((), ()))
    sides = (
        (k_own, v_own, bias_own, dk_one, dv_one),
        (k_other, v_other, bias_other, dk_two, dv_two),
    )

    def body(head, carry):
        start, base = head_window(head, head_dim, width)
        window = pl.ds(base, WINDOW)
        lane = lax.broadcasted_iota(jnp.int32, (1, WINDOW), 1) + base
        inside = (lane >= start) & (lane < start + head_dim)
        keep = inside.astype(BF16)
        query = q_ref[:, window] * keep
        grad = do_ref[:, window] * keep
        lse = lse_ref[pl.ds(head, 1), :]

        def put(ref, value):
            ref[:, window] = jnp.where(inside, value, ref[:, window].astype(F32)).astype(ref.dtype)

        probs, prods = [], []
        delta = None
        for k_ref, v_ref, bias, _, _ in sides:
            scores = lax.dot_general(k_ref[:, window], query, across, preferred_element_type=F32)
            prob = jnp.exp2(scores * scale + bias[...] - lse)
            prob_grad = lax.dot_general(v_ref[:, window], grad, across, preferred_element_type=F32)
            prod = prob * prob_grad
            part = jnp.sum(prod, axis=0, keepdims=True)
            delta = part if delta is None else delta + part
            probs.append(prob)
            prods.append(prod)
        dq = None
        for (k_ref, _, _, dk, dv), prob, prod in zip(sides, probs, prods, strict=True):
            put(dv, jnp.dot(prob.astype(BF16), grad, preferred_element_type=F32))
            score_grad = (prod - prob * delta).astype(BF16)
            put(dk, jnp.dot(score_grad, query, preferred_element_type=F32) * factor)
            part = lax.dot_general(
                score_grad, k_ref[:, window], DOWN, preferred_element_type=F32
            )
            dq = part if dq is None else dq + part
        put(dq_ref, dq * factor)
        return carry

    lax.fori_loop(low, high, body, 0)


def backward_kernel(*refs):
    for ref in refs[-5:]:
        ref[...] = jnp.zeros_like(ref)
    backward_heads(0, HEADS, *refs)


def attend_back(queries, k_own, v_own, k_other, v_other, grad, lse, bias_own, bias_other):
    tokens, width = queries.shape
    shape = (tokens, width)
    return pl.pallas_call(
        backward_kernel,
        out_shape=[
            jax.ShapeDtypeStruct(shape, BF16),
            jax.ShapeDtypeStruct(shape, F32),
            jax.ShapeDtypeStruct(shape, F32),
            jax.ShapeDtypeStruct(shape, BF16),
            jax.ShapeDtypeStruct(shape, BF16),
        ],
        compiler_params=pltpu.CompilerParams(vmem_limit_bytes=60 * 1024 * 1024),
        name="attend_back",
    )(queries, k_own, v_own, k_other, v_other, grad, lse, bias_own, bias_other)


def dot(left, right):
    return jnp.dot(left, right, preferred_element_type=F32)


def dot_t(left, right):
    return lax.dot_general(left, right, (((1,), (1,)), ((), ())), preferred_element_type=F32)


def norm_parts(inputs):
    centred = inputs - jnp.mean(inputs, axis=-1, keepdims=True)
    rate = lax.rsqrt(jnp.mean(centred * centred, axis=-1, keepdims=True) + EPS)
    return centred * rate, rate


def norm_back(grad, normed, rate):
    return rate * (
        grad
        - jnp.mean(grad, axis=-1, keepdims=True)
        - normed * jnp.mean(grad * normed, axis=-1, keepdims=True)
    )


def gelu_parts(inputs):
    inner = jnp.tanh(GELU_C * (inputs + 0.044715 * inputs * inputs * inputs))
    value = 0.5 * inputs * (1.0 + inner)
    slope = 0.5 * (1.0 + inner) + 0.5 * inputs * (1.0 - inner * inner) * GELU_C * (
        1.0 + 3.0 * 0.044715 * inputs * inputs
    )
    return value, slope


def column_sum(array):
    return jnp.sum(array.astype(F32), axis=0)


def shards(
    tokens,
    condition,
    valid_mask,
    teacher,
    out_grad,
    mod_weight,
    mod_bias,
    qkv_weight,
    qkv_bias,
    out_weight,
    out_bias,
    up_weight,
    up_bias,
    down_weight,
    down_bias,
):
    reps, fsdp, seq = lax.axis_size("rep"), lax.axis_size("fsdp"), lax.axis_size("seq")
    fast = (reps, fsdp, seq) == (2, 4, 4)
    latents, span, width = tokens.shape
    assert 2 * latents == seq and latents == 2
    place_f, place_s = lax.axis_index("fsdp"), lax.axis_index("seq")
    total_tokens = latents * span * reps * fsdp * seq

    biases = jnp.concatenate([mod_bias, qkv_bias, out_bias, up_bias, down_bias])
    shard_rows = mod_weight.shape[0]
    cond_row = pick(condition, place_s % 2)
    keep_mask = valid_mask.astype(F32)

    if fast:
        inputs_low, valid_all, mod_parts, bias_all, qkv_full, out_full = enter(
            tokens,
            keep_mask.reshape(latents, 1, span),
            condition.astype(F32).reshape(latents, fsdp, 1, shard_rows),
            biases.astype(F32)[None],
            mod_weight,
            qkv_weight,
            out_weight,
        )
        inputs_low = inputs_low.reshape(-1, width)
        valid_all = valid_all.reshape(2, -1)
        keyvalid, valid_other = pick(valid_all, place_f % 2), pick(valid_all, 1 - place_f % 2)
        mod_row = jnp.sum(mod_parts, axis=(0, 1))
        bias_all = bias_all[:, 0]
    else:
        inputs_low = to_latent(tokens)
        keyvalid = to_latent(keep_mask)
        valid_other = flip(keyvalid, "fsdp", 1)
        counted = lax.psum(jnp.sum(keep_mask), ("rep", "fsdp", "seq")).reshape(1, 1)
        own_row = jnp.where(place_f % 2 == place_s // 2, cond_row, flip(cond_row, "fsdp", 1))
        cond_pair = lax.all_gather(own_row, "fsdp", axis=0)[::2]
        silu_pair = jax.nn.silu(cond_pair.astype(F32)).astype(BF16)
        silu_cols = lax.dynamic_slice_in_dim(silu_pair, place_f * shard_rows, shard_rows, 1)
        mod_row = pick(lax.psum(dot(silu_cols, mod_weight), "fsdp"), place_f // 2)
        bias_all = lax.all_gather(biases, "fsdp", axis=0).astype(F32)
        qkv_full, out_full = gather_weight(qkv_weight), gather_weight(out_weight)
        up_full, down_full = gather_weight(up_weight), gather_weight(down_weight)
        teacher_own, out_grad_own = to_latent(teacher), to_latent(out_grad)
    mask_own = (keyvalid - 1.0) * (-NEG)
    mask_other = (valid_other - 1.0) * (-NEG)

    cuts = [0]
    for bias in (mod_bias, qkv_bias, out_bias, up_bias, down_bias):
        cuts.append(cuts[-1] + bias.shape[0])
    mod_b, qkv_b, out_b, up_b, down_b = (
        bias_all[:, low:high].reshape(-1) for low, high in zip(cuts[:-1], cuts[1:], strict=True)
    )
    pieces = (mod_row + mod_b).reshape(6, 1, width)
    shift_one, scale_one, gate_one, shift_two, scale_two, gate_two = (pieces[i] for i in range(6))

    inputs = inputs_low.astype(F32)
    if fast:
        (
            hidden_one,
            queries,
            keys_own,
            values_own,
            attended,
            lse,
            keys_other,
            values_other,
            hidden_two,
            counted,
            up_full,
            down_full,
            teacher_own,
            out_grad_own,
            middle,
            branch,
            activated,
            slope,
        ) = attend_and_gather(
            inputs_low,
            (
                shift_one,
                scale_one,
                qkv_b[None, :width],
                qkv_b[None, width:],
                mask_own[None],
                mask_other[None],
                gate_one,
                out_b[None],
                shift_two,
                scale_two,
                up_b[None],
                jnp.full((1, LANES), jnp.sum(valid_all)),
            ),
            qkv_full,
            out_full,
            up_weight,
            down_weight,
            teacher,
            out_grad,
        )
        counted = counted[:, :1]
        teacher_own = teacher_own.reshape(-1, width)
        out_grad_own = out_grad_own.reshape(-1, width)
    else:
        normed_one, rate_one = norm_parts(inputs)
        hidden_one = (normed_one * (1.0 + scale_one) + shift_one).astype(BF16)
        projected = dot(hidden_one, qkv_full)
        queries = (projected[:, :width] + qkv_b[:width]).astype(BF16)
        keys_own = projected[:, width : 2 * width].astype(BF16)
        values_own = (projected[:, 2 * width :] + qkv_b[width:]).astype(BF16)
        keys_other, values_other = flip(keys_own, "fsdp", 1), flip(values_own, "fsdp", 1)
        attended, lse = attend(
            queries,
            keys_own,
            values_own,
            keys_other,
            values_other,
            mask_own[None],
            mask_other[None],
        )
        branch = dot(attended, out_full) + out_b
        middle = inputs + gate_one * branch
        normed_two, rate_two = norm_parts(middle)
        hidden_two = (normed_two * (1.0 + scale_two) + shift_two).astype(BF16)
        up_pre = dot(hidden_two, up_full) + up_b
        activated, slope = gelu_parts(up_pre)
        activated = activated.astype(BF16)
    mlp_out = dot(activated, down_full) + down_b
    output = middle + gate_two * mlp_out
    block_out = output.astype(BF16)
    differ = (output - teacher_own.astype(F32)) * keyvalid[:, None]
    error = jnp.sum(differ * differ)

    grad_out = out_grad_own.astype(F32) + total_tokens / counted * differ
    grad_mlp = (grad_out * gate_two).astype(BF16)
    gate_two_grad = jnp.sum(grad_out * mlp_out, axis=0, keepdims=True)

    def slices(array):
        return array.reshape(array.shape[0], fsdp, -1).transpose(1, 0, 2)

    def weight_grad(left, right):
        whole = lax.dot_general(left, right, DOWN, preferred_element_type=F32)
        mine = lax.psum_scatter(whole.astype(BF16), "fsdp", scatter_dimension=0, tiled=True)
        return lax.psum(mine, ("rep", "seq")).astype(F32)

    cond_part = jnp.where(place_f % 2 == place_s // 2, cond_row.astype(F32), 0.0)[None]
    length = (11 + up_weight.shape[1] // width) * width
    if fast:
        (
            attended_grad,
            branch_grad,
            middle_grad,
            sums,
            error_sum,
            up_total,
            down_final,
            _,
            block_out,
        ) = middle_back(
            (
                grad_mlp,
                grad_out,
                middle,
                branch,
                scale_two,
                gate_one,
                jnp.full((1, LANES), error),
            ),
            activated,
            slope,
            slices(hidden_two),
            down_full,
            up_full,
            out_full,
            block_out.reshape(2, span, width),
        )
        err_total = error_sum[:, :1]
        rows, cond_parts, up_final, tail_final, tokens_grad = finish(
            (
                branch_grad,
                up_total,
                middle_grad,
                inputs_low,
                scale_one,
                queries,
                keys_own,
                values_own,
                keys_other,
                values_other,
                attended_grad,
                lse.T,
                mask_own[:, None],
                mask_other[:, None],
                sums,
                gate_two_grad,
                cond_part,
            ),
            slices(attended),
            slices(hidden_one),
            mod_weight,
            qkv_full,
            (2, span, width),
        )
        rows = rows.reshape(-1, ROW_PARTS * width)[:, :length]
        down_g = down_final.reshape(down_weight.shape).astype(F32)
        up_g = spread(up_final.reshape(4, -1, width))
        tail_final = tail_final.reshape(4, -1, width)
        out_g = tail_final[0].astype(F32)
        qkv_g = spread(tail_final[1:])
    else:
        upper_grad = (dot_t(grad_mlp, down_full) * slope).astype(BF16)
        hidden_two_grad = dot_t(upper_grad, up_full)
        scaled_two = hidden_two_grad * (1.0 + scale_two)
        middle_grad = grad_out + norm_back(scaled_two, normed_two, rate_two)
        branch_grad = (middle_grad * gate_one).astype(BF16)
        attended_grad = dot_t(branch_grad, out_full).astype(BF16)
        query_grad, key_part, value_part, key_away, value_away = attend_back(
            queries,
            keys_own,
            values_own,
            keys_other,
            values_other,
            attended_grad,
            lse.T,
            mask_own[:, None],
            mask_other[:, None],
        )
        key_grad = (key_part + flip(key_away, "fsdp", 1).astype(F32)).astype(BF16)
        value_grad = (value_part + flip(value_away, "fsdp", 1).astype(F32)).astype(BF16)
        err_total = lax.psum(error, ("rep", "fsdp", "seq")).reshape(1, 1)
        block_out = from_latent(block_out)
        qkv_grad = jnp.concatenate([query_grad, key_grad, value_grad], axis=-1)
        hidden_one_grad = dot_t(qkv_grad, qkv_full)
        scaled_one = hidden_one_grad * (1.0 + scale_one)
        tokens_grad = middle_grad + norm_back(scaled_one, normed_one, rate_one)
        tokens_grad = tokens_grad.astype(BF16)
        row = jnp.concatenate(
            [
                column_sum(hidden_one_grad),
                column_sum(hidden_one_grad * normed_one),
                column_sum(middle_grad * branch),
                column_sum(hidden_two_grad),
                column_sum(hidden_two_grad * normed_two),
                gate_two_grad[0],
                column_sum(branch_grad),
                column_sum(upper_grad),
                column_sum(grad_mlp),
                column_sum(query_grad),
                column_sum(value_grad),
                cond_part[0],
            ]
        )
        row = row + flip(row, "fsdp", 1)
        rows = gather_rows(row)
        tokens_grad = from_latent(tokens_grad)
        down_g = weight_grad(activated, grad_mlp)
        up_g = weight_grad(hidden_two, upper_grad)
        out_g = weight_grad(attended, branch_grad)
        qkv_g = weight_grad(hidden_one, qkv_grad)

    mod_grad = rows[:, : 6 * width]
    silu_all = jax.nn.silu(rows[:, -width:]).astype(BF16)
    silu_own = lax.dynamic_slice_in_dim(silu_all, place_f * shard_rows, shard_rows, 1)
    mod_wgrad = lax.dot_general(
        silu_own.astype(F32),
        mod_grad,
        (((0,), (0,)), ((), ())),
        precision=HIGHEST,
        preferred_element_type=F32,
    )
    bias_sum = jnp.sum(rows[:, 6 * width : -width], axis=0)

    def own_bias(low, size):
        own = size // fsdp
        return lax.dynamic_slice_in_dim(bias_sum, low + place_f * own, own, 0)

    up_size = up_b.shape[0]
    out_bg = own_bias(0, width)
    up_bg = own_bias(width, up_size)
    down_bg = own_bias(width + up_size, width)
    qkv_bg = own_bias(2 * width + up_size, 2 * width)
    mod_own = mod_bias.shape[0]
    mod_bg = lax.dynamic_slice_in_dim(jnp.sum(mod_grad, axis=0), place_f * mod_own, mod_own, 0)

    if fast:
        found = cond_parts
    else:
        replica = lax.axis_index("rep")
        per_rep = mod_grad.shape[0] // reps
        own_rep = lax.dynamic_slice_in_dim(mod_grad, replica * per_rep, per_rep, 0)
        silu_grad = lax.dot_general(
            own_rep,
            mod_weight.astype(F32),
            (((1,), (1,)), ((), ())),
            precision=HIGHEST,
            preferred_element_type=F32,
        )
        owners = silu_grad.reshape(fsdp, latents, shard_rows)
        found = lax.all_to_all(owners, "fsdp", 0, 0, tiled=True)
    silu_grad = found.transpose(1, 0, 2).reshape(latents, width)
    conds = condition.astype(F32)
    sigmoid = 1.0 / (1.0 + jnp.exp(-conds))
    condition_grad = silu_grad * (sigmoid * (1.0 + conds * (1.0 - sigmoid)))

    loss_value = (err_total / (width * counted))[0, 0]
    return (
        block_out,
        loss_value,
        tokens_grad,
        condition_grad,
        mod_wgrad,
        mod_bg,
        qkv_g,
        qkv_bg,
        out_g,
        out_bg,
        up_g,
        up_bg,
        down_g,
        down_bg,
    )


def solution(mesh):
    batch = P(("rep", "fsdp"), "seq", None)
    matrix, vector = P("fsdp", None), P("fsdp")
    params = (matrix, vector) * 5
    return jax.shard_map(
        shards,
        mesh=mesh,
        in_specs=(batch, P(("rep", "fsdp"), None), P(("rep", "fsdp"), "seq"), batch, batch)
        + params,
        out_specs=(batch, P(), batch, P(("rep", "fsdp"), None)) + params,
        check_vma=False,
    )
```

```python
import functools

import jax
import jax.numpy as jnp
from jax import lax
from jax.experimental import pallas as pl
from jax.experimental.pallas import tpu as pltpu
from jax.sharding import PartitionSpec as P

HEADS = 16

EPS = 1e-06
GELU_C = 0.7978845608028654
HIGHEST = lax.Precision.HIGHEST
LOG2E = 1.4426950408889634
NEG = -1e30
BF16 = jnp.bfloat16
F32 = jnp.float32
WINDOW = 256
LANES = 128


def flip(array, axis, bit):
    size = lax.axis_size(axis)
    return lax.ppermute(array, axis, [(i, i ^ bit) for i in range(size)])


def pick(array, index):
    return lax.dynamic_index_in_dim(array, index, 0, keepdims=False)


def in_order(first, second, swapped):
    return jnp.where(swapped, jnp.stack([second, first]), jnp.stack([first, second]))


def to_latent(array):
    seq, fsdp = lax.axis_size("seq"), lax.axis_size("fsdp")
    place = lax.axis_index("seq")
    arrived = []
    for turn in range(2):
        pairs = []
        for f in range(fsdp):
            for s in range(seq):
                pair, core = f // 2, f % 2
                target = (pair * 2 + s // 2, 2 * core + (s + turn) % 2)
                pairs.append((f * seq + s, target[0] * seq + target[1]))
        block = pick(array, (place + turn) % 2)
        arrived.append(lax.ppermute(block, ("fsdp", "seq"), pairs))
    both = in_order(arrived[0], arrived[1], place % 2 == 1)
    return both.reshape((-1,) + both.shape[2:])


def from_latent(array):
    seq, fsdp = lax.axis_size("seq"), lax.axis_size("fsdp")
    place = lax.axis_index("seq")
    halves = array.reshape((2, array.shape[0] // 2) + array.shape[1:])
    arrived = []
    for turn in range(2):
        pairs = []
        for f in range(fsdp):
            for s in range(seq):
                pair, core = f // 2, f % 2
                slot = (s + turn) % 2
                target = (pair * 2 + s // 2, 2 * core + slot)
                pairs.append((f * seq + s, target[0] * seq + target[1]))
        arrived.append(lax.ppermute(pick(halves, (place + turn) % 2), ("fsdp", "seq"), pairs))
    return in_order(arrived[0], arrived[1], place % 2 == 1)


def gather_rows(row):
    fsdp = lax.axis_size("fsdp")
    everything = lax.all_gather(row, ("rep", "fsdp", "seq"), axis=0)
    everything = everything.reshape((-1, fsdp // 2, 2, lax.axis_size("seq")) + row.shape)
    return everything[:, :, 0].reshape((-1,) + row.shape)


def gather_weight(weight):
    return lax.all_gather(weight, "fsdp", axis=0, tiled=True)


MESH = pl.DeviceIdType.MESH


class Spot:
    def __init__(self):
        self.x, self.f, self.s = (lax.axis_index(name) for name in ("rep", "fsdp", "seq"))
        self.core = self.f % 2
        self.pair = self.f // 2

    def other(self, bit):
        if bit == 3:
            return 3 - self.f
        return self.f + bit - 2 * bit * ((self.f // bit) % 2)

    def fsdp(self, bit):
        return (self.x, self.other(bit), self.s)

    def rep(self, bit=0):
        return (1 - self.x, self.other(bit) if bit else self.f, self.s)

    def seq(self, step):
        return (self.x, self.f, lax.rem(self.s + step, 4))

    def token_target(self, turn):
        block = lax.rem(self.s + turn, 2)
        return (self.x, 2 * self.pair + self.s // 2, 2 * self.core + block), block


def greet(devices):
    barrier = pltpu.get_barrier_semaphore()
    for device in devices:
        pl.semaphore_signal(barrier, inc=1, device_id=device, device_id_type=MESH)
    pl.semaphore_wait(barrier, len(devices))


def column_group(spot):
    found = [(spot.x, spot.other(1), spot.s)]
    for step in range(1, 4):
        found.append(spot.seq(step))
        found.append((spot.x, spot.other(1), lax.rem(spot.s + step, 4)))
    return found


class Sender:
    def __init__(self, send_sems, recv_sems):
        self.send_sems, self.recv_sems = send_sems, recv_sems
        self.used = 0
        self.open = []

    def slot(self):
        self.used += 1
        return self.used - 1

    def start(self, slot, source, target, device):
        copy = pltpu.make_async_remote_copy(
            source, target, self.send_sems.at[slot], self.recv_sems.at[slot], device, MESH
        )
        copy.start()
        self.open.append(copy)

    def start_if(self, wanted, send_slot, recv_slot, source, target, device):
        copy = pltpu.make_async_remote_copy(
            source, target, self.send_sems.at[send_slot], self.recv_sems.at[recv_slot], device, MESH
        )
        pl.when(wanted)(lambda: copy.start())
        return wanted, copy

    def slots(self, count):
        self.used += count
        return self.used - count

    def sent(self, slot, view):
        pltpu.make_async_copy(view, view, self.send_sems.at[slot]).wait()

    def arrived(self, slot, view):
        pltpu.make_async_copy(view, view, self.recv_sems.at[slot]).wait()

    def finish(self):
        for copy in self.open:
            copy.wait_send()
        self.open = []


class Locals:
    def __init__(self, sems):
        self.sems = sems
        self.used = 0
        self.open = []

    def start(self, source, target):
        copy = pltpu.make_async_copy(source, target, self.sems.at[self.used])
        self.used += 1
        copy.start()
        return copy


class TokenMove:
    def __init__(self, sender, spot, source, target):
        self.sender, self.spot, self.source, self.target = sender, spot, source, target
        self.slots = [sender.slot(), sender.slot()]

    def start(self):
        spot = self.spot
        self.remote = []
        for turn, slot in enumerate(self.slots):
            device, block = spot.token_target(turn)
            stays = (device[1] == spot.f) & (device[2] == spot.s)
            source = self.source.at[block]
            target = self.target.at[lax.rem(spot.s, 2)]
            remote = pltpu.make_async_remote_copy(
                source,
                target,
                self.sender.send_sems.at[slot],
                self.sender.recv_sems.at[slot],
                device,
                MESH,
            )
            local = pltpu.make_async_copy(source, target, self.sender.recv_sems.at[slot])
            pl.when(jnp.logical_not(stays))(lambda remote=remote: remote.start())
            pl.when(stays)(lambda local=local: local.start())
            self.remote.append((stays, remote))

    def finish(self):
        for turn, slot in enumerate(self.slots):
            self.sender.arrived(slot, self.target.at[lax.rem(self.spot.s + turn, 2)])
        for stays, remote in self.remote:
            pl.when(jnp.logical_not(stays))(lambda remote=remote: remote.wait_send())


class WeightMove:
    def __init__(self, sender, local, spot, own, full, stage, chunks):
        self.sender, self.local, self.spot = sender, local, spot
        self.own, self.full, self.stage = own, full, stage
        self.rows, self.chunks = own.shape[0], chunks
        self.half = self.rows // 2
        self.tall = self.half // chunks
        self.slots = {
            kind: [sender.slot() for _ in range(1 if kind == "core" else chunks)]
            for kind in ("core", "far", "side", "far_core", "side_core")
        }

    def view(self, bits, side, chunk):
        shard = self.spot.other(bits) if bits else self.spot.f
        half = self.spot.x if side == 0 else 1 - self.spot.x
        start = shard * self.rows + half * self.half + chunk * self.tall
        return self.full.at[pl.ds(pl.multiple_of(start, 16), self.tall)]

    def shard_view(self, bits):
        shard = self.spot.other(bits) if bits else self.spot.f
        return self.full.at[pl.ds(pl.multiple_of(shard * self.rows, 16), self.rows)]

    def start_far(self):
        spot = self.spot
        for chunk, slot in enumerate(self.slots["far"]):
            start = pl.multiple_of(spot.x * self.half + chunk * self.tall, 16)
            self.sender.start(
                slot, self.own.at[pl.ds(start, self.tall)], self.view(0, 0, chunk), spot.fsdp(2)
            )

    def start_near(self):
        self.sender.start(self.slots["core"][0], self.own, self.shard_view(0), self.spot.fsdp(1))
        self.load = self.local.start(self.own, self.stage)

    def store(self):
        self.load.wait()
        self.kept = self.local.start(self.stage, self.shard_view(0))

    def pass_far(self, chunk):
        view = self.view(2, 0, chunk)
        self.sender.arrived(self.slots["far"][chunk], view)
        self.sender.start(self.slots["side"][chunk], view, view, self.spot.rep())
        self.sender.start(self.slots["far_core"][chunk], view, view, self.spot.fsdp(1))

    def pass_side(self, chunk):
        view = self.view(2, 1, chunk)
        self.sender.arrived(self.slots["side"][chunk], view)
        self.sender.start(self.slots["side_core"][chunk], view, view, self.spot.fsdp(1))

    def finish(self):
        self.kept.wait()
        self.sender.arrived(self.slots["core"][0], self.shard_view(1))
        for chunk in range(self.chunks):
            self.sender.arrived(self.slots["far_core"][chunk], self.view(3, 0, chunk))
            self.sender.arrived(self.slots["side_core"][chunk], self.view(3, 1, chunk))


def entry_kernel(
    tokens,
    valid,
    cond,
    biases,
    mod_weight,
    qkv_weight,
    out_weight,
    tokens_own,
    valid_all,
    mod_parts,
    bias_all,
    qkv_full,
    out_full,
    mod_held,
    cond_held,
    partial,
    qkv_stage,
    out_stage,
    send_sems,
    recv_sems,
    local_sems,
):
    spot = Spot()
    sender, local = Sender(send_sems, recv_sems), Locals(local_sems)
    mod_load = local.start(mod_weight, mod_held)
    greet(column_group(spot) + [spot.fsdp(2), spot.fsdp(3), spot.rep()])

    row = lax.rem(spot.s, 2)
    cond_slots, bias_slots = {}, {}
    for bit in (1, 2, 3):
        cond_slots[bit], bias_slots[bit] = sender.slot(), sender.slot()
        target = spot.other(bit)
        sender.start(
            cond_slots[bit], cond.at[row, target], cond_held.at[spot.f], spot.fsdp(bit)
        )
    for bit in (1, 2, 3):
        sender.start(bias_slots[bit], biases, bias_all.at[spot.f], spot.fsdp(bit))
    cond_own = local.start(cond.at[row, spot.f], cond_held.at[spot.f])
    bias_own = local.start(biases, bias_all.at[spot.f])

    qkv = WeightMove(sender, local, spot, qkv_weight, qkv_full, qkv_stage, 3)
    out = WeightMove(sender, local, spot, out_weight, out_full, out_stage, 1)
    mod_slots = {bit: sender.slot() for bit in (1, 2, 3)}
    move = TokenMove(sender, spot, tokens, tokens_own)
    valid_base = [sender.slot() for _ in range(4)][0]
    valid_open = []
    for turn in range(2):
        device, block = spot.token_target(turn)
        for core in range(2):
            goal = (device[0], 2 * spot.pair + core, device[2])
            stays = (goal[1] == spot.f) & (goal[2] == spot.s)
            source, target = valid.at[block], valid_all.at[spot.s]
            arrival = recv_sems.at[valid_base + spot.s]
            remote = pltpu.make_async_remote_copy(
                source, target, send_sems.at[valid_base + 2 * turn + core], arrival, goal, MESH
            )
            near = pltpu.make_async_copy(source, target, arrival)
            pl.when(jnp.logical_not(stays))(lambda remote=remote: remote.start())
            pl.when(stays)(lambda near=near: near.start())
            valid_open.append((stays, remote))
    move.start()
    qkv.start_far()
    qkv.start_near()
    out.start_near()

    cond_own.wait()
    for bit in (1, 2, 3):
        sender.arrived(cond_slots[bit], cond_held.at[spot.other(bit)])
    first, second = cond_held[spot.s // 2], cond_held[2 + spot.s // 2]
    which = lax.broadcasted_iota(jnp.int32, (16, first.shape[-1]), 0)
    conds = jnp.where(which == 0, first, second)
    silu = (conds / (1.0 + jnp.exp(-conds))).astype(BF16)
    mod_load.wait()
    width = mod_held.shape[1] // 6
    for piece in range(6):
        columns = slice(piece * width, (piece + 1) * width)
        product = jnp.dot(silu, mod_held[:, columns], preferred_element_type=F32)
        partial[0, :, columns] = product[0:1]
        partial[1, :, columns] = product[1:2]
    for bit in (1, 2, 3):
        pair = spot.pair if bit == 1 else 1 - spot.pair
        sender.start(
            mod_slots[bit], partial.at[pair], mod_parts.at[spot.f], spot.fsdp(bit)
        )
    mod_own = local.start(partial.at[spot.pair], mod_parts.at[spot.f])
    out.start_far()
    qkv.store()
    out.store()
    for chunk in range(3):
        qkv.pass_far(chunk)
        if chunk:
            qkv.pass_side(chunk - 1)
    qkv.pass_side(2)
    out.pass_far(0)
    out.pass_side(0)

    bias_own.wait()
    mod_own.wait()
    for bit in (1, 2, 3):
        sender.arrived(bias_slots[bit], bias_all.at[spot.other(bit)])
        sender.arrived(mod_slots[bit], mod_parts.at[spot.other(bit)])
    for place in range(4):
        sender.arrived(valid_base + place, valid_all.at[place])
    for stays, remote in valid_open:
        pl.when(jnp.logical_not(stays))(lambda remote=remote: remote.wait_send())
    move.finish()
    qkv.finish()
    out.finish()
    sender.finish()


def sems(count):
    return pltpu.SemaphoreType.DMA((count,))


def enter(tokens, valid, cond, biases, mod_weight, qkv_weight, out_weight):
    anywhere = pl.BlockSpec(memory_space=pl.ANY)
    return pl.pallas_call(
        entry_kernel,
        out_shape=[
            jax.ShapeDtypeStruct(tokens.shape, tokens.dtype),
            jax.ShapeDtypeStruct((4,) + valid.shape[1:], F32),
            jax.ShapeDtypeStruct((4, 1, mod_weight.shape[1]), F32),
            jax.ShapeDtypeStruct((4,) + biases.shape, F32),
            jax.ShapeDtypeStruct((4 * qkv_weight.shape[0], qkv_weight.shape[1]), BF16),
            jax.ShapeDtypeStruct((4 * out_weight.shape[0], out_weight.shape[1]), BF16),
        ],
        in_specs=[anywhere] * 7,
        out_specs=[anywhere] * 6,
        scratch_shapes=[
            pltpu.VMEM(mod_weight.shape, BF16),
            pltpu.VMEM((4,) + cond.shape[2:], F32),
            pltpu.VMEM((2, 1, mod_weight.shape[1]), F32),
            pltpu.VMEM(qkv_weight.shape, BF16),
            pltpu.VMEM(out_weight.shape, BF16),
            sems(40),
            sems(40),
            sems(12),
        ],
        compiler_params=pltpu.CompilerParams(
            collective_id=1, has_side_effects=True, vmem_limit_bytes=67043328
        ),
        name="enter",
    )(tokens, valid, cond, biases, mod_weight, qkv_weight, out_weight)


class TokenReturn:
    def __init__(self, sender, spot, source, target):
        self.sender, self.spot, self.source, self.target = sender, spot, source, target
        self.slots = [sender.slot(), sender.slot()]

    def start(self):
        spot = self.spot
        self.remote = []
        for turn, slot in enumerate(self.slots):
            half = lax.rem(spot.s + turn, 2)
            device = (spot.x, 2 * spot.pair + spot.s // 2, 2 * spot.core + half)
            stays = (device[1] == spot.f) & (device[2] == spot.s)
            source, target = self.source.at[half], self.target.at[lax.rem(spot.s, 2)]
            arrival = self.sender.recv_sems.at[slot]
            remote = pltpu.make_async_remote_copy(
                source, target, self.sender.send_sems.at[slot], arrival, device, MESH
            )
            local = pltpu.make_async_copy(source, target, arrival)
            pl.when(jnp.logical_not(stays))(lambda remote=remote: remote.start())
            pl.when(stays)(lambda local=local: local.start())
            self.remote.append((stays, remote))

    def finish(self):
        for turn, slot in enumerate(self.slots):
            self.sender.arrived(slot, self.target.at[lax.rem(self.spot.s + turn, 2)])
        for stays, remote in self.remote:
            pl.when(jnp.logical_not(stays))(lambda remote=remote: remote.wait_send())


ORDER = (0, 3, 1, 2)
STRIP = 64


def row_norm(inputs):
    centred = inputs - jnp.mean(inputs, axis=-1, keepdims=True)
    rate = lax.rsqrt(jnp.mean(centred * centred, axis=-1, keepdims=True) + EPS)
    return centred * rate, rate


class ColumnStream:
    def __init__(self, local, source, held, width):
        self.local, self.source, self.held, self.width = local, source, held, width
        self.base = local.used
        local.used += 2

    def copy(self, j):
        return pltpu.make_async_copy(
            self.source.at[:, pl.ds(j * self.width, self.width)],
            self.held.at[j % 2],
            self.local.sems.at[self.base + j % 2],
        )

    def start(self, j):
        self.copy(j).start()

    def wait(self, j):
        self.copy(j).wait()
        return self.held[j % 2]


class GradMove:
    def __init__(self, sender, local, spot, far, side, depth, total, final):
        self.sender, self.local, self.spot = sender, local, spot
        self.far, self.side, self.depth, self.total, self.final = far, side, depth, total, final
        self.tall = total.shape[0]
        self.y, self.x, self.z, self.g, self.fx = (sender.slots(4) for _ in range(5))
        self.kept = local.used
        local.used += 1
        self.z_open = []

    def send_far(self, j, give):
        self.sender.start(self.y + j, give, self.far.at[j], self.spot.fsdp(2))

    def half(self, side):
        return pl.ds(pl.multiple_of(side * self.tall, 16), self.tall)

    def fold(self, j, kept, arrives=True):
        if arrives:
            self.sender.arrived(self.y + j, self.far.at[j])
        self.far[j] = (self.far[j].astype(F32) + kept.astype(F32)).astype(BF16)
        self.sender.start(
            self.x + j, self.far.at[j, self.half(1 - self.spot.x)], self.side.at[j], self.spot.rep()
        )

    def cross(self, j):
        spot = self.spot
        self.sender.arrived(self.x + j, self.side.at[j])
        mine = self.far[j, self.half(spot.x), :].astype(F32)
        self.side[j] = (mine + self.side[j].astype(F32)).astype(BF16)
        step = lax.rem(spot.s - j + 4, 4)
        index = jnp.maximum(step - 1, 0)
        self.z_open.append(
            self.sender.start_if(
                spot.s != j,
                self.z + j,
                self.z + index,
                self.side.at[j],
                self.depth.at[index],
                (spot.x, spot.f, j),
            )
        )

    def gather(self, j):
        @pl.when(self.spot.s == j)
        def _():
            total = self.side[j].astype(F32)
            for index in range(3):
                self.sender.arrived(self.z + index, self.depth.at[index])
                total = total + self.depth[index].astype(F32)
            self.total[...] = total.astype(BF16)

    def give_back(self, j):
        spot, sender = self.spot, self.sender
        target = self.final.at[j, spot.x]

        @pl.when(spot.s == j)
        def _():
            for step in range(1, 4):
                pltpu.make_async_remote_copy(
                    self.total,
                    target,
                    sender.send_sems.at[self.g + step],
                    sender.recv_sems.at[self.g + j],
                    (spot.x, spot.f, (j + step) % 4),
                    MESH,
                ).start()
            pltpu.make_async_remote_copy(
                self.total,
                target,
                sender.send_sems.at[self.fx + j],
                sender.recv_sems.at[self.fx + j],
                spot.rep(),
                MESH,
            ).start()
            pltpu.make_async_copy(self.total, target, self.local.sems.at[self.kept]).start()

    def settle(self, j):
        self.gather(j)
        self.give_back(j)

    def pass_on(self, j):
        spot, sender = self.spot, self.sender
        target = self.final.at[j, spot.x]

        @pl.when(spot.s != j)
        def _():
            sender.arrived(self.g + j, target)
            pltpu.make_async_remote_copy(
                target,
                target,
                sender.send_sems.at[self.fx + j],
                sender.recv_sems.at[self.fx + j],
                spot.rep(),
                MESH,
            ).start()

    def finish_sums(self):
        for wanted, copy in self.z_open:
            pl.when(wanted)(lambda copy=copy: copy.wait_send())

    def finish_back(self):
        spot, sender = self.spot, self.sender
        for j in range(4):
            sender.arrived(self.fx + j, self.final.at[j, 1 - spot.x])
            sender.sent(self.fx + j, self.total)
        for step in range(1, 4):
            sender.sent(self.g + step, self.total)
        pltpu.make_async_copy(self.total, self.total, self.local.sems.at[self.kept]).wait()

    def finish(self):
        self.finish_sums()
        self.finish_back()


DOWN = (((0,), (0,)), ((), ()))


def outer(left_own, left_other, right_own, right_other):
    total = lax.dot_general(left_own, right_own, DOWN, preferred_element_type=F32)
    return total + lax.dot_general(left_other, right_other, DOWN, preferred_element_type=F32)


def lane_block(index, size):
    return pl.ds(pl.multiple_of(index * size, LANES), size)


def middle_kernel(
    grad_mlp,
    grad_out,
    middle,
    branch,
    stretch,
    gate,
    error_in,
    activated,
    slope,
    hidden,
    down_full,
    up_full,
    out_full,
    block_out,
    attended_grad,
    branch_grad,
    middle_grad,
    sums,
    error_out,
    up_total,
    down_final,
    upper_other,
    block_back,
    act_give,
    act_keep,
    act_give_other,
    act_keep_other,
    mlp_other,
    hid,
    held,
    slopes,
    uppers,
    others,
    hidden_grad,
    out_held,
    give,
    kept,
    far,
    side,
    depth,
    total,
    up_far,
    up_side,
    up_depth,
    errors,
    send_sems,
    recv_sems,
    local_sems,
):
    spot = Spot()
    sender, local = Sender(send_sems, recv_sems), Locals(local_sems)
    tokens, width = grad_mlp.shape
    shard = activated.shape[1] // 4
    f, core = spot.f, spot.fsdp(1)
    loads = [
        local.start(activated.at[:, lane_block(spot.other(2), shard)], act_give),
        local.start(activated.at[:, lane_block(f, shard)], act_keep),
        local.start(hidden.at[spot.other(2)], hid.at[0]),
        local.start(hidden.at[f], hid.at[1]),
    ]
    out_load = local.start(out_full, out_held)
    base = local.used
    local.used += 6

    def weight_copy(number, which):
        units = pl.ds(ORDER[number] * width, width)
        if which == 0:
            return pltpu.make_async_copy(down_full.at[units], held.at[0], local.sems.at[base])
        if which == 1:
            slot = number % 2
            return pltpu.make_async_copy(
                slope.at[:, units], slopes.at[slot], local.sems.at[base + 1 + slot]
            )
        return pltpu.make_async_copy(up_full.at[:, units], held.at[1], local.sems.at[base + 3])

    def other_copy(number):
        slot = number % 2
        return pltpu.make_async_copy(
            upper_other.at[ORDER[number]], others.at[slot], local.sems.at[base + 4 + slot]
        )

    for which in range(3):
        weight_copy(0, which).start()
    greet(column_group(spot) + [spot.fsdp(2), spot.rep()])
    error_slots = [sender.slot() for _ in range(3)]
    error_z = sender.slots(4)
    sender.start(error_slots[0], error_in, errors.at[4], core)
    pieces = [sender.slot() for _ in range(5)]
    upper_slots = sender.slots(4)
    sender.start(
        pieces[0], activated.at[:, lane_block(spot.other(3), shard)], act_give_other, core
    )
    sender.start(pieces[1], grad_mlp, mlp_other, core)
    sender.start(
        pieces[2], activated.at[:, lane_block(spot.other(1), shard)], act_keep_other, core
    )
    sender.start(pieces[3], hidden.at[spot.other(3)], hid.at[2], core)
    sender.start(pieces[4], hidden.at[spot.other(1)], hid.at[3], core)
    back = TokenReturn(sender, spot, block_out, block_back)
    down = GradMove(sender, local, spot, far, side, depth, total, down_final)
    up = GradMove(sender, local, spot, up_far, up_side, up_depth, up_total, None)

    sender.arrived(error_slots[0], errors.at[4])
    errors[5] = error_in[...] + errors[4]
    sender.start(error_slots[1], errors.at[5], errors.at[6], spot.fsdp(2))
    for load in loads[:2]:
        load.wait()
    sender.arrived(pieces[0], act_give_other)
    sender.arrived(error_slots[1], errors.at[6])
    errors[7] = errors[5] + errors[6]
    sender.start(error_slots[2], errors.at[7], errors.at[8], spot.rep())
    sender.arrived(pieces[1], mlp_other)
    block = 384

    def fill(target, left, left_other):
        def body(i, carry):
            columns = lane_block(i, block)
            rows = pl.ds(pl.multiple_of(i * block, 16), block)
            target[rows, :] = outer(
                left[:, columns], left_other[:, columns], grad_mlp[...], mlp_other[...]
            ).astype(BF16)
            return carry

        lax.fori_loop(0, shard // block, body, 0)

    tall = shard // 4
    fill(give.at[0], act_give, act_give_other)
    for j in ORDER:
        down.send_far(j, give.at[0, pl.ds(j * tall, tall)])
    sender.arrived(error_slots[2], errors.at[8])
    errors[spot.s] = errors[7] + errors[8]
    error_open = []
    for step in range(1, 4):
        copy = pltpu.make_async_remote_copy(
            errors.at[spot.s],
            errors.at[spot.s],
            send_sems.at[error_z + step],
            recv_sems.at[error_z + spot.s],
            spot.seq(step),
            MESH,
        )
        copy.start()
        error_open.append(copy)
    back.start()
    sender.arrived(pieces[2], act_keep_other)
    fill(kept.at[0], act_keep, act_keep_other)

    across = (((1,), (1,)), ((), ()))
    sums[...] = jnp.zeros_like(sums)

    def upper(number):
        j = ORDER[number]
        weight_copy(number, 0).wait()
        weight_copy(number, 1).wait()
        grad = lax.dot_general(grad_mlp[...], held[0], across, preferred_element_type=F32)
        grad = (grad * slopes[number % 2].astype(F32)).astype(BF16)
        uppers[j] = grad
        sender.start(upper_slots + j, uppers.at[j], upper_other.at[j], core)
        if number < 3:
            weight_copy(number + 1, 0).start()
            weight_copy(number + 1, 1).start()
        weight_copy(number, 2).wait()
        product = lax.dot_general(uppers[j], held[1], across, preferred_element_type=F32)
        if number == 0:
            hidden_grad[...] = product
        else:
            hidden_grad[...] += product
        if number < 3:
            weight_copy(number + 1, 2).start()
        sums[5 + j : 6 + j, :] = jnp.sum(uppers[j].astype(F32), axis=0, keepdims=True)

    def up_outer(number):
        j = ORDER[number]
        other_copy(number).wait()
        if number < 3:
            sender.arrived(upper_slots + ORDER[number + 1], upper_other.at[ORDER[number + 1]])
            other_copy(number + 1).start()
        rows = pl.ds(j * tall, tall)
        right_other = others[number % 2]
        give[1, rows, :] = outer(hid[0], hid[2], uppers[j], right_other).astype(BF16)
        up.send_far(j, give.at[1, rows])
        kept[1, rows, :] = outer(hid[1], hid[3], uppers[j], right_other).astype(BF16)

    def fold(group, index, j):
        group.fold(j, kept[index, pl.ds(j * tall, tall), :])

    a, b, c, d = ORDER
    upper(0)
    fold(down, 0, a)
    upper(1)
    down.cross(a)
    upper(2)
    fold(down, 0, b)
    upper(3)
    down.cross(b)
    for load in loads[2:]:
        load.wait()
    for slot, place in ((3, 2), (4, 3)):
        sender.arrived(pieces[slot], hid.at[place])
    sender.arrived(upper_slots + a, upper_other.at[a])
    other_copy(0).start()
    up_outer(0)
    up_outer(1)
    fold(down, 0, c)
    up_outer(2)
    up_outer(3)
    down.cross(c)
    down.settle(a)

    def strip_step(i, found):
        strip = pl.ds(pl.multiple_of(i * STRIP, STRIP), STRIP)
        normed, rate = row_norm(middle[strip, :])
        grad = hidden_grad[strip, :]
        scaled = grad * (1.0 + stretch[...])
        result = grad_out[strip, :] + rate * (
            scaled
            - jnp.mean(scaled, axis=-1, keepdims=True)
            - normed * jnp.mean(scaled * normed, axis=-1, keepdims=True)
        )
        middle_grad[strip, :] = result
        low = (result * gate[...]).astype(BF16)
        branch_grad[strip, :] = low
        terms = (
            result * branch[strip, :],
            grad,
            grad * normed,
            low.astype(F32),
            grad_mlp[strip, :].astype(F32),
        )
        return tuple(
            kept_sum + jnp.sum(term, axis=0, keepdims=True)
            for kept_sum, term in zip(found, terms, strict=True)
        )

    zero = jnp.zeros((1, width), F32)
    found = lax.fori_loop(0, tokens // STRIP, strip_step, (zero,) * 5)
    for place, value in zip((0, 1, 2, 4, 9), found, strict=True):
        sums[place : place + 1, :] = value
    fold(down, 0, d)
    out_load.wait()
    attended_grad[...] = lax.dot_general(
        branch_grad[...], out_held[...], across, preferred_element_type=F32
    ).astype(BF16)
    down.cross(d)
    down.settle(b)
    fold(up, 1, a)
    down.settle(c)
    up.cross(a)
    fold(up, 1, b)
    down.settle(d)
    up.cross(b)
    down.pass_on(a)
    fold(up, 1, c)
    down.pass_on(b)
    up.cross(c)
    down.pass_on(c)
    for place in range(4):

        @pl.when(spot.s != place)
        def _():
            sender.arrived(error_z + place, errors.at[place])

    error_out[...] = errors[0] + errors[1] + errors[2] + errors[3]
    for copy in error_open:
        copy.wait_send()
    fold(up, 1, d)
    down.pass_on(d)
    up.cross(d)
    up.gather(a)
    up.gather(b)
    up.gather(c)
    back.finish()
    down.finish()
    up.gather(d)
    up.finish_sums()
    sender.finish()


def middle_back(near_operands, activated, slope, hidden, down_full, up_full, out_full, block_out):
    grad_mlp = near_operands[0]
    error = near_operands[-1]
    tokens, width = grad_mlp.shape
    shape = (tokens, width)
    shard = activated.shape[1] // 4
    tall = shard // 4
    anywhere = pl.BlockSpec(memory_space=pl.ANY)
    near = pl.BlockSpec(memory_space=pltpu.VMEM)
    piece = (tall // 2, width)
    return pl.pallas_call(
        middle_kernel,
        out_shape=[
            jax.ShapeDtypeStruct(shape, BF16),
            jax.ShapeDtypeStruct(shape, BF16),
            jax.ShapeDtypeStruct(shape, F32),
            jax.ShapeDtypeStruct((ROW_PARTS, width), F32),
            jax.ShapeDtypeStruct(error.shape, F32),
            jax.ShapeDtypeStruct(piece, BF16),
            jax.ShapeDtypeStruct((4, 2) + piece, BF16),
            jax.ShapeDtypeStruct((4,) + shape, BF16),
            jax.ShapeDtypeStruct(block_out.shape, BF16),
        ],
        in_specs=[near] * len(near_operands) + [anywhere] * 7,
        out_specs=[near] * 6 + [anywhere] * 3,
        scratch_shapes=[
            pltpu.VMEM((tokens, shard), BF16),
            pltpu.VMEM((tokens, shard), BF16),
            pltpu.VMEM((tokens, shard), BF16),
            pltpu.VMEM((tokens, shard), BF16),
            pltpu.VMEM(shape, BF16),
            pltpu.VMEM((4,) + hidden.shape[1:], BF16),
            pltpu.VMEM((2, width, width), BF16),
            pltpu.VMEM((2,) + shape, BF16),
            pltpu.VMEM((4,) + shape, BF16),
            pltpu.VMEM((2,) + shape, BF16),
            pltpu.VMEM(shape, F32),
            pltpu.VMEM(out_full.shape, BF16),
            pltpu.VMEM((2, shard, width), BF16),
            pltpu.VMEM((2, shard, width), BF16),
            pltpu.VMEM((4, tall, width), BF16),
            pltpu.VMEM((4,) + piece, BF16),
            pltpu.VMEM((3,) + piece, BF16),
            pltpu.VMEM(piece, BF16),
            pltpu.VMEM((4, tall, width), BF16),
            pltpu.VMEM((4,) + piece, BF16),
            pltpu.VMEM((3,) + piece, BF16),
            pltpu.VMEM((9,) + error.shape, F32),
            sems(72),
            sems(72),
            sems(20),
        ],
        compiler_params=pltpu.CompilerParams(
            collective_id=3, has_side_effects=True, vmem_limit_bytes=67043328
        ),
        name="middle_back",
    )(*near_operands, activated, slope, hidden, down_full, up_full, out_full, block_out)


ROW_PARTS = 16


def finish_kernel(*refs):
    (
        branch_grad,
        up_total,
        middle_grad,
        inputs,
        stretch,
        q_ref,
        k_own,
        v_own,
        k_other,
        v_other,
        do_ref,
        lse_ref,
        bias_own,
        bias_other,
        sums_in,
        gate_sum,
        cond_part,
        attended,
        hidden,
        mod_weight,
        qkv_full,
        rows,
        cond_parts,
        up_final,
        tail_final,
        tokens_back,
        branch_other,
        qkv_grad,
        qkv_other,
        att,
        hid,
        mod_held,
        qkv_held,
        hidden_grad,
        dv_one,
        dk_two,
        dv_two,
        dk_in,
        dv_in,
        tokens_grad,
        give,
        far,
        side,
        depth,
        total,
        row,
        row_in,
        cond_send,
        send_sems,
        recv_sems,
        local_sems,
    ) = refs
    spot = Spot()
    sender, local = Sender(send_sems, recv_sems), Locals(local_sems)
    width = branch_grad.shape[1]
    f, core = spot.f, spot.fsdp(1)
    loads = [
        local.start(attended.at[spot.other(2)], att.at[0]),
        local.start(attended.at[f], att.at[1]),
        local.start(hidden.at[spot.other(2)], hid.at[0]),
        local.start(hidden.at[f], hid.at[1]),
    ]
    mod_load = local.start(mod_weight, mod_held)
    stream = ColumnStream(local, qkv_full, qkv_held, width)
    stream.start(0)
    stream.start(1)
    greet(column_group(spot) + [spot.fsdp(2), spot.fsdp(3), spot.rep()])
    slots = [sender.slot() for _ in range(6)]
    qkv_slots = sender.slots(3)
    sender.start(slots[0], attended.at[spot.other(3)], att.at[2], core)
    sender.start(slots[1], branch_grad, branch_other, core)
    sender.start(slots[2], hidden.at[spot.other(3)], hid.at[2], core)
    sender.start(slots[4], attended.at[spot.other(1)], att.at[3], core)
    sender.start(slots[5], hidden.at[spot.other(1)], hid.at[3], core)
    up = GradMove(sender, local, spot, None, None, None, up_total, up_final)
    tail = GradMove(sender, local, spot, far, side, depth, total, tail_final)
    back = TokenReturn(sender, spot, tokens_grad, tokens_back)
    row_slot = sender.slot()
    row_z, row_y, row_x = sender.slots(4), sender.slot(), sender.slot()
    cond_slots = {bit: sender.slot() for bit in (1, 2, 3)}
    dk_slot, dv_slot = sender.slot(), sender.slot()
    for j in ORDER:
        up.give_back(j)
    for load in loads:
        load.wait()

    def operands(j):
        if j == 0:
            return att, branch_grad[...], branch_other[...]
        return hid, qkv_grad[3 - j], qkv_other[3 - j]

    def give_far(j):
        left, right, right_other = operands(j)
        give[j] = outer(left[0], left[2], right, right_other).astype(BF16)
        tail.send_far(j, give.at[j])

    a, b, c, d = ORDER
    sender.arrived(slots[0], att.at[2])
    sender.arrived(slots[1], branch_other)
    give_far(a)
    data = (
        q_ref,
        k_own,
        v_own,
        k_other,
        v_other,
        do_ref,
        lse_ref,
        bias_own,
        bias_other,
        qkv_grad.at[0],
        hidden_grad,
        dv_one,
        dk_two,
        dv_two,
    )
    sender.arrived(slots[4], att.at[3])

    def fold(j):
        left, right, right_other = operands(j)
        tail.fold(j, outer(left[1], left[3], right, right_other))

    backward_heads(0, 5, *data)
    up.pass_on(a)
    backward_heads(5, 10, *data)
    fold(a)
    up.pass_on(b)
    backward_heads(10, HEADS, *data)
    sender.start(qkv_slots, qkv_grad.at[0], qkv_other.at[0], core)
    sender.start(dv_slot, dv_two, dv_in, core)
    sender.start(dk_slot, dk_two, dk_in, core)
    sender.arrived(slots[2], hid.at[2])
    sender.arrived(slots[5], hid.at[3])
    sender.arrived(qkv_slots, qkv_other.at[0])
    give_far(b)
    sender.arrived(dv_slot, dv_in)
    qkv_grad[2] = (dv_one[...] + dv_in[...].astype(F32)).astype(BF16)
    sender.start(qkv_slots + 2, qkv_grad.at[2], qkv_other.at[2], core)
    sender.arrived(dk_slot, dk_in)
    qkv_grad[1] = (hidden_grad[...] + dk_in[...].astype(F32)).astype(BF16)
    sender.start(qkv_slots + 1, qkv_grad.at[1], qkv_other.at[1], core)
    tail.cross(a)
    sender.arrived(qkv_slots + 2, qkv_other.at[2])
    give_far(c)
    sender.arrived(qkv_slots + 1, qkv_other.at[1])
    give_far(d)

    across = (((1,), (1,)), ((), ()))
    for j in range(3):
        product = lax.dot_general(qkv_grad[j], stream.wait(j), across, preferred_element_type=F32)
        if j == 0:
            hidden_grad[...] = product
            stream.start(2)
        else:
            hidden_grad[...] += product
    fold(b)

    def norm_step(i, sums):
        strip = pl.ds(pl.multiple_of(i * STRIP, STRIP), STRIP)
        normed, rate = row_norm(inputs[strip, :].astype(F32))
        grad = hidden_grad[strip, :]
        scaled = grad * (1.0 + stretch[...])
        result = middle_grad[strip, :] + rate * (
            scaled
            - jnp.mean(scaled, axis=-1, keepdims=True)
            - normed * jnp.mean(scaled * normed, axis=-1, keepdims=True)
        )
        tokens_grad[i // per_half, pl.ds(pl.multiple_of((i % per_half) * STRIP, STRIP), STRIP), :] = (
            result.astype(BF16)
        )
        return (
            sums[0] + jnp.sum(grad, axis=0, keepdims=True),
            sums[1] + jnp.sum(grad * normed, axis=0, keepdims=True),
            sums[2] + jnp.sum(qkv_grad[0, strip, :].astype(F32), axis=0, keepdims=True),
            sums[3] + jnp.sum(qkv_grad[2, strip, :].astype(F32), axis=0, keepdims=True),
        )

    per_half = tokens_grad.shape[1] // STRIP
    zero = jnp.zeros((1, width), F32)
    sums = lax.fori_loop(0, 2 * per_half, norm_step, (zero,) * 4)
    row[0:2, :] = jnp.concatenate(sums[:2], axis=0)
    row[2:, :] = sums_in[: ROW_PARTS - 2, :]
    row[5:6, :] = gate_sum[...]
    row[12:15, :] = jnp.concatenate(sums[2:] + (cond_part[...],), axis=0)
    sender.start(row_slot, row, row_in, core)
    sender.arrived(row_slot, row_in)
    column = (spot.x * 2 + spot.pair) * 4
    rows[column + spot.s] = row[...] + row_in[...]
    row_open = []
    for step in range(1, 4):
        copy = pltpu.make_async_remote_copy(
            rows.at[column + spot.s],
            rows.at[column + spot.s],
            send_sems.at[row_z + step],
            recv_sems.at[row_z + spot.s],
            spot.seq(step),
            MESH,
        )
        copy.start()
        row_open.append(copy)
    tail.cross(b)
    fold(c)
    up.pass_on(c)
    tail.cross(c)
    tail.settle(a)
    fold(d)
    up.pass_on(d)
    tail.cross(d)
    tail.settle(b)
    for place in range(4):

        @pl.when(spot.s != place)
        def _():
            sender.arrived(row_z + place, rows.at[column + place])

    span = pl.ds(column, 4)
    sender.start(row_y, rows.at[span], rows.at[span], spot.fsdp(2))
    tail.settle(c)
    back.start()
    far_column = (spot.x * 2 + 1 - spot.pair) * 4
    sender.arrived(row_y, rows.at[pl.ds(far_column, 4)])
    half = pl.ds(spot.x * 8, 8)
    sender.start(row_x, rows.at[half], rows.at[half], spot.rep())

    mod_load.wait()
    products = jnp.zeros((16, mod_held.shape[0]), F32)
    for part in range(6):
        grad = rows[half, part, :]
        high = grad.astype(BF16)
        low = (grad - high.astype(F32)).astype(BF16)
        products += lax.dot_general(
            jnp.concatenate([high, low], axis=0),
            mod_held[:, part * width : (part + 1) * width],
            (((1,), (1,)), ((), ())),
            preferred_element_type=F32,
        )
    silu_grad = products[:8] + products[8:]
    for latent in range(8):
        cond_send[latent // 2, latent % 2 : latent % 2 + 1, :] = silu_grad[latent : latent + 1]
    cond_parts[f] = cond_send[f]
    for bit in (1, 2, 3):
        sender.start(
            cond_slots[bit], cond_send.at[spot.other(bit)], cond_parts.at[f], spot.fsdp(bit)
        )

    tail.pass_on(a)
    tail.settle(d)
    tail.pass_on(b)
    tail.pass_on(c)
    tail.pass_on(d)
    for bit in (1, 2, 3):
        sender.arrived(cond_slots[bit], cond_parts.at[spot.other(bit)])
    sender.arrived(row_x, rows.at[pl.ds((1 - spot.x) * 8, 8)])
    for copy in row_open:
        copy.wait_send()
    back.finish()
    up.finish_back()
    tail.finish()
    sender.finish()


def finish(near_operands, attended, hidden, mod_weight, qkv_full, token_shape):
    branch_grad, up_total = near_operands[:2]
    tokens, width = branch_grad.shape
    shape = (tokens, width)
    piece = up_total.shape
    anywhere = pl.BlockSpec(memory_space=pl.ANY)
    near = pl.BlockSpec(memory_space=pltpu.VMEM)
    final = jax.ShapeDtypeStruct((4, 2) + piece, BF16)
    tall = 2 * piece[0]
    return pl.pallas_call(
        finish_kernel,
        out_shape=[
            jax.ShapeDtypeStruct((16, ROW_PARTS, width), F32),
            jax.ShapeDtypeStruct((4, 2, mod_weight.shape[0]), F32),
            final,
            final,
            jax.ShapeDtypeStruct(token_shape, BF16),
        ],
        in_specs=[near] * len(near_operands) + [anywhere] * 4,
        out_specs=[near] * 2 + [anywhere] * 3,
        scratch_shapes=[
            pltpu.VMEM(shape, BF16),
            pltpu.VMEM((3,) + shape, BF16),
            pltpu.VMEM((3,) + shape, BF16),
            pltpu.VMEM((4,) + attended.shape[1:], BF16),
            pltpu.VMEM((4,) + hidden.shape[1:], BF16),
            pltpu.VMEM(mod_weight.shape, BF16),
            pltpu.VMEM((2, width, width), BF16),
            pltpu.VMEM(shape, F32),
            pltpu.VMEM(shape, F32),
            pltpu.VMEM(shape, BF16),
            pltpu.VMEM(shape, BF16),
            pltpu.VMEM(shape, BF16),
            pltpu.VMEM(shape, BF16),
            pltpu.VMEM(token_shape, BF16),
            pltpu.VMEM((4, tall, width), BF16),
            pltpu.VMEM((4, tall, width), BF16),
            pltpu.VMEM((4,) + piece, BF16),
            pltpu.VMEM((3,) + piece, BF16),
            pltpu.VMEM(piece, BF16),
            pltpu.VMEM((ROW_PARTS, width), F32),
            pltpu.VMEM((ROW_PARTS, width), F32),
            pltpu.VMEM((4, 2, mod_weight.shape[0]), F32),
            sems(72),
            sems(72),
            sems(24),
        ],
        compiler_params=pltpu.CompilerParams(
            collective_id=4, has_side_effects=True, vmem_limit_bytes=67043328
        ),
        name="finish",
    )(*near_operands, attended, hidden, mod_weight, qkv_full)


def spread_kernel(block, out):
    out[...] = block[0].astype(F32)


def spread(blocks, order):
    rows, width = blocks.shape[1:]
    count = len(order)
    first, step = order[0], order[1] - order[0]
    return pl.pallas_call(
        spread_kernel,
        grid=(count,),
        out_shape=jax.ShapeDtypeStruct((rows, count * width), F32),
        in_specs=[pl.BlockSpec((1, rows, width), lambda j: (first + step * j, 0, 0))],
        out_specs=pl.BlockSpec((rows, width), lambda j: (0, j)),
        name="spread",
    )(blocks)


def head_window(head, head_dim, width):
    start = head * head_dim
    base = jnp.minimum(start // LANES, (width - WINDOW) // LANES) * LANES
    base = pl.multiple_of(base, LANES)
    return start, base


def forward_heads(
    low,
    high,
    q_ref,
    k_own,
    v_own,
    k_other,
    v_other,
    bias_own,
    bias_other,
    out_ref,
    lse_ref,
):
    tokens, width = q_ref.shape
    head_dim = width // HEADS
    blocks = 2
    tall = tokens // blocks
    scale = head_dim ** (-0.5) * LOG2E
    b_own, b_other = bias_own[...], bias_other[...]
    dims = (((1,), (1,)), ((), ()))

    def body(head, carry):
        start, base = head_window(head, head_dim, width)
        window = pl.ds(base, WINDOW)
        lane = lax.broadcasted_iota(jnp.int32, (1, WINDOW), 1) + base
        inside = (lane >= start) & (lane < start + head_dim)
        keep = inside.astype(BF16)
        spot = lax.broadcasted_iota(jnp.int32, (1, LANES), 1) == head
        key_one, key_two = k_own[:, window], k_other[:, window]
        val_one, val_two = v_own[:, window] * keep, v_other[:, window] * keep
        for block in range(blocks):
            rows = pl.ds(block * tall, tall)
            query = q_ref[rows, window] * keep
            one = lax.dot_general(query, key_one, dims, preferred_element_type=F32)
            two = lax.dot_general(query, key_two, dims, preferred_element_type=F32)
            one = one * scale + b_own
            two = two * scale + b_other
            top = jnp.maximum(
                jnp.max(one, axis=1, keepdims=True), jnp.max(two, axis=1, keepdims=True)
            )
            one = jnp.exp2(one - top)
            two = jnp.exp2(two - top)
            total = jnp.sum(one, axis=1, keepdims=True) + jnp.sum(two, axis=1, keepdims=True)
            mixed = jnp.dot(one.astype(BF16), val_one, preferred_element_type=F32)
            mixed += jnp.dot(two.astype(BF16), val_two, preferred_element_type=F32)
            mixed = mixed * (1.0 / total)
            out_ref[rows, window] = jnp.where(
                inside, mixed, out_ref[rows, window].astype(F32)
            ).astype(out_ref.dtype)
            lse_ref[rows, :] = jnp.where(spot, top + jnp.log2(total), lse_ref[rows, :])
        return carry

    lax.fori_loop(low, high, body, 0)


def forward_kernel(*refs):
    out_ref, lse_ref = refs[-2:]
    out_ref[...] = jnp.zeros_like(out_ref)
    lse_ref[...] = jnp.zeros_like(lse_ref)
    forward_heads(0, HEADS, *refs)


def forward_send_kernel(
    inputs,
    shift,
    stretch,
    q_bias,
    v_bias,
    bias_own,
    bias_other,
    gate,
    out_bias,
    shift_two,
    stretch_two,
    up_bias,
    count_in,
    qkv_full,
    out_full,
    up_weight,
    down_weight,
    teacher,
    out_grad,
    hidden,
    q_ref,
    k_own,
    v_own,
    out_ref,
    lse_ref,
    k_other,
    v_other,
    hidden_two,
    count_out,
    up_full,
    down_full,
    teacher_own,
    out_grad_own,
    middle_out,
    branch_out,
    activated,
    slope,
    qkv_held,
    middle,
    branch,
    upper,
    values,
    slopes,
    counts,
    count_sum,
    far_counts,
    up_stage,
    down_stage,
    send_sems,
    recv_sems,
    local_sems,
):
    spot = Spot()
    sender, local = Sender(send_sems, recv_sems), Locals(local_sems)
    width = q_ref.shape[1]
    stream = ColumnStream(local, qkv_full, qkv_held, width)
    stream.start(0)
    stream.start(1)
    greet(column_group(spot) + [spot.fsdp(2), spot.rep(), spot.rep(2)])
    count_slots = [sender.slot() for _ in range(3)]
    for step in range(1, 4):
        sender.start(count_slots[step - 1], count_in, counts.at[step - 1], spot.seq(step))
    key_slot, value_slot = sender.slot(), sender.slot()
    moves = [
        TokenMove(sender, spot, teacher, teacher_own),
        TokenMove(sender, spot, out_grad, out_grad_own),
    ]
    up = WeightMove(sender, local, spot, up_weight, up_full, up_stage, 3)
    down = WeightMove(sender, local, spot, down_weight, down_full, down_stage, 4)
    far_slots = [sender.slot() for _ in range(3)]

    up.start_far()
    down.start_far()
    for move in moves:
        move.start()

    def normalise(i, carry):
        rows = pl.ds(pl.multiple_of(i * STRIP, STRIP), STRIP)
        normed, _ = row_norm(inputs[rows, :].astype(F32))
        hidden[rows, :] = (normed * (1.0 + stretch[...]) + shift[...]).astype(BF16)
        return carry

    lax.fori_loop(0, q_ref.shape[0] // STRIP, normalise, 0)
    q_ref[...] = (
        jnp.dot(hidden[...], stream.wait(0), preferred_element_type=F32) + q_bias[...]
    ).astype(BF16)
    stream.start(2)
    k_own[...] = jnp.dot(hidden[...], stream.wait(1), preferred_element_type=F32).astype(BF16)
    sender.start(key_slot, k_own, k_other, spot.fsdp(1))
    v_own[...] = (
        jnp.dot(hidden[...], stream.wait(2), preferred_element_type=F32) + v_bias[...]
    ).astype(BF16)
    sender.start(value_slot, v_own, v_other, spot.fsdp(1))
    up.start_near()
    down.start_near()
    out_load = pltpu.make_async_copy(out_full, qkv_held.at[1], local.sems.at[stream.base + 1])
    out_load.start()

    total = count_in[...]
    for step in range(1, 4):
        sender.arrived(count_slots[step - 1], counts.at[step - 1])
        total = total + counts[step - 1]
    count_sum[...] = total
    for number, device in enumerate((spot.fsdp(2), spot.rep(), spot.rep(2))):
        sender.start(far_slots[number], count_sum, far_counts.at[number], device)
    up.pass_far(0)
    out_ref[...] = jnp.zeros_like(out_ref)
    lse_ref[...] = jnp.zeros_like(lse_ref)
    sender.arrived(key_slot, k_other)
    sender.arrived(value_slot, v_other)
    data = (q_ref, k_own, v_own, k_other, v_other, bias_own, bias_other, out_ref, lse_ref)
    forward_heads(0, 8, *data)
    up.store()
    down.store()
    up.pass_far(1)
    up.pass_side(0)
    forward_heads(8, HEADS, *data)
    up.pass_far(2)
    up.pass_side(1)
    down.pass_far(0)

    out_load.wait()
    branch[...] = (
        jnp.dot(out_ref[...], qkv_held[1], preferred_element_type=F32) + out_bias[...]
    )

    def norm_two(i, carry):
        rows = pl.ds(pl.multiple_of(i * STRIP, STRIP), STRIP)
        result = inputs[rows, :].astype(F32) + gate[...] * branch[rows, :]
        middle[rows, :] = result
        normed, _ = row_norm(result)
        hidden_two[rows, :] = (normed * (1.0 + stretch_two[...]) + shift_two[...]).astype(BF16)
        return carry

    lax.fori_loop(0, q_ref.shape[0] // STRIP, norm_two, 0)
    stored = [local.start(middle, middle_out), local.start(branch, branch_out)]
    up.pass_side(2)
    down.pass_far(1)
    down.pass_side(0)
    up.finish()

    up_stream = ColumnStream(local, up_full, qkv_held, width)
    up_stream.start(0)
    up_stream.start(1)
    kept = []
    for j in range(4):
        columns = slice(j * width, (j + 1) * width)
        upper[...] = jnp.dot(hidden_two[...], up_stream.wait(j), preferred_element_type=F32)
        if j < 2:
            up_stream.start(j + 2)
            down.pass_far(j + 2)
            down.pass_side(j + 1)
        else:
            for copy in kept[j - 2]:
                copy.wait()
        if j == 2:
            down.pass_side(3)

        def activate(i, carry):
            rows = pl.ds(pl.multiple_of(i * STRIP, STRIP), STRIP)
            value, rise = gelu_parts(upper[rows, :] + up_bias[:, columns])
            values[j % 2, rows, :] = value.astype(BF16)
            slopes[j % 2, rows, :] = rise.astype(BF16)
            return carry

        lax.fori_loop(0, q_ref.shape[0] // STRIP, activate, 0)
        kept.append(
            (
                local.start(values.at[j % 2], activated.at[:, pl.ds(j * width, width)]),
                local.start(slopes.at[j % 2], slope.at[:, pl.ds(j * width, width)]),
            )
        )
    for copy in stored + list(kept[2] + kept[3]):
        copy.wait()
    total = count_sum[...]
    for number in range(3):
        sender.arrived(far_slots[number], far_counts.at[number])
        total = total + far_counts[number]
    count_out[...] = total
    for move in moves:
        move.finish()
    down.finish()
    sender.finish()


def attend_and_gather(
    inputs, near_operands, qkv_full, out_full, up_weight, down_weight, teacher, out_grad
):
    tokens, width = inputs.shape
    count = near_operands[-1]
    anywhere = pl.BlockSpec(memory_space=pl.ANY)
    near = pl.BlockSpec(memory_space=pltpu.VMEM)
    shape = (tokens, width)
    return pl.pallas_call(
        forward_send_kernel,
        out_shape=[jax.ShapeDtypeStruct(shape, BF16)] * 5
        + [
            jax.ShapeDtypeStruct((tokens, LANES), F32),
            jax.ShapeDtypeStruct(shape, BF16),
            jax.ShapeDtypeStruct(shape, BF16),
            jax.ShapeDtypeStruct(shape, BF16),
            jax.ShapeDtypeStruct(count.shape, F32),
            jax.ShapeDtypeStruct((4 * up_weight.shape[0], up_weight.shape[1]), BF16),
            jax.ShapeDtypeStruct((4 * down_weight.shape[0], down_weight.shape[1]), BF16),
            jax.ShapeDtypeStruct(teacher.shape, BF16),
            jax.ShapeDtypeStruct(out_grad.shape, BF16),
            jax.ShapeDtypeStruct(shape, F32),
            jax.ShapeDtypeStruct(shape, F32),
            jax.ShapeDtypeStruct((tokens, up_weight.shape[1]), BF16),
            jax.ShapeDtypeStruct((tokens, up_weight.shape[1]), BF16),
        ],
        in_specs=[near] * (1 + len(near_operands)) + [anywhere] * 6,
        out_specs=[near] * 10 + [anywhere] * 8,
        scratch_shapes=[
            pltpu.VMEM((2, width, width), BF16),
            pltpu.VMEM(shape, F32),
            pltpu.VMEM(shape, F32),
            pltpu.VMEM(shape, F32),
            pltpu.VMEM((2,) + shape, BF16),
            pltpu.VMEM((2,) + shape, BF16),
            pltpu.VMEM((3,) + count.shape, F32),
            pltpu.VMEM(count.shape, F32),
            pltpu.VMEM((3,) + count.shape, F32),
            pltpu.VMEM(up_weight.shape, BF16),
            pltpu.VMEM(down_weight.shape, BF16),
            sems(48),
            sems(48),
            sems(24),
        ],
        compiler_params=pltpu.CompilerParams(
            collective_id=2, has_side_effects=True, vmem_limit_bytes=67043328
        ),
        name="attend_and_gather",
    )(inputs, *near_operands, qkv_full, out_full, up_weight, down_weight, teacher, out_grad)


def attend(queries, k_own, v_own, k_other, v_other, bias_own, bias_other):
    tokens, width = queries.shape
    return pl.pallas_call(
        forward_kernel,
        out_shape=[
            jax.ShapeDtypeStruct((tokens, width), BF16),
            jax.ShapeDtypeStruct((tokens, LANES), F32),
        ],
        compiler_params=pltpu.CompilerParams(vmem_limit_bytes=48 * 1024 * 1024),
        cost_estimate=pl.CostEstimate(
            flops=16 * tokens * tokens * 2 * WINDOW * 4,
            transcendentals=HEADS * tokens * tokens * 2,
            bytes_accessed=6 * tokens * width * 2,
        ),
        name="attend",
    )(queries, k_own, v_own, k_other, v_other, bias_own, bias_other)


def backward_heads(
    low,
    high,
    q_ref,
    k_own,
    v_own,
    k_other,
    v_other,
    do_ref,
    lse_ref,
    bias_own,
    bias_other,
    dq_ref,
    dk_one,
    dv_one,
    dk_two,
    dv_two,
):
    tokens, width = q_ref.shape
    head_dim = width // HEADS
    factor = head_dim ** (-0.5)
    scale = factor * LOG2E
    across = (((1,), (1,)), ((), ()))
    sides = (
        (k_own, v_own, bias_own, dk_one, dv_one),
        (k_other, v_other, bias_other, dk_two, dv_two),
    )

    def body(head, carry):
        start, base = head_window(head, head_dim, width)
        window = pl.ds(base, WINDOW)
        lane = lax.broadcasted_iota(jnp.int32, (1, WINDOW), 1) + base
        inside = (lane >= start) & (lane < start + head_dim)
        keep = inside.astype(BF16)
        query = q_ref[:, window] * keep
        grad = do_ref[:, window] * keep
        lse = lse_ref[pl.ds(head, 1), :]

        def put(ref, value):
            ref[:, window] = jnp.where(inside, value, ref[:, window].astype(F32)).astype(ref.dtype)

        probs, prods = [], []
        delta = None
        for k_ref, v_ref, bias, _, _ in sides:
            scores = lax.dot_general(k_ref[:, window], query, across, preferred_element_type=F32)
            prob = jnp.exp2(scores * scale + bias[...] - lse)
            prob_grad = lax.dot_general(v_ref[:, window], grad, across, preferred_element_type=F32)
            prod = prob * prob_grad
            part = jnp.sum(prod, axis=0, keepdims=True)
            delta = part if delta is None else delta + part
            probs.append(prob)
            prods.append(prod)
        dq = None
        for (k_ref, _, _, dk, dv), prob, prod in zip(sides, probs, prods, strict=True):
            put(dv, jnp.dot(prob.astype(BF16), grad, preferred_element_type=F32))
            score_grad = (prod - prob * delta).astype(BF16)
            put(dk, jnp.dot(score_grad, query, preferred_element_type=F32) * factor)
            part = lax.dot_general(
                score_grad, k_ref[:, window], DOWN, preferred_element_type=F32
            )
            dq = part if dq is None else dq + part
        put(dq_ref, dq * factor)
        return carry

    lax.fori_loop(low, high, body, 0)


def backward_kernel(*refs):
    for ref in refs[-5:]:
        ref[...] = jnp.zeros_like(ref)
    backward_heads(0, HEADS, *refs)


def attend_back(queries, k_own, v_own, k_other, v_other, grad, lse, bias_own, bias_other):
    tokens, width = queries.shape
    shape = (tokens, width)
    return pl.pallas_call(
        backward_kernel,
        out_shape=[
            jax.ShapeDtypeStruct(shape, BF16),
            jax.ShapeDtypeStruct(shape, F32),
            jax.ShapeDtypeStruct(shape, F32),
            jax.ShapeDtypeStruct(shape, BF16),
            jax.ShapeDtypeStruct(shape, BF16),
        ],
        compiler_params=pltpu.CompilerParams(vmem_limit_bytes=60 * 1024 * 1024),
        name="attend_back",
    )(queries, k_own, v_own, k_other, v_other, grad, lse, bias_own, bias_other)


def dot(left, right):
    return jnp.dot(left, right, preferred_element_type=F32)


def dot_t(left, right):
    return lax.dot_general(left, right, (((1,), (1,)), ((), ())), preferred_element_type=F32)


def norm_parts(inputs):
    centred = inputs - jnp.mean(inputs, axis=-1, keepdims=True)
    rate = lax.rsqrt(jnp.mean(centred * centred, axis=-1, keepdims=True) + EPS)
    return centred * rate, rate


def norm_back(grad, normed, rate):
    return rate * (
        grad
        - jnp.mean(grad, axis=-1, keepdims=True)
        - normed * jnp.mean(grad * normed, axis=-1, keepdims=True)
    )


def gelu_parts(inputs):
    inner = jnp.tanh(GELU_C * (inputs + 0.044715 * inputs * inputs * inputs))
    value = 0.5 * inputs * (1.0 + inner)
    slope = 0.5 * (1.0 + inner) + 0.5 * inputs * (1.0 - inner * inner) * GELU_C * (
        1.0 + 3.0 * 0.044715 * inputs * inputs
    )
    return value, slope


def column_sum(array):
    return jnp.sum(array.astype(F32), axis=0)


def shards(
    tokens,
    condition,
    valid_mask,
    teacher,
    out_grad,
    mod_weight,
    mod_bias,
    qkv_weight,
    qkv_bias,
    out_weight,
    out_bias,
    up_weight,
    up_bias,
    down_weight,
    down_bias,
):
    reps, fsdp, seq = lax.axis_size("rep"), lax.axis_size("fsdp"), lax.axis_size("seq")
    fast = (reps, fsdp, seq) == (2, 4, 4)
    latents, span, width = tokens.shape
    assert 2 * latents == seq and latents == 2
    place_f, place_s = lax.axis_index("fsdp"), lax.axis_index("seq")
    total_tokens = latents * span * reps * fsdp * seq

    biases = jnp.concatenate([mod_bias, qkv_bias, out_bias, up_bias, down_bias])
    shard_rows = mod_weight.shape[0]
    cond_row = pick(condition, place_s % 2)
    keep_mask = valid_mask.astype(F32)

    if fast:
        inputs_low, valid_all, mod_parts, bias_all, qkv_full, out_full = enter(
            tokens,
            keep_mask.reshape(latents, 1, span),
            condition.astype(F32).reshape(latents, fsdp, 1, shard_rows),
            biases.astype(F32)[None],
            mod_weight,
            qkv_weight,
            out_weight,
        )
        inputs_low = inputs_low.reshape(-1, width)
        valid_all = valid_all.reshape(2, -1)
        keyvalid, valid_other = pick(valid_all, place_f % 2), pick(valid_all, 1 - place_f % 2)
        mod_row = jnp.sum(mod_parts, axis=(0, 1))
        bias_all = bias_all[:, 0]
    else:
        inputs_low = to_latent(tokens)
        keyvalid = to_latent(keep_mask)
        valid_other = flip(keyvalid, "fsdp", 1)
        counted = lax.psum(jnp.sum(keep_mask), ("rep", "fsdp", "seq")).reshape(1, 1)
        own_row = jnp.where(place_f % 2 == place_s // 2, cond_row, flip(cond_row, "fsdp", 1))
        cond_pair = lax.all_gather(own_row, "fsdp", axis=0)[::2]
        silu_pair = jax.nn.silu(cond_pair.astype(F32)).astype(BF16)
        silu_cols = lax.dynamic_slice_in_dim(silu_pair, place_f * shard_rows, shard_rows, 1)
        mod_row = pick(lax.psum(dot(silu_cols, mod_weight), "fsdp"), place_f // 2)
        bias_all = lax.all_gather(biases, "fsdp", axis=0).astype(F32)
        qkv_full, out_full = gather_weight(qkv_weight), gather_weight(out_weight)
        up_full, down_full = gather_weight(up_weight), gather_weight(down_weight)
        teacher_own, out_grad_own = to_latent(teacher), to_latent(out_grad)
    mask_own = (keyvalid - 1.0) * (-NEG)
    mask_other = (valid_other - 1.0) * (-NEG)

    cuts = [0]
    for bias in (mod_bias, qkv_bias, out_bias, up_bias, down_bias):
        cuts.append(cuts[-1] + bias.shape[0])
    mod_b, qkv_b, out_b, up_b, down_b = (
        bias_all[:, low:high].reshape(-1) for low, high in zip(cuts[:-1], cuts[1:], strict=True)
    )
    pieces = (mod_row + mod_b).reshape(6, 1, width)
    shift_one, scale_one, gate_one, shift_two, scale_two, gate_two = (pieces[i] for i in range(6))

    inputs = inputs_low.astype(F32)
    if fast:
        (
            hidden_one,
            queries,
            keys_own,
            values_own,
            attended,
            lse,
            keys_other,
            values_other,
            hidden_two,
            counted,
            up_full,
            down_full,
            teacher_own,
            out_grad_own,
            middle,
            branch,
            activated,
            slope,
        ) = attend_and_gather(
            inputs_low,
            (
                shift_one,
                scale_one,
                qkv_b[None, :width],
                qkv_b[None, width:],
                mask_own[None],
                mask_other[None],
                gate_one,
                out_b[None],
                shift_two,
                scale_two,
                up_b[None],
                jnp.full((1, LANES), jnp.sum(valid_all)),
            ),
            qkv_full,
            out_full,
            up_weight,
            down_weight,
            teacher,
            out_grad,
        )
        counted = counted[:, :1]
        teacher_own = teacher_own.reshape(-1, width)
        out_grad_own = out_grad_own.reshape(-1, width)
    else:
        normed_one, rate_one = norm_parts(inputs)
        hidden_one = (normed_one * (1.0 + scale_one) + shift_one).astype(BF16)
        projected = dot(hidden_one, qkv_full)
        queries = (projected[:, :width] + qkv_b[:width]).astype(BF16)
        keys_own = projected[:, width : 2 * width].astype(BF16)
        values_own = (projected[:, 2 * width :] + qkv_b[width:]).astype(BF16)
        keys_other, values_other = flip(keys_own, "fsdp", 1), flip(values_own, "fsdp", 1)
        attended, lse = attend(
            queries,
            keys_own,
            values_own,
            keys_other,
            values_other,
            mask_own[None],
            mask_other[None],
        )
        branch = dot(attended, out_full) + out_b
        middle = inputs + gate_one * branch
        normed_two, rate_two = norm_parts(middle)
        hidden_two = (normed_two * (1.0 + scale_two) + shift_two).astype(BF16)
        up_pre = dot(hidden_two, up_full) + up_b
        activated, slope = gelu_parts(up_pre)
        activated = activated.astype(BF16)
    mlp_out = dot(activated, down_full) + down_b
    output = middle + gate_two * mlp_out
    block_out = output.astype(BF16)
    differ = (output - teacher_own.astype(F32)) * keyvalid[:, None]
    error = jnp.sum(differ * differ)

    grad_out = out_grad_own.astype(F32) + total_tokens / counted * differ
    grad_mlp = (grad_out * gate_two).astype(BF16)
    gate_two_grad = jnp.sum(grad_out * mlp_out, axis=0, keepdims=True)

    def slices(array):
        return array.reshape(array.shape[0], fsdp, -1).transpose(1, 0, 2)

    def weight_grad(left, right):
        whole = lax.dot_general(left, right, DOWN, preferred_element_type=F32)
        mine = lax.psum_scatter(whole.astype(BF16), "fsdp", scatter_dimension=0, tiled=True)
        return lax.psum(mine, ("rep", "seq")).astype(F32)

    cond_part = jnp.where(place_f % 2 == place_s // 2, cond_row.astype(F32), 0.0)[None]
    length = (11 + up_weight.shape[1] // width) * width
    if fast:
        (
            attended_grad,
            branch_grad,
            middle_grad,
            sums,
            error_sum,
            up_total,
            down_final,
            _,
            block_out,
        ) = middle_back(
            (
                grad_mlp,
                grad_out,
                middle,
                branch,
                scale_two,
                gate_one,
                jnp.full((1, LANES), error),
            ),
            activated,
            slope,
            slices(hidden_two),
            down_full,
            up_full,
            out_full,
            block_out.reshape(2, span, width),
        )
        err_total = error_sum[:, :1]
        rows, cond_parts, up_final, tail_final, tokens_grad = finish(
            (
                branch_grad,
                up_total,
                middle_grad,
                inputs_low,
                scale_one,
                queries,
                keys_own,
                values_own,
                keys_other,
                values_other,
                attended_grad,
                lse.T,
                mask_own[:, None],
                mask_other[:, None],
                sums,
                gate_two_grad,
                cond_part,
            ),
            slices(attended),
            slices(hidden_one),
            mod_weight,
            qkv_full,
            (2, span, width),
        )
        rows = rows.reshape(-1, ROW_PARTS * width)[:, :length]
        down_g = down_final.reshape(down_weight.shape).astype(F32)
        up_g = spread(up_final.reshape(4, -1, width), (0, 1, 2, 3))
        tail_final = tail_final.reshape(4, -1, width)
        out_g = tail_final[0].astype(F32)
        qkv_g = spread(tail_final, (3, 2, 1))
    else:
        upper_grad = (dot_t(grad_mlp, down_full) * slope).astype(BF16)
        hidden_two_grad = dot_t(upper_grad, up_full)
        scaled_two = hidden_two_grad * (1.0 + scale_two)
        middle_grad = grad_out + norm_back(scaled_two, normed_two, rate_two)
        branch_grad = (middle_grad * gate_one).astype(BF16)
        attended_grad = dot_t(branch_grad, out_full).astype(BF16)
        query_grad, key_part, value_part, key_away, value_away = attend_back(
            queries,
            keys_own,
            values_own,
            keys_other,
            values_other,
            attended_grad,
            lse.T,
            mask_own[:, None],
            mask_other[:, None],
        )
        key_grad = (key_part + flip(key_away, "fsdp", 1).astype(F32)).astype(BF16)
        value_grad = (value_part + flip(value_away, "fsdp", 1).astype(F32)).astype(BF16)
        err_total = lax.psum(error, ("rep", "fsdp", "seq")).reshape(1, 1)
        block_out = from_latent(block_out)
        qkv_grad = jnp.concatenate([query_grad, key_grad, value_grad], axis=-1)
        hidden_one_grad = dot_t(qkv_grad, qkv_full)
        scaled_one = hidden_one_grad * (1.0 + scale_one)
        tokens_grad = middle_grad + norm_back(scaled_one, normed_one, rate_one)
        tokens_grad = tokens_grad.astype(BF16)
        row = jnp.concatenate(
            [
                column_sum(hidden_one_grad),
                column_sum(hidden_one_grad * normed_one),
                column_sum(middle_grad * branch),
                column_sum(hidden_two_grad),
                column_sum(hidden_two_grad * normed_two),
                gate_two_grad[0],
                column_sum(branch_grad),
                column_sum(upper_grad),
                column_sum(grad_mlp),
                column_sum(query_grad),
                column_sum(value_grad),
                cond_part[0],
            ]
        )
        row = row + flip(row, "fsdp", 1)
        rows = gather_rows(row)
        tokens_grad = from_latent(tokens_grad)
        down_g = weight_grad(activated, grad_mlp)
        up_g = weight_grad(hidden_two, upper_grad)
        out_g = weight_grad(attended, branch_grad)
        qkv_g = weight_grad(hidden_one, qkv_grad)

    mod_grad = rows[:, : 6 * width]
    silu_all = jax.nn.silu(rows[:, -width:]).astype(BF16)
    silu_own = lax.dynamic_slice_in_dim(silu_all, place_f * shard_rows, shard_rows, 1)
    mod_wgrad = lax.dot_general(
        silu_own.astype(F32),
        mod_grad,
        (((0,), (0,)), ((), ())),
        precision=HIGHEST,
        preferred_element_type=F32,
    )
    bias_sum = jnp.sum(rows[:, 6 * width : -width], axis=0)

    def own_bias(low, size):
        own = size // fsdp
        return lax.dynamic_slice_in_dim(bias_sum, low + place_f * own, own, 0)

    up_size = up_b.shape[0]
    out_bg = own_bias(0, width)
    up_bg = own_bias(width, up_size)
    down_bg = own_bias(width + up_size, width)
    qkv_bg = own_bias(2 * width + up_size, 2 * width)
    mod_own = mod_bias.shape[0]
    mod_bg = lax.dynamic_slice_in_dim(jnp.sum(mod_grad, axis=0), place_f * mod_own, mod_own, 0)

    if fast:
        found = cond_parts
    else:
        replica = lax.axis_index("rep")
        per_rep = mod_grad.shape[0] // reps
        own_rep = lax.dynamic_slice_in_dim(mod_grad, replica * per_rep, per_rep, 0)
        silu_grad = lax.dot_general(
            own_rep,
            mod_weight.astype(F32),
            (((1,), (1,)), ((), ())),
            precision=HIGHEST,
            preferred_element_type=F32,
        )
        owners = silu_grad.reshape(fsdp, latents, shard_rows)
        found = lax.all_to_all(owners, "fsdp", 0, 0, tiled=True)
    silu_grad = found.transpose(1, 0, 2).reshape(latents, width)
    conds = condition.astype(F32)
    sigmoid = 1.0 / (1.0 + jnp.exp(-conds))
    condition_grad = silu_grad * (sigmoid * (1.0 + conds * (1.0 - sigmoid)))

    loss_value = (err_total / (width * counted))[0, 0]
    return (
        block_out,
        loss_value,
        tokens_grad,
        condition_grad,
        mod_wgrad,
        mod_bg,
        qkv_g,
        qkv_bg,
        out_g,
        out_bg,
        up_g,
        up_bg,
        down_g,
        down_bg,
    )


def solution(mesh):
    batch = P(("rep", "fsdp"), "seq", None)
    matrix, vector = P("fsdp", None), P("fsdp")
    params = (matrix, vector) * 5
    return jax.shard_map(
        shards,
        mesh=mesh,
        in_specs=(batch, P(("rep", "fsdp"), None), P(("rep", "fsdp"), "seq"), batch, batch)
        + params,
        out_specs=(batch, P(), batch, P(("rep", "fsdp"), None)) + params,
        check_vma=False,
    )
```
